32 devices in a mesh: dp: 8 (over y, x, core), mp: 4 (over z).
Axes of the slice: x: 2, y: 2, z: 4, core: 2. Of those that a mesh axis runs over, the one named last changes fastest.
Arguments:
- layer_input: bfloat16 [16384, 1024], P(('dp', 'mp')), may hold values from -9 to 9
- segment_ids: int32 [8, 2048], P('dp'), may hold values from 0 to 10, as said below
- grad_out: bfloat16 [16384, 1024], P(('dp', 'mp')), may hold values from -6 to 6
- qkv_weight: bfloat16 [1024, 3, 1024], P('dp', None, 'mp'), may hold values from -0.1875 to 0.1875
- attn_weight: bfloat16 [1024, 1024], P('dp', 'mp'), may hold values from -3 to 3
- inner_weight: bfloat16 [1024, 2, 2624], P('dp', None, 'mp'), may hold values from -0.1875 to 0.1875
- outer_weight: bfloat16 [1024, 2624], P('dp', 'mp'), may hold values from -0.25 to 0.25
- attn_gain: float32 [1024], replicated, may hold values from 0.1 to 1.9
- mlp_gain: float32 [1024], replicated, may hold values from 0.1 to 1.9
Outputs:
- layer_output: bfloat16 [16384, 1024], P(('dp', 'mp'))
- input_grad: float32 [16384, 1024], P(('dp', 'mp'))
- qkv_grad: float32 [1024, 3, 1024], P('dp', None, 'mp')
- attn_grad: float32 [1024, 1024], P('dp', 'mp')
- inner_grad: float32 [1024, 2, 2624], P('dp', None, 'mp')
- outer_grad: float32 [1024, 2624], P('dp', 'mp')
- attn_gain_grad: float32 [1024], replicated
- mlp_gain_grad: float32 [1024], replicated
- rms_values: float32 [4], replicated
The draws below stay inside these ranges and needn't reach their ends.
Inputs may be any that keep to these rules, and one draw needn't show every extreme that they name: `segment_ids`: along each sequence the numbers never fall; the nonzero ones count the documents from 1 at the sequence's start, each document of 200 to 2000 tokens; zeros fill the tail after the last document, if any. Some sequence holds 2048 // 200 documents.
All inputs are finite; a program needn't handle non-finite values.
Results may differ from the reference program's by a relative error of at most 0.018.
Values may be sent and summed in bfloat16 or wider, within the bound.
A program may use at most 192 MiB of HBM per device.

```python
import math
import jax
import jax.numpy as jnp
from jax import lax

D = 1024
HEADS = 16
HEAD_DIM = 64
FF = 2624
SEQ = 2048
DOC_MIN = 200
DOC_MAX = 2000
NSEQ = 8
TOKENS = 16384


def draw_layer_input(key, part):
    placed = lax.broadcasted_iota(jnp.float32, (TOKENS, D), 0) / TOKENS
    base = jnp.clip(jax.random.normal(key, (TOKENS, D), jnp.float32), -5.0, 5.0)
    return (base * (0.6 + 1.2 * placed)).astype(jnp.bfloat16)


def draw_segment_ids(key, part):
    doc_count = SEQ // DOC_MIN + 1
    lengths = jax.random.randint(key, (NSEQ, doc_count), DOC_MIN, DOC_MAX + 1)
    seq_rows = lax.broadcasted_iota(jnp.int32, (NSEQ, doc_count), 0)
    doc_cols = lax.broadcasted_iota(jnp.int32, (NSEQ, doc_count), 1)
    lengths = jnp.where((seq_rows == 0) & (doc_cols == 0), DOC_MAX, lengths)
    lengths = jnp.where(seq_rows == 1, DOC_MIN, lengths)
    ends = jnp.cumsum(lengths, axis=1)
    fitted = jnp.where(ends <= SEQ, ends, jnp.zeros_like(ends))
    last_end = jnp.max(fitted, axis=1)
    places = lax.broadcasted_iota(jnp.int32, (NSEQ, SEQ), 1)
    number = 1 + jnp.sum((ends[:, None, :] <= places[:, :, None]).astype(jnp.int32), axis=2)
    return jnp.where(places < last_end[:, None], number, jnp.zeros_like(number))


def with_spikes(values, key, source, target, blocks, factor):
    owner, partner = [(jnp.arange(values.shape[position]) // (values.shape[position] // blocks)).reshape([-1 if axis == position else 1 for axis in range(values.ndim)]) for position in (source, target)]
    chosen = jax.random.permutation(key, blocks)[partner]
    strong = (owner == chosen) | (owner == (partner + blocks // 2) % blocks)
    return jnp.where(strong, factor * values, values)


def levels(key, extent, pieces, least, high):
    def one(axis_at, blocks):
        heights = jax.random.uniform(jax.random.fold_in(jax.random.fold_in(key, 6), axis_at), (blocks,), jnp.float32, least / len(pieces), high / len(pieces))
        return jnp.repeat(jnp.exp(heights), extent[axis_at] // blocks).reshape((-1,) + (1,) * (len(extent) - axis_at - 1))

    level = one(*pieces[0])
    for cut in pieces[1:]:
        level = level * one(*cut)
    return level


def gaussian(rng, shape, scale, most, shards=(), kind=jnp.bfloat16):
    drawn = scale * jax.random.normal(rng, shape, jnp.float32)
    if shards:
        drawn = drawn * levels(rng, shape, shards, -0.22, 0.18)
    return jnp.clip(drawn, -most, most).astype(kind)


def bell_draw_with(own_key, extent, deviation, bound, cuts, heavy, held_as=jnp.bfloat16):
    array = deviation * jax.random.normal(own_key, extent, jnp.float32)
    if cuts:
        array = array * levels(own_key, extent, cuts, -0.22, 0.18)
    return jnp.clip(with_spikes(array, jax.random.fold_in(own_key, 3), *heavy), -bound, bound).astype(held_as)


def setup_inputs(seed: int = 0) -> dict:
    arg_keys = jax.random.split(jax.random.key(seed), 10)
    return {
        "layer_input": draw_layer_input(jax.random.fold_in(arg_keys[9], 71), 0),
        "segment_ids": draw_segment_ids(jax.random.fold_in(arg_keys[9], 71), 0),
        "grad_out": bell_draw_with(arg_keys[2], (TOKENS, D), 1.0, 6.0, ((0, 32),), (0, 1, 32, 2.75)),
        "qkv_weight": gaussian(arg_keys[3], (D, 3, D), D ** -0.5, 0.1875, ((0, 8), (2, 4))),
        "attn_weight": gaussian(arg_keys[4], (D, D), (max(4, D // 256)) ** -0.5, 3.0, ((0, 8), (1, 4))),
        "inner_weight": gaussian(arg_keys[5], (D, 2, FF), D ** -0.5, 0.1875, ((0, 8), (2, 4))),
        "outer_weight": gaussian(arg_keys[6], (D, FF), (FF // 4) ** -0.5, 0.25, ((0, 8), (1, 4))),
        "attn_gain": jnp.clip(1.0 + 0.18 * jax.random.normal(arg_keys[7], (D,), jnp.float32), 0.1, 1.9),
        "mlp_gain": jnp.clip(1.0 + 0.18 * jax.random.normal(arg_keys[8], (D,), jnp.float32), 0.1, 1.9),
    }


@jax.custom_vjp
def low(v):
    return lax.optimization_barrier(v.astype(jnp.bfloat16)).astype(jnp.float32)

@jax.custom_vjp
def low_back(v):
    return v

def low_keep(v):
    return (low(v), None)

def low_pass(kept, grad):
    return (grad,)

def back_keep(v):
    return (v, None)

def back_low(kept, grad):
    return (low(grad),)
low.defvjp(low_keep, low_pass)
low_back.defvjp(back_keep, back_low)
NORM_EPS = 1e-05
ROPE_BASE = 160000.0
MASKED_SCORE = -1e+30
HIGHEST = lax.Precision.HIGHEST

def layer_norm(values, gain):
    centre = lax.optimization_barrier(jnp.mean(values, axis=-1, keepdims=True))
    shifted = values - centre
    spread = lax.optimization_barrier(jnp.mean(shifted * shifted, axis=-1, keepdims=True))
    return shifted * lax.rsqrt(spread + NORM_EPS) * gain

def doc_positions(segment):
    length = segment.shape[0]
    places = jnp.arange(length, dtype=jnp.int32)
    before = jnp.concatenate([jnp.full((1,), -1, jnp.int32), segment[:-1]])
    starts = jnp.where(segment != before, places, jnp.zeros_like(places))
    return places - lax.cummax(starts, axis=0)

def rope_angles(segment):
    half_dim = HEAD_DIM // 2
    frequency = jnp.exp(jnp.arange(half_dim, dtype=jnp.float32) * (-2.0 * math.log(ROPE_BASE) / HEAD_DIM))
    return doc_positions(segment).astype(jnp.float32)[:, None] * frequency[None, :]

def rotary(values, angle):
    half_dim = values.shape[-1] // 2
    cosine = jnp.cos(angle)[:, None, :]
    sine_part = jnp.sin(angle)[:, None, :]
    first_half = values[..., :half_dim]
    second_half = values[..., half_dim:]
    return jnp.concatenate([first_half * cosine - second_half * sine_part, second_half * cosine + first_half * sine_part], axis=-1)

def attend(query_rot, key_rot, value_rows, segment):
    length = query_rot.shape[0]
    block_rows = min(512, length)
    score_scale = HEAD_DIM ** (-0.5)

    def one_block(block_index):
        row_start = block_index * block_rows
        q_rows = lax.dynamic_slice_in_dim(query_rot, row_start, block_rows)
        seg_rows = lax.dynamic_slice_in_dim(segment, row_start, block_rows)
        live_rows = seg_rows != 0
        allowed = (seg_rows[:, None] == segment[None, :]) & live_rows[:, None]
        scores = low_back(jnp.einsum('qhe,khe->hqk', q_rows, key_rot, precision=HIGHEST) * score_scale)
        masked = jnp.where(allowed[None], scores, MASKED_SCORE)
        row_top = jnp.where(live_rows[None, :], lax.optimization_barrier(jnp.max(masked, axis=-1)), 0.0)
        weights = jnp.exp(masked - row_top[..., None])
        row_total = jnp.where(live_rows[None, :], lax.optimization_barrier(jnp.sum(weights, axis=-1)), 1.0)
        attn_prob = low(weights / row_total[..., None])
        return jnp.einsum('hqk,khe->qhe', attn_prob, value_rows, precision=HIGHEST)
    blocks = lax.map(jax.checkpoint(one_block), jnp.arange(length // block_rows, dtype=jnp.int32))
    return blocks.reshape(length, HEADS * HEAD_DIM)

def reference(layer_input, segment_ids, grad_out, qkv_weight, attn_weight, inner_weight, outer_weight, attn_gain, mlp_gain):

    def forward(inputs, qkv_w, attn_w, inner_w, outer_w, gain_attn, gain_mlp):

        def one_sequence(sums, packed):
            tokens, segment = packed
            length = tokens.shape[0]
            head_shape = (length, HEADS, HEAD_DIM)
            angle = rope_angles(segment)
            normed = low(layer_norm(tokens, gain_attn))
            qkv_all = low_back(jnp.einsum('ld,dcf->lcf', normed, qkv_w, precision=HIGHEST))
            query_rot = low(rotary(qkv_all[:, 0].reshape(head_shape), angle))
            key_rot = low(rotary(qkv_all[:, 1].reshape(head_shape), angle))
            value_rows = low(qkv_all[:, 2].reshape(head_shape))
            heads_out = low(low_back(attend(query_rot, key_rot, value_rows, segment)))
            attn_out = low_back(jnp.dot(heads_out, attn_w.T, precision=HIGHEST))
            middle = tokens + attn_out
            inner_in = low(layer_norm(middle, gain_mlp))
            gates = low_back(jnp.einsum('ld,dcf->lcf', inner_in, inner_w, precision=HIGHEST))
            hidden = low(jax.nn.gelu(gates[:, 0], approximate=False) * gates[:, 1])
            mlp_out = low_back(jnp.dot(hidden, outer_w.T, precision=HIGHEST))
            live_rows = (segment != 0).astype(jnp.float32)[:, None]
            squares = jnp.stack([jnp.sum(live_rows * tokens * tokens), jnp.sum(live_rows * attn_out * attn_out), jnp.sum(live_rows * middle * middle), jnp.sum(live_rows * mlp_out * mlp_out)])
            return (sums + squares, middle + mlp_out)
        sums, outputs = lax.scan(one_sequence, jnp.zeros((4,), jnp.float32), (inputs.reshape(NSEQ, SEQ, D), segment_ids))
        return (outputs.reshape(TOKENS, D), sums)
    floats = (layer_input.astype(jnp.float32), qkv_weight.astype(jnp.float32), attn_weight.astype(jnp.float32), inner_weight.astype(jnp.float32), outer_weight.astype(jnp.float32), attn_gain, mlp_gain)
    layer_output, pullback, sums = jax.vjp(forward, *floats, has_aux=True)
    grads = pullback(grad_out.astype(jnp.float32))
    live_count = jnp.sum((segment_ids != 0).astype(jnp.float32))
    rms_values = jnp.sqrt(sums / (live_count * D))
    return (layer_output.astype(jnp.bfloat16), grads[0], grads[1], grads[2], grads[3], grads[4], grads[5], grads[6], rms_values)
```

```python
import functools
import math

import jax
import jax.numpy as jnp
from jax import lax
from jax.experimental import pallas as pl
from jax.experimental.pallas import tpu as pltpu
from jax.sharding import PartitionSpec as P

HEAD_DIM = 64
NORM_EPS = 1e-05
ROPE_BASE = 160000.0
BIG = 1e30
LANES = 128
BF = jnp.bfloat16
F32 = jnp.float32
VMEM_LIMIT = 60 * 1024 * 1024


def dot_nn(a, b):
    return lax.dot_general(a, b, (((1,), (0,)), ((), ())), preferred_element_type=F32)


def dot_nt(a, b):
    return lax.dot_general(a, b, (((1,), (1,)), ((), ())), preferred_element_type=F32)


def dot_tn(a, b):
    return lax.dot_general(a, b, (((0,), (0,)), ((), ())), preferred_element_type=F32)


def norm_stats(values):
    centre = jnp.mean(values, axis=-1, keepdims=True)
    shifted = values - centre
    spread = jnp.mean(shifted * shifted, axis=-1, keepdims=True)
    scale = lax.rsqrt(spread + NORM_EPS)
    return shifted * scale, scale


def norm_back(vhat, scale, gain, grad):
    u = grad * gain
    mean_u = jnp.mean(u, axis=-1, keepdims=True)
    mean_uv = jnp.mean(u * vhat, axis=-1, keepdims=True)
    return scale * (u - mean_u - vhat * mean_uv)


def doc_positions(segment):
    length = segment.shape[0]
    places = jnp.arange(length, dtype=jnp.int32)
    before = jnp.concatenate([jnp.full((1,), -1, jnp.int32), segment[:-1]])
    starts = jnp.where(segment != before, places, jnp.zeros_like(places))
    return places - lax.cummax(starts, axis=0)


def rope_tables(segment):
    half = HEAD_DIM // 2
    lane = jnp.arange(LANES, dtype=jnp.int32)
    frequency = jnp.exp(
        (lane % half).astype(F32) * (-2.0 * math.log(ROPE_BASE) / HEAD_DIM)
    )
    angle = doc_positions(segment).astype(F32)[:, None] * frequency[None, :]
    first = (lane % HEAD_DIM < half)[None, :]
    sine = jnp.sin(angle)
    return jnp.cos(angle), jnp.where(first, -sine, sine)


def swap_halves(values):
    lane = lax.broadcasted_iota(jnp.int32, values.shape, 1)
    first = lane % HEAD_DIM < HEAD_DIM // 2
    back = pltpu.roll(values, LANES - HEAD_DIM // 2, 1)
    ahead = pltpu.roll(values, HEAD_DIM // 2, 1)
    return jnp.where(first, back, ahead)


def qkv_kernel(x_ref, gain_ref, w_ref, cos_ref, sin_ref, n_ref, q_ref, k_ref, v_ref):
    vhat, unused = norm_stats(x_ref[...].astype(F32))
    normed = (vhat * gain_ref[...]).astype(BF)
    n_ref[...] = normed
    cols = q_ref.shape[1]
    flat = dot_nn(normed, w_ref[...])
    cosine = cos_ref[...]
    sine = sin_ref[...]
    for part, out in ((0, q_ref), (1, k_ref)):
        for at in range(0, cols, LANES):
            u = flat[:, part * cols + at : part * cols + at + LANES]
            out[:, at : at + LANES] = (u * cosine + swap_halves(u) * sine).astype(BF)
    v_ref[...] = flat[:, 2 * cols :].astype(BF)


def qkv_call(x_all, gain, weight, cosine, sine):
    tokens, model = x_all.shape
    cols = weight.shape[1] // 3
    rows = 512
    whole = lambda i: (0, 0)
    block = lambda i: (i, 0)
    return pl.pallas_call(
        qkv_kernel,
        grid=(tokens // rows,),
        in_specs=[
            pl.BlockSpec((rows, model), block),
            pl.BlockSpec((1, model), whole),
            pl.BlockSpec(weight.shape, whole),
            pl.BlockSpec((rows, LANES), block),
            pl.BlockSpec((rows, LANES), block),
        ],
        out_specs=[
            pl.BlockSpec((rows, model), block),
            pl.BlockSpec((rows, cols), block),
            pl.BlockSpec((rows, cols), block),
            pl.BlockSpec((rows, cols), block),
        ],
        out_shape=[
            jax.ShapeDtypeStruct((tokens, model), BF),
            jax.ShapeDtypeStruct((tokens, cols), BF),
            jax.ShapeDtypeStruct((tokens, cols), BF),
            jax.ShapeDtypeStruct((tokens, cols), BF),
        ],
        compiler_params=pltpu.CompilerParams(vmem_limit_bytes=VMEM_LIMIT),
        cost_estimate=pl.CostEstimate(
            flops=2 * tokens * model * 3 * cols, bytes_accessed=16 << 20, transcendentals=0
        ),
        name="qkv",
    )(x_all, gain, weight, cosine, sine)


def attn_fwd_kernel(q_ref, k_ref, v_ref, qaux_ref, kaux_ref, live_ref, o_ref, qa_ref, ka_ref, s_ref):
    step = pl.program_id(0)
    keys = k_ref.shape[0]
    rows = q_ref.shape[0]
    chunk = 512
    lane_k = lax.broadcasted_iota(jnp.int32, (keys, LANES), 1)
    lane = lax.broadcasted_iota(jnp.int32, (rows, LANES), 1)

    @pl.when(step == 0)
    def _():
        k = k_ref[...]
        kaux = kaux_ref[...]
        ka_ref[0] = jnp.where(lane_k < HEAD_DIM, k, kaux)
        ka_ref[1] = jnp.where(lane_k >= HEAD_DIM, k, kaux)

    q = q_ref[...] * jnp.asarray(HEAD_DIM**-0.5, BF)
    qaux = qaux_ref[...]
    live = live_ref[...]
    outs = []
    for head in range(2):
        mine = (lane < HEAD_DIM) if head == 0 else (lane >= HEAD_DIM)
        qa = jnp.where(mine, q, qaux)
        top = None
        for at in range(0, keys, chunk):
            s = dot_nt(qa, ka_ref[head, at : at + chunk, :])
            s_ref[:, at : at + chunk] = s
            part = jnp.max(s, axis=-1, keepdims=True)
            top = part if top is None else jnp.maximum(top, part)
        total = jnp.zeros((rows, 1), F32)
        mixed = jnp.zeros((rows, LANES), F32)
        for at in range(0, keys, chunk):
            p = jnp.exp(s_ref[:, at : at + chunk] - top)
            total += jnp.sum(p, axis=-1, keepdims=True)
            mixed += dot_nn(p.astype(BF), v_ref[at : at + chunk, :])
        outs.append(mixed * (live / total))
        log_sum = jnp.where(live > 0, top + jnp.log(total), BIG)
        high = log_sum.astype(BF)
        rest = log_sum - high.astype(F32)
        mid = rest.astype(BF)
        low = (rest - mid.astype(F32)).astype(BF)
        t = lane % HEAD_DIM
        aux = jnp.where(t == 16, -high, jnp.where(t == 17, -mid, jnp.where(t == 18, -low, qaux)))
        qa_ref[head] = jnp.where(mine, q, aux)
    o_ref[...] = jnp.where(lane < HEAD_DIM, outs[0], outs[1]).astype(BF)


def attn_fwd_call(q, k, v, qaux, kaux, live, pair):
    tokens = q.shape[0]
    rows = 256
    whole = lambda i: (0, 0)
    block = lambda i: (i, 0)
    return pl.pallas_call(
        attn_fwd_kernel,
        grid=(tokens // rows,),
        in_specs=[
            pl.BlockSpec((rows, LANES), lambda i: (i, pair)),
            pl.BlockSpec((tokens, LANES), lambda i: (0, pair)),
            pl.BlockSpec((tokens, LANES), lambda i: (0, pair)),
            pl.BlockSpec((rows, LANES), block),
            pl.BlockSpec((tokens, LANES), whole),
            pl.BlockSpec((rows, 1), block),
        ],
        out_specs=[
            pl.BlockSpec((rows, LANES), block),
            pl.BlockSpec((2, rows, LANES), lambda i: (0, i, 0)),
            pl.BlockSpec((2, tokens, LANES), lambda i: (0, 0, 0)),
        ],
        out_shape=[
            jax.ShapeDtypeStruct((tokens, LANES), BF),
            jax.ShapeDtypeStruct((2, tokens, LANES), BF),
            jax.ShapeDtypeStruct((2, tokens, LANES), BF),
        ],
        scratch_shapes=[pltpu.VMEM((rows, tokens), F32)],
        compiler_params=pltpu.CompilerParams(vmem_limit_bytes=VMEM_LIMIT),
        cost_estimate=pl.CostEstimate(
            flops=8 * tokens * tokens * LANES, bytes_accessed=4 << 20, transcendentals=0
        ),
        name="attn_fwd",
    )(q, k, v, qaux, kaux, live)


def attn_bwd_kernel(
    qa_ref, ka_ref, v_ref, do_ref, o_ref, cosq_ref, sinq_ref, cosk_ref, sink_ref,
    dq_ref, dk_ref, dv_ref, va_ref, kt_ref, dk_acc, dv_acc,
):
    step = pl.program_id(0)
    keys = v_ref.shape[0]
    rows = do_ref.shape[0]
    chunk = 512
    lane_k = lax.broadcasted_iota(jnp.int32, (keys, LANES), 1)
    lane = lax.broadcasted_iota(jnp.int32, (rows, LANES), 1)
    zero = jnp.zeros((), BF)

    @pl.when(step == 0)
    def _():
        v = v_ref[...]
        ones = jnp.where(lane_k % HEAD_DIM < 3, jnp.ones((), BF), zero)
        for head in range(2):
            mine = (lane_k < HEAD_DIM) if head == 0 else (lane_k >= HEAD_DIM)
            va_ref[head] = jnp.where(mine, v, ones)
            own = jnp.where(mine, ka_ref[head], zero).astype(F32)
            kt_ref[head] = own.T.astype(BF)
        dk_acc[...] = jnp.zeros_like(dk_acc)
        dv_acc[...] = jnp.zeros_like(dv_acc)

    grad = do_ref[...]
    product = grad.astype(F32) * o_ref[...].astype(F32)
    turned = jnp.zeros((LANES, rows), F32)
    for head in range(2):
        mine = (lane < HEAD_DIM) if head == 0 else (lane >= HEAD_DIM)
        delta = jnp.sum(jnp.where(mine, product, 0.0), axis=-1, keepdims=True)
        high = delta.astype(BF)
        rest = delta - high.astype(F32)
        mid = rest.astype(BF)
        low = (rest - mid.astype(F32)).astype(BF)
        t = lane % HEAD_DIM
        aux = jnp.where(t == 0, -high, jnp.where(t == 1, -mid, jnp.where(t == 2, -low, zero)))
        grad_aug = jnp.where(mine, grad, aux)
        grad_own = jnp.where(mine, grad, zero)
        qa = qa_ref[head]
        q_own = jnp.where(mine, qa, zero)
        for at in range(0, keys, chunk):
            some = slice(at, at + chunk)
            prob = jnp.exp(dot_nt(ka_ref[head, some, :], qa))
            back = dot_nt(va_ref[head, some, :], grad_aug)
            score_grad = (prob * back).astype(BF)
            dv_acc[some, :] += dot_nn(prob.astype(BF), grad_own)
            dk_acc[some, :] += dot_nn(score_grad, q_own)
            turned += dot_nn(kt_ref[head, :, some], score_grad)
    dq = turned.T * (HEAD_DIM**-0.5)
    dq_ref[...] = (dq * cosq_ref[...] - swap_halves(dq) * sinq_ref[...]).astype(BF)

    @pl.when(step == pl.num_programs(0) - 1)
    def _():
        dk = dk_acc[...]
        dk_ref[...] = (dk * cosk_ref[...] - swap_halves(dk) * sink_ref[...]).astype(BF)
        dv_ref[...] = dv_acc[...].astype(BF)


def attn_bwd_call(qa, ka, v, grad, o, cosine, sine, pair):
    tokens = v.shape[0]
    rows = 256
    whole = lambda i: (0, 0)
    block = lambda i: (i, 0)
    return pl.pallas_call(
        attn_bwd_kernel,
        grid=(tokens // rows,),
        in_specs=[
            pl.BlockSpec((2, rows, LANES), lambda i: (0, i, 0)),
            pl.BlockSpec((2, tokens, LANES), lambda i: (0, 0, 0)),
            pl.BlockSpec((tokens, LANES), lambda i: (0, pair)),
            pl.BlockSpec((rows, LANES), block),
            pl.BlockSpec((rows, LANES), block),
            pl.BlockSpec((rows, LANES), block),
            pl.BlockSpec((rows, LANES), block),
            pl.BlockSpec((tokens, LANES), whole),
            pl.BlockSpec((tokens, LANES), whole),
        ],
        out_specs=[
            pl.BlockSpec((rows, LANES), block),
            pl.BlockSpec((tokens, LANES), whole),
            pl.BlockSpec((tokens, LANES), whole),
        ],
        out_shape=[jax.ShapeDtypeStruct((tokens, LANES), BF)] * 3,
        scratch_shapes=[
            pltpu.VMEM((2, tokens, LANES), BF),
            pltpu.VMEM((2, LANES, tokens), BF),
            pltpu.VMEM((tokens, LANES), F32),
            pltpu.VMEM((tokens, LANES), F32),
        ],
        compiler_params=pltpu.CompilerParams(vmem_limit_bytes=VMEM_LIMIT),
        cost_estimate=pl.CostEstimate(
            flops=20 * tokens * tokens * LANES, bytes_accessed=6 << 20, transcendentals=0
        ),
        name="attn_bwd",
    )(qa, ka, v, grad, o, cosine, sine, cosine, sine)


def ffn_kernel(x_ref, g_ref, w_ref, mlp_ref, back_ref, dw_ref):
    step = pl.program_id(0)
    blocks = w_ref.shape[0]

    def weight(part):
        return jnp.concatenate([w_ref[d, 0, part] for d in range(blocks)], axis=-1)

    x = x_ref[...]
    grad = g_ref[...]
    w_act, w_lin, w_out = weight(0), weight(1), weight(2)
    act_in = dot_nt(w_act, x)
    linear = dot_nt(w_lin, x)
    hidden_grad = dot_nt(w_out, grad)
    cdf = 0.5 * (1.0 + lax.erf(act_in * (2.0**-0.5)))
    act = act_in * cdf
    slope = cdf + act_in * jnp.exp(-0.5 * act_in * act_in) * ((2.0 * math.pi) ** -0.5)
    hidden = (act * linear).astype(BF)
    d_act = (hidden_grad * linear * slope).astype(BF)
    d_lin = (hidden_grad * act).astype(BF)

    def put(part, value):
        value = value.astype(BF)
        for d in range(blocks):
            dw_ref[d, 0, part] = value[:, d * LANES : (d + 1) * LANES]

    put(2, dot_nn(hidden, grad))
    put(0, dot_nn(d_act, x))
    put(1, dot_nn(d_lin, x))
    mlp = dot_tn(hidden, w_out)
    back = dot_tn(d_act, w_act) + dot_tn(d_lin, w_lin)

    @pl.when(step == 0)
    def _():
        mlp_ref[...] = mlp
        back_ref[...] = back

    @pl.when(step > 0)
    def _():
        mlp_ref[...] += mlp
        back_ref[...] += back


def ffn_call(x, grad, weights):
    tokens, model = x.shape
    blocks, quarters, parts, units, unused = weights.shape
    whole = lambda i: (0, 0)
    wide = pl.BlockSpec((blocks, 1, parts, units, LANES), lambda i: (0, i, 0, 0, 0))
    return pl.pallas_call(
        ffn_kernel,
        grid=(quarters,),
        in_specs=[pl.BlockSpec((tokens, model), whole), pl.BlockSpec((tokens, model), whole), wide],
        out_specs=[pl.BlockSpec((tokens, model), whole), pl.BlockSpec((tokens, model), whole), wide],
        out_shape=[
            jax.ShapeDtypeStruct((tokens, model), F32),
            jax.ShapeDtypeStruct((tokens, model), F32),
            jax.ShapeDtypeStruct(weights.shape, BF),
        ],
        compiler_params=pltpu.CompilerParams(vmem_limit_bytes=VMEM_LIMIT),
        cost_estimate=pl.CostEstimate(
            flops=18 * tokens * model * units * quarters,
            bytes_accessed=36 << 20,
            transcendentals=0,
        ),
        name="ffn",
    )(x, grad, weights)


def pieces_along(values, ways):
    here = values
    below, above = [], []
    up, down = here, here
    for hop in range(1, ways):
        up = lax.ppermute(up, "mp", [(i, i + 1) for i in range(hop - 1, ways - 1)])
        down = lax.ppermute(down, "mp", [(i, i - 1) for i in range(1, ways - hop + 1)])
        below.append(up)
        above.append(down)
    line = jnp.concatenate(below[::-1] + [here] + above, axis=0)
    rows = values.shape[0]
    at = (ways - 1 - lax.axis_index("mp")) * rows
    return lax.dynamic_slice_in_dim(line, at, ways * rows, axis=0)


def swap_rows(values, ways):
    rows = values.shape[0] // ways
    me = lax.axis_index("mp")
    blocks = values.reshape(ways, rows, values.shape[1])
    out = jnp.zeros_like(blocks)
    own = lax.dynamic_index_in_dim(blocks, me, 0, keepdims=False)
    out = lax.dynamic_update_index_in_dim(out, own, me, 0)
    for k in range(1, ways):
        sent = lax.dynamic_index_in_dim(blocks, (me + k) % ways, 0, keepdims=False)
        got = lax.ppermute(sent, "mp", [(i, (i + k) % ways) for i in range(ways)])
        out = lax.dynamic_update_index_in_dim(out, got, (me - k) % ways, 0)
    return out


def add_low(a, b):
    return (a.astype(F32) + b.astype(F32)).astype(BF)


def pick(values, at, axis):
    return lax.dynamic_index_in_dim(values, at, axis, keepdims=False)


def sum_slabs(values):
    dp = lax.axis_index("dp")
    core, x, y = dp % 2, (dp // 2) % 2, dp // 4
    flip = lambda bit: [(i, i ^ bit) for i in range(8)]
    rows = values.shape[2]
    g = values.reshape(2, 2, 2, 4, rows, LANES)
    g = add_low(pick(g, core, 2), lax.ppermute(pick(g, 1 - core, 2), "dp", flip(1)))
    a, b = g[:, :, :2], g[:, :, 2:]
    a = add_low(pick(a, x, 1), lax.ppermute(pick(a, 1 - x, 1), "dp", flip(2)))
    b = add_low(pick(b, y, 0), lax.ppermute(pick(b, 1 - y, 0), "dp", flip(4)))
    a = add_low(pick(a, y, 0), lax.ppermute(pick(a, 1 - y, 0), "dp", flip(4)))
    b = add_low(pick(b, x, 0), lax.ppermute(pick(b, 1 - x, 0), "dp", flip(2)))
    g = jnp.concatenate([a, b], axis=0)
    me = lax.axis_index("mp")
    total = pick(g, me, 0).astype(F32)
    for k in range(1, 4):
        sent = pick(g, (me + k) % 4, 0)
        total += lax.ppermute(sent, "mp", [(i, (i + k) % 4) for i in range(4)]).astype(F32)
    return total


def sum_small(values, sizes):
    for axis, size in sizes:
        total = values
        for k in range(1, size):
            total += lax.ppermute(values, axis, [(i, (i + k) % size) for i in range(size)])
        values = total
    return values


def local(
    sizes,
    layer_input,
    segment_ids,
    grad_out,
    qkv_weight,
    attn_weight,
    inner_weight,
    outer_weight,
    attn_gain,
    mlp_gain,
):
    dps, mps = sizes
    rows, model = layer_input.shape
    segment = segment_ids[0]
    length = segment.shape[0]
    head_cols = qkv_weight.shape[2]
    units = inner_weight.shape[2]
    wide = model // LANES
    me = lax.axis_index("mp")
    my_start = me * rows
    tokens = layer_input.astype(F32)

    part = jnp.concatenate(
        [inner_weight.transpose(1, 2, 0), outer_weight.T[None]], axis=0
    )
    attn_part = attn_weight.T
    qkv_part = qkv_weight.reshape(qkv_weight.shape[0], 3 * head_cols)
    qkv_mine = lax.all_gather(qkv_part, "dp", axis=0, tiled=True)

    def every(values):
        got = lax.all_gather(values, ("dp", "mp"), axis=0)
        if dps != wide:
            lanes = values.shape[-1]
            got = got.reshape((dps, mps) + values.shape)
            got = got.reshape((wide, dps // wide, mps) + values.shape)
            got = jnp.moveaxis(got, 1, -2)
            return got.reshape((wide, mps) + values.shape[:-1] + (LANES,))
        return got.reshape((dps, mps) + values.shape)

    def shared(values):
        if dps == wide:
            return sum_slabs(values)
        lanes = LANES * wide // dps
        cut = values.reshape(values.shape[:-1] + (dps // wide, lanes))
        cut = jnp.moveaxis(cut, -2, 1).reshape((dps * mps,) + values.shape[2:-1] + (lanes,))
        return lax.psum_scatter(
            cut.astype(F32), ("dp", "mp"), scatter_dimension=0, tiled=True
        )[0]

    attn_all = every(attn_part)
    ffn_all = every(part)
    attn_t = attn_all.transpose(1, 2, 0, 3).reshape(model, model)

    cosine, sine = rope_tables(segment)
    lane = jnp.arange(LANES, dtype=jnp.int32) % HEAD_DIM
    same = segment[:, None] == lane[None, :]
    qaux = jnp.where(same | (lane >= 16)[None, :], 0.0, -BIG).astype(BF)
    kaux = jnp.where(same & (lane < 16)[None, :], 1.0, 0.0)
    kaux = jnp.where(((lane >= 16) & (lane < 19))[None, :], 1.0, kaux).astype(BF)
    live = (segment != 0).astype(F32)[:, None]
    live_mine = lax.dynamic_slice_in_dim(live, my_start, rows)

    x_all = pieces_along(layer_input, mps)
    normed_all, q, k, v = qkv_call(x_all, attn_gain[None], qkv_mine, cosine, sine)

    pairs = head_cols // LANES
    kept, heads = [], []
    for pair in range(pairs):
        o, qa, ka = attn_fwd_call(q, k, v, qaux, kaux, live, pair)
        kept.append((o, qa, ka))
        heads.append(swap_rows(o, mps))
    heads_out = jnp.stack(heads, axis=1)
    heads_out = heads_out.transpose(2, 0, 1, 3).reshape(rows, model)
    attn_out = dot_nn(heads_out, attn_t)
    middle = tokens + attn_out
    vhat, scale = norm_stats(middle)
    inner_in = (vhat * mlp_gain).astype(BF)
    mlp_out, inner_in_grad, ffn_grad = ffn_call(inner_in, grad_out, ffn_all)
    layer_output = (middle + mlp_out).astype(BF)
    squares = jnp.stack(
        [jnp.sum(live_mine * a * a) for a in (tokens, attn_out, middle, mlp_out)]
        + [jnp.sum(live_mine)]
    )
    ffn_sum = shared(ffn_grad.reshape(wide, mps, 3 * units, LANES)).reshape(3, units, -1)

    mlp_gain_part = jnp.sum(inner_in_grad * vhat, axis=0)
    middle_grad = grad_out.astype(F32) + norm_back(vhat, scale, mlp_gain, inner_in_grad)
    middle_low = middle_grad.astype(BF)
    heads_grad = dot_nt(middle_low, attn_t).astype(BF)
    attn_grad = dot_tn(heads_out, middle_low).astype(BF)
    attn_slab = attn_grad.reshape(mps, model // mps, wide, LANES).transpose(2, 0, 1, 3)
    attn_sum = shared(attn_slab)

    by_owner = heads_grad.reshape(rows, mps, pairs, LANES)
    returned, own = [], []
    for pair in range(pairs):
        sent = by_owner[:, :, pair].transpose(1, 0, 2).reshape(mps * rows, LANES)
        grad = swap_rows(sent, mps).reshape(length, LANES)
        o, qa, ka = kept[pair]
        parts = attn_bwd_call(qa, ka, v, grad, o, cosine, sine, pair)
        low = jnp.concatenate(parts, axis=1)
        own.append(parts)
        returned.append(swap_rows(low, mps))
    qkv_low = jnp.concatenate([own[p][c] for c in range(3) for p in range(pairs)], axis=1)
    qkv_grad = dot_tn(normed_all, qkv_low)
    qkv_sum = lax.psum_scatter(qkv_grad, "dp", scatter_dimension=0, tiled=True)

    qkv_full = lax.all_gather(qkv_part, ("dp", "mp"), axis=0).reshape(
        dps, mps, -1, 3, pairs, LANES
    )
    normed_grad = jnp.zeros((rows, model), F32)
    for pair in range(pairs):
        w = qkv_full[:, :, :, :, pair].transpose(1, 3, 4, 0, 2).reshape(mps, 3 * LANES, model)
        for z in range(mps):
            normed_grad += dot_nn(returned[pair][z], w[z])
    vhat_in, scale_in = norm_stats(tokens)
    attn_gain_part = jnp.sum(normed_grad * vhat_in, axis=0)
    input_grad = middle_grad + norm_back(vhat_in, scale_in, attn_gain, normed_grad)

    small = jnp.stack([attn_gain_part, mlp_gain_part, jnp.pad(squares, (0, model - 5))])
    if dps == wide:
        small = sum_small(small, (("dp", dps), ("mp", mps)))
    else:
        small = lax.psum(small, ("dp", "mp"))
    rms_values = jnp.sqrt(small[2, :4] / (small[2, 4] * model))
    return (
        layer_output,
        input_grad,
        qkv_sum.reshape(-1, 3, head_cols),
        attn_sum.T,
        ffn_sum[:2].transpose(2, 0, 1),
        ffn_sum[2].T,
        small[0],
        small[1],
        rms_values,
    )


def solution(mesh):
    sizes = (mesh.shape["dp"], mesh.shape["mp"])
    return jax.shard_map(
        functools.partial(local, sizes),
        mesh=mesh,
        in_specs=(
            P(("dp", "mp"), None),
            P("dp", None),
            P(("dp", "mp"), None),
            P("dp", None, "mp"),
            P("dp", "mp"),
            P("dp", None, "mp"),
            P("dp", "mp"),
            P(),
            P(),
        ),
        out_specs=(
            P(("dp", "mp"), None),
            P(("dp", "mp"), None),
            P("dp", None, "mp"),
            P("dp", "mp"),
            P("dp", None, "mp"),
            P("dp", "mp"),
            P(),
            P(),
            P(),
        ),
        check_vma=False,
    )
```

```python
import functools
import math

import jax
import jax.numpy as jnp
from jax import lax
from jax.experimental import pallas as pl
from jax.experimental.pallas import tpu as pltpu
from jax.sharding import PartitionSpec as P

HEAD_DIM = 64
NORM_EPS = 1e-05
ROPE_BASE = 160000.0
BIG = 1e30
LANES = 128
WAYS = 4
BF = jnp.bfloat16
F32 = jnp.float32
VMEM_LIMIT = 56 * 1024 * 1024


def dot_nn(a, b):
    return lax.dot_general(a, b, (((1,), (0,)), ((), ())), preferred_element_type=F32)


def dot_nt(a, b):
    return lax.dot_general(a, b, (((1,), (1,)), ((), ())), preferred_element_type=F32)


def dot_tn(a, b):
    return lax.dot_general(a, b, (((0,), (0,)), ((), ())), preferred_element_type=F32)


def norm_stats(values):
    centre = jnp.mean(values, axis=-1, keepdims=True)
    shifted = values - centre
    spread = jnp.mean(shifted * shifted, axis=-1, keepdims=True)
    scale = lax.rsqrt(spread + NORM_EPS)
    return shifted * scale, scale


def norm_back(vhat, scale, gain, grad):
    u = grad * gain
    mean_u = jnp.mean(u, axis=-1, keepdims=True)
    mean_uv = jnp.mean(u * vhat, axis=-1, keepdims=True)
    return scale * (u - mean_u - vhat * mean_uv)


def doc_positions(segment):
    length = segment.shape[0]
    places = jnp.arange(length, dtype=jnp.int32)
    before = jnp.concatenate([jnp.full((1,), -1, jnp.int32), segment[:-1]])
    starts = jnp.where(segment != before, places, jnp.zeros_like(places))
    return places - lax.cummax(starts, axis=0)


def rope_tables(positions):
    half = HEAD_DIM // 2
    lane = jnp.arange(LANES, dtype=jnp.int32)
    frequency = jnp.exp((lane % half).astype(F32) * (-2.0 * math.log(ROPE_BASE) / HEAD_DIM))
    angle = positions.astype(F32)[:, None] * frequency[None, :]
    first = (lane % HEAD_DIM < half)[None, :]
    sine = jnp.sin(angle)
    return jnp.cos(angle), jnp.where(first, -sine, sine)


def swap_halves(values):
    lane = lax.broadcasted_iota(jnp.int32, values.shape, 1)
    first = lane % HEAD_DIM < HEAD_DIM // 2
    back = pltpu.roll(values, LANES - HEAD_DIM // 2, 1)
    ahead = pltpu.roll(values, HEAD_DIM // 2, 1)
    return jnp.where(first, back, ahead)


def choose(at, values):
    out = values[0]
    for i in range(1, len(values)):
        out = jnp.where(at == i, values[i], out)
    return out


def params():
    return pltpu.CompilerParams(vmem_limit_bytes=VMEM_LIMIT)


def cost(flops, mib):
    return pl.CostEstimate(flops=int(flops), bytes_accessed=int(mib * 2**20), transcendentals=0)


def call(kernel, scalars, grid, in_specs, out_specs, out_shape, scratch, estimate, name):
    spec = pltpu.PrefetchScalarGridSpec(
        num_scalar_prefetch=1,
        grid=grid,
        in_specs=in_specs,
        out_specs=out_specs,
        scratch_shapes=scratch,
    )
    return functools.partial(
        pl.pallas_call(
            kernel,
            grid_spec=spec,
            out_shape=out_shape,
            compiler_params=params(),
            cost_estimate=estimate,
            name=name,
        ),
        scalars,
    )


def full(shape):
    return pl.BlockSpec(shape, lambda i, s: (0,) * len(shape))


def shape_of(shape, dtype):
    return jax.ShapeDtypeStruct(shape, dtype)


def side_by_side(ref, *at):
    return jnp.concatenate([ref[(d, *at)] for d in range(ref.shape[0])], axis=-1)


def qkv_kernel(s_ref, x_ref, gain_ref, w_ref, cos_ref, sin_ref, n_ref, q_ref, k_ref, v_ref):
    vhat, unused = norm_stats(x_ref[...].astype(F32))
    normed = (vhat * gain_ref[...]).astype(BF)
    n_ref[...] = normed
    flat = dot_nt(normed, side_by_side(w_ref, 0))
    cosine = cos_ref[...]
    sine = sin_ref[...]
    for pair in range(q_ref.shape[1] // LANES):
        here = slice(pair * LANES, (pair + 1) * LANES)
        for part, out in ((0, q_ref), (1, k_ref)):
            at = (pair * 3 + part) * LANES
            u = flat[:, at : at + LANES]
            out[:, here] = (u * cosine + swap_halves(u) * sine).astype(BF)
        at = (pair * 3 + 2) * LANES
        v_ref[:, here] = flat[:, at : at + LANES].astype(BF)


def qkv_call(scalars, x, gain, weight, cosine, sine):
    tokens, model = x.shape
    rows = tokens // WAYS
    wide, unused, cols3, unused = weight.shape
    cols = cols3 // 3
    block = lambda width: pl.BlockSpec((rows, width), lambda i, s: (i, 0))
    return call(
        qkv_kernel,
        scalars,
        (WAYS,),
        [
            block(model),
            full((1, model)),
            pl.BlockSpec((wide, 1, cols3, LANES), lambda i, s: (0, s[2], 0, 0)),
            block(LANES),
            block(LANES),
        ],
        [block(model)] + [block(cols)] * 3,
        [shape_of((tokens, model), BF)] + [shape_of((tokens, cols), BF)] * 3,
        [],
        cost(2 * tokens * model * cols3, 14),
        "qkv",
    )(x, gain, weight, cosine, sine)


def attn_fwd_kernel(s_ref, *refs):
    q_ref, k_ref, v_ref, qaux_ref, kaux_ref, live_ref = refs[:6]
    o_refs, qa_ref, ka_ref, s_scr = refs[6:10], refs[10], refs[11], refs[12]
    step = pl.program_id(0)
    rows = q_ref.shape[0]
    chunk = k_ref.shape[0] // WAYS
    per = chunk // rows
    piece = step // per
    lane_k = lax.broadcasted_iota(jnp.int32, (chunk, LANES), 1)
    lane = lax.broadcasted_iota(jnp.int32, (rows, LANES), 1)

    @pl.when(step == 0)
    def _():
        for m in range(WAYS):
            some = slice(m * chunk, (m + 1) * chunk)
            k = k_ref[some, :]
            kaux = kaux_ref[some, :]
            ka_ref[0, some, :] = jnp.where(lane_k < HEAD_DIM, k, kaux)
            ka_ref[1, some, :] = jnp.where(lane_k >= HEAD_DIM, k, kaux)

    q = q_ref[...] * jnp.asarray(HEAD_DIM**-0.5, BF)
    qaux = qaux_ref[...]
    live = live_ref[...]
    outs = []
    for head in range(2):
        mine = (lane < HEAD_DIM) if head == 0 else (lane >= HEAD_DIM)
        qa = jnp.where(mine, q, qaux)
        top = None
        for m in range(WAYS):
            some = slice(m * chunk, (m + 1) * chunk)
            s = dot_nt(qa, ka_ref[head, some, :])
            s_scr[:, some] = s
            part = jnp.max(s, axis=-1, keepdims=True)
            top = part if top is None else jnp.maximum(top, part)
        total = jnp.zeros((rows, 1), F32)
        mixed = jnp.zeros((rows, LANES), F32)
        for m in range(WAYS):
            p = jnp.exp(s_scr[:, m * chunk : (m + 1) * chunk] - top)
            total += jnp.sum(p, axis=-1, keepdims=True)
            mixed += dot_nn(p.astype(BF), v_ref[m * chunk : (m + 1) * chunk, :])
        outs.append(mixed * (live / total))
        log_sum = jnp.where(live > 0, top + jnp.log(total), BIG)
        high = log_sum.astype(BF)
        rest = log_sum - high.astype(F32)
        mid = rest.astype(BF)
        low = (rest - mid.astype(F32)).astype(BF)
        t = lane % HEAD_DIM
        aux = jnp.where(t == 16, -high, jnp.where(t == 17, -mid, jnp.where(t == 18, -low, qaux)))
        qa_ref[head] = jnp.where(mine, q, aux)
    out = jnp.where(lane < HEAD_DIM, outs[0], outs[1]).astype(BF)
    for m in range(WAYS):

        @pl.when(piece == m)
        def _(m=m):
            o_refs[m][...] = out


def piece_block(m, rows, per):
    return pl.BlockSpec((rows, LANES), lambda i, s: (jnp.clip(i - per * m, 0, per - 1), 0))


def attn_fwd_call(scalars, q, k, v, qaux, kaux, live, pair):
    tokens = q.shape[0]
    chunk = tokens // WAYS
    rows = 256
    per = chunk // rows
    fixed = pl.BlockSpec((tokens, LANES), lambda i, s: (0, pair))
    block = pl.BlockSpec((rows, LANES), lambda i, s: (i, 0))
    outs = call(
        attn_fwd_kernel,
        scalars,
        (tokens // rows,),
        [
            pl.BlockSpec((rows, LANES), lambda i, s: (i, pair)),
            fixed,
            fixed,
            block,
            full((tokens, LANES)),
            pl.BlockSpec((rows, 1), lambda i, s: (i, 0)),
        ],
        [piece_block(m, rows, per) for m in range(WAYS)]
        + [pl.BlockSpec((2, rows, LANES), lambda i, s: (0, i, 0)), full((2, tokens, LANES))],
        [shape_of((chunk, LANES), BF)] * WAYS + [shape_of((2, tokens, LANES), BF)] * 2,
        [pltpu.VMEM((rows, tokens), F32)],
        cost(16 * tokens * tokens * LANES, 4),
        "attn_fwd",
    )(q, k, v, qaux, kaux, live)
    return outs[:WAYS], outs[WAYS], outs[WAYS + 1]


def attn_bwd_kernel(s_ref, *refs):
    qa_ref, ka_ref = refs[:2]
    v_ref, do_refs, o_refs = refs[2], refs[3:7], refs[7:11]
    cosq_ref, sinq_ref, cosk_ref, sink_ref = refs[11:15]
    out_refs = refs[15:19]
    va_ref, kt_ref, dk_acc, dv_acc = refs[19:23]
    step = pl.program_id(0)
    rows = do_refs[0].shape[0]
    chunk = v_ref.shape[0] // WAYS
    per = chunk // rows
    piece = step // per
    lane_k = lax.broadcasted_iota(jnp.int32, (chunk, LANES), 1)
    lane = lax.broadcasted_iota(jnp.int32, (rows, LANES), 1)
    zero = jnp.zeros((), BF)

    @pl.when(step == 0)
    def _():
        ones = jnp.where(lane_k % HEAD_DIM < 3, jnp.ones((), BF), zero)
        for m in range(WAYS):
            some = slice(m * chunk, (m + 1) * chunk)
            v = v_ref[some, :]
            for head in range(2):
                mine = (lane_k < HEAD_DIM) if head == 0 else (lane_k >= HEAD_DIM)
                va_ref[head, some, :] = jnp.where(mine, v, ones)
                own = jnp.where(mine, ka_ref[head, some, :], zero).astype(F32)
                kt_ref[head, :, some] = own.T.astype(BF)
        dk_acc[...] = jnp.zeros_like(dk_acc)
        dv_acc[...] = jnp.zeros_like(dv_acc)

    grad = choose(piece, [r[...] for r in do_refs])
    out = choose(piece, [r[...] for r in o_refs])
    product = grad.astype(F32) * out.astype(F32)
    turned = jnp.zeros((LANES, rows), F32)
    for head in range(2):
        mine = (lane < HEAD_DIM) if head == 0 else (lane >= HEAD_DIM)
        delta = jnp.sum(jnp.where(mine, product, 0.0), axis=-1, keepdims=True)
        high = delta.astype(BF)
        rest = delta - high.astype(F32)
        mid = rest.astype(BF)
        low = (rest - mid.astype(F32)).astype(BF)
        t = lane % HEAD_DIM
        aux = jnp.where(t == 0, -high, jnp.where(t == 1, -mid, jnp.where(t == 2, -low, zero)))
        grad_aug = jnp.where(mine, grad, aux)
        grad_own = jnp.where(mine, grad, zero)
        qa = qa_ref[head]
        q_own = jnp.where(mine, qa, zero)
        for m in range(WAYS):
            some = slice(m * chunk, (m + 1) * chunk)
            prob = jnp.exp(dot_nt(ka_ref[head, some, :], qa))
            back = dot_nt(va_ref[head, some, :], grad_aug)
            score_grad = (prob * back).astype(BF)
            dv_acc[some, :] += dot_nn(prob.astype(BF), grad_own)
            dk_acc[some, :] += dot_nn(score_grad, q_own)
            turned += dot_nn(kt_ref[head, :, some], score_grad)
    dq = turned.T * (HEAD_DIM**-0.5)
    dq = (dq * cosq_ref[...] - swap_halves(dq) * sinq_ref[...]).astype(BF)
    for m in range(WAYS):

        @pl.when(piece == m)
        def _(m=m):
            here = pl.ds(pl.multiple_of((step - m * per) * rows, rows), rows)
            out_refs[m][here, :LANES] = dq

    @pl.when(step == pl.num_programs(0) - 1)
    def _():
        for m in range(WAYS):
            some = slice(m * chunk, (m + 1) * chunk)
            dk = dk_acc[some, :]
            dk = dk * cosk_ref[some, :] - swap_halves(dk) * sink_ref[some, :]
            out_refs[m][:, LANES : 2 * LANES] = dk.astype(BF)
            out_refs[m][:, 2 * LANES :] = dv_acc[some, :].astype(BF)


def attn_bwd_call(scalars, qa, ka, v, grad, o, cosine, sine, pair):
    tokens = v.shape[0]
    chunk = tokens // WAYS
    rows = 256
    per = chunk // rows
    moving = [piece_block(m, rows, per) for m in range(WAYS)]
    block = pl.BlockSpec((rows, LANES), lambda i, s: (i, 0))
    return call(
        attn_bwd_kernel,
        scalars,
        (tokens // rows,),
        [pl.BlockSpec((2, rows, LANES), lambda i, s: (0, i, 0)), full((2, tokens, LANES))]
        + [pl.BlockSpec((tokens, LANES), lambda i, s: (0, pair))]
        + moving * 2
        + [block, block, full((tokens, LANES)), full((tokens, LANES))],
        [full((chunk, 3 * LANES))] * WAYS,
        [shape_of((chunk, 3 * LANES), BF)] * WAYS,
        [
            pltpu.VMEM((2, tokens, LANES), BF),
            pltpu.VMEM((2, LANES, tokens), BF),
            pltpu.VMEM((tokens, LANES), F32),
            pltpu.VMEM((tokens, LANES), F32),
        ],
        cost(28 * tokens * tokens * LANES, 8),
        "attn_bwd",
    )(qa, ka, v, *grad, *o, cosine, sine, cosine, sine)


def middle_kernel(s_ref, *refs):
    o_refs = refs[:8]
    x_ref, w_ref, gain_ref, live_ref, middle_ref, inner_ref, square_ref = refs[8:]
    z = s_ref[0]
    tokens = x_ref[...].astype(F32)
    attn_out = jnp.zeros(tokens.shape, F32)
    for m in range(WAYS):
        o = jnp.concatenate([o_refs[2 * m][...], o_refs[2 * m + 1][...]], axis=-1)
        attn_out += dot_nn(o, side_by_side(w_ref, z ^ m))
    middle = tokens + attn_out
    vhat, unused = norm_stats(middle)
    middle_ref[...] = middle
    inner_ref[...] = (vhat * gain_ref[...]).astype(BF)
    live = live_ref[...]
    square_ref[...] = jnp.concatenate(
        [jnp.sum(live * a * a, axis=0, keepdims=True) for a in (tokens, attn_out, middle)]
        + [jnp.zeros((5, tokens.shape[1]), F32)],
        axis=0,
    )


def middle_call(scalars, heads, x, weight, gain, live):
    rows, model = x.shape
    wide = weight.shape[0]
    depth = model // WAYS
    return call(
        middle_kernel,
        scalars,
        (1,),
        [full((rows, LANES))] * 8
        + [
            full((rows, model)),
            full((wide, WAYS, depth, LANES)),
            full((1, model)),
            full((rows, 1)),
        ],
        [full((rows, model)), full((rows, model)), full((8, model))],
        [shape_of((rows, model), F32), shape_of((rows, model), BF), shape_of((8, model), F32)],
        [],
        cost(2 * rows * model * model, 8),
        "middle",
    )(*heads, x, weight, gain, live)


def middle_back_kernel(
    s_ref, middle_ref, mlp_ref, back_ref, grad_ref, w_ref, gain_ref, live_ref,
    output_ref, mgrad_ref, low_ref, small_ref, *hg_refs,
):
    z = s_ref[0]
    middle = middle_ref[...]
    mlp = mlp_ref[...]
    back = back_ref[...]
    vhat, scale = norm_stats(middle)
    middle_grad = grad_ref[...].astype(F32) + norm_back(vhat, scale, gain_ref[...], back)
    low = middle_grad.astype(BF)
    for m in range(WAYS):
        hg = dot_nt(low, side_by_side(w_ref, z ^ m)).astype(BF)
        hg_refs[2 * m][...] = hg[:, :LANES]
        hg_refs[2 * m + 1][...] = hg[:, LANES:]
    mgrad_ref[...] = middle_grad
    low_ref[...] = low
    output_ref[...] = (middle + mlp).astype(BF)
    small_ref[...] = jnp.concatenate(
        [
            jnp.sum(live_ref[...] * mlp * mlp, axis=0, keepdims=True),
            jnp.sum(back * vhat, axis=0, keepdims=True),
            jnp.zeros((6, mlp.shape[1]), F32),
        ],
        axis=0,
    )


def middle_back_call(scalars, middle, mlp, back, grad, weight, gain, live):
    rows, model = middle.shape
    wide = weight.shape[0]
    depth = model // WAYS
    outs = call(
        middle_back_kernel,
        scalars,
        (1,),
        [full((rows, model))] * 4
        + [full((wide, WAYS, depth, LANES)), full((1, model)), full((rows, 1))],
        [full((rows, model))] * 3 + [full((8, model))] + [full((rows, LANES))] * 8,
        [
            shape_of((rows, model), BF),
            shape_of((rows, model), F32),
            shape_of((rows, model), BF),
            shape_of((8, model), F32),
        ]
        + [shape_of((rows, LANES), BF)] * 8,
        [],
        cost(2 * rows * model * model, 12),
        "middle_back",
    )(middle, mlp, back, grad, weight, gain, live)
    return outs[:4], outs[4:]


def own_first(core, values):
    cut = [values[:, at : at + LANES] for at in range(0, values.shape[1], LANES)]
    turned = [cut[i ^ 1] for i in range(len(cut))]
    return jnp.where(core == 0, values, jnp.concatenate(turned, axis=-1))


def put_slabs(keep_ref, send_ref, value, *at):
    for d in range(value.shape[1] // LANES):
        ref = send_ref if d % 2 else keep_ref
        ref[(d // 2, *at)] = value[:, d * LANES : (d + 1) * LANES]


def attn_grad_kernel(s_ref, *refs):
    o_refs, low_ref, keep_ref, send_ref = refs[:8], refs[8], refs[9], refs[10]
    low = own_first(s_ref[1], low_ref[...])
    for m in range(WAYS):
        o = jnp.concatenate([o_refs[2 * m][...], o_refs[2 * m + 1][...]], axis=-1)
        put_slabs(keep_ref, send_ref, dot_tn(o, low).astype(BF), s_ref[0] ^ m)


def attn_grad_call(scalars, heads, low):
    rows, model = low.shape
    shape = (model // LANES // 2, WAYS, model // WAYS, LANES)
    return call(
        attn_grad_kernel,
        scalars,
        (1,),
        [full((rows, LANES))] * 8 + [full((rows, model))],
        [full(shape)] * 2,
        [shape_of(shape, BF)] * 2,
        [],
        cost(2 * rows * model * model, 6),
        "attn_grad",
    )(*heads, low)


def ffn_kernel(s_ref, x_ref, g_ref, wa_ref, wb_ref, mlp_ref, back_ref, keep_ref, send_ref):
    step = pl.program_id(0)
    units = wb_ref.shape[2] // 2
    skip = wa_ref.shape[2] - units
    w_act = side_by_side(wa_ref, 0, slice(skip, skip + units))
    w_lin = side_by_side(wb_ref, 0, slice(0, units))
    w_out = side_by_side(wb_ref, 0, slice(units, 2 * units))
    x = x_ref[...]
    grad = g_ref[...]
    act_in = dot_nt(w_act, x)
    linear = dot_nt(w_lin, x)
    hidden_grad = dot_nt(w_out, grad)
    cdf = 0.5 * (1.0 + lax.erf(act_in * (2.0**-0.5)))
    act = act_in * cdf
    slope = cdf + act_in * jnp.exp(-0.5 * act_in * act_in) * ((2.0 * math.pi) ** -0.5)
    hidden = (act * linear).astype(BF)
    d_act = (hidden_grad * linear * slope).astype(BF)
    d_lin = (hidden_grad * act).astype(BF)
    x = own_first(s_ref[1], x)
    grad = own_first(s_ref[1], grad)
    for part, value in ((0, dot_nn(d_act, x)), (1, dot_nn(d_lin, x)), (2, dot_nn(hidden, grad))):
        some = slice(part * units, (part + 1) * units)
        put_slabs(keep_ref, send_ref, value.astype(BF), 0, some)
    mlp = dot_tn(hidden, w_out)
    back = dot_tn(d_act, w_act) + dot_tn(d_lin, w_lin)

    @pl.when(step == 0)
    def _():
        mlp_ref[...] = mlp
        back_ref[...] = back

    @pl.when(step > 0)
    def _():
        mlp_ref[...] += mlp
        back_ref[...] += back


def ffn_call(scalars, x, grad, pack_a, pack_b):
    tokens, model = x.shape
    wide, quarters, depth_a, unused = pack_a.shape
    depth_b = pack_b.shape[2]
    units = depth_b // 2
    out = (wide // 2, quarters, 3 * units, LANES)
    part = pl.BlockSpec((wide // 2, 1, 3 * units, LANES), lambda i, s: (0, i, 0, 0))
    weight = lambda depth: pl.BlockSpec((wide, 1, depth, LANES), lambda i, s: (0, i, 0, 0))
    return call(
        ffn_kernel,
        scalars,
        (quarters,),
        [full((tokens, model))] * 2 + [weight(depth_a), weight(depth_b)],
        [full((tokens, model))] * 2 + [part] * 2,
        [shape_of((tokens, model), F32)] * 2 + [shape_of(out, BF)] * 2,
        [],
        cost(18 * tokens * model * units * quarters, 40),
        "ffn",
    )(x, grad, pack_a, pack_b)


def qkv_grad_kernel(s_ref, *refs):
    low_refs, normed_ref, keep_ref, send_ref = refs[:4], refs[4], refs[5], refs[6]
    rows = low_refs[0].shape[0]
    total = None
    for m in range(WAYS):
        part = dot_tn(low_refs[m][...], normed_ref[m * rows : (m + 1) * rows, :])
        total = part if total is None else total + part
    value = total.astype(BF)
    for d in range(value.shape[1] // LANES):
        slab = value[:, d * LANES : (d + 1) * LANES]
        x = (d // 2) % 2
        at = d // 4 * 2 + d % 2

        @pl.when(s_ref[3] == x)
        def _():
            keep_ref[at] = slab

        @pl.when(s_ref[3] != x)
        def _():
            send_ref[at] = slab


def qkv_grad_call(scalars, low, normed):
    tokens, model = normed.shape
    rows, cols = low[0].shape
    shape = (model // LANES // 2, cols, LANES)
    return call(
        qkv_grad_kernel,
        scalars,
        (1,),
        [full((rows, cols))] * WAYS + [full((tokens, model))],
        [full(shape)] * 2,
        [shape_of(shape, BF)] * 2,
        [],
        cost(2 * WAYS * rows * model * cols, 7),
        "qkv_grad",
    )(*low, normed)


def input_grad_kernel(s_ref, *refs):
    low_refs = refs[:8]
    w_ref, x_ref, mgrad_ref, gain_ref, grad_ref, gain_part_ref = refs[8:]
    z = s_ref[0]
    normed_grad = jnp.zeros(x_ref.shape, F32)
    for m in range(WAYS):
        w = side_by_side(w_ref, z ^ m)
        for pair in range(2):
            at = pair * 3 * LANES
            normed_grad += dot_nn(low_refs[2 * m + pair][...], w[at : at + 3 * LANES, :])
    vhat, scale = norm_stats(x_ref[...].astype(F32))
    gain_part_ref[...] = jnp.sum(normed_grad * vhat, axis=0, keepdims=True)
    grad_ref[...] = mgrad_ref[...] + norm_back(vhat, scale, gain_ref[...], normed_grad)


def input_grad_call(scalars, low, weight, x, middle_grad, gain):
    rows, model = x.shape
    return call(
        input_grad_kernel,
        scalars,
        (1,),
        [full((rows, 3 * LANES))] * 8
        + [full(weight.shape), full((rows, model)), full((rows, model)), full((1, model))],
        [full((rows, model)), full((1, model))],
        [shape_of((rows, model), F32), shape_of((1, model), F32)],
        [],
        cost(6 * rows * model * model, 14),
        "input_grad",
    )(*low, weight, x, middle_grad, gain)


MESH = pl.DeviceIdType.MESH
UP, DOWN, TO_X, TO_Y, TO_D, CORE_OWN, CORE_X, CORE_Y, CORE_D = range(9)
FROM_Z, FROM_X, FROM_Y, FROM_D = range(4)


def gather_kernel(x_ref, *refs, packs):
    parts, x_all, outs = refs[:packs], refs[packs], refs[packs + 1 : 2 * packs + 1]
    sends, recvs, cores, locals_, token_send, token_recv = refs[2 * packs + 1 :]
    dp, z = lax.axis_index("dp"), lax.axis_index("mp")
    core, xb, yb = dp % 2, (dp // 2) % 2, dp // 4
    at_c, at_x, at_y = dp + 1 - 2 * core, dp + 2 - 4 * xb, dp + 4 - 8 * yb
    at_d = at_x + at_y - dp
    group = z // 2
    quarter = z + 2 * core - 4 * core * group

    def flip1(q):
        return q + 1 - 2 * (q % 2)

    def attention_of(m):
        h = z if m == 0 else flip1(z)
        a, g = h // 2, core
        return dp - core + a + g - 2 * a * g, 2 * core + h % 2

    def owner_of(m):
        return dp - core + group, (quarter if m == 0 else flip1(quarter))

    barrier = pltpu.get_barrier_semaphore()

    def greet(device, when=None):
        def signal():
            pl.semaphore_signal(barrier, inc=1, device_id=device, device_id_type=MESH)

        signal() if when is None else pl.when(when)(signal)

    greet((at_c, z))
    greet((at_x, z))
    greet((at_y, z))
    greet((dp, z + 1), z < WAYS - 1)
    greet((dp, z - 1), z > 0)
    here = []
    for m in range(2):
        to_dp, to_z = attention_of(m)
        from_dp, from_z = owner_of(m)
        stays = jnp.logical_and(to_dp == dp, to_z == z)
        here.append((to_dp, to_z, stays))
        greet((from_dp, from_z), jnp.logical_not(jnp.logical_and(from_dp == dp, from_z == z)))
    count = 3 + (z < WAYS - 1).astype(jnp.int32) + (z > 0).astype(jnp.int32)
    for m in range(2):
        count += 1 - here[m][2].astype(jnp.int32)
    pl.semaphore_wait(barrier, count)

    def remote(src, dst, send, recv, device):
        return pltpu.make_async_remote_copy(
            src_ref=src, dst_ref=dst, send_sem=send, recv_sem=recv,
            device_id=device, device_id_type=MESH,
        )

    def copy(p, kind, s, src=None):
        who = {CORE_X: at_x, CORE_Y: at_y, CORE_D: at_d}.get(kind, dp)
        if kind == TO_D:
            who = jnp.where(s < 2, at_x, at_y)
        slab = outs[p].at[who, s]
        send = sends.at[p, kind, s]
        if kind == UP:
            recv, device = recvs.at[p, FROM_Z, s], (dp, z + 1)
        elif kind == DOWN:
            recv, device = recvs.at[p, FROM_Z, s], (dp, z - 1)
        elif kind == TO_X:
            recv, device = recvs.at[p, FROM_X, s], (at_x, z)
        elif kind == TO_Y:
            recv, device = recvs.at[p, FROM_Y, s], (at_y, z)
        elif kind == TO_D:
            recv, device = recvs.at[p, FROM_D, s], (jnp.where(s < 2, at_y, at_x), z)
        else:
            recv, device = cores.at[p, kind - CORE_OWN, s], (at_c, z)
        return remote(slab if src is None else src, slab, send, recv, device)

    def arrived(p, sem, who, s):
        slab = outs[p].at[who, s]
        remote(slab, slab, sends.at[p, UP, s], sem, (at_c, z)).wait_recv()

    def spread(p, s, src=None):
        copy(p, TO_X, s, src).start()
        copy(p, TO_Y, s, src).start()
        copy(p, CORE_OWN, s, src).start()

    def begin(p):
        src = parts[p]
        pl.when(z < WAYS - 1)(lambda: copy(p, UP, z, src).start())
        pl.when(z > 0)(lambda: copy(p, DOWN, z, src).start())
        spread(p, z, src)
        pltpu.make_async_copy(src, outs[p].at[dp, z], locals_.at[p]).start()

    def line(p, hop):
        def below():
            s = z - hop
            arrived(p, recvs.at[p, FROM_Z, s], dp, s)
            pl.when(z < WAYS - 1)(lambda: copy(p, UP, s).start())
            spread(p, s)

        def above():
            s = z + hop
            arrived(p, recvs.at[p, FROM_Z, s], dp, s)
            pl.when(z > 0)(lambda: copy(p, DOWN, s).start())
            spread(p, s)

        pl.when(z >= hop)(below)
        pl.when(z + hop < WAYS)(above)

    def plane(p, hop):
        def one(s):
            arrived(p, recvs.at[p, FROM_X, s], at_x, s)
            copy(p, CORE_X, s).start()
            pl.when(s < 2)(lambda: copy(p, TO_D, s).start())
            arrived(p, recvs.at[p, FROM_Y, s], at_y, s)
            copy(p, CORE_Y, s).start()
            pl.when(s >= 2)(lambda: copy(p, TO_D, s).start())

        if hop == 0:
            one(z)
        else:
            pl.when(z >= hop)(lambda: one(z - hop))
            pl.when(z + hop < WAYS)(lambda: one(z + hop))

    def corner(p, hop):
        def one(s):
            arrived(p, recvs.at[p, FROM_D, s], at_d, s)
            copy(p, CORE_D, s).start()

        if hop == 0:
            one(z)
        else:
            pl.when(z >= hop)(lambda: one(z - hop))
            pl.when(z + hop < WAYS)(lambda: one(z + hop))

    def finish(p):
        for s in range(WAYS):
            for kind in range(4):
                twin = (at_c, at_x + at_c - dp, at_y + at_c - dp, at_d + at_c - dp)[kind]
                arrived(p, cores.at[p, kind, s], twin, s)
        pltpu.make_async_copy(parts[p], outs[p].at[dp, z], locals_.at[p]).wait()
        for s in range(WAYS):
            pl.when(jnp.logical_and(z < WAYS - 1, s <= z))(lambda s=s: copy(p, UP, s).wait_send())
            pl.when(jnp.logical_and(z > 0, s >= z))(lambda s=s: copy(p, DOWN, s).wait_send())
            for kind in range(TO_X, CORE_D + 1):
                copy(p, kind, s).wait_send()

    def token(m):
        to_dp, to_z, stays = here[m]
        far = remote(x_ref, x_all.at[m], token_send.at[m], token_recv.at[m], (to_dp, to_z))
        near = pltpu.make_async_copy(x_ref, x_all.at[m], token_recv.at[m])
        return far, near, stays

    def pass_on(m):
        return remote(
            x_all.at[m], x_all.at[m + 2], token_send.at[m + 2], token_recv.at[m + 2], (at_c, z)
        )

    begin(0)
    for m in range(2):
        far, near, stays = token(m)
        pl.when(stays)(near.start)
        pl.when(jnp.logical_not(stays))(far.start)
    for p in range(1, packs):
        begin(p)
    for hop in range(1, WAYS):
        line(0, hop)
    for hop in range(WAYS):
        plane(0, hop)
    for m in range(2):
        token(m)[0].wait_recv()
        pass_on(m).start()
    for hop in range(WAYS):
        corner(0, hop)
    for p in range(1, packs):
        for hop in range(1, WAYS):
            line(p, hop)
        for hop in range(WAYS):
            plane(p, hop)
        for hop in range(WAYS):
            corner(p, hop)
    for m in range(2):
        pass_on(m).wait()
        far, near, stays = token(m)
        pl.when(jnp.logical_not(stays))(far.wait_send)
    for p in range(packs):
        finish(p)


def gather_call(x, parts, dps):
    rows, model = x.shape
    packs = len(parts)
    anywhere = pl.BlockSpec(memory_space=pl.ANY)
    out = pl.pallas_call(
        functools.partial(gather_kernel, packs=packs),
        in_specs=[anywhere] * (1 + packs),
        out_specs=[anywhere] * (1 + packs),
        out_shape=[shape_of((WAYS, rows, model), BF)]
        + [shape_of((dps, WAYS) + part.shape, BF) for part in parts],
        scratch_shapes=[
            pltpu.SemaphoreType.DMA((packs, 9, WAYS)),
            pltpu.SemaphoreType.DMA((packs, 4, WAYS)),
            pltpu.SemaphoreType.DMA((packs, 4, WAYS)),
            pltpu.SemaphoreType.DMA((packs,)),
            pltpu.SemaphoreType.DMA((WAYS,)),
            pltpu.SemaphoreType.DMA((WAYS,)),
        ],
        compiler_params=pltpu.CompilerParams(collective_id=0, has_side_effects=True),
        name="gather",
    )(x, *parts)
    return out[0].reshape(WAYS * rows, model), out[1:]


def after(value, *others):
    return lax.optimization_barrier((value, *others))[0]


def add_low(a, b):
    return (a.astype(F32) + b.astype(F32)).astype(BF)


def pick(values, at, axis=0):
    return lax.dynamic_index_in_dim(values, at, axis, keepdims=False)


def flip(values, bit, dps):
    return lax.ppermute(values, "dp", [(i, i ^ bit) for i in range(dps)])


def to_attention(values, m, dps, back=False):
    pairs = []
    for dp in range(dps):
        group = dp % 2
        for t in range(WAYS):
            quarter = t ^ m
            there = (dp - group + ((quarter // 2) ^ group)) * WAYS + 2 * group + quarter % 2
            pairs.append((there, dp * WAYS + t) if back else (dp * WAYS + t, there))
    return lax.ppermute(values, ("dp", "mp"), pairs)


class Sum:
    def __init__(self, keep, send, place):
        self.place = place
        self.keep = keep.reshape((2, 2) + keep.shape[1:])
        self.got = flip(send, 1, 8).reshape(self.keep.shape)

    def planes(self):
        core, x, y, me = self.place
        half = self.keep.shape[2] // 2
        a = [v[:, :, :half] for v in (self.keep, self.got)]
        b = [v[:, :, half:] for v in (self.keep, self.got)]
        self.a = add_low(pick(a[0], x, 1), pick(a[1], x, 1))
        self.b = add_low(pick(b[0], y, 0), pick(b[1], y, 0))
        send_a = add_low(pick(a[0], 1 - x, 1), pick(a[1], 1 - x, 1))
        send_b = add_low(pick(b[0], 1 - y, 0), pick(b[1], 1 - y, 0))
        self.got_a = flip(send_a, 2, 8)
        self.got_b = flip(send_b, 4, 8)
        return send_a, send_b

    def planes_again(self):
        core, x, y, me = self.place
        send_a = add_low(pick(self.a, 1 - y), pick(self.got_a, 1 - y))
        send_b = add_low(pick(self.b, 1 - x), pick(self.got_b, 1 - x))
        self.a = add_low(pick(self.a, y), pick(self.got_a, y))
        self.b = add_low(pick(self.b, x), pick(self.got_b, x))
        self.got_a = flip(send_a, 4, 8)
        self.got_b = flip(send_b, 2, 8)
        return send_a, send_b

    def line(self):
        core, x, y, me = self.place
        g = jnp.concatenate([add_low(self.a, self.got_a), add_low(self.b, self.got_b)], axis=0)
        sent = [pick(g, (me + k) % WAYS) for k in range(1, WAYS)]
        self.own = pick(g, me)
        self.parts = [
            lax.ppermute(sent[k - 1], "mp", [(i, (i + k) % WAYS) for i in range(WAYS)])
            for k in range(1, WAYS)
        ]
        return tuple(sent)

    def total(self):
        out = self.own.astype(F32)
        for part in self.parts:
            out += part.astype(F32)
        return out


def sum_small(values, sizes):
    for axis, size in sizes:
        total = values
        for k in range(1, size):
            total += lax.ppermute(values, axis, [(i, (i + k) % size) for i in range(size)])
        values = total
    return values


def local(
    sizes,
    layer_input,
    segment_ids,
    grad_out,
    qkv_weight,
    attn_weight,
    inner_weight,
    outer_weight,
    attn_gain,
    mlp_gain,
):
    dps, mps = sizes
    rows, model = layer_input.shape
    head_cols = qkv_weight.shape[2]
    units = inner_weight.shape[2]
    pairs = head_cols // LANES
    wide = model // LANES
    special = dps == wide
    me = lax.axis_index("mp")
    dp = lax.axis_index("dp")
    core, x_at, y_at = dp % 2, (dp // 2) % 2, dp // 4
    group = me // 2
    quarter = me ^ (2 * core)
    scalars = jnp.stack([me, core, quarter, x_at]).astype(jnp.int32)
    place = (core, x_at, y_at, me)

    def every(values):
        got = lax.all_gather(values, ("dp", "mp"), axis=0)
        if not special:
            ratio = dps // wide
            got = got.reshape((wide, ratio, mps) + values.shape)
            return jnp.moveaxis(got, 1, -2).reshape((wide, mps, values.shape[0], LANES))
        return got.reshape((dps, mps) + values.shape)

    qkv_part = qkv_weight.transpose(1, 2, 0).reshape(3, pairs, LANES, -1)
    qkv_part = qkv_part.transpose(1, 0, 2, 3).reshape(3 * head_cols, -1)
    inner_t = inner_weight.transpose(1, 2, 0)
    outer_t = outer_weight.T
    attn_depth = model // mps
    part_a = jnp.concatenate([attn_weight.T, inner_t[0]], axis=0)
    part_b = jnp.concatenate([inner_t[1], outer_t], axis=0)
    if special:
        x_all, (qkv_all, pack_a, pack_b) = gather_call(layer_input, [qkv_part, part_a, part_b], dps)
    else:
        x_pieces = [to_attention(layer_input, m, dps) for m in range(WAYS)]
        x_all = jnp.concatenate(x_pieces, axis=0)
        qkv_all, pack_a, pack_b = every(qkv_part), every(part_a), every(part_b)

    mine = segment_ids[0]
    other = flip(mine, 1, dps)
    segment = jnp.where(group == core, mine, other)
    order = [pick(segment.reshape(WAYS, rows), quarter ^ m) for m in range(WAYS)]
    positions = doc_positions(segment).reshape(WAYS, rows)
    positions = jnp.concatenate([pick(positions, quarter ^ m) for m in range(WAYS)])
    segment = jnp.concatenate(order)
    cosine, sine = rope_tables(positions)
    lane = jnp.arange(LANES, dtype=jnp.int32) % HEAD_DIM
    same = segment[:, None] == lane[None, :]
    qaux = jnp.where(same | (lane >= 16)[None, :], 0.0, -BIG).astype(BF)
    kaux = jnp.where(same & (lane < 16)[None, :], 1.0, 0.0)
    kaux = jnp.where(((lane >= 16) & (lane < 19))[None, :], 1.0, kaux).astype(BF)
    live = (segment != 0).astype(F32)[:, None]
    live_mine = (pick(mine.reshape(WAYS, rows), me) != 0).astype(F32)[:, None]

    normed, q, k, v = qkv_call(scalars, x_all, attn_gain[None], qkv_all, cosine, sine)

    kept, heads = [], [None] * (2 * WAYS)
    for pair in range(pairs):
        o, qa, ka = attn_fwd_call(scalars, q, k, v, qaux, kaux, live, pair)
        kept.append((o, qa, ka))
        for m in range(WAYS):
            heads[2 * m + pair] = to_attention(o[m], m, dps, back=True)
    middle, inner_in, squares = middle_call(
        scalars, heads, layer_input, pack_a, mlp_gain[None], live_mine
    )
    mlp_out, inner_back, keep_f, send_f = ffn_call(scalars, inner_in, grad_out, pack_a, pack_b)
    if special:
        sum_f = Sum(keep_f, send_f, place)
    (layer_output, middle_grad, middle_low, small), heads_grad = middle_back_call(
        scalars, middle, mlp_out, inner_back, grad_out, pack_a, mlp_gain[None], live_mine
    )
    grads = [
        [to_attention(heads_grad[2 * m + pair], m, dps) for m in range(WAYS)]
        for pair in range(pairs)
    ]
    keep_c, send_c = attn_grad_call(scalars, heads, middle_low)
    if special:
        sum_c = Sum(keep_c, send_c, place)

    returned, low = [None] * (2 * WAYS), []
    qkv_sums = []
    for pair in range(pairs):
        o, qa, ka = kept[pair]
        grad = grads[pair]
        if special:
            if pair == 0:
                waits = sum_f.planes()
            else:
                waits = (*sum_f.planes_again(), *sum_c.planes())
            grad = [after(grad[0], *waits), *grad[1:]]
        parts = attn_bwd_call(scalars, qa, ka, v, grad, o, cosine, sine, pair)
        for m in range(WAYS):
            returned[2 * m + pair] = to_attention(parts[m], m, dps, back=True)
        low.append(parts)
        keep, send = qkv_grad_call(scalars, parts, normed)
        if special:
            got = flip(send, 2, 8)
            total = [v.reshape(2, 2, -1, LANES) for v in (keep, got)]
            sent = add_low(pick(total[0], 1 - y_at), pick(total[1], 1 - y_at))
            got = flip(sent, 4, 8)
            total = add_low(
                add_low(pick(total[0], y_at), pick(total[1], y_at)), got
            )
            parts = []
            for turn in range(2):
                steps = []
                for i in range(dps):
                    for z in range(mps):
                        g, h = z // 2, z ^ (2 * (i % 2))
                        there = (i - i % 2 + (g ^ turn)) * mps + h
                        steps.append((i * mps + z, there))
                parts.append(lax.ppermute(pick(total, group ^ turn), ("dp", "mp"), steps))
            qkv_sums.append(parts[0].astype(F32) + parts[1].astype(F32))
        else:
            both = [jnp.where(x_at == i, keep, send) for i in range(2)]
            both = jnp.stack([b.reshape(wide // 4, 2, -1, LANES) for b in both], axis=1)
            both = both.reshape(wide, -1, LANES)
            slot = (jnp.arange(WAYS) == quarter)[None, :, None, None]
            qkv_sums.append(jnp.where(slot, both[:, None], jnp.zeros((), BF)))

    if special:
        sum_f.line()
        sum_c.planes_again()
        sum_c.line()
        ffn_sum, attn_sum = sum_f.total(), sum_c.total()
        qkv_sum = jnp.concatenate(qkv_sums, axis=0)
    else:

        def join(keep, send):
            both = [jnp.where(core == i, keep, send) for i in range(2)]
            return jnp.stack(both, axis=1).reshape((wide,) + keep.shape[1:])

        def shared(values):
            ratio = dps // wide
            lanes = LANES // ratio
            cut = values.reshape(values.shape[:-1] + (ratio, lanes))
            cut = jnp.moveaxis(cut, -2, 1).reshape(dps * mps, -1, lanes)
            return lax.psum_scatter(
                cut.astype(F32), ("dp", "mp"), scatter_dimension=0, tiled=True
            )[0]

        ffn_sum = shared(join(keep_f, send_f))
        attn_sum = shared(join(keep_c, send_c))
        qkv_sum = shared(jnp.concatenate(qkv_sums, axis=2))

    input_grad, attn_gain_part = input_grad_call(
        scalars, returned, qkv_all, layer_input, middle_grad, attn_gain[None]
    )

    sums = jnp.concatenate([jnp.sum(squares[:3], axis=1), jnp.sum(small[:1], axis=1)])
    sums = jnp.concatenate([sums, jnp.sum(live_mine)[None], jnp.zeros((model - 5,), F32)])
    early = jnp.stack([small[1], sums])
    if special:
        ways = (("dp", dps), ("mp", mps))
        early = sum_small(early, ways)
        attn_gain_grad = sum_small(attn_gain_part, ways)[0]
    else:
        early, attn_gain_grad = lax.psum((early, attn_gain_part[0]), ("dp", "mp"))
    rms_values = jnp.sqrt(early[1, :4] / (early[1, 4] * model))

    qkv_sum = qkv_sum.reshape(pairs, 3, LANES, -1).transpose(3, 1, 0, 2)
    ffn_sum = ffn_sum.reshape(3, units, -1)
    return (
        layer_output,
        input_grad,
        qkv_sum.reshape(-1, 3, head_cols),
        attn_sum.T,
        ffn_sum[:2].transpose(2, 0, 1),
        ffn_sum[2].T,
        attn_gain_grad,
        early[0],
        rms_values,
    )


def solution(mesh):
    sizes = (mesh.shape["dp"], mesh.shape["mp"])
    both = ("dp", "mp")
    whole = (P(both, None), P("dp", None, "mp"), P("dp", "mp"))
    return jax.shard_map(
        functools.partial(local, sizes),
        mesh=mesh,
        in_specs=(
            whole[0],
            P("dp", None),
            whole[0],
            whole[1],
            whole[2],
            whole[1],
            whole[2],
            P(),
            P(),
        ),
        out_specs=(
            whole[0],
            whole[0],
            whole[1],
            whole[2],
            whole[1],
            whole[2],
            P(),
            P(),
            P(),
        ),
        check_vma=False,
    )
```

```python
import functools
import math

import jax
import jax.numpy as jnp
from jax import lax
from jax.experimental import pallas as pl
from jax.experimental.pallas import tpu as pltpu
from jax.sharding import PartitionSpec as P

HEAD_DIM = 64
NORM_EPS = 1e-05
ROPE_BASE = 160000.0
BIG = 1e30
LANES = 128
WAYS = 4
BF = jnp.bfloat16
F32 = jnp.float32
VMEM_LIMIT = 56 * 1024 * 1024


def dot_nn(a, b):
    return lax.dot_general(a, b, (((1,), (0,)), ((), ())), preferred_element_type=F32)


def dot_nt(a, b):
    return lax.dot_general(a, b, (((1,), (1,)), ((), ())), preferred_element_type=F32)


def dot_tn(a, b):
    return lax.dot_general(a, b, (((0,), (0,)), ((), ())), preferred_element_type=F32)


def norm_stats(values):
    centre = jnp.mean(values, axis=-1, keepdims=True)
    shifted = values - centre
    spread = jnp.mean(shifted * shifted, axis=-1, keepdims=True)
    scale = lax.rsqrt(spread + NORM_EPS)
    return shifted * scale, scale


def norm_back(vhat, scale, gain, grad):
    u = grad * gain
    mean_u = jnp.mean(u, axis=-1, keepdims=True)
    mean_uv = jnp.mean(u * vhat, axis=-1, keepdims=True)
    return scale * (u - mean_u - vhat * mean_uv)


def doc_positions(segment):
    length = segment.shape[0]
    places = jnp.arange(length, dtype=jnp.int32)
    before = jnp.concatenate([jnp.full((1,), -1, jnp.int32), segment[:-1]])
    starts = jnp.where(segment != before, places, jnp.zeros_like(places))
    return places - lax.cummax(starts, axis=0)


def swap_halves(values):
    lane = lax.broadcasted_iota(jnp.int32, values.shape, 1)
    first = lane % HEAD_DIM < HEAD_DIM // 2
    back = pltpu.roll(values, LANES - HEAD_DIM // 2, 1)
    ahead = pltpu.roll(values, HEAD_DIM // 2, 1)
    return jnp.where(first, back, ahead)


def choose(at, values):
    out = values[0]
    for i in range(1, len(values)):
        out = jnp.where(at == i, values[i], out)
    return out


def params():
    return pltpu.CompilerParams(vmem_limit_bytes=VMEM_LIMIT)


def cost(flops, mib):
    return pl.CostEstimate(flops=int(flops), bytes_accessed=int(mib * 2**20), transcendentals=0)


def call(kernel, scalars, grid, in_specs, out_specs, out_shape, scratch, estimate, name):
    spec = pltpu.PrefetchScalarGridSpec(
        num_scalar_prefetch=1,
        grid=grid,
        in_specs=in_specs,
        out_specs=out_specs,
        scratch_shapes=scratch,
    )
    return functools.partial(
        pl.pallas_call(
            kernel,
            grid_spec=spec,
            out_shape=out_shape,
            compiler_params=params(),
            cost_estimate=estimate,
            name=name,
        ),
        scalars,
    )


def full(shape):
    return pl.BlockSpec(shape, lambda i, s: (0,) * len(shape))


def shape_of(shape, dtype):
    return jax.ShapeDtypeStruct(shape, dtype)


def side_by_side(ref, *at):
    return jnp.concatenate([ref[(d, *at)] for d in range(ref.shape[0])], axis=-1)


STEP = 256


def table_piece(m, info, out):
    rows = info.shape[0]
    here = slice(m * rows, (m + 1) * rows)
    segment, position = info[:, 0:1], info[:, 1:2]
    lane = lax.broadcasted_iota(jnp.int32, (1, LANES), 1)
    half = HEAD_DIM // 2
    frequency = jnp.exp((lane % half).astype(F32) * (-2.0 * math.log(ROPE_BASE) / HEAD_DIM))
    angle = position * frequency
    sine = jnp.sin(angle)
    out.cosine[here, :] = jnp.cos(angle)
    out.sine[here, :] = jnp.where(lane % HEAD_DIM < half, -sine, sine)
    t = lane % HEAD_DIM
    same = segment == t.astype(F32)
    masked = jnp.where(same, 0.0, -BIG)
    out.qaux[here, :] = jnp.where(t >= 16, 0.0, masked).astype(BF)
    found = jnp.where(same, 1.0, 0.0)
    counted = jnp.where(t < 19, 1.0, 0.0)
    out.kaux[here, :] = jnp.where(t < 16, found, counted).astype(BF)
    out.live[here, :] = jnp.where(segment != 0.0, 1.0, 0.0)


def qkv_piece(m, x, gain, weight, out):
    rows = x.shape[0]
    here = slice(m * rows, (m + 1) * rows)
    vhat, unused = norm_stats(x.astype(F32))
    normed = (vhat * gain).astype(BF)
    out.normed[here, :] = normed
    flat = dot_nt(normed, weight)
    cosine, sine = out.cosine[here, :], out.sine[here, :]
    kaux = out.kaux[here, :]
    lane = lax.broadcasted_iota(jnp.int32, (rows, LANES), 1)
    for pair in range(flat.shape[1] // (3 * LANES)):
        q, k, v = [
            flat[:, at : at + LANES] for at in range(pair * 3 * LANES, (pair + 1) * 3 * LANES, LANES)
        ]
        q = (q * cosine + swap_halves(q) * sine).astype(BF)
        k = (k * cosine + swap_halves(k) * sine).astype(BF)
        out.q[pair, here, :] = q * jnp.asarray(HEAD_DIM**-0.5, BF)
        out.ka[pair, 0, here, :] = jnp.where(lane < HEAD_DIM, k, kaux)
        out.ka[pair, 1, here, :] = jnp.where(lane >= HEAD_DIM, k, kaux)
        out.v[pair, here, :] = v.astype(BF)


def attn_step(pair, step, out):
    tokens = out.v.shape[1]
    chunk = 512
    here = pl.ds(pl.multiple_of(step * STEP, STEP), STEP)
    lane = lax.broadcasted_iota(jnp.int32, (STEP, LANES), 1)
    t = lane % HEAD_DIM
    q = out.q[pair, here, :]
    qaux = out.qaux[here, :]
    live = out.live[here, :]
    outs = []
    for head in range(2):
        mine = (lane < HEAD_DIM) if head == 0 else (lane >= HEAD_DIM)
        qa = jnp.where(mine, q, qaux)
        top = None
        for at in range(0, tokens, chunk):
            s = dot_nt(qa, out.ka[pair, head, at : at + chunk, :])
            out.scores[:, at : at + chunk] = s
            part = jnp.max(s, axis=-1, keepdims=True)
            top = part if top is None else jnp.maximum(top, part)
        total = jnp.zeros((STEP, 1), F32)
        mixed = jnp.zeros((STEP, LANES), F32)
        for at in range(0, tokens, chunk):
            p = jnp.exp(out.scores[:, at : at + chunk] - top)
            total += jnp.sum(p, axis=-1, keepdims=True)
            mixed += dot_nn(p.astype(BF), out.v[pair, at : at + chunk, :])
        outs.append(mixed * (live / total))
        log_sum = jnp.where(live > 0, top + jnp.log(total), BIG)
        high = log_sum.astype(BF)
        rest = log_sum - high.astype(F32)
        mid = rest.astype(BF)
        low = (rest - mid.astype(F32)).astype(BF)
        aux = jnp.where(t == 16, -high, jnp.where(t == 17, -mid, jnp.where(t == 18, -low, qaux)))
        out.qa[pair, head, here, :] = jnp.where(mine, q, aux)
    out.o[pair, here, :] = jnp.where(lane < HEAD_DIM, outs[0], outs[1]).astype(BF)


class Kept:
    names = ("normed", "cosine", "sine", "qa", "ka", "v", "o", "q", "qaux", "kaux", "live", "scores")

    def __init__(self, refs):
        for name, ref in zip(self.names, refs):
            setattr(self, name, ref)


def kept_shapes(tokens, model, pairs):
    outs = [
        shape_of((tokens, model), BF),
        shape_of((tokens, LANES), F32),
        shape_of((tokens, LANES), F32),
        shape_of((pairs, 2, tokens, LANES), BF),
        shape_of((pairs, 2, tokens, LANES), BF),
        shape_of((pairs, tokens, LANES), BF),
        shape_of((pairs, tokens, LANES), BF),
    ]
    scratch = [
        pltpu.VMEM((pairs, tokens, LANES), BF),
        pltpu.VMEM((tokens, LANES), BF),
        pltpu.VMEM((tokens, LANES), BF),
        pltpu.VMEM((tokens, 1), F32),
        pltpu.VMEM((STEP, tokens), F32),
    ]
    return outs, scratch


def alone_kernel(x_ref, info_ref, gain_ref, w_ref, *refs):
    out = Kept(refs)
    for m in range(WAYS):
        table_piece(m, info_ref[m], out)
        qkv_piece(m, x_ref[m], gain_ref[...], side_by_side(w_ref), out)

    def body(step, carry):
        per = out.v.shape[1] // STEP
        attn_step(step // per, step % per, out)
        return carry

    lax.fori_loop(0, out.v.shape[0] * out.v.shape[1] // STEP, body, 0)


def alone_call(x, info, gain, weight, pairs):
    outs, scratch = kept_shapes(WAYS * x.shape[1], x.shape[2], pairs)
    return pl.pallas_call(
        alone_kernel,
        in_specs=[pl.BlockSpec(memory_space=pltpu.VMEM)] * 4,
        out_specs=[pl.BlockSpec(memory_space=pltpu.VMEM)] * len(outs),
        out_shape=outs,
        scratch_shapes=scratch,
        compiler_params=params(),
        name="forward",
    )(x, info, gain, weight)


def piece_block(m, rows, per):
    return pl.BlockSpec((rows, LANES), lambda i, s: (jnp.clip(i - per * m, 0, per - 1), 0))


def attn_bwd_kernel(s_ref, *refs):
    qa_ref, ka_ref, v_ref, o_ref, do_refs = refs[0], refs[1], refs[2], refs[3], refs[4:8]
    cosq_ref, sinq_ref, cosk_ref, sink_ref = refs[8:12]
    out_refs = refs[12:16]
    va_ref, kt_ref, dk_acc, dv_acc = refs[16:20]
    step = pl.program_id(0)
    rows = do_refs[0].shape[0]
    chunk = v_ref.shape[0] // WAYS
    per = chunk // rows
    piece = step // per
    lane_k = lax.broadcasted_iota(jnp.int32, (chunk, LANES), 1)
    lane = lax.broadcasted_iota(jnp.int32, (rows, LANES), 1)
    zero = jnp.zeros((), BF)

    @pl.when(step == 0)
    def _():
        ones = jnp.where(lane_k % HEAD_DIM < 3, jnp.ones((), BF), zero)
        for m in range(WAYS):
            some = slice(m * chunk, (m + 1) * chunk)
            v = v_ref[some, :]
            for head in range(2):
                mine = (lane_k < HEAD_DIM) if head == 0 else (lane_k >= HEAD_DIM)
                va_ref[head, some, :] = jnp.where(mine, v, ones)
                own = jnp.where(mine, ka_ref[head, some, :], zero).astype(F32)
                kt_ref[head, :, some] = own.T.astype(BF)
        dk_acc[...] = jnp.zeros_like(dk_acc)
        dv_acc[...] = jnp.zeros_like(dv_acc)

    grad = choose(piece, [r[...] for r in do_refs])
    out = o_ref[...]
    product = grad.astype(F32) * out.astype(F32)
    turned = jnp.zeros((LANES, rows), F32)
    for head in range(2):
        mine = (lane < HEAD_DIM) if head == 0 else (lane >= HEAD_DIM)
        delta = jnp.sum(jnp.where(mine, product, 0.0), axis=-1, keepdims=True)
        high = delta.astype(BF)
        rest = delta - high.astype(F32)
        mid = rest.astype(BF)
        low = (rest - mid.astype(F32)).astype(BF)
        t = lane % HEAD_DIM
        aux = jnp.where(t == 0, -high, jnp.where(t == 1, -mid, jnp.where(t == 2, -low, zero)))
        grad_aug = jnp.where(mine, grad, aux)
        grad_own = jnp.where(mine, grad, zero)
        qa = qa_ref[head]
        q_own = jnp.where(mine, qa, zero)
        for m in range(WAYS):
            some = slice(m * chunk, (m + 1) * chunk)
            prob = jnp.exp(dot_nt(ka_ref[head, some, :], qa))
            back = dot_nt(va_ref[head, some, :], grad_aug)
            score_grad = (prob * back).astype(BF)
            dv_acc[some, :] += dot_nn(prob.astype(BF), grad_own)
            dk_acc[some, :] += dot_nn(score_grad, q_own)
            turned += dot_nn(kt_ref[head, :, some], score_grad)
    dq = turned.T * (HEAD_DIM**-0.5)
    dq = (dq * cosq_ref[...] - swap_halves(dq) * sinq_ref[...]).astype(BF)
    for m in range(WAYS):

        @pl.when(piece == m)
        def _(m=m):
            here = pl.ds(pl.multiple_of((step - m * per) * rows, rows), rows)
            out_refs[m][here, :LANES] = dq

    @pl.when(step == pl.num_programs(0) - 1)
    def _():
        for m in range(WAYS):
            some = slice(m * chunk, (m + 1) * chunk)
            dk = dk_acc[some, :]
            dk = dk * cosk_ref[some, :] - swap_halves(dk) * sink_ref[some, :]
            out_refs[m][:, LANES : 2 * LANES] = dk.astype(BF)
            out_refs[m][:, 2 * LANES :] = dv_acc[some, :].astype(BF)


def attn_bwd_call(scalars, qa, ka, v, grad, o, cosine, sine, pair):
    tokens = v.shape[1]
    chunk = tokens // WAYS
    rows = 256
    per = chunk // rows
    moving = [piece_block(m, rows, per) for m in range(WAYS)]
    block = pl.BlockSpec((rows, LANES), lambda i, s: (i, 0))
    return call(
        attn_bwd_kernel,
        scalars,
        (tokens // rows,),
        [
            pl.BlockSpec((None, 2, rows, LANES), lambda i, s: (pair, 0, i, 0)),
            pl.BlockSpec((None, 2, tokens, LANES), lambda i, s: (pair, 0, 0, 0)),
            pl.BlockSpec((None, tokens, LANES), lambda i, s: (pair, 0, 0)),
            pl.BlockSpec((None, rows, LANES), lambda i, s: (pair, i, 0)),
        ]
        + moving
        + [block, block, full((tokens, LANES)), full((tokens, LANES))],
        [full((chunk, 3 * LANES))] * WAYS,
        [shape_of((chunk, 3 * LANES), BF)] * WAYS,
        [
            pltpu.VMEM((2, tokens, LANES), BF),
            pltpu.VMEM((2, LANES, tokens), BF),
            pltpu.VMEM((tokens, LANES), F32),
            pltpu.VMEM((tokens, LANES), F32),
        ],
        cost(28 * tokens * tokens * LANES, 8),
        "attn_bwd",
    )(qa, ka, v, o, *grad, cosine, sine, cosine, sine)


def middle_kernel(s_ref, *refs):
    o_ref, x_ref, w_ref, gain_ref, live_ref, middle_ref, inner_ref, square_ref = refs
    z = s_ref[0]
    tokens = x_ref[...].astype(F32)
    attn_out = jnp.zeros(tokens.shape, F32)
    for m in range(WAYS):
        o = jnp.concatenate([o_ref[m, 0], o_ref[m, 1]], axis=-1)
        attn_out += dot_nn(o, side_by_side(w_ref, z ^ m))
    middle = tokens + attn_out
    vhat, unused = norm_stats(middle)
    middle_ref[...] = middle
    inner_ref[...] = (vhat * gain_ref[...]).astype(BF)
    live = live_ref[...]
    square_ref[...] = jnp.concatenate(
        [jnp.sum(live * a * a, axis=0, keepdims=True) for a in (tokens, attn_out, middle)]
        + [jnp.zeros((5, tokens.shape[1]), F32)],
        axis=0,
    )


def middle_call(scalars, heads, x, weight, gain, live):
    rows, model = x.shape
    wide = weight.shape[0]
    depth = model // WAYS
    return call(
        middle_kernel,
        scalars,
        (1,),
        [
            full(heads.shape),
            full((rows, model)),
            full((wide, WAYS, depth, LANES)),
            full((1, model)),
            full((rows, 1)),
        ],
        [full((rows, model)), full((rows, model)), full((8, model))],
        [shape_of((rows, model), F32), shape_of((rows, model), BF), shape_of((8, model), F32)],
        [],
        cost(2 * rows * model * model, 8),
        "middle",
    )(heads, x, weight, gain, live)


def middle_back_kernel(
    s_ref, middle_ref, mlp_ref, back_ref, grad_ref, w_ref, gain_ref, live_ref,
    output_ref, mgrad_ref, low_ref, small_ref, hg_ref,
):
    z = s_ref[0]
    middle = middle_ref[...]
    mlp = mlp_ref[...]
    back = back_ref[...]
    vhat, scale = norm_stats(middle)
    middle_grad = grad_ref[...].astype(F32) + norm_back(vhat, scale, gain_ref[...], back)
    low = middle_grad.astype(BF)
    for m in range(WAYS):
        hg = dot_nt(low, side_by_side(w_ref, z ^ m)).astype(BF)
        hg_ref[m, 0] = hg[:, :LANES]
        hg_ref[m, 1] = hg[:, LANES:]
    mgrad_ref[...] = middle_grad
    low_ref[...] = low
    output_ref[...] = (middle + mlp).astype(BF)
    small_ref[...] = jnp.concatenate(
        [
            jnp.sum(live_ref[...] * mlp * mlp, axis=0, keepdims=True),
            jnp.sum(back * vhat, axis=0, keepdims=True),
            jnp.zeros((6, mlp.shape[1]), F32),
        ],
        axis=0,
    )


def middle_back_call(scalars, middle, mlp, back, grad, weight, gain, live):
    rows, model = middle.shape
    wide = weight.shape[0]
    depth = model // WAYS
    heads = (WAYS, depth // LANES, rows, LANES)
    return call(
        middle_back_kernel,
        scalars,
        (1,),
        [full((rows, model))] * 4
        + [full((wide, WAYS, depth, LANES)), full((1, model)), full((rows, 1))],
        [full((rows, model))] * 3 + [full((8, model)), full(heads)],
        [
            shape_of((rows, model), BF),
            shape_of((rows, model), F32),
            shape_of((rows, model), BF),
            shape_of((8, model), F32),
            shape_of(heads, BF),
        ],
        [],
        cost(2 * rows * model * model, 12),
        "middle_back",
    )(middle, mlp, back, grad, weight, gain, live)


def own_first(core, values):
    cut = [values[:, at : at + LANES] for at in range(0, values.shape[1], LANES)]
    turned = [cut[i ^ 1] for i in range(len(cut))]
    return jnp.where(core == 0, values, jnp.concatenate(turned, axis=-1))


def ffn_kernel(
    s_ref, x_ref, g_ref, wa_ref, wb_ref, mlp_ref, back_ref, sum_ref, *scratch, swap
):
    step = pl.program_id(0)
    steps = pl.num_programs(0)
    units = wb_ref.shape[2] // 2
    skip = wa_ref.shape[2] - units
    if swap:
        away, got, send_sem, recv_sem = scratch
        dp, z = lax.axis_index("dp"), lax.axis_index("mp")
        core = dp % 2
        other = (dp + 1 - 2 * core, z)

        @pl.when(step == 0)
        def _():
            barrier = pltpu.get_barrier_semaphore()
            pl.semaphore_signal(barrier, inc=1, device_id=other, device_id_type=MESH)
            pl.semaphore_wait(barrier, 1)

        def give(i):
            return remote(away.at[i % 2], got.at[i], send_sem.at[i % 2], recv_sem.at[i], other)

        def take(i):
            give(i).wait_recv()
            for d in range(sum_ref.shape[1]):
                sum_ref[i, d] += got[i, d]

        @pl.when(step >= 2)
        def _():
            give(step - 2).wait_send()
    else:
        core = s_ref[1]
    w_act = side_by_side(wa_ref, 0, slice(skip, skip + units))
    w_lin = side_by_side(wb_ref, 0, slice(0, units))
    w_out = side_by_side(wb_ref, 0, slice(units, 2 * units))
    x = x_ref[...]
    grad = g_ref[...]
    act_in = dot_nt(w_act, x)
    linear = dot_nt(w_lin, x)
    hidden_grad = dot_nt(w_out, grad)
    cdf = 0.5 * (1.0 + lax.erf(act_in * (2.0**-0.5)))
    act = act_in * cdf
    slope = cdf + act_in * jnp.exp(-0.5 * act_in * act_in) * ((2.0 * math.pi) ** -0.5)
    hidden = (act * linear).astype(BF)
    d_act = (hidden_grad * linear * slope).astype(BF)
    d_lin = (hidden_grad * act).astype(BF)
    x = own_first(core, x)
    grad = own_first(core, grad)
    for part, value in ((0, dot_nn(d_act, x)), (1, dot_nn(d_lin, x)), (2, dot_nn(hidden, grad))):
        some = slice(part * units, (part + 1) * units)
        value = value.astype(BF)
        for d in range(value.shape[1] // LANES):
            slab = value[:, d * LANES : (d + 1) * LANES]
            if not swap:
                sum_ref[step, d // 2, d % 2, some] = slab
            elif d % 2:
                away[step % 2, d // 2, some] = slab
            else:
                sum_ref[step, d // 2, some] = slab
    if swap:
        give(step).start()
    mlp = dot_tn(hidden, w_out)
    back = dot_tn(d_act, w_act) + dot_tn(d_lin, w_lin)

    @pl.when(step == 0)
    def _():
        mlp_ref[...] = mlp
        back_ref[...] = back

    @pl.when(step > 0)
    def _():
        mlp_ref[...] += mlp
        back_ref[...] += back

    if swap:

        @pl.when(step >= 1)
        def _():
            take(step - 1)

        @pl.when(step == steps - 1)
        def _():
            take(step)
            give(step - 1).wait_send()
            give(step).wait_send()


def ffn_call(scalars, x, grad, pack_a, pack_b, swap):
    tokens, model = x.shape
    wide, quarters, depth_a, unused = pack_a.shape
    depth_b = pack_b.shape[2]
    units = depth_b // 2
    out = (quarters, wide // 2) + (() if swap else (2,)) + (3 * units, LANES)
    weight = lambda depth: pl.BlockSpec((wide, 1, depth, LANES), lambda i, s: (0, i, 0, 0))
    whole = lambda: pl.BlockSpec(memory_space=pltpu.VMEM)
    scratch = [
        pltpu.VMEM((2,) + out[1:], BF),
        pltpu.VMEM(out, BF),
        pltpu.SemaphoreType.DMA((2,)),
        pltpu.SemaphoreType.DMA((quarters,)),
    ]
    spec = pltpu.PrefetchScalarGridSpec(
        num_scalar_prefetch=1,
        grid=(quarters,),
        in_specs=[whole(), whole(), weight(depth_a), weight(depth_b)],
        out_specs=[whole()] * 3,
        scratch_shapes=scratch if swap else [],
    )
    extra = dict(collective_id=1, has_side_effects=True) if swap else {}
    return pl.pallas_call(
        functools.partial(ffn_kernel, swap=swap),
        grid_spec=spec,
        out_shape=[shape_of((tokens, model), F32)] * 2 + [shape_of(out, BF)],
        compiler_params=pltpu.CompilerParams(vmem_limit_bytes=VMEM_LIMIT, **extra),
        cost_estimate=cost(18 * tokens * model * units * quarters, 40),
        name="ffn",
    )(scalars, x, grad, pack_a, pack_b)


MESH = pl.DeviceIdType.MESH
UP, DOWN, TO_X, TO_Y, TO_D, CORE_OWN, CORE_X, CORE_Y, CORE_D = range(9)
FROM_Z, FROM_X, FROM_Y, FROM_D = range(4)


class Place:
    def __init__(self):
        self.dp, self.z = lax.axis_index("dp"), lax.axis_index("mp")
        self.core, self.x, self.y = self.dp % 2, (self.dp // 2) % 2, self.dp // 4
        self.at_c = self.dp + 1 - 2 * self.core
        self.at_x = self.dp + 2 - 4 * self.x
        self.at_y = self.dp + 4 - 8 * self.y
        self.at_d = self.at_x + self.at_y - self.dp
        self.group = self.z // 2
        self.far_z = self.z + 2 - 4 * self.group
        self.quarter = self.z + self.core * (self.far_z - self.z)

    @staticmethod
    def mix(q, m):
        return (q + m) % 2 + 2 * ((q // 2 + m // 2) % 2)

    def stays(self, a, b):
        return jnp.logical_and(a == self.dp, b == self.z)

    def attention_of(self, m):
        h = self.mix(self.z, m)
        a, b = self.dp - self.core + (h // 2 + self.core) % 2, 2 * self.core + h % 2
        return a, b, self.stays(a, b)

    def owner_of(self, m):
        a, b = self.dp - self.core + self.group, self.mix(self.quarter, m)
        return a, b, self.stays(a, b)


def remote(src, dst, send, recv, device):
    return pltpu.make_async_remote_copy(
        src_ref=src, dst_ref=dst, send_sem=send, recv_sem=recv,
        device_id=device, device_id_type=MESH,
    )


class Move:
    def __init__(self, src, dst, send, recv, place):
        a, b, self.stays = place
        self.far = lambda: remote(src, dst, send, recv, (a, b))
        self.near = lambda: pltpu.make_async_copy(src, dst, recv)

    def start(self):
        pl.when(self.stays)(lambda: self.near().start())
        pl.when(jnp.logical_not(self.stays))(lambda: self.far().start())

    def wait_recv(self):
        self.far().wait_recv()

    def wait_send(self):
        pl.when(jnp.logical_not(self.stays))(lambda: self.far().wait_send())


def forward_kernel(x_ref, info_ref, gain_ref, qkv_ref, *refs, packs):
    parts, outs, heads_ref = refs[:packs], refs[packs : 2 * packs], refs[2 * packs]
    saved, refs = refs[2 * packs + 1 : 2 * packs + 7], refs[2 * packs + 7 :]
    qa, o, normed, cosine, sine, ka, v, q, qaux, kaux, live, scores = refs[:12]
    kept = Kept((normed, cosine, sine, qa, ka, v, o, q, qaux, kaux, live, scores))
    x_all, w_ref, infos = refs[12:15]
    (
        sends, recvs, cores, locals_, token_send, token_recv, head_send, head_recv,
        q_send, q_recv, save_sem,
    ) = refs[15:]
    dp, z = lax.axis_index("dp"), lax.axis_index("mp")
    core, xb, yb = dp % 2, (dp // 2) % 2, dp // 4
    at_c, at_x, at_y = dp + 1 - 2 * core, dp + 2 - 4 * xb, dp + 4 - 8 * yb
    at_d = at_x + at_y - dp
    group = z // 2
    far_z = z + 2 - 4 * group
    quarter = z + core * (far_z - z)

    def mix(q, m):
        return (q + m) % 2 + 2 * ((q // 2 + m // 2) % 2)

    def attention_of(m):
        h = mix(z, m)
        return dp - core + (h // 2 + core) % 2, 2 * core + h % 2

    def owner_of(m):
        return dp - core + group, mix(quarter, m)

    barrier = pltpu.get_barrier_semaphore()

    def greet(device, when=None):
        def signal():
            pl.semaphore_signal(barrier, inc=1, device_id=device, device_id_type=MESH)

        signal() if when is None else pl.when(when)(signal)

    greet((at_c, z))
    greet((at_x, z))
    greet((at_y, z))
    greet((dp, far_z))
    greet((dp, z + 1), z < WAYS - 1)
    greet((dp, z - 1), z > 0)
    count = 4 + (z < WAYS - 1).astype(jnp.int32) + (z > 0).astype(jnp.int32)
    here, there = [], []
    for m in range(WAYS):
        for of, found in ((attention_of, here), (owner_of, there)):
            a, b = of(m)
            stays = jnp.logical_and(a == dp, b == z)
            found.append((a, b, stays))
            greet((a, b), jnp.logical_not(stays))
            count += 1 - stays.astype(jnp.int32)
    pl.semaphore_wait(barrier, count)

    def remote(src, dst, send, recv, device):
        return pltpu.make_async_remote_copy(
            src_ref=src, dst_ref=dst, send_sem=send, recv_sem=recv,
            device_id=device, device_id_type=MESH,
        )

    def copy(p, kind, s, src=None):
        who = {CORE_X: at_x, CORE_Y: at_y, CORE_D: at_d}.get(kind, dp)
        if kind == TO_D:
            who = jnp.where(s < 2, at_x, at_y)
        slab = outs[p].at[who, s]
        send = sends.at[p, kind, s]
        if kind == UP:
            recv, device = recvs.at[p, FROM_Z, s], (dp, z + 1)
        elif kind == DOWN:
            recv, device = recvs.at[p, FROM_Z, s], (dp, z - 1)
        elif kind == TO_X:
            recv, device = recvs.at[p, FROM_X, s], (at_x, z)
        elif kind == TO_Y:
            recv, device = recvs.at[p, FROM_Y, s], (at_y, z)
        elif kind == TO_D:
            recv, device = recvs.at[p, FROM_D, s], (jnp.where(s < 2, at_y, at_x), z)
        else:
            recv, device = cores.at[p, kind - CORE_OWN, s], (at_c, z)
        return remote(slab if src is None else src, slab, send, recv, device)

    def arrived(p, sem, who, s):
        slab = outs[p].at[who, s]
        remote(slab, slab, sends.at[p, UP, s], sem, (at_c, z)).wait_recv()

    def spread(p, s, src=None):
        copy(p, TO_X, s, src).start()
        copy(p, TO_Y, s, src).start()
        copy(p, CORE_OWN, s, src).start()

    def begin(p):
        src = parts[p]
        spread(p, z, src)
        pltpu.make_async_copy(src, outs[p].at[dp, z], locals_.at[p]).start()

    def begin_line(p):
        src = parts[p]
        pl.when(z < WAYS - 1)(lambda: copy(p, UP, z, src).start())
        pl.when(z > 0)(lambda: copy(p, DOWN, z, src).start())

    def reach(p, hop):
        def one(s):
            arrived(p, recvs.at[p, FROM_Z, s], dp, s)
            spread(p, s)

        pl.when(z >= hop)(lambda: one(z - hop))
        pl.when(z + hop < WAYS)(lambda: one(z + hop))

    def ahead(p, hop):
        pl.when(jnp.logical_and(z >= hop, z < WAYS - 1))(lambda: copy(p, UP, z - hop).start())
        pl.when(jnp.logical_and(z + hop < WAYS, z > 0))(lambda: copy(p, DOWN, z + hop).start())

    def line(p, hop):
        reach(p, hop)
        if hop < WAYS - 1:
            ahead(p, hop)

    def plane(p, hop):
        def one(s):
            arrived(p, recvs.at[p, FROM_X, s], at_x, s)
            copy(p, CORE_X, s).start()
            pl.when(s < 2)(lambda: copy(p, TO_D, s).start())
            arrived(p, recvs.at[p, FROM_Y, s], at_y, s)
            copy(p, CORE_Y, s).start()
            pl.when(s >= 2)(lambda: copy(p, TO_D, s).start())

        if hop == 0:
            one(z)
        else:
            pl.when(z >= hop)(lambda: one(z - hop))
            pl.when(z + hop < WAYS)(lambda: one(z + hop))

    def corner(p, hop):
        def one(s):
            arrived(p, recvs.at[p, FROM_D, s], at_d, s)
            copy(p, CORE_D, s).start()

        if hop == 0:
            one(z)
        else:
            pl.when(z >= hop)(lambda: one(z - hop))
            pl.when(z + hop < WAYS)(lambda: one(z + hop))

    def from_core(p):
        for s in range(WAYS):
            for kind in range(4):
                twin = (at_c, at_x + at_c - dp, at_y + at_c - dp, at_d + at_c - dp)[kind]
                arrived(p, cores.at[p, kind, s], twin, s)
        pltpu.make_async_copy(parts[p], outs[p].at[dp, z], locals_.at[p]).wait()

    def finish(p):
        for s in range(WAYS):
            pl.when(jnp.logical_and(z < WAYS - 1, s <= z))(lambda s=s: copy(p, UP, s).wait_send())
            pl.when(jnp.logical_and(z > 0, s >= z))(lambda s=s: copy(p, DOWN, s).wait_send())
            for kind in range(TO_X, CORE_D + 1):
                copy(p, kind, s).wait_send()

    def token(m):
        to_dp, to_z, stays = here[m]

        def far():
            return remote(x_ref, x_all.at[m], token_send.at[m], token_recv.at[m], (to_dp, to_z))

        def near():
            return pltpu.make_async_copy(x_ref, x_all.at[m], token_recv.at[m])

        return far, near, stays

    def pass_on(m):
        return remote(
            x_all.at[m], x_all.at[m + 2], token_send.at[m + 2], token_recv.at[m + 2], (at_c, z)
        )

    def swap_info():
        return remote(info_ref, infos.at[1], token_send.at[WAYS], token_recv.at[WAYS], (at_c, z))

    def own_info():
        return pltpu.make_async_copy(info_ref, infos.at[0], locals_.at[packs])

    def q_copy(kind, i=0, src=None):
        who = {"z": dp, "x": dp, "y": dp, "c": dp, "cx": at_x, "cy": at_y, "cd": at_d}.get(kind)
        if kind == "d":
            who = at_x if i == 0 else at_y
        device = {"z": (dp, far_z), "x": (at_x, z), "y": (at_y, z)}.get(kind, (at_c, z))
        if kind == "d":
            device = (at_y, z) if i == 0 else (at_x, z)
        slot = {"z": 0, "x": 1, "y": 3, "d": 5, "c": 7, "cx": 8, "cy": 9, "cd": 10}[kind]
        if kind in ("x", "y", "d"):
            slot += i
        if kind == "z":
            i = 1
        if kind[0] == "c":
            i = 1 - core
        dst = w_ref.at[i, who]
        return remote(dst if src is None else src, dst, q_send.at[slot], q_recv.at[slot], device)

    def q_arrived(kind, i=0):
        q_copy(kind, i).wait_recv()

    def own_q():
        return pltpu.make_async_copy(qkv_ref, w_ref.at[0, dp], locals_.at[packs + 1])

    q_kinds = [("z", 0), ("x", 0), ("x", 1), ("y", 0), ("y", 1), ("d", 0), ("d", 1)]
    q_kinds += [("c", 0), ("cx", 0), ("cy", 0), ("cd", 0)]

    keeps = [w_ref.at[core], normed, cosine, sine, ka, v]

    def save(i):
        return pltpu.make_async_copy(keeps[i], saved[i], save_sem.at[i])

    rows = x_ref.shape[0]

    def head(pair, m, owner):
        src = kept.o.at[pair, pl.ds(m * rows, rows)]
        dst = heads_ref.at[m, pair]
        to_dp, to_z, stays = owner

        def far():
            return remote(
                src, dst, head_send.at[m, pair], head_recv.at[m, pair], (to_dp, to_z)
            )

        def near():
            return pltpu.make_async_copy(src, dst, head_recv.at[m, pair])

        return far, near, stays

    def start(item):
        far, near, stays = item
        pl.when(stays)(lambda: near().start())
        pl.when(jnp.logical_not(stays))(lambda: far().start())

    def end_send(item):
        far, near, stays = item
        pl.when(jnp.logical_not(stays))(lambda: far().wait_send())

    q_copy("z", 0, qkv_ref).start()
    q_copy("x", 0, qkv_ref).start()
    q_copy("y", 0, qkv_ref).start()
    own_q().start()
    for m in range(2):
        start(token(m))
    swap_info().start()
    own_info().start()
    for p in range(packs):
        begin(p)
        begin_line(p)
    own_info().wait()
    swap_info().wait()
    own_q().wait()
    q_arrived("x", 0)
    q_copy("d", 0).start()
    q_arrived("z")
    q_copy("x", 1).start()
    q_copy("y", 1).start()
    away = (group + core) % 2
    for m in range(WAYS):
        table_piece(m, infos[away, mix(quarter, m)], kept)
    q_arrived("y", 0)
    q_copy("c").start()
    plane(0, 0)
    q_arrived("x", 1)
    q_copy("cx").start()
    q_arrived("y", 1)
    q_copy("d", 1).start()
    q_copy("cy").start()
    plane(1, 0)
    q_arrived("d", 0)
    q_arrived("d", 1)
    q_copy("cd").start()
    reach(0, 1)
    corner(0, 0)
    reach(1, 1)
    corner(1, 0)
    for kind in ("c", "cx", "cy", "cd"):
        q_arrived(kind)
    save(0).start()
    save(2).start()
    save(3).start()
    for m in range(2):
        token(m)[0]().wait_recv()
        pass_on(m).start()
    for p in range(packs):
        ahead(p, 1)
        plane(p, 1)
    for m in range(WAYS):
        if m >= 2:
            pass_on(m - 2).wait_recv()
        weight = jnp.concatenate([w_ref[core, d] for d in range(w_ref.shape[1])], axis=-1)
        qkv_piece(m, x_all[m], gain_ref[...], weight, kept)
        if m == 2:
            line(0, 2)
            corner(0, 1)
    save(1).start()
    save(4).start()
    save(5).start()

    events = {
        1: [(line, 1, 2), (corner, 1, 1)],
        4: [(line, 0, 3), (plane, 0, 2)],
        7: [(line, 1, 3), (plane, 1, 2)],
        9: [(corner, 0, 2)],
        11: [(plane, 0, 3)],
        13: [(corner, 1, 2)],
    }
    steps = kept.v.shape[1] // STEP
    pairs = kept.v.shape[0]
    per = steps // WAYS

    def body(i, carry):
        for at, todo in events.items():

            @pl.when(i == at)
            def _(todo=todo):
                for what, p, hop in todo:
                    what(p, hop)

        pair = i // steps
        step = i % steps
        attn_step(pair, step, kept)
        m = step // per

        @pl.when(step % per == per - 1)
        def _():
            a, b = dp - core + group, mix(quarter, m)
            start(head(pair, m, (a, b, jnp.logical_and(a == dp, b == z))))

        return carry

    lax.fori_loop(0, pairs * steps, body, 0)
    plane(1, 3)
    corner(0, 3)
    corner(1, 3)
    for p in range(packs):
        from_core(p)
    for m in range(WAYS):
        for pair in range(pairs):
            head(pair, m, there[m])[0]().wait_recv()
            end_send(head(pair, m, there[m]))
    for m in range(2):
        pass_on(m).wait_send()
        end_send(token(m))
    for p in range(packs):
        finish(p)
    for kind, i in q_kinds:
        q_copy(kind, i).wait_send()
    for i in range(len(keeps)):
        save(i).wait()


def forward_call(x, info, gain, qkv_part, parts, dps, pairs):
    rows, model = x.shape
    packs = len(parts)
    anywhere = pl.BlockSpec(memory_space=pl.ANY)
    vmem = pl.BlockSpec(memory_space=pltpu.VMEM)
    outs, scratch = kept_shapes(WAYS * rows, model, pairs)
    normed, cosine, sine, qa, ka, v, o = outs
    hold = [normed, cosine, sine, ka, v]
    weight = (dps,) + qkv_part.shape
    out = pl.pallas_call(
        functools.partial(forward_kernel, packs=packs),
        in_specs=[anywhere, anywhere, vmem] + [anywhere] * (1 + packs),
        out_specs=[anywhere] * (packs + 7) + [vmem] * 2,
        out_shape=[shape_of((dps, WAYS) + part.shape, BF) for part in parts]
        + [shape_of((WAYS, pairs, rows, LANES), BF), shape_of(weight, BF)]
        + hold
        + [qa, o],
        scratch_shapes=[pltpu.VMEM(h.shape, h.dtype) for h in hold]
        + scratch
        + [
            pltpu.VMEM((WAYS, rows, model), BF),
            pltpu.VMEM((2,) + weight, BF),
            pltpu.VMEM((2, WAYS, rows, LANES), F32),
            pltpu.SemaphoreType.DMA((packs, 9, WAYS)),
            pltpu.SemaphoreType.DMA((packs, 4, WAYS)),
            pltpu.SemaphoreType.DMA((packs, 4, WAYS)),
            pltpu.SemaphoreType.DMA((packs + 2,)),
            pltpu.SemaphoreType.DMA((WAYS + 1,)),
            pltpu.SemaphoreType.DMA((WAYS + 1,)),
            pltpu.SemaphoreType.DMA((WAYS, pairs)),
            pltpu.SemaphoreType.DMA((WAYS, pairs)),
            pltpu.SemaphoreType.DMA((11,)),
            pltpu.SemaphoreType.DMA((11,)),
            pltpu.SemaphoreType.DMA((6,)),
        ],
        compiler_params=pltpu.CompilerParams(
            collective_id=0, has_side_effects=True, vmem_limit_bytes=VMEM_LIMIT
        ),
        name="forward",
    )(x, info, gain, qkv_part, *parts)
    packs_out, out = out[:packs], out[packs:]
    heads, weight, normed, cosine, sine, ka, v, qa, o = out
    return packs_out, heads, weight, (normed, cosine, sine, qa, ka, v, o)


def attn_back_begin(pair, k):
    chunk = 512
    lane = lax.broadcasted_iota(jnp.int32, (chunk, LANES), 1)
    zero = jnp.zeros((), BF)
    ones = jnp.where(lane % HEAD_DIM < 3, jnp.ones((), BF), zero)
    for at in range(0, k.dk.shape[0], chunk):
        some = slice(at, at + chunk)
        v = k.v[pair, some, :]
        for head in range(2):
            mine = (lane < HEAD_DIM) if head == 0 else (lane >= HEAD_DIM)
            k.va[head, some, :] = jnp.where(mine, v, ones)
            own = jnp.where(mine, k.ka[pair, head, some, :], zero).astype(F32)
            k.kt[head, :, some] = own.T.astype(BF)
    k.dk[...] = jnp.zeros_like(k.dk)
    k.dv[...] = jnp.zeros_like(k.dv)


def attn_back_step(pair, step, grad, k):
    chunk = 512
    here = pl.ds(pl.multiple_of(step * STEP, STEP), STEP)
    lane = lax.broadcasted_iota(jnp.int32, (STEP, LANES), 1)
    zero = jnp.zeros((), BF)
    t = lane % HEAD_DIM
    product = grad.astype(F32) * k.o[pair, here, :].astype(F32)
    turned = jnp.zeros((LANES, STEP), F32)
    for head in range(2):
        mine = (lane < HEAD_DIM) if head == 0 else (lane >= HEAD_DIM)
        delta = jnp.sum(jnp.where(mine, product, 0.0), axis=-1, keepdims=True)
        high = delta.astype(BF)
        rest = delta - high.astype(F32)
        mid = rest.astype(BF)
        low = (rest - mid.astype(F32)).astype(BF)
        aux = jnp.where(t == 0, -high, jnp.where(t == 1, -mid, jnp.where(t == 2, -low, zero)))
        grad_aug = jnp.where(mine, grad, aux)
        grad_own = jnp.where(mine, grad, zero)
        qa = k.qa[pair, head, here, :]
        q_own = jnp.where(mine, qa, zero)
        for at in range(0, k.dk.shape[0], chunk):
            some = slice(at, at + chunk)
            prob = jnp.exp(dot_nt(k.ka[pair, head, some, :], qa))
            back = dot_nt(k.va[head, some, :], grad_aug)
            score_grad = (prob * back).astype(BF)
            k.dv[some, :] += dot_nn(prob.astype(BF), grad_own)
            k.dk[some, :] += dot_nn(score_grad, q_own)
            turned += dot_nn(k.kt[head, :, some], score_grad)
    dq = turned.T * (HEAD_DIM**-0.5)
    dq = dq * k.cosine[here, :] - swap_halves(dq) * k.sine[here, :]
    k.low[pair, 0, here, :] = dq.astype(BF)


def attn_back_end(pair, k):
    chunk = 512
    for at in range(0, k.dk.shape[0], chunk):
        some = slice(at, at + chunk)
        dk = k.dk[some, :]
        dk = dk * k.cosine[some, :] - swap_halves(dk) * k.sine[some, :]
        k.low[pair, 1, some, :] = dk.astype(BF)
        k.low[pair, 2, some, :] = k.dv[some, :].astype(BF)


def low_piece(pair, m, k, rows):
    some = slice(m * rows, (m + 1) * rows)
    return jnp.concatenate([k.low[pair, c, some, :] for c in range(3)], axis=-1)


class Back:
    names = ("qa", "ka", "v", "o", "cosine", "sine", "low", "va", "kt", "dk", "dv")

    def __init__(self, refs):
        for name, ref in zip(self.names, refs):
            setattr(self, name, ref)


class Chain:
    def __init__(self, p, source, kept, r1, r2, rz, send, recv):
        self.p, self.source, self.kept = p, source, kept
        self.r1, self.r2, self.rz, self.send, self.recv = r1, r2, rz, send, recv

    def slab(self, q, slot, away):
        x, y = self.p.x, self.p.y
        if q < 2:
            return (y if slot else 1 - y) * 2 + (1 - x if away else x)
        return (1 - y if away else y) * 2 + (x if slot else 1 - x)

    def near(self, q, second=False):
        p = self.p
        return (p.at_x, p.z) if (q < 2) != second else (p.at_y, p.z)

    def stage1(self, q, slot):
        src = self.source(q, self.slab(q, slot, True))
        at = q * 2 + slot
        return remote(src, self.r1.at[q, slot], self.send.at[at], self.recv.at[at], self.near(q))

    def stage2(self, q):
        at = 8 + q
        src = self.kept(q, 0, self.slab(q, 0, False))
        return remote(src, self.r2.at[q], self.send.at[at], self.recv.at[at], self.near(q, True))

    def first(self, q):
        self.stage1(q, 0).start()
        self.stage1(q, 1).start()

    def second(self, q):
        self.stage1(q, 0).wait_recv()
        ref = self.kept(q, 0, self.slab(q, 0, False))
        ref[...] += self.r1[q, 0]
        self.stage2(q).start()
        self.stage1(q, 1).wait_recv()
        self.own(q)[...] += self.r1[q, 1]

    def own(self, q):
        return self.kept(q, 1, self.slab(q, 1, False))

    def third(self, q):
        self.stage2(q).wait_recv()
        self.own(q)[...] += self.r2[q]

    def lined(self, q, down):
        z = self.p.z
        at = q if down else q + 1
        return remote(
            self.own(q), self.rz.at[at], self.send.at[12 + q], self.recv.at[12 + at],
            (self.p.dp, z - 1 if down else z + 1),
        )

    def line(self, hop, quarters):
        z = self.p.z
        for q in quarters:
            if q < WAYS - hop:

                @pl.when(z == WAYS - hop)
                def _(q=q):
                    if hop > 1:
                        self.lined(q, True).wait_recv()
                        self.own(q)[...] += self.rz[q]
                    self.lined(q, True).start()

            if q > hop - 1:

                @pl.when(z == hop - 1)
                def _(q=q):
                    if hop > 1:
                        self.lined(q, False).wait_recv()
                        self.own(q)[...] += self.rz[q + 1]
                    self.lined(q, False).start()

    def last(self, out_ref):
        z = self.p.z
        for q in range(WAYS):

            @pl.when(z == q)
            def _(q=q):
                total = self.own(q)[...].astype(F32)
                if q < WAYS - 1:
                    self.lined(q, True).wait_recv()
                    total += self.rz[q].astype(F32)
                if q > 0:
                    self.lined(q, False).wait_recv()
                    total += self.rz[q + 1].astype(F32)
                out_ref[...] = total

    def finish(self):
        z = self.p.z
        for q in range(WAYS):
            self.stage1(q, 0).wait_send()
            self.stage1(q, 1).wait_send()
            self.stage2(q).wait_send()
            pl.when(q < z)(lambda q=q: self.lined(q, True).wait_send())
            pl.when(q > z)(lambda q=q: self.lined(q, False).wait_send())


def backward_kernel(
    hg_ref, sum_ref, normed_ref, w_ref, x_ref, mgrad_ref, low_ref, heads_ref,
    qa, ka, v, o, cosine, sine, gain_ref, small_ref,
    grad_ref, ffn_ref, attn_ref, qkv_ref, total_ref,
    do_ref, low, va, kt, dk, dv, normed, weight, x_in, mgrad,
    f_kept, f_r1, f_r2, f_rz, a_sum, a_got, a_r1, a_r2, a_rz,
    q_sum, q_rx, q_ry, q_rz, g_core, g_here, s_own, s_dp, s_mp,
    load_sem, do_send, do_recv, f_send, f_recv, a_send, a_recv, c_send, c_recv,
    q_send, q_recv, g_send, g_recv, s_send, s_recv,
):
    p = Place()
    dp, z, core = p.dp, p.z, p.core
    rows = x_ref.shape[0]
    pairs = v.shape[0]
    k = Back((qa, ka, v, o, cosine, sine, low, va, kt, dk, dv))

    def qkv_to(turn):
        a, b = dp - core + (p.group + turn) % 2, p.quarter
        return a, b, p.stays(a, b)

    def qkv_from(g):
        a, b = dp - core + (z // 2 + g) % 2, 2 * g + z % 2
        return a, b, p.stays(a, b)

    def other_dp(turn):
        return (dp + turn) % 8, z

    def other_mp(turn):
        return dp, (z + turn) % WAYS

    barrier = pltpu.get_barrier_semaphore()
    count = jnp.int32(0)

    def greet(device, skip=None):
        def signal():
            pl.semaphore_signal(barrier, inc=1, device_id=device, device_id_type=MESH)

        if skip is None:
            signal()
            return 1
        pl.when(jnp.logical_not(skip))(signal)
        return 1 - skip.astype(jnp.int32)

    for turn in range(1, 8):
        count += greet(other_dp(turn))
    for turn in range(1, WAYS):
        count += greet(other_mp(turn))
    for m in range(WAYS):
        for a, b, stays in (p.attention_of(m), p.owner_of(m)):
            count += greet((a, b), stays)
    for i in range(2):
        for a, b, stays in (qkv_to(i), qkv_from(i)):
            count += greet((a, b), stays)
    pl.semaphore_wait(barrier, count)

    def head_grad(m, pair, place):
        return Move(
            hg_ref.at[m, pair], do_ref.at[m, pair], do_send.at[m, pair], do_recv.at[m, pair], place
        )

    for pair in range(pairs):
        for m in range(WAYS):
            head_grad(m, pair, p.attention_of(m)).start()

    ffn = Chain(
        p, lambda q, i: sum_ref.at[q, i], lambda q, slot, i: f_kept.at[q, slot],
        f_r1, f_r2, f_rz, f_send, f_recv,
    )
    ffn.first(0)
    ffn.first(2)
    loads = []

    def load(src, dst):
        copy = pltpu.make_async_copy(src, dst, load_sem.at[len(loads)])
        copy.start()
        loads.append(copy)

    for q in range(WAYS):
        for slot in range(2):
            load(sum_ref.at[q, ffn.slab(q, slot, False)], f_kept.at[q, slot])
    load(normed_ref, normed)
    load(w_ref, weight)
    load(x_ref, x_in)
    load(mgrad_ref, mgrad)

    low_here = own_first(core, low_ref[...])
    for m in range(WAYS):
        mixed = jnp.concatenate([heads_ref[m, 0], heads_ref[m, 1]], axis=-1)
        value = dot_tn(mixed, low_here).astype(BF)
        h = p.mix(z, m)
        for d in range(value.shape[1] // LANES):
            a_sum[d % 2, h, d // 2] = value[:, d * LANES : (d + 1) * LANES]
    swap = remote(a_sum.at[1], a_got, c_send.at[0], c_recv.at[0], (p.at_c, z))
    swap.start()
    attn_back_begin(0, k)
    swap.wait()
    for q in range(WAYS):
        a_sum[0, q] += a_got[q]
    attn = Chain(
        p, lambda q, i: a_sum.at[0, q, i], lambda q, slot, i: a_sum.at[0, q, i],
        a_r1, a_r2, a_rz, a_send, a_recv,
    )
    for q in range(WAYS):
        attn.first(q)
    for copy in loads[:8]:
        copy.wait()

    def qkv_x(pair, yy):
        at = (p.y if yy else 1 - p.y) * 4 + (1 - p.x) * 2
        return remote(
            q_sum.at[pair, pl.ds(at, 2)], q_rx.at[pair, yy],
            q_send.at[pair, yy], q_recv.at[pair, yy], (p.at_x, z),
        )

    def qkv_y(pair):
        at = (1 - p.y) * 4 + p.x * 2
        return remote(
            q_sum.at[pair, pl.ds(at, 2)], q_ry.at[pair],
            q_send.at[pair, 2], q_recv.at[pair, 2], (p.at_y, z),
        )

    def qkv_z(pair, turn, g, place):
        at = p.y * 4 + p.x * 2 + (p.group + turn) % 2
        return Move(
            q_sum.at[pair, at], q_rz.at[pair, g],
            q_send.at[pair, 3 + turn], q_recv.at[pair, 3 + g], place,
        )

    def qkv_first(pair):
        total = None
        for m in range(WAYS):
            part = dot_tn(low_piece(pair, m, k, rows), normed[m * rows : (m + 1) * rows, :])
            total = part if total is None else total + part
        value = total.astype(BF)
        for d in range(value.shape[1] // LANES):
            q_sum[pair, d] = value[:, d * LANES : (d + 1) * LANES]
        qkv_x(pair, 0).start()
        qkv_x(pair, 1).start()

    def qkv_second(pair):
        qkv_x(pair, 0).wait_recv()
        at = (1 - p.y) * 4 + p.x * 2
        for i in range(2):
            q_sum[pair, at + i] += q_rx[pair, 0, i]
        qkv_y(pair).start()
        qkv_x(pair, 1).wait_recv()
        at = p.y * 4 + p.x * 2
        for i in range(2):
            q_sum[pair, at + i] += q_rx[pair, 1, i]

    def qkv_third(pair):
        qkv_y(pair).wait_recv()
        at = p.y * 4 + p.x * 2
        for i in range(2):
            q_sum[pair, at + i] += q_ry[pair, i]
        for turn in range(2):
            qkv_z(pair, turn, p.group, qkv_to(turn)).start()

    def pair_end():
        attn_back_end(0, k)
        attn_back_begin(1, k)
        for copy in loads[8:]:
            copy.wait()
        qkv_first(0)

    events = {
        3: [(ffn.second, 0), (ffn.second, 2), (ffn.first, 1), (ffn.first, 3)],
        4: [(attn.second, q) for q in range(WAYS)],
        6: [(attn.third, q) for q in range(WAYS)] + [(attn.line, 1, range(WAYS))],
        7: [(attn.line, 2, range(WAYS))],
        8: [(pair_end,)],
        9: [(attn.line, 3, range(WAYS)), (ffn.third, 0), (ffn.third, 2)],
        10: [(ffn.line, 1, (0, 2)), (qkv_second, 0)],
        11: [(ffn.second, 1), (ffn.second, 3)],
        12: [(ffn.line, 2, (0, 2)), (qkv_third, 0)],
        14: [(ffn.line, 3, (0, 2)), (ffn.third, 1), (ffn.third, 3), (ffn.line, 1, (1, 3))],
    }
    steps = v.shape[1] // STEP
    per = rows // STEP

    def body(i, carry):
        for at, todo in events.items():

            @pl.when(i == at)
            def _(todo=todo):
                for what, *args in todo:
                    what(*args)

        pair, step = i // steps, i % steps
        m = step // per

        @pl.when(step % per == 0)
        def _():
            head_grad(m, pair, p.owner_of(0)).wait_recv()

        at = pl.multiple_of((step - m * per) * STEP, STEP)
        attn_back_step(pair, step, do_ref[m, pair, pl.ds(at, STEP), :], k)
        return carry

    lax.fori_loop(0, pairs * steps, body, 0)
    attn_back_end(1, k)

    joined = jnp.concatenate([weight[d] for d in range(weight.shape[0])], axis=-1)

    def piece_grad(m):
        out = None
        for pair in range(pairs):
            at = pair * 3 * LANES
            part = dot_nn(low_piece(pair, m, k, rows), joined[at : at + 3 * LANES, :])
            out = part if out is None else out + part
        return out.astype(BF)

    def to_core(m):
        return remote(
            normed.at[pl.ds((m + 2) * rows, rows)], g_core.at[m],
            g_send.at[m], g_recv.at[m], (p.at_c, z),
        )

    def to_owner(m, place):
        return Move(
            normed.at[pl.ds(m * rows, rows)], g_here.at[m], g_send.at[2 + m], g_recv.at[2 + m], place
        )

    qkv_first(1)
    for m in range(2):
        normed[(m + 2) * rows : (m + 3) * rows, :] = piece_grad(m + 2)
        to_core(m).start()
    for m in range(2):
        own = piece_grad(m)
        to_core(m).wait_recv()
        normed[m * rows : (m + 1) * rows, :] = own + g_core[m]
        to_owner(m, p.owner_of(m)).start()
    ffn.line(2, (1, 3))
    qkv_second(1)
    ffn.line(3, (1, 3))
    attn.last(attn_ref)
    qkv_third(1)
    ffn.last(ffn_ref)
    vhat, scale = norm_stats(x_in[...].astype(F32))
    for pair in range(pairs):
        for g in range(2):
            qkv_z(pair, 0, g, qkv_from(g)).wait_recv()
        qkv_ref[pair] = q_rz[pair, 0].astype(F32) + q_rz[pair, 1].astype(F32)
    for m in range(2):
        to_owner(m, p.attention_of(m)).wait_recv()
    normed_grad = g_here[0].astype(F32) + g_here[1].astype(F32)
    gain_part = jnp.sum(normed_grad * vhat, axis=0, keepdims=True)
    s_own[...] = jnp.concatenate([gain_part, small_ref[1:, :]], axis=0)

    def sum_dp(turn):
        return remote(
            s_own, s_dp.at[turn], s_send.at[turn], s_recv.at[turn], other_dp(turn)
        )

    def sum_mp(turn):
        return remote(
            s_dp.at[0], s_mp.at[turn], s_send.at[8 + turn], s_recv.at[8 + turn], other_mp(turn)
        )

    for turn in range(1, 8):
        sum_dp(turn).start()
    grad_ref[...] = mgrad[...] + norm_back(vhat, scale, gain_ref[...], normed_grad)
    total = s_own[...]
    for turn in range(1, 8):
        sum_dp(turn).wait_recv()
        total += s_dp[turn]
    s_dp[0] = total
    for turn in range(1, WAYS):
        sum_mp(turn).start()
    for turn in range(1, WAYS):
        sum_mp(turn).wait_recv()
        total += s_mp[turn]
    total_ref[...] = total

    for turn in range(1, 8):
        sum_dp(turn).wait_send()
    for turn in range(1, WAYS):
        sum_mp(turn).wait_send()
    for m in range(2):
        to_core(m).wait_send()
        to_owner(m, p.owner_of(m)).wait_send()
    for m in range(WAYS):
        for pair in range(pairs):
            head_grad(m, pair, p.attention_of(m)).wait_send()
    for pair in range(pairs):
        qkv_x(pair, 0).wait_send()
        qkv_x(pair, 1).wait_send()
        qkv_y(pair).wait_send()
        for turn in range(2):
            qkv_z(pair, turn, p.group, qkv_to(turn)).wait_send()
    ffn.finish()
    attn.finish()


def backward_call(heads_grad, ffn_sum, kept, weight, x, middle_grad, low, heads, gain, small):
    normed, cosine, sine, qa, ka, v, o = kept
    rows, model = x.shape
    pairs, tokens, unused = v.shape
    wide, cols3, unused = weight.shape
    units = ffn_sum.shape[2]
    depth = model // WAYS
    third = cols3 // pairs
    anywhere = pl.BlockSpec(memory_space=pl.ANY)
    vmem = pl.BlockSpec(memory_space=pltpu.VMEM)
    buf = lambda *shape, kind=BF: pltpu.VMEM(shape, kind)
    sems = lambda *shape: pltpu.SemaphoreType.DMA(shape)
    return pl.pallas_call(
        backward_kernel,
        in_specs=[anywhere] * 6 + [vmem] * 10,
        out_specs=[vmem] * 5,
        out_shape=[
            shape_of((rows, model), F32),
            shape_of((units, LANES), F32),
            shape_of((depth, LANES), F32),
            shape_of((pairs, third, LANES), F32),
            shape_of(small.shape, F32),
        ],
        scratch_shapes=[
            buf(WAYS, pairs, rows, LANES),
            buf(pairs, 3, tokens, LANES),
            buf(2, tokens, LANES),
            buf(2, LANES, tokens),
            buf(tokens, LANES, kind=F32),
            buf(tokens, LANES, kind=F32),
            buf(tokens, model),
            buf(wide, cols3, LANES),
            buf(rows, model),
            buf(rows, model, kind=F32),
            buf(WAYS, 2, units, LANES),
            buf(WAYS, 2, units, LANES),
            buf(WAYS, units, LANES),
            buf(WAYS + 1, units, LANES),
            buf(2, WAYS, wide // 2, depth, LANES),
            buf(WAYS, wide // 2, depth, LANES),
            buf(WAYS, 2, depth, LANES),
            buf(WAYS, depth, LANES),
            buf(WAYS + 1, depth, LANES),
            buf(pairs, wide, third, LANES),
            buf(pairs, 2, 2, third, LANES),
            buf(pairs, 2, third, LANES),
            buf(pairs, 2, third, LANES),
            buf(2, rows, model),
            buf(2, rows, model),
            buf(*small.shape, kind=F32),
            buf(8, *small.shape, kind=F32),
            buf(WAYS, *small.shape, kind=F32),
            sems(12),
            sems(WAYS, pairs),
            sems(WAYS, pairs),
            sems(16),
            sems(17),
            sems(16),
            sems(17),
            sems(1),
            sems(1),
            sems(pairs, 5),
            sems(pairs, 5),
            sems(4),
            sems(4),
            sems(12),
            sems(12),
        ],
        compiler_params=pltpu.CompilerParams(
            collective_id=2, has_side_effects=True, vmem_limit_bytes=62 * 1024 * 1024
        ),
        name="backward",
    )(
        heads_grad, ffn_sum, normed, weight, x, middle_grad, low, heads,
        qa, ka, v, o, cosine, sine, gain, small,
    )


def pick(values, at, axis=0):
    return lax.dynamic_index_in_dim(values, at, axis, keepdims=False)


def flip(values, bit, dps):
    return lax.ppermute(values, "dp", [(i, i ^ bit) for i in range(dps)])


def to_attention(values, m, dps, back=False):
    pairs = []
    for dp in range(dps):
        group = dp % 2
        for t in range(WAYS):
            quarter = t ^ m
            there = (dp - group + ((quarter // 2) ^ group)) * WAYS + 2 * group + quarter % 2
            pairs.append((there, dp * WAYS + t) if back else (dp * WAYS + t, there))
    return lax.ppermute(values, ("dp", "mp"), pairs)


def local(
    sizes,
    layer_input,
    segment_ids,
    grad_out,
    qkv_weight,
    attn_weight,
    inner_weight,
    outer_weight,
    attn_gain,
    mlp_gain,
):
    dps, mps = sizes
    rows, model = layer_input.shape
    head_cols = qkv_weight.shape[2]
    units = inner_weight.shape[2]
    pairs = head_cols // LANES
    wide = model // LANES
    special = dps == wide
    me = lax.axis_index("mp")
    dp = lax.axis_index("dp")
    core = dp % 2
    group = me // 2
    quarter = me ^ (2 * core)
    scalars = jnp.stack([me, core if special else 0, quarter]).astype(jnp.int32)

    def every(values):
        got = lax.all_gather(values.T, "dp", axis=0, tiled=True).T
        got = got.reshape(-1, wide, LANES).transpose(1, 0, 2)
        return lax.all_gather(got, "mp", axis=1)

    qkv_part = qkv_weight.transpose(1, 2, 0).reshape(3, pairs, LANES, -1)
    qkv_part = qkv_part.transpose(1, 0, 2, 3).reshape(3 * head_cols, -1)
    inner_t = inner_weight.transpose(1, 2, 0)
    outer_t = outer_weight.T
    attn_depth = model // mps
    part_a = jnp.concatenate([attn_weight.T, inner_t[0]], axis=0)
    part_b = jnp.concatenate([inner_t[1], outer_t], axis=0)
    mine = segment_ids[0]
    info = jnp.stack([mine, doc_positions(mine)], axis=1).astype(F32)
    info = jnp.pad(info, ((0, 0), (0, LANES - 2))).reshape(WAYS, rows, LANES)
    live_mine = (pick(mine.reshape(WAYS, rows), me) != 0).astype(F32)[:, None]
    if special:
        (pack_a, pack_b), heads, qkv_own, kept = forward_call(
            layer_input, info, attn_gain[None], qkv_part, [part_a, part_b], dps, pairs
        )
    else:
        x_all = jnp.stack([to_attention(layer_input, m, dps) for m in range(WAYS)])
        qkv_all, pack_a, pack_b = every(qkv_part), every(part_a), every(part_b)
        info = jnp.where(group == core, info, flip(info, 1, dps))
        info = jnp.stack([pick(info, quarter ^ m) for m in range(WAYS)])
        kept = alone_call(x_all, info, attn_gain[None], pick(qkv_all, quarter, 1), pairs)
        heads = kept[6].reshape(pairs, WAYS, rows, LANES)
        heads = [to_attention(heads[:, m], m, dps, back=True) for m in range(WAYS)]
        heads = jnp.stack(heads)
    normed, cosine, sine, qa, ka, v, o = kept

    middle, inner_in, squares = middle_call(
        scalars, heads, layer_input, pack_a, mlp_gain[None], live_mine
    )
    mlp_out, inner_back, ffn_sum = ffn_call(
        scalars, inner_in, grad_out, pack_a, pack_b, special
    )
    layer_output, middle_grad, middle_low, small, heads_grad = middle_back_call(
        scalars, middle, mlp_out, inner_back, grad_out, pack_a, mlp_gain[None], live_mine
    )
    sums = [jnp.sum(squares[:3], axis=1), jnp.sum(small[0])[None], jnp.sum(live_mine)[None]]
    sums = jnp.concatenate(sums + [jnp.zeros((model - 5,), F32)])
    small = jnp.concatenate([small[:2], sums[None], jnp.zeros((5, model), F32)])
    if special:
        input_grad, ffn_sum, attn_sum, qkv_sum, small = backward_call(
            heads_grad, ffn_sum, kept, qkv_own, layer_input, middle_grad, middle_low, heads,
            attn_gain[None], small,
        )
        qkv_sum = qkv_sum.reshape(3 * head_cols, -1)
    else:
        lows = []
        for pair in range(pairs):
            grad = [to_attention(heads_grad[m, pair], m, dps) for m in range(WAYS)]
            low = attn_bwd_call(scalars, qa, ka, v, grad, o, cosine, sine, pair)
            lows.append(jnp.concatenate(low, axis=0))
        low = jnp.concatenate(lows, axis=1)
        own = pick(qkv_all, quarter, 1)
        own = jnp.concatenate([own[d] for d in range(wide)], axis=-1)
        normed_grad = dot_nn(low, own).astype(BF).reshape(WAYS, rows, model)
        normed_grad = sum(
            to_attention(normed_grad[m], m, dps, back=True).astype(F32) for m in range(WAYS)
        )

        def scatter(values):
            cut = lax.psum_scatter(values, "mp", scatter_dimension=0)
            return lax.psum_scatter(cut.T, "dp", scatter_dimension=0, tiled=True).T

        slot = (jnp.arange(mps) == quarter)[:, None, None]
        qkv_sum = scatter(jnp.where(slot, dot_tn(low, normed)[None], 0.0))
        mixed = jnp.stack([pick(heads, me ^ h) for h in range(mps)])
        mixed = mixed.transpose(0, 2, 1, 3).reshape(mps, rows, -1)
        attn_sum = scatter(jnp.stack([dot_tn(mixed[h], middle_low) for h in range(mps)]))
        ffn_sum = ffn_sum.reshape(mps, wide, 3 * units, LANES).transpose(0, 2, 1, 3)
        ffn_sum = scatter(ffn_sum.reshape(mps, 3 * units, model).astype(F32))
        vhat, scale = norm_stats(layer_input.astype(F32))
        input_grad = middle_grad + norm_back(vhat, scale, attn_gain, normed_grad)
        small = small.at[0].set(jnp.sum(normed_grad * vhat, axis=0))
        small = lax.psum(small, ("dp", "mp"))
    rms_values = jnp.sqrt(small[2, :4] / (small[2, 4] * model))

    qkv_sum = qkv_sum.reshape(pairs, 3, LANES, -1).transpose(3, 1, 0, 2)
    ffn_sum = ffn_sum.reshape(3, units, -1)
    return (
        layer_output,
        input_grad,
        qkv_sum.reshape(-1, 3, head_cols),
        attn_sum.T,
        ffn_sum[:2].transpose(2, 0, 1),
        ffn_sum[2].T,
        small[0],
        small[1],
        rms_values,
    )


def solution(mesh):
    sizes = (mesh.shape["dp"], mesh.shape["mp"])
    both = ("dp", "mp")
    whole = (P(both, None), P("dp", None, "mp"), P("dp", "mp"))
    return jax.shard_map(
        functools.partial(local, sizes),
        mesh=mesh,
        in_specs=(
            whole[0],
            P("dp", None),
            whole[0],
            whole[1],
            whole[2],
            whole[1],
            whole[2],
            P(),
            P(),
        ),
        out_specs=(
            whole[0],
            whole[0],
            whole[1],
            whole[2],
            whole[1],
            whole[2],
            P(),
            P(),
            P(),
        ),
        check_vma=False,
    )
```

```python
import functools
import math

import jax
import jax.numpy as jnp
from jax import lax
from jax.experimental import pallas as pl
from jax.experimental.pallas import tpu as pltpu
from jax.sharding import PartitionSpec as P

HEAD_DIM = 64
NORM_EPS = 1e-05
ROPE_BASE = 160000.0
BIG = 1e30
LANES = 128
WAYS = 4
BF = jnp.bfloat16
F32 = jnp.float32
VMEM_LIMIT = 56 * 1024 * 1024


def dot_nn(a, b):
    return lax.dot_general(a, b, (((1,), (0,)), ((), ())), preferred_element_type=F32)


def dot_nt(a, b):
    return lax.dot_general(a, b, (((1,), (1,)), ((), ())), preferred_element_type=F32)


def dot_tn(a, b):
    return lax.dot_general(a, b, (((0,), (0,)), ((), ())), preferred_element_type=F32)


def norm_stats(values):
    centre = jnp.mean(values, axis=-1, keepdims=True)
    shifted = values - centre
    spread = jnp.mean(shifted * shifted, axis=-1, keepdims=True)
    scale = lax.rsqrt(spread + NORM_EPS)
    return shifted * scale, scale


def norm_back(vhat, scale, gain, grad):
    u = grad * gain
    mean_u = jnp.mean(u, axis=-1, keepdims=True)
    mean_uv = jnp.mean(u * vhat, axis=-1, keepdims=True)
    return scale * (u - mean_u - vhat * mean_uv)


def doc_positions(segment):
    length = segment.shape[0]
    places = jnp.arange(length, dtype=jnp.int32)
    before = jnp.concatenate([jnp.full((1,), -1, jnp.int32), segment[:-1]])
    starts = jnp.where(segment != before, places, jnp.zeros_like(places))
    return places - lax.cummax(starts, axis=0)


def swap_halves(values):
    lane = lax.broadcasted_iota(jnp.int32, values.shape, 1)
    first = lane % HEAD_DIM < HEAD_DIM // 2
    back = pltpu.roll(values, LANES - HEAD_DIM // 2, 1)
    ahead = pltpu.roll(values, HEAD_DIM // 2, 1)
    return jnp.where(first, back, ahead)


def choose(at, values):
    out = values[0]
    for i in range(1, len(values)):
        out = jnp.where(at == i, values[i], out)
    return out


def params():
    return pltpu.CompilerParams(vmem_limit_bytes=VMEM_LIMIT)


def cost(flops, mib):
    return pl.CostEstimate(flops=int(flops), bytes_accessed=int(mib * 2**20), transcendentals=0)


def call(kernel, scalars, grid, in_specs, out_specs, out_shape, scratch, estimate, name):
    spec = pltpu.PrefetchScalarGridSpec(
        num_scalar_prefetch=1,
        grid=grid,
        in_specs=in_specs,
        out_specs=out_specs,
        scratch_shapes=scratch,
    )
    return functools.partial(
        pl.pallas_call(
            kernel,
            grid_spec=spec,
            out_shape=out_shape,
            compiler_params=params(),
            cost_estimate=estimate,
            name=name,
        ),
        scalars,
    )


def full(shape):
    return pl.BlockSpec(shape, lambda i, s: (0,) * len(shape))


def shape_of(shape, dtype):
    return jax.ShapeDtypeStruct(shape, dtype)


def side_by_side(ref, *at):
    return jnp.concatenate([ref[(d, *at)] for d in range(ref.shape[0])], axis=-1)


STEP = 256


def table_piece(m, info, out):
    rows = info.shape[0]
    here = slice(m * rows, (m + 1) * rows)
    segment, position = info[:, 0:1], info[:, 1:2]
    lane = lax.broadcasted_iota(jnp.int32, (1, LANES), 1)
    half = HEAD_DIM // 2
    frequency = jnp.exp((lane % half).astype(F32) * (-2.0 * math.log(ROPE_BASE) / HEAD_DIM))
    angle = position * frequency
    sine = jnp.sin(angle)
    out.cosine[here, :] = jnp.cos(angle)
    out.sine[here, :] = jnp.where(lane % HEAD_DIM < half, -sine, sine)
    t = lane % HEAD_DIM
    same = segment == t.astype(F32)
    masked = jnp.where(same, 0.0, -BIG)
    out.qaux[here, :] = jnp.where(t >= 16, 0.0, masked).astype(BF)
    found = jnp.where(same, 1.0, 0.0)
    counted = jnp.where(t < 19, 1.0, 0.0)
    out.kaux[here, :] = jnp.where(t < 16, found, counted).astype(BF)
    out.live[here, :] = jnp.where(segment != 0.0, 1.0, 0.0)


def qkv_piece(m, x, gain, weight, out):
    rows = x.shape[0]
    here = slice(m * rows, (m + 1) * rows)
    vhat, unused = norm_stats(x.astype(F32))
    normed = (vhat * gain).astype(BF)
    out.normed[here, :] = normed
    flat = dot_nt(normed, weight)
    cosine, sine = out.cosine[here, :], out.sine[here, :]
    kaux = out.kaux[here, :]
    lane = lax.broadcasted_iota(jnp.int32, (rows, LANES), 1)
    for pair in range(flat.shape[1] // (3 * LANES)):
        q, k, v = [
            flat[:, at : at + LANES] for at in range(pair * 3 * LANES, (pair + 1) * 3 * LANES, LANES)
        ]
        q = (q * cosine + swap_halves(q) * sine).astype(BF)
        k = (k * cosine + swap_halves(k) * sine).astype(BF)
        out.q[pair, here, :] = q * jnp.asarray(HEAD_DIM**-0.5, BF)
        out.ka[pair, 0, here, :] = jnp.where(lane < HEAD_DIM, k, kaux)
        out.ka[pair, 1, here, :] = jnp.where(lane >= HEAD_DIM, k, kaux)
        out.v[pair, here, :] = v.astype(BF)


def attn_step(pair, step, out):
    tokens = out.v.shape[1]
    chunk = 512
    here = pl.ds(pl.multiple_of(step * STEP, STEP), STEP)
    lane = lax.broadcasted_iota(jnp.int32, (STEP, LANES), 1)
    t = lane % HEAD_DIM
    q = out.q[pair, here, :]
    qaux = out.qaux[here, :]
    live = out.live[here, :]
    outs = []
    for head in range(2):
        mine = (lane < HEAD_DIM) if head == 0 else (lane >= HEAD_DIM)
        qa = jnp.where(mine, q, qaux)
        top = None
        for at in range(0, tokens, chunk):
            s = dot_nt(qa, out.ka[pair, head, at : at + chunk, :])
            out.scores[:, at : at + chunk] = s
            part = jnp.max(s, axis=-1, keepdims=True)
            top = part if top is None else jnp.maximum(top, part)
        total = jnp.zeros((STEP, 1), F32)
        mixed = jnp.zeros((STEP, LANES), F32)
        for at in range(0, tokens, chunk):
            p = jnp.exp(out.scores[:, at : at + chunk] - top)
            total += jnp.sum(p, axis=-1, keepdims=True)
            mixed += dot_nn(p.astype(BF), out.v[pair, at : at + chunk, :])
        outs.append(mixed * (live / total))
        log_sum = jnp.where(live > 0, top + jnp.log(total), BIG)
        high = log_sum.astype(BF)
        rest = log_sum - high.astype(F32)
        mid = rest.astype(BF)
        low = (rest - mid.astype(F32)).astype(BF)
        aux = jnp.where(t == 16, -high, jnp.where(t == 17, -mid, jnp.where(t == 18, -low, qaux)))
        out.qa[pair, head, here, :] = jnp.where(mine, q, aux)
    out.o[pair, here, :] = jnp.where(lane < HEAD_DIM, outs[0], outs[1]).astype(BF)


class Kept:
    names = ("normed", "cosine", "sine", "qa", "ka", "v", "o", "q", "qaux", "kaux", "live", "scores")

    def __init__(self, refs):
        for name, ref in zip(self.names, refs):
            setattr(self, name, ref)


def kept_shapes(tokens, model, pairs):
    outs = [
        shape_of((tokens, model), BF),
        shape_of((tokens, LANES), F32),
        shape_of((tokens, LANES), F32),
        shape_of((pairs, 2, tokens, LANES), BF),
        shape_of((pairs, 2, tokens, LANES), BF),
        shape_of((pairs, tokens, LANES), BF),
        shape_of((pairs, tokens, LANES), BF),
    ]
    scratch = [
        pltpu.VMEM((pairs, tokens, LANES), BF),
        pltpu.VMEM((tokens, LANES), BF),
        pltpu.VMEM((tokens, LANES), BF),
        pltpu.VMEM((tokens, 1), F32),
        pltpu.VMEM((STEP, tokens), F32),
    ]
    return outs, scratch


def alone_kernel(x_ref, info_ref, gain_ref, w_ref, *refs):
    out = Kept(refs)
    for m in range(WAYS):
        table_piece(m, info_ref[m], out)
        qkv_piece(m, x_ref[m], gain_ref[...], side_by_side(w_ref), out)

    def body(step, carry):
        per = out.v.shape[1] // STEP
        attn_step(step // per, step % per, out)
        return carry

    lax.fori_loop(0, out.v.shape[0] * out.v.shape[1] // STEP, body, 0)


def alone_call(x, info, gain, weight, pairs):
    outs, scratch = kept_shapes(WAYS * x.shape[1], x.shape[2], pairs)
    return pl.pallas_call(
        alone_kernel,
        in_specs=[pl.BlockSpec(memory_space=pltpu.VMEM)] * 4,
        out_specs=[pl.BlockSpec(memory_space=pltpu.VMEM)] * len(outs),
        out_shape=outs,
        scratch_shapes=scratch,
        compiler_params=params(),
        name="forward",
    )(x, info, gain, weight)


def piece_block(m, rows, per):
    return pl.BlockSpec((rows, LANES), lambda i, s: (jnp.clip(i - per * m, 0, per - 1), 0))


def attn_bwd_kernel(s_ref, *refs):
    qa_ref, ka_ref, v_ref, o_ref, do_refs = refs[0], refs[1], refs[2], refs[3], refs[4:8]
    cosq_ref, sinq_ref, cosk_ref, sink_ref = refs[8:12]
    out_refs = refs[12:16]
    va_ref, kt_ref, dk_acc, dv_acc = refs[16:20]
    step = pl.program_id(0)
    rows = do_refs[0].shape[0]
    chunk = v_ref.shape[0] // WAYS
    per = chunk // rows
    piece = step // per
    lane_k = lax.broadcasted_iota(jnp.int32, (chunk, LANES), 1)
    lane = lax.broadcasted_iota(jnp.int32, (rows, LANES), 1)
    zero = jnp.zeros((), BF)

    @pl.when(step == 0)
    def _():
        ones = jnp.where(lane_k % HEAD_DIM < 3, jnp.ones((), BF), zero)
        for m in range(WAYS):
            some = slice(m * chunk, (m + 1) * chunk)
            v = v_ref[some, :]
            for head in range(2):
                mine = (lane_k < HEAD_DIM) if head == 0 else (lane_k >= HEAD_DIM)
                va_ref[head, some, :] = jnp.where(mine, v, ones)
                own = jnp.where(mine, ka_ref[head, some, :], zero).astype(F32)
                kt_ref[head, :, some] = own.T.astype(BF)
        dk_acc[...] = jnp.zeros_like(dk_acc)
        dv_acc[...] = jnp.zeros_like(dv_acc)

    grad = choose(piece, [r[...] for r in do_refs])
    out = o_ref[...]
    product = grad.astype(F32) * out.astype(F32)
    turned = jnp.zeros((LANES, rows), F32)
    for head in range(2):
        mine = (lane < HEAD_DIM) if head == 0 else (lane >= HEAD_DIM)
        delta = jnp.sum(jnp.where(mine, product, 0.0), axis=-1, keepdims=True)
        high = delta.astype(BF)
        rest = delta - high.astype(F32)
        mid = rest.astype(BF)
        low = (rest - mid.astype(F32)).astype(BF)
        t = lane % HEAD_DIM
        aux = jnp.where(t == 0, -high, jnp.where(t == 1, -mid, jnp.where(t == 2, -low, zero)))
        grad_aug = jnp.where(mine, grad, aux)
        grad_own = jnp.where(mine, grad, zero)
        qa = qa_ref[head]
        q_own = jnp.where(mine, qa, zero)
        for m in range(WAYS):
            some = slice(m * chunk, (m + 1) * chunk)
            prob = jnp.exp(dot_nt(ka_ref[head, some, :], qa))
            back = dot_nt(va_ref[head, some, :], grad_aug)
            score_grad = (prob * back).astype(BF)
            dv_acc[some, :] += dot_nn(prob.astype(BF), grad_own)
            dk_acc[some, :] += dot_nn(score_grad, q_own)
            turned += dot_nn(kt_ref[head, :, some], score_grad)
    dq = turned.T * (HEAD_DIM**-0.5)
    dq = (dq * cosq_ref[...] - swap_halves(dq) * sinq_ref[...]).astype(BF)
    for m in range(WAYS):

        @pl.when(piece == m)
        def _(m=m):
            here = pl.ds(pl.multiple_of((step - m * per) * rows, rows), rows)
            out_refs[m][here, :LANES] = dq

    @pl.when(step == pl.num_programs(0) - 1)
    def _():
        for m in range(WAYS):
            some = slice(m * chunk, (m + 1) * chunk)
            dk = dk_acc[some, :]
            dk = dk * cosk_ref[some, :] - swap_halves(dk) * sink_ref[some, :]
            out_refs[m][:, LANES : 2 * LANES] = dk.astype(BF)
            out_refs[m][:, 2 * LANES :] = dv_acc[some, :].astype(BF)


def attn_bwd_call(scalars, qa, ka, v, grad, o, cosine, sine, pair):
    tokens = v.shape[1]
    chunk = tokens // WAYS
    rows = 256
    per = chunk // rows
    moving = [piece_block(m, rows, per) for m in range(WAYS)]
    block = pl.BlockSpec((rows, LANES), lambda i, s: (i, 0))
    return call(
        attn_bwd_kernel,
        scalars,
        (tokens // rows,),
        [
            pl.BlockSpec((None, 2, rows, LANES), lambda i, s: (pair, 0, i, 0)),
            pl.BlockSpec((None, 2, tokens, LANES), lambda i, s: (pair, 0, 0, 0)),
            pl.BlockSpec((None, tokens, LANES), lambda i, s: (pair, 0, 0)),
            pl.BlockSpec((None, rows, LANES), lambda i, s: (pair, i, 0)),
        ]
        + moving
        + [block, block, full((tokens, LANES)), full((tokens, LANES))],
        [full((chunk, 3 * LANES))] * WAYS,
        [shape_of((chunk, 3 * LANES), BF)] * WAYS,
        [
            pltpu.VMEM((2, tokens, LANES), BF),
            pltpu.VMEM((2, LANES, tokens), BF),
            pltpu.VMEM((tokens, LANES), F32),
            pltpu.VMEM((tokens, LANES), F32),
        ],
        cost(28 * tokens * tokens * LANES, 8),
        "attn_bwd",
    )(qa, ka, v, o, *grad, cosine, sine, cosine, sine)


def own_first(core, values):
    cut = [values[:, at : at + LANES] for at in range(0, values.shape[1], LANES)]
    turned = [cut[i ^ 1] for i in range(len(cut))]
    return jnp.where(core == 0, values, jnp.concatenate(turned, axis=-1))


MESH = pl.DeviceIdType.MESH
UP, DOWN, TO_X, TO_Y, TO_D, CORE_OWN, CORE_X, CORE_Y, CORE_D = range(9)
FROM_Z, FROM_X, FROM_Y, FROM_D = range(4)


class Place:
    def __init__(self):
        self.dp, self.z = lax.axis_index("dp"), lax.axis_index("mp")
        self.core, self.x, self.y = self.dp % 2, (self.dp // 2) % 2, self.dp // 4
        self.at_c = self.dp + 1 - 2 * self.core
        self.at_x = self.dp + 2 - 4 * self.x
        self.at_y = self.dp + 4 - 8 * self.y
        self.at_d = self.at_x + self.at_y - self.dp
        self.group = self.z // 2
        self.far_z = self.z + 2 - 4 * self.group
        self.quarter = self.z + self.core * (self.far_z - self.z)

    @staticmethod
    def mix(q, m):
        return (q + m) % 2 + 2 * ((q // 2 + m // 2) % 2)

    def stays(self, a, b):
        return jnp.logical_and(a == self.dp, b == self.z)

    def attention_of(self, m):
        h = self.mix(self.z, m)
        a, b = self.dp - self.core + (h // 2 + self.core) % 2, 2 * self.core + h % 2
        return a, b, self.stays(a, b)

    def owner_of(self, m):
        a, b = self.dp - self.core + self.group, self.mix(self.quarter, m)
        return a, b, self.stays(a, b)


def remote(src, dst, send, recv, device):
    return pltpu.make_async_remote_copy(
        src_ref=src, dst_ref=dst, send_sem=send, recv_sem=recv,
        device_id=device, device_id_type=MESH,
    )


class Move:
    def __init__(self, src, dst, send, recv, place):
        a, b, self.stays = place
        self.far = lambda: remote(src, dst, send, recv, (a, b))
        self.near = lambda: pltpu.make_async_copy(src, dst, recv)

    def start(self):
        pl.when(self.stays)(lambda: self.near().start())
        pl.when(jnp.logical_not(self.stays))(lambda: self.far().start())

    def wait_recv(self):
        self.far().wait_recv()

    def wait_send(self):
        pl.when(jnp.logical_not(self.stays))(lambda: self.far().wait_send())


def forward_kernel(x_ref, info_ref, gain_ref, qkv_ref, *refs, packs):
    parts, outs, heads_ref = refs[:packs], refs[packs : 2 * packs], refs[2 * packs]
    saved, refs = refs[2 * packs + 1 : 2 * packs + 7], refs[2 * packs + 7 :]
    qa, o, normed, cosine, sine, ka, v, q, qaux, kaux, live, scores = refs[:12]
    kept = Kept((normed, cosine, sine, qa, ka, v, o, q, qaux, kaux, live, scores))
    x_all, w_ref, infos = refs[12:15]
    (
        sends, recvs, cores, locals_, token_send, token_recv, head_send, head_recv,
        q_send, q_recv, save_sem,
    ) = refs[15:]
    dp, z = lax.axis_index("dp"), lax.axis_index("mp")
    core, xb, yb = dp % 2, (dp // 2) % 2, dp // 4
    at_c, at_x, at_y = dp + 1 - 2 * core, dp + 2 - 4 * xb, dp + 4 - 8 * yb
    at_d = at_x + at_y - dp
    group = z // 2
    far_z = z + 2 - 4 * group
    quarter = z + core * (far_z - z)

    def mix(q, m):
        return (q + m) % 2 + 2 * ((q // 2 + m // 2) % 2)

    def attention_of(m):
        h = mix(z, m)
        return dp - core + (h // 2 + core) % 2, 2 * core + h % 2

    def owner_of(m):
        return dp - core + group, mix(quarter, m)

    barrier = pltpu.get_barrier_semaphore()

    def greet(device, when=None):
        def signal():
            pl.semaphore_signal(barrier, inc=1, device_id=device, device_id_type=MESH)

        signal() if when is None else pl.when(when)(signal)

    greet((at_c, z))
    greet((at_x, z))
    greet((at_y, z))
    greet((dp, far_z))
    greet((dp, z + 1), z < WAYS - 1)
    greet((dp, z - 1), z > 0)
    count = 4 + (z < WAYS - 1).astype(jnp.int32) + (z > 0).astype(jnp.int32)
    here, there = [], []
    for m in range(WAYS):
        for of, found in ((attention_of, here), (owner_of, there)):
            a, b = of(m)
            stays = jnp.logical_and(a == dp, b == z)
            found.append((a, b, stays))
            greet((a, b), jnp.logical_not(stays))
            count += 1 - stays.astype(jnp.int32)
    pl.semaphore_wait(barrier, count)

    def remote(src, dst, send, recv, device):
        return pltpu.make_async_remote_copy(
            src_ref=src, dst_ref=dst, send_sem=send, recv_sem=recv,
            device_id=device, device_id_type=MESH,
        )

    def copy(p, kind, s, src=None):
        who = {CORE_X: at_x, CORE_Y: at_y, CORE_D: at_d}.get(kind, dp)
        if kind == TO_D:
            who = jnp.where(s < 2, at_x, at_y)
        slab = outs[p].at[who, s]
        send = sends.at[p, kind, s]
        if kind == UP:
            recv, device = recvs.at[p, FROM_Z, s], (dp, z + 1)
        elif kind == DOWN:
            recv, device = recvs.at[p, FROM_Z, s], (dp, z - 1)
        elif kind == TO_X:
            recv, device = recvs.at[p, FROM_X, s], (at_x, z)
        elif kind == TO_Y:
            recv, device = recvs.at[p, FROM_Y, s], (at_y, z)
        elif kind == TO_D:
            recv, device = recvs.at[p, FROM_D, s], (jnp.where(s < 2, at_y, at_x), z)
        else:
            recv, device = cores.at[p, kind - CORE_OWN, s], (at_c, z)
        return remote(slab if src is None else src, slab, send, recv, device)

    def arrived(p, sem, who, s):
        slab = outs[p].at[who, s]
        remote(slab, slab, sends.at[p, UP, s], sem, (at_c, z)).wait_recv()

    def spread(p, s, src=None):
        copy(p, TO_X, s, src).start()
        copy(p, TO_Y, s, src).start()
        copy(p, CORE_OWN, s, src).start()

    def begin(p):
        src = parts[p]
        spread(p, z, src)
        pltpu.make_async_copy(src, outs[p].at[dp, z], locals_.at[p]).start()

    def begin_line(p):
        src = parts[p]
        pl.when(z < WAYS - 1)(lambda: copy(p, UP, z, src).start())
        pl.when(z > 0)(lambda: copy(p, DOWN, z, src).start())

    def reach(p, hop):
        def one(s):
            arrived(p, recvs.at[p, FROM_Z, s], dp, s)
            spread(p, s)

        pl.when(z >= hop)(lambda: one(z - hop))
        pl.when(z + hop < WAYS)(lambda: one(z + hop))

    def ahead(p, hop):
        pl.when(jnp.logical_and(z >= hop, z < WAYS - 1))(lambda: copy(p, UP, z - hop).start())
        pl.when(jnp.logical_and(z + hop < WAYS, z > 0))(lambda: copy(p, DOWN, z + hop).start())

    def line(p, hop):
        reach(p, hop)
        if hop < WAYS - 1:
            ahead(p, hop)

    def plane(p, hop):
        def one(s):
            arrived(p, recvs.at[p, FROM_X, s], at_x, s)
            copy(p, CORE_X, s).start()
            pl.when(s < 2)(lambda: copy(p, TO_D, s).start())
            arrived(p, recvs.at[p, FROM_Y, s], at_y, s)
            copy(p, CORE_Y, s).start()
            pl.when(s >= 2)(lambda: copy(p, TO_D, s).start())

        if hop == 0:
            one(z)
        else:
            pl.when(z >= hop)(lambda: one(z - hop))
            pl.when(z + hop < WAYS)(lambda: one(z + hop))

    def corner(p, hop):
        def one(s):
            arrived(p, recvs.at[p, FROM_D, s], at_d, s)
            copy(p, CORE_D, s).start()

        if hop == 0:
            one(z)
        else:
            pl.when(z >= hop)(lambda: one(z - hop))
            pl.when(z + hop < WAYS)(lambda: one(z + hop))

    def from_core(p):
        for s in range(WAYS):
            for kind in range(4):
                twin = (at_c, at_x + at_c - dp, at_y + at_c - dp, at_d + at_c - dp)[kind]
                arrived(p, cores.at[p, kind, s], twin, s)
        pltpu.make_async_copy(parts[p], outs[p].at[dp, z], locals_.at[p]).wait()

    def finish(p):
        for s in range(WAYS):
            pl.when(jnp.logical_and(z < WAYS - 1, s <= z))(lambda s=s: copy(p, UP, s).wait_send())
            pl.when(jnp.logical_and(z > 0, s >= z))(lambda s=s: copy(p, DOWN, s).wait_send())
            for kind in range(TO_X, CORE_D + 1):
                copy(p, kind, s).wait_send()

    def token(m):
        to_dp, to_z, stays = here[m]

        def far():
            return remote(x_ref, x_all.at[m], token_send.at[m], token_recv.at[m], (to_dp, to_z))

        def near():
            return pltpu.make_async_copy(x_ref, x_all.at[m], token_recv.at[m])

        return far, near, stays

    def pass_on(m):
        return remote(
            x_all.at[m], x_all.at[m + 2], token_send.at[m + 2], token_recv.at[m + 2], (at_c, z)
        )

    def swap_info():
        return remote(info_ref, infos.at[1], token_send.at[WAYS], token_recv.at[WAYS], (at_c, z))

    def own_info():
        return pltpu.make_async_copy(info_ref, infos.at[0], locals_.at[packs])

    def q_copy(kind, i=0, src=None):
        who = {"z": dp, "x": dp, "y": dp, "c": dp, "cx": at_x, "cy": at_y, "cd": at_d}.get(kind)
        if kind == "d":
            who = at_x if i == 0 else at_y
        device = {"z": (dp, far_z), "x": (at_x, z), "y": (at_y, z)}.get(kind, (at_c, z))
        if kind == "d":
            device = (at_y, z) if i == 0 else (at_x, z)
        slot = {"z": 0, "x": 1, "y": 3, "d": 5, "c": 7, "cx": 8, "cy": 9, "cd": 10}[kind]
        if kind in ("x", "y", "d"):
            slot += i
        if kind == "z":
            i = 1
        if kind[0] == "c":
            i = 1 - core
        dst = w_ref.at[i, who]
        return remote(dst if src is None else src, dst, q_send.at[slot], q_recv.at[slot], device)

    def q_arrived(kind, i=0):
        q_copy(kind, i).wait_recv()

    def own_q():
        return pltpu.make_async_copy(qkv_ref, w_ref.at[0, dp], locals_.at[packs + 1])

    q_kinds = [("z", 0), ("x", 0), ("x", 1), ("y", 0), ("y", 1), ("d", 0), ("d", 1)]
    q_kinds += [("c", 0), ("cx", 0), ("cy", 0), ("cd", 0)]

    keeps = [w_ref.at[core], normed, cosine, sine, ka, v]

    def save(i):
        return pltpu.make_async_copy(keeps[i], saved[i], save_sem.at[i])

    rows = x_ref.shape[0]

    def head(pair, m, owner):
        src = kept.o.at[pair, pl.ds(m * rows, rows)]
        dst = heads_ref.at[m, pair]
        to_dp, to_z, stays = owner

        def far():
            return remote(
                src, dst, head_send.at[m, pair], head_recv.at[m, pair], (to_dp, to_z)
            )

        def near():
            return pltpu.make_async_copy(src, dst, head_recv.at[m, pair])

        return far, near, stays

    def start(item):
        far, near, stays = item
        pl.when(stays)(lambda: near().start())
        pl.when(jnp.logical_not(stays))(lambda: far().start())

    def end_send(item):
        far, near, stays = item
        pl.when(jnp.logical_not(stays))(lambda: far().wait_send())

    q_copy("z", 0, qkv_ref).start()
    q_copy("x", 0, qkv_ref).start()
    q_copy("y", 0, qkv_ref).start()
    own_q().start()
    for m in range(2):
        start(token(m))
    swap_info().start()
    own_info().start()
    for p in range(packs):
        begin(p)
        begin_line(p)
    own_info().wait()
    swap_info().wait()
    own_q().wait()
    q_arrived("x", 0)
    q_copy("d", 0).start()
    q_arrived("z")
    q_copy("x", 1).start()
    q_copy("y", 1).start()
    away = (group + core) % 2
    for m in range(WAYS):
        table_piece(m, infos[away, mix(quarter, m)], kept)
    q_arrived("y", 0)
    q_copy("c").start()
    plane(0, 0)
    q_arrived("x", 1)
    q_copy("cx").start()
    q_arrived("y", 1)
    q_copy("d", 1).start()
    q_copy("cy").start()
    plane(1, 0)
    q_arrived("d", 0)
    q_arrived("d", 1)
    q_copy("cd").start()
    reach(0, 1)
    corner(0, 0)
    reach(1, 1)
    corner(1, 0)
    for kind in ("c", "cx", "cy", "cd"):
        q_arrived(kind)
    save(0).start()
    save(2).start()
    save(3).start()
    for m in range(2):
        token(m)[0]().wait_recv()
        pass_on(m).start()
    for p in range(packs):
        ahead(p, 1)
        plane(p, 1)
    for m in range(WAYS):
        if m >= 2:
            pass_on(m - 2).wait_recv()
        weight = jnp.concatenate([w_ref[core, d] for d in range(w_ref.shape[1])], axis=-1)
        qkv_piece(m, x_all[m], gain_ref[...], weight, kept)
        if m == 2:
            line(0, 2)
            corner(0, 1)
    save(1).start()
    save(4).start()
    save(5).start()

    events = {
        1: [(line, 1, 2), (corner, 1, 1)],
        4: [(line, 0, 3), (plane, 0, 2)],
        7: [(line, 1, 3), (plane, 1, 2)],
        9: [(corner, 0, 2)],
        11: [(plane, 0, 3)],
        13: [(corner, 1, 2)],
    }
    steps = kept.v.shape[1] // STEP
    pairs = kept.v.shape[0]
    per = steps // WAYS

    def body(i, carry):
        for at, todo in events.items():

            @pl.when(i == at)
            def _(todo=todo):
                for what, p, hop in todo:
                    what(p, hop)

        pair = i // steps
        step = i % steps
        attn_step(pair, step, kept)
        m = step // per

        @pl.when(step % per == per - 1)
        def _():
            a, b = dp - core + group, mix(quarter, m)
            start(head(pair, m, (a, b, jnp.logical_and(a == dp, b == z))))

        return carry

    lax.fori_loop(0, pairs * steps, body, 0)
    plane(1, 3)
    corner(0, 3)
    corner(1, 3)
    for p in range(packs):
        from_core(p)
    for m in range(WAYS):
        for pair in range(pairs):
            head(pair, m, there[m])[0]().wait_recv()
            end_send(head(pair, m, there[m]))
    for m in range(2):
        pass_on(m).wait_send()
        end_send(token(m))
    for p in range(packs):
        finish(p)
    for kind, i in q_kinds:
        q_copy(kind, i).wait_send()
    for i in range(len(keeps)):
        save(i).wait()


def forward_call(x, info, gain, qkv_part, parts, dps, pairs):
    rows, model = x.shape
    packs = len(parts)
    anywhere = pl.BlockSpec(memory_space=pl.ANY)
    vmem = pl.BlockSpec(memory_space=pltpu.VMEM)
    outs, scratch = kept_shapes(WAYS * rows, model, pairs)
    normed, cosine, sine, qa, ka, v, o = outs
    hold = [normed, cosine, sine, ka, v]
    weight = (dps,) + qkv_part.shape
    out = pl.pallas_call(
        functools.partial(forward_kernel, packs=packs),
        in_specs=[anywhere, anywhere, vmem] + [anywhere] * (1 + packs),
        out_specs=[anywhere] * (packs + 7) + [vmem] * 2,
        out_shape=[shape_of((dps, WAYS) + part.shape, BF) for part in parts]
        + [shape_of((WAYS, pairs, rows, LANES), BF), shape_of(weight, BF)]
        + hold
        + [qa, o],
        scratch_shapes=[pltpu.VMEM(h.shape, h.dtype) for h in hold]
        + scratch
        + [
            pltpu.VMEM((WAYS, rows, model), BF),
            pltpu.VMEM((2,) + weight, BF),
            pltpu.VMEM((2, WAYS, rows, LANES), F32),
            pltpu.SemaphoreType.DMA((packs, 9, WAYS)),
            pltpu.SemaphoreType.DMA((packs, 4, WAYS)),
            pltpu.SemaphoreType.DMA((packs, 4, WAYS)),
            pltpu.SemaphoreType.DMA((packs + 2,)),
            pltpu.SemaphoreType.DMA((WAYS + 1,)),
            pltpu.SemaphoreType.DMA((WAYS + 1,)),
            pltpu.SemaphoreType.DMA((WAYS, pairs)),
            pltpu.SemaphoreType.DMA((WAYS, pairs)),
            pltpu.SemaphoreType.DMA((11,)),
            pltpu.SemaphoreType.DMA((11,)),
            pltpu.SemaphoreType.DMA((6,)),
        ],
        compiler_params=pltpu.CompilerParams(
            collective_id=0, has_side_effects=True, vmem_limit_bytes=VMEM_LIMIT
        ),
        name="forward",
    )(x, info, gain, qkv_part, *parts)
    packs_out, out = out[:packs], out[packs:]
    heads, weight, normed, cosine, sine, ka, v, qa, o = out
    return packs_out, heads, weight, (normed, cosine, sine, qa, ka, v, o)


def attn_back_begin(pair, k):
    chunk = 512
    lane = lax.broadcasted_iota(jnp.int32, (chunk, LANES), 1)
    zero = jnp.zeros((), BF)
    ones = jnp.where(lane % HEAD_DIM < 3, jnp.ones((), BF), zero)
    for at in range(0, k.dk.shape[0], chunk):
        some = slice(at, at + chunk)
        v = k.v[pair, some, :]
        for head in range(2):
            mine = (lane < HEAD_DIM) if head == 0 else (lane >= HEAD_DIM)
            k.va[head, some, :] = jnp.where(mine, v, ones)
            own = jnp.where(mine, k.ka[pair, head, some, :], zero).astype(F32)
            k.kt[head, :, some] = own.T.astype(BF)
    k.dk[...] = jnp.zeros_like(k.dk)
    k.dv[...] = jnp.zeros_like(k.dv)


def attn_back_step(pair, step, grad, k):
    chunk = 512
    here = pl.ds(pl.multiple_of(step * STEP, STEP), STEP)
    lane = lax.broadcasted_iota(jnp.int32, (STEP, LANES), 1)
    zero = jnp.zeros((), BF)
    t = lane % HEAD_DIM
    product = grad.astype(F32) * k.o[pair, here, :].astype(F32)
    turned = jnp.zeros((LANES, STEP), F32)
    for head in range(2):
        mine = (lane < HEAD_DIM) if head == 0 else (lane >= HEAD_DIM)
        delta = jnp.sum(jnp.where(mine, product, 0.0), axis=-1, keepdims=True)
        high = delta.astype(BF)
        rest = delta - high.astype(F32)
        mid = rest.astype(BF)
        low = (rest - mid.astype(F32)).astype(BF)
        aux = jnp.where(t == 0, -high, jnp.where(t == 1, -mid, jnp.where(t == 2, -low, zero)))
        grad_aug = jnp.where(mine, grad, aux)
        grad_own = jnp.where(mine, grad, zero)
        qa = k.qa[pair, head, here, :]
        q_own = jnp.where(mine, qa, zero)
        for at in range(0, k.dk.shape[0], chunk):
            some = slice(at, at + chunk)
            prob = jnp.exp(dot_nt(k.ka[pair, head, some, :], qa))
            back = dot_nt(k.va[head, some, :], grad_aug)
            score_grad = (prob * back).astype(BF)
            k.dv[some, :] += dot_nn(prob.astype(BF), grad_own)
            k.dk[some, :] += dot_nn(score_grad, q_own)
            turned += dot_nn(k.kt[head, :, some], score_grad)
    dq = turned.T * (HEAD_DIM**-0.5)
    dq = dq * k.cosine[here, :] - swap_halves(dq) * k.sine[here, :]
    k.low[pair, 0, here, :] = dq.astype(BF)


def attn_back_end(pair, k):
    chunk = 512
    for at in range(0, k.dk.shape[0], chunk):
        some = slice(at, at + chunk)
        dk = k.dk[some, :]
        dk = dk * k.cosine[some, :] - swap_halves(dk) * k.sine[some, :]
        k.low[pair, 1, some, :] = dk.astype(BF)
        k.low[pair, 2, some, :] = k.dv[some, :].astype(BF)


def low_piece(pair, m, k, rows):
    some = slice(m * rows, (m + 1) * rows)
    return jnp.concatenate([k.low[pair, c, some, :] for c in range(3)], axis=-1)


class Back:
    names = ("qa", "ka", "v", "o", "cosine", "sine", "low", "va", "kt", "dk", "dv")

    def __init__(self, refs):
        for name, ref in zip(self.names, refs):
            setattr(self, name, ref)


class Chain:
    def __init__(self, p, source, kept, r1, r2, rz, send, recv):
        self.p, self.source, self.kept = p, source, kept
        self.r1, self.r2, self.rz, self.send, self.recv = r1, r2, rz, send, recv

    def slab(self, q, slot, away):
        x, y = self.p.x, self.p.y
        if q < 2:
            return (y if slot else 1 - y) * 2 + (1 - x if away else x)
        return (1 - y if away else y) * 2 + (x if slot else 1 - x)

    def near(self, q, second=False):
        p = self.p
        return (p.at_x, p.z) if (q < 2) != second else (p.at_y, p.z)

    def stage1(self, q, slot):
        src = self.source(q, self.slab(q, slot, True))
        at = q * 2 + slot
        return remote(src, self.r1.at[q, slot], self.send.at[at], self.recv.at[at], self.near(q))

    def stage2(self, q):
        at = 8 + q
        src = self.kept(q, 0, self.slab(q, 0, False))
        return remote(src, self.r2.at[q], self.send.at[at], self.recv.at[at], self.near(q, True))

    def first(self, q):
        self.stage1(q, 0).start()
        self.stage1(q, 1).start()

    def second(self, q, done=False):
        if not done:
            self.stage1(q, 0).wait_recv()
        ref = self.kept(q, 0, self.slab(q, 0, False))
        ref[...] += self.r1[q, 0]
        self.stage2(q).start()
        if not done:
            self.stage1(q, 1).wait_recv()
        self.own(q)[...] += self.r1[q, 1]

    def own(self, q):
        return self.kept(q, 1, self.slab(q, 1, False))

    def third(self, q):
        self.stage2(q).wait_recv()
        self.own(q)[...] += self.r2[q]

    def lined(self, q, down):
        z = self.p.z
        at = q if down else q + 1
        return remote(
            self.own(q), self.rz.at[at], self.send.at[12 + q], self.recv.at[12 + at],
            (self.p.dp, z - 1 if down else z + 1),
        )

    def line(self, hop, quarters):
        z = self.p.z
        for q in quarters:
            if q < WAYS - hop:

                @pl.when(z == WAYS - hop)
                def _(q=q):
                    if hop > 1:
                        self.lined(q, True).wait_recv()
                        self.own(q)[...] += self.rz[q]
                    self.lined(q, True).start()

            if q > hop - 1:

                @pl.when(z == hop - 1)
                def _(q=q):
                    if hop > 1:
                        self.lined(q, False).wait_recv()
                        self.own(q)[...] += self.rz[q + 1]
                    self.lined(q, False).start()

    def last(self, out_ref):
        z = self.p.z
        for q in range(WAYS):

            @pl.when(z == q)
            def _(q=q):
                total = self.own(q)[...].astype(F32)
                if q < WAYS - 1:
                    self.lined(q, True).wait_recv()
                    total += self.rz[q].astype(F32)
                if q > 0:
                    self.lined(q, False).wait_recv()
                    total += self.rz[q + 1].astype(F32)
                out_ref[...] = total

    def finish(self, done=()):
        z = self.p.z
        for q in range(WAYS):
            if q not in done:
                self.stage1(q, 0).wait_send()
                self.stage1(q, 1).wait_send()
            self.stage2(q).wait_send()
            pl.when(q < z)(lambda q=q: self.lined(q, True).wait_send())
            pl.when(q > z)(lambda q=q: self.lined(q, False).wait_send())


DONE = (0, 2)


def turn_of(step):
    return 2 * (step % 2) + step // 2


def mlp_kernel(
    s_ref, heads_ref, x_ref, g_ref, gain_ref, live_ref, pack_ref, wa_ref, wb_ref,
    output_ref, mgrad_ref, low_ref, small_ref, hg_ref, sum_ref, r1_ref, *scratch, swap
):
    w_attn, middle, inner, mlp, back, grads, load_sem = scratch[:7]
    step = pl.program_id(0)
    steps = pl.num_programs(0)
    quarter = turn_of(step)
    units = wb_ref.shape[2] // 2
    skip = wa_ref.shape[2] - units
    z = s_ref[0]
    core = s_ref[1]
    load = pltpu.make_async_copy(pack_ref.at[:, :, :skip], w_attn, load_sem.at[0])
    if swap:
        away, got, send_sem, recv_sem, f_send, f_recv = scratch[7:]
        p = Place()
        core = p.core
        other = (p.at_c, p.z)
        chain = Chain(
            p, lambda q, i: grads.at[q, i], None, None, None, None, f_send, f_recv
        )

        @pl.when(step == 0)
        def _():
            barrier = pltpu.get_barrier_semaphore()
            for device in (other, (p.at_x, p.z), (p.at_y, p.z)):
                pl.semaphore_signal(barrier, inc=1, device_id=device, device_id_type=MESH)
            pl.semaphore_wait(barrier, 3)

        def give(i):
            return remote(
                away.at[i % 2], got.at[i % 2], send_sem.at[i % 2], recv_sem.at[i % 2], other
            )

        def stage1(i, slot):
            q = DONE[i]
            at = i * 2 + slot
            return remote(
                grads.at[q, chain.slab(q, slot, True)], r1_ref.at[i, slot],
                f_send.at[at], f_recv.at[at], chain.near(q),
            )

        def take(i):
            q = turn_of(i)
            give(i).wait_recv()
            for d in range(grads.shape[1]):
                grads[q, d] += got[i % 2, d]
            pltpu.make_async_copy(grads.at[q], sum_ref.at[q], load_sem.at[1 + i]).start()
            for j in range(len(DONE)):

                @pl.when(i == j)
                def _(j=j):
                    stage1(j, 0).start()
                    stage1(j, 1).start()

    @pl.when(step == 0)
    def _():
        load.start()
        tokens = x_ref[...].astype(F32)
        attn_out = jnp.zeros(tokens.shape, F32)
        load.wait()
        for m in range(WAYS):
            o = jnp.concatenate([heads_ref[m, 0], heads_ref[m, 1]], axis=-1)
            attn_out += dot_nn(o, side_by_side(w_attn, z ^ m))
        total = tokens + attn_out
        vhat, unused = norm_stats(total)
        middle[...] = total
        inner[...] = (vhat * gain_ref[...]).astype(BF)
        live = live_ref[...]
        lane = lax.broadcasted_iota(jnp.int32, (1, tokens.shape[1]), 1)
        sums = jnp.where(lane == 4, jnp.sum(live), 0.0)
        for i, values in enumerate((tokens, attn_out, total)):
            sums = jnp.where(lane == i, jnp.sum(live * values * values), sums)
        small_ref[...] = jnp.zeros_like(small_ref)
        small_ref[2:3, :] = sums

    w_act = side_by_side(wa_ref, 0, slice(skip, skip + units))
    w_lin = side_by_side(wb_ref, 0, slice(0, units))
    w_out = side_by_side(wb_ref, 0, slice(units, 2 * units))
    x = inner[...]
    grad = g_ref[...]
    act_in = dot_nt(w_act, x)
    linear = dot_nt(w_lin, x)
    hidden_grad = dot_nt(w_out, grad)
    cdf = 0.5 * (1.0 + lax.erf(act_in * (2.0**-0.5)))
    act = act_in * cdf
    slope = cdf + act_in * jnp.exp(-0.5 * act_in * act_in) * ((2.0 * math.pi) ** -0.5)
    hidden = (act * linear).astype(BF)
    d_act = (hidden_grad * linear * slope).astype(BF)
    d_lin = (hidden_grad * act).astype(BF)
    if swap:
        pl.when(step >= 1)(lambda: take(step - 1))
        pl.when(step >= 2)(lambda: give(step - 2).wait_send())
    x_mine = own_first(core, x)
    g_mine = own_first(core, grad)
    pieces = (dot_nn(d_act, x_mine), dot_nn(d_lin, x_mine), dot_nn(hidden, g_mine))
    for part, value in enumerate(pieces):
        some = slice(part * units, (part + 1) * units)
        value = value.astype(BF)
        for d in range(value.shape[1] // LANES):
            slab = value[:, d * LANES : (d + 1) * LANES]
            if not swap:
                sum_ref[quarter, d // 2, d % 2, some] = slab
            elif d % 2:
                away[step % 2, d // 2, some] = slab
            else:
                grads[quarter, d // 2, some] = slab
    if swap:
        give(step).start()
    more_mlp = dot_tn(hidden, w_out)
    more_back = dot_tn(d_act, w_act) + dot_tn(d_lin, w_lin)

    @pl.when(step == 0)
    def _():
        mlp[...] = more_mlp
        back[...] = more_back

    @pl.when(step > 0)
    def _():
        mlp[...] += more_mlp
        back[...] += more_back

    @pl.when(step == steps - 1)
    def _():
        if swap:
            take(step)
        vhat, scale = norm_stats(middle[...])
        into = back[...]
        middle_grad = g_ref[...].astype(F32) + norm_back(vhat, scale, gain_ref[...], into)
        low = middle_grad.astype(BF)
        for m in range(WAYS):
            hg = dot_nt(low, side_by_side(w_attn, z ^ m)).astype(BF)
            hg_ref[m, 0] = hg[:, :LANES]
            hg_ref[m, 1] = hg[:, LANES:]
        mgrad_ref[...] = middle_grad
        low_ref[...] = low
        out = mlp[...]
        output_ref[...] = (middle[...] + out).astype(BF)
        lane = lax.broadcasted_iota(jnp.int32, (1, out.shape[1]), 1)
        square = jnp.sum(live_ref[...] * out * out)
        small_ref[2:3, :] = jnp.where(lane == 3, square, small_ref[2:3, :])
        small_ref[1:2, :] = jnp.sum(into * vhat, axis=0, keepdims=True)
        if swap:
            give(step - 1).wait_send()
            give(step).wait_send()
            for i in range(WAYS):
                q = turn_of(i)
                pltpu.make_async_copy(grads.at[q], sum_ref.at[q], load_sem.at[1 + i]).wait()
            for i in range(len(DONE)):
                for slot in range(2):
                    stage1(i, slot).wait()


def mlp_call(scalars, heads, x, grad, gain, live, pack_a, pack_b, swap):
    tokens, model = x.shape
    wide, quarters, depth_a, unused = pack_a.shape
    units = pack_b.shape[2] // 2
    depth = model // WAYS
    out = (quarters, wide // 2) + (() if swap else (2,)) + (3 * units, LANES)
    whole = pl.BlockSpec(memory_space=pltpu.VMEM)
    anywhere = pl.BlockSpec(memory_space=pl.ANY)
    weight = lambda rows: pl.BlockSpec((wide, 1, rows, LANES), lambda i, s: (0, turn_of(i), 0, 0))
    sems = lambda *shape: pltpu.SemaphoreType.DMA(shape)
    scratch = [
        pltpu.VMEM((wide, quarters, depth, LANES), BF),
        pltpu.VMEM((tokens, model), F32),
        pltpu.VMEM((tokens, model), BF),
        pltpu.VMEM((tokens, model), F32),
        pltpu.VMEM((tokens, model), F32),
        pltpu.VMEM(out if swap else (8, LANES), BF),
        sems(1 + WAYS),
    ]
    if swap:
        scratch += [pltpu.VMEM((2,) + out[1:], BF)] * 2 + [sems(2), sems(2), sems(6), sems(6)]
    r1 = (len(DONE), 2, 3 * units, LANES) if swap else (8, LANES)
    spec = pltpu.PrefetchScalarGridSpec(
        num_scalar_prefetch=1,
        grid=(quarters,),
        in_specs=[whole] * 5 + [anywhere, weight(depth_a), weight(2 * units)],
        out_specs=[whole] * 5 + [anywhere if swap else whole, anywhere],
        scratch_shapes=scratch,
    )
    extra = dict(collective_id=1, has_side_effects=True) if swap else {}
    return pl.pallas_call(
        functools.partial(mlp_kernel, swap=swap),
        grid_spec=spec,
        out_shape=[
            shape_of((tokens, model), BF),
            shape_of((tokens, model), F32),
            shape_of((tokens, model), BF),
            shape_of((8, model), F32),
            shape_of((WAYS, depth // LANES, tokens, LANES), BF),
            shape_of(out, BF),
            shape_of(r1, BF),
        ],
        compiler_params=pltpu.CompilerParams(vmem_limit_bytes=62 * 1024 * 1024, **extra),
        cost_estimate=cost(22 * tokens * model * units * quarters, 40),
        name="mlp",
    )(scalars, heads, x, grad, gain, live, pack_a, pack_a, pack_b)


def backward_kernel(
    hg_ref, sum_ref, r1_ref, normed_ref, w_ref, x_ref, mgrad_ref, low_ref, heads_ref,
    qa, ka, v, o, cosine, sine, gain_ref, small_ref,
    grad_ref, ffn_ref, attn_ref, qkv_ref, total_ref,
    do_ref, low, va, kt, dk, dv, normed, weight, x_in, mgrad,
    f_kept0, f_r10, f_r20, f_rz0, f_kept1, f_r11, f_r21, f_rz1,
    a_sum, a_got, a_r1, a_r2, a_rz,
    q_sum, q_rx, q_ry, q_rz, g_core, g_here, s_own, s_dp, s_mp,
    load_sem, do_send, do_recv, f_send, f_recv, a_send, a_recv, c_send, c_recv,
    q_send, q_recv, g_send, g_recv, s_send, s_recv,
):
    p = Place()
    dp, z, core = p.dp, p.z, p.core
    rows = x_ref.shape[0]
    pairs = v.shape[0]
    k = Back((qa, ka, v, o, cosine, sine, low, va, kt, dk, dv))

    def qkv_to(turn):
        a, b = dp - core + (p.group + turn) % 2, p.quarter
        return a, b, p.stays(a, b)

    def qkv_from(g):
        a, b = dp - core + (z // 2 + g) % 2, 2 * g + z % 2
        return a, b, p.stays(a, b)

    def other_dp(turn):
        return (dp + turn) % 8, z

    def other_mp(turn):
        return dp, (z + turn) % WAYS

    barrier = pltpu.get_barrier_semaphore()
    count = jnp.int32(0)

    def greet(device, skip=None):
        def signal():
            pl.semaphore_signal(barrier, inc=1, device_id=device, device_id_type=MESH)

        if skip is None:
            signal()
            return 1
        pl.when(jnp.logical_not(skip))(signal)
        return 1 - skip.astype(jnp.int32)

    for turn in range(1, 8):
        count += greet(other_dp(turn))
    for turn in range(1, WAYS):
        count += greet(other_mp(turn))
    for m in range(WAYS):
        for a, b, stays in (p.attention_of(m), p.owner_of(m)):
            count += greet((a, b), stays)
    for i in range(2):
        for a, b, stays in (qkv_to(i), qkv_from(i)):
            count += greet((a, b), stays)
    pl.semaphore_wait(barrier, count)

    def head_grad(m, pair, place):
        return Move(
            hg_ref.at[m, pair], do_ref.at[m, pair], do_send.at[m, pair], do_recv.at[m, pair], place
        )

    for pair in range(pairs):
        for m in range(WAYS):
            head_grad(m, pair, p.attention_of(m)).start()

    def half(h):
        kept, r1, r2, rz = ((f_kept0, f_r10, f_r20, f_rz0), (f_kept1, f_r11, f_r21, f_rz1))[h]
        some = pl.ds(h * f_kept0.shape[2], kept.shape[2])
        return Chain(
            p, lambda q, i: sum_ref.at[q, i, some], lambda q, slot, i: kept.at[q, slot],
            r1, r2, rz, f_send.at[h], f_recv.at[h],
        )

    ffn = [half(0), half(1)]
    loads = []

    def load(src, dst):
        copy = pltpu.make_async_copy(src, dst, load_sem.at[len(loads)])
        copy.start()
        loads.append(copy)
        return copy

    def fetch(h, q):
        kept, r1 = (f_kept0, f_r10) if h == 0 else (f_kept1, f_r11)
        some = pl.ds(h * f_kept0.shape[2], kept.shape[2])
        copies = []
        for slot in range(2):
            copies.append(load(sum_ref.at[q, ffn[h].slab(q, slot, False), some], kept.at[q, slot]))
        if q in DONE:
            copies.append(load(r1_ref.at[DONE.index(q), :, some], r1.at[q]))
        return copies

    fetched = {(h, q): fetch(h, q) for q in (0, 2, 1, 3) for h in range(2)}

    def second(h, q):
        for copy in fetched[h, q]:
            copy.wait()
        ffn[h].second(q, q in DONE)

    def third(h, *quarters):
        for q in quarters:
            ffn[h].third(q)

    def line(h, hop, *quarters):
        ffn[h].line(hop, quarters)

    for h in range(2):
        second(h, 0)
        second(h, 2)
        ffn[h].first(1)
        ffn[h].first(3)
    late = [load(normed_ref, normed), load(w_ref, weight), load(x_ref, x_in)]
    late.append(load(mgrad_ref, mgrad))

    low_here = own_first(core, low_ref[...])
    for m in range(WAYS):
        mixed = jnp.concatenate([heads_ref[m, 0], heads_ref[m, 1]], axis=-1)
        value = dot_tn(mixed, low_here).astype(BF)
        h = p.mix(z, m)
        for d in range(value.shape[1] // LANES):
            a_sum[d % 2, h, d // 2] = value[:, d * LANES : (d + 1) * LANES]
    swap = remote(a_sum.at[1], a_got, c_send.at[0], c_recv.at[0], (p.at_c, z))
    swap.start()
    attn_back_begin(0, k)
    swap.wait()
    for q in range(WAYS):
        a_sum[0, q] += a_got[q]
    attn = Chain(
        p, lambda q, i: a_sum.at[0, q, i], lambda q, slot, i: a_sum.at[0, q, i],
        a_r1, a_r2, a_rz, a_send, a_recv,
    )
    for q in range(WAYS):
        attn.first(q)

    def qkv_x(pair, yy):
        at = (p.y if yy else 1 - p.y) * 4 + (1 - p.x) * 2
        return remote(
            q_sum.at[pair, pl.ds(at, 2)], q_rx.at[pair, yy],
            q_send.at[pair, yy], q_recv.at[pair, yy], (p.at_x, z),
        )

    def qkv_y(pair):
        at = (1 - p.y) * 4 + p.x * 2
        return remote(
            q_sum.at[pair, pl.ds(at, 2)], q_ry.at[pair],
            q_send.at[pair, 2], q_recv.at[pair, 2], (p.at_y, z),
        )

    def qkv_z(pair, turn, g, place):
        at = p.y * 4 + p.x * 2 + (p.group + turn) % 2
        return Move(
            q_sum.at[pair, at], q_rz.at[pair, g],
            q_send.at[pair, 3 + turn], q_recv.at[pair, 3 + g], place,
        )

    def qkv_first(pair):
        total = None
        for m in range(WAYS):
            part = dot_tn(low_piece(pair, m, k, rows), normed[m * rows : (m + 1) * rows, :])
            total = part if total is None else total + part
        value = total.astype(BF)
        for d in range(value.shape[1] // LANES):
            q_sum[pair, d] = value[:, d * LANES : (d + 1) * LANES]
        qkv_x(pair, 0).start()
        qkv_x(pair, 1).start()

    def qkv_second(pair):
        qkv_x(pair, 0).wait_recv()
        at = (1 - p.y) * 4 + p.x * 2
        for i in range(2):
            q_sum[pair, at + i] += q_rx[pair, 0, i]
        qkv_y(pair).start()
        qkv_x(pair, 1).wait_recv()
        at = p.y * 4 + p.x * 2
        for i in range(2):
            q_sum[pair, at + i] += q_rx[pair, 1, i]

    def qkv_third(pair):
        qkv_y(pair).wait_recv()
        at = p.y * 4 + p.x * 2
        for i in range(2):
            q_sum[pair, at + i] += q_ry[pair, i]
        for turn in range(2):
            qkv_z(pair, turn, p.group, qkv_to(turn)).start()

    def pair_end():
        attn_back_end(0, k)
        attn_back_begin(1, k)
        for copy in late:
            copy.wait()
        qkv_first(0)

    every = range(WAYS)
    events = {
        1: [(third, 0, 0, 2), (line, 0, 1, 0, 2)],
        2: [(third, 1, 0, 2), (line, 1, 1, 0, 2)],
        3: [(line, 0, 2, 0, 2)],
        4: [(attn.second, q) for q in every],
        5: [(second, 0, 1), (second, 0, 3), (line, 1, 2, 0, 2)],
        6: [(line, 0, 3, 0, 2)] + [(attn.third, q) for q in every] + [(attn.line, 1, every)],
        7: [(line, 1, 3, 0, 2), (attn.line, 2, every)],
        8: [(second, 1, 1), (second, 1, 3), (attn.line, 3, every), (pair_end,)],
        9: [(third, 0, 1, 3), (line, 0, 1, 1, 3)],
        10: [(qkv_second, 0)],
        11: [(line, 0, 2, 1, 3), (third, 1, 1, 3), (line, 1, 1, 1, 3)],
        12: [(qkv_third, 0)],
        13: [(line, 0, 3, 1, 3), (line, 1, 2, 1, 3)],
        15: [(line, 1, 3, 1, 3)],
    }
    steps = v.shape[1] // STEP
    per = rows // STEP

    def body(i, carry):
        for at, todo in events.items():

            @pl.when(i == at)
            def _(todo=todo):
                for what, *args in todo:
                    what(*args)

        pair, step = i // steps, i % steps
        m = step // per

        @pl.when(step % per == 0)
        def _():
            head_grad(m, pair, p.owner_of(0)).wait_recv()

        at = pl.multiple_of((step - m * per) * STEP, STEP)
        attn_back_step(pair, step, do_ref[m, pair, pl.ds(at, STEP), :], k)
        return carry

    lax.fori_loop(0, pairs * steps, body, 0)
    attn_back_end(1, k)

    joined = jnp.concatenate([weight[d] for d in range(weight.shape[0])], axis=-1)

    def piece_grad(m):
        out = None
        for pair in range(pairs):
            at = pair * 3 * LANES
            part = dot_nn(low_piece(pair, m, k, rows), joined[at : at + 3 * LANES, :])
            out = part if out is None else out + part
        return out.astype(BF)

    def to_core(m):
        return remote(
            normed.at[pl.ds((m + 2) * rows, rows)], g_core.at[m],
            g_send.at[m], g_recv.at[m], (p.at_c, z),
        )

    def to_owner(m, place):
        return Move(
            normed.at[pl.ds(m * rows, rows)], g_here.at[m], g_send.at[2 + m], g_recv.at[2 + m], place
        )

    qkv_first(1)
    for m in range(2):
        normed[(m + 2) * rows : (m + 3) * rows, :] = piece_grad(m + 2)
        to_core(m).start()
    for m in range(2):
        own = piece_grad(m)
        to_core(m).wait_recv()
        normed[m * rows : (m + 1) * rows, :] = own + g_core[m]
        to_owner(m, p.owner_of(m)).start()
    qkv_second(1)
    attn.last(attn_ref)
    qkv_third(1)
    cut = f_kept0.shape[2]
    ffn[0].last(ffn_ref.at[:cut])
    ffn[1].last(ffn_ref.at[cut:])
    vhat, scale = norm_stats(x_in[...].astype(F32))
    for pair in range(pairs):
        for g in range(2):
            qkv_z(pair, 0, g, qkv_from(g)).wait_recv()
        qkv_ref[pair] = q_rz[pair, 0].astype(F32) + q_rz[pair, 1].astype(F32)
    for m in range(2):
        to_owner(m, p.attention_of(m)).wait_recv()
    normed_grad = g_here[0].astype(F32) + g_here[1].astype(F32)
    gain_part = jnp.sum(normed_grad * vhat, axis=0, keepdims=True)
    s_own[...] = jnp.concatenate([gain_part, small_ref[1:, :]], axis=0)

    def sum_dp(turn):
        return remote(
            s_own, s_dp.at[turn], s_send.at[turn], s_recv.at[turn], other_dp(turn)
        )

    def sum_mp(turn):
        return remote(
            s_dp.at[0], s_mp.at[turn], s_send.at[8 + turn], s_recv.at[8 + turn], other_mp(turn)
        )

    for turn in range(1, 8):
        sum_dp(turn).start()
    grad_ref[...] = mgrad[...] + norm_back(vhat, scale, gain_ref[...], normed_grad)
    total = s_own[...]
    for turn in range(1, 8):
        sum_dp(turn).wait_recv()
        total += s_dp[turn]
    s_dp[0] = total
    for turn in range(1, WAYS):
        sum_mp(turn).start()
    for turn in range(1, WAYS):
        sum_mp(turn).wait_recv()
        total += s_mp[turn]
    total_ref[...] = total

    for turn in range(1, 8):
        sum_dp(turn).wait_send()
    for turn in range(1, WAYS):
        sum_mp(turn).wait_send()
    for m in range(2):
        to_core(m).wait_send()
        to_owner(m, p.owner_of(m)).wait_send()
    for m in range(WAYS):
        for pair in range(pairs):
            head_grad(m, pair, p.attention_of(m)).wait_send()
    for pair in range(pairs):
        qkv_x(pair, 0).wait_send()
        qkv_x(pair, 1).wait_send()
        qkv_y(pair).wait_send()
        for turn in range(2):
            qkv_z(pair, turn, p.group, qkv_to(turn)).wait_send()
    ffn[0].finish(DONE)
    ffn[1].finish(DONE)
    attn.finish()


def backward_call(heads_grad, ffn_sum, r1, kept, weight, x, middle_grad, low, heads, gain, small):
    normed, cosine, sine, qa, ka, v, o = kept
    rows, model = x.shape
    pairs, tokens, unused = v.shape
    wide, cols3, unused = weight.shape
    units = ffn_sum.shape[2]
    depth = model // WAYS
    third = cols3 // pairs
    part = (units // 32 + 1) * 16
    anywhere = pl.BlockSpec(memory_space=pl.ANY)
    vmem = pl.BlockSpec(memory_space=pltpu.VMEM)
    buf = lambda *shape, kind=BF: pltpu.VMEM(shape, kind)
    sems = lambda *shape: pltpu.SemaphoreType.DMA(shape)
    return pl.pallas_call(
        backward_kernel,
        in_specs=[anywhere] * 7 + [vmem] * 10,
        out_specs=[vmem] * 5,
        out_shape=[
            shape_of((rows, model), F32),
            shape_of((units, LANES), F32),
            shape_of((depth, LANES), F32),
            shape_of((pairs, third, LANES), F32),
            shape_of(small.shape, F32),
        ],
        scratch_shapes=[
            buf(WAYS, pairs, rows, LANES),
            buf(pairs, 3, tokens, LANES),
            buf(2, tokens, LANES),
            buf(2, LANES, tokens),
            buf(tokens, LANES, kind=F32),
            buf(tokens, LANES, kind=F32),
            buf(tokens, model),
            buf(wide, cols3, LANES),
            buf(rows, model),
            buf(rows, model, kind=F32),
            *[
                buf(*lead, cut, LANES)
                for cut in (part, units - part)
                for lead in ((WAYS, 2), (WAYS, 2), (WAYS,), (WAYS + 1,))
            ],
            buf(2, WAYS, wide // 2, depth, LANES),
            buf(WAYS, wide // 2, depth, LANES),
            buf(WAYS, 2, depth, LANES),
            buf(WAYS, depth, LANES),
            buf(WAYS + 1, depth, LANES),
            buf(pairs, wide, third, LANES),
            buf(pairs, 2, 2, third, LANES),
            buf(pairs, 2, third, LANES),
            buf(pairs, 2, third, LANES),
            buf(2, rows, model),
            buf(2, rows, model),
            buf(*small.shape, kind=F32),
            buf(8, *small.shape, kind=F32),
            buf(WAYS, *small.shape, kind=F32),
            sems(26),
            sems(WAYS, pairs),
            sems(WAYS, pairs),
            sems(2, 16),
            sems(2, 17),
            sems(16),
            sems(17),
            sems(1),
            sems(1),
            sems(pairs, 5),
            sems(pairs, 5),
            sems(4),
            sems(4),
            sems(12),
            sems(12),
        ],
        compiler_params=pltpu.CompilerParams(
            collective_id=2, has_side_effects=True, vmem_limit_bytes=62 * 1024 * 1024
        ),
        name="backward",
    )(
        heads_grad, ffn_sum, r1, normed, weight, x, middle_grad, low, heads,
        qa, ka, v, o, cosine, sine, gain, small,
    )


def pick(values, at, axis=0):
    return lax.dynamic_index_in_dim(values, at, axis, keepdims=False)


def flip(values, bit, dps):
    return lax.ppermute(values, "dp", [(i, i ^ bit) for i in range(dps)])


def to_attention(values, m, dps, back=False):
    pairs = []
    for dp in range(dps):
        group = dp % 2
        for t in range(WAYS):
            quarter = t ^ m
            there = (dp - group + ((quarter // 2) ^ group)) * WAYS + 2 * group + quarter % 2
            pairs.append((there, dp * WAYS + t) if back else (dp * WAYS + t, there))
    return lax.ppermute(values, ("dp", "mp"), pairs)


def local(
    sizes,
    layer_input,
    segment_ids,
    grad_out,
    qkv_weight,
    attn_weight,
    inner_weight,
    outer_weight,
    attn_gain,
    mlp_gain,
):
    dps, mps = sizes
    rows, model = layer_input.shape
    head_cols = qkv_weight.shape[2]
    units = inner_weight.shape[2]
    pairs = head_cols // LANES
    wide = model // LANES
    special = dps == wide
    me = lax.axis_index("mp")
    dp = lax.axis_index("dp")
    core = dp % 2
    group = me // 2
    quarter = me ^ (2 * core)
    scalars = jnp.stack([me, core if special else 0, quarter]).astype(jnp.int32)

    def every(values):
        got = lax.all_gather(values.T, "dp", axis=0, tiled=True).T
        got = got.reshape(-1, wide, LANES).transpose(1, 0, 2)
        return lax.all_gather(got, "mp", axis=1)

    qkv_part = qkv_weight.transpose(1, 2, 0).reshape(3, pairs, LANES, -1)
    qkv_part = qkv_part.transpose(1, 0, 2, 3).reshape(3 * head_cols, -1)
    inner_t = inner_weight.transpose(1, 2, 0)
    outer_t = outer_weight.T
    attn_depth = model // mps
    part_a = jnp.concatenate([attn_weight.T, inner_t[0]], axis=0)
    part_b = jnp.concatenate([inner_t[1], outer_t], axis=0)
    mine = segment_ids[0]
    info = jnp.stack([mine, doc_positions(mine)], axis=1).astype(F32)
    info = jnp.pad(info, ((0, 0), (0, LANES - 2))).reshape(WAYS, rows, LANES)
    live_mine = (pick(mine.reshape(WAYS, rows), me) != 0).astype(F32)[:, None]
    if special:
        (pack_a, pack_b), heads, qkv_own, kept = forward_call(
            layer_input, info, attn_gain[None], qkv_part, [part_a, part_b], dps, pairs
        )
    else:
        x_all = jnp.stack([to_attention(layer_input, m, dps) for m in range(WAYS)])
        qkv_all, pack_a, pack_b = every(qkv_part), every(part_a), every(part_b)
        info = jnp.where(group == core, info, flip(info, 1, dps))
        info = jnp.stack([pick(info, quarter ^ m) for m in range(WAYS)])
        kept = alone_call(x_all, info, attn_gain[None], pick(qkv_all, quarter, 1), pairs)
        heads = kept[6].reshape(pairs, WAYS, rows, LANES)
        heads = [to_attention(heads[:, m], m, dps, back=True) for m in range(WAYS)]
        heads = jnp.stack(heads)
    normed, cosine, sine, qa, ka, v, o = kept

    layer_output, middle_grad, middle_low, small, heads_grad, ffn_sum, ffn_got = mlp_call(
        scalars, heads, layer_input, grad_out, mlp_gain[None], live_mine, pack_a, pack_b, special
    )
    if special:
        input_grad, ffn_sum, attn_sum, qkv_sum, small = backward_call(
            heads_grad, ffn_sum, ffn_got, kept, qkv_own, layer_input, middle_grad, middle_low, heads,
            attn_gain[None], small,
        )
        qkv_sum = qkv_sum.reshape(3 * head_cols, -1)
    else:
        lows = []
        for pair in range(pairs):
            grad = [to_attention(heads_grad[m, pair], m, dps) for m in range(WAYS)]
            low = attn_bwd_call(scalars, qa, ka, v, grad, o, cosine, sine, pair)
            lows.append(jnp.concatenate(low, axis=0))
        low = jnp.concatenate(lows, axis=1)
        own = pick(qkv_all, quarter, 1)
        own = jnp.concatenate([own[d] for d in range(wide)], axis=-1)
        normed_grad = dot_nn(low, own).astype(BF).reshape(WAYS, rows, model)
        normed_grad = sum(
            to_attention(normed_grad[m], m, dps, back=True).astype(F32) for m in range(WAYS)
        )

        def scatter(values):
            cut = lax.psum_scatter(values, "mp", scatter_dimension=0)
            return lax.psum_scatter(cut.T, "dp", scatter_dimension=0, tiled=True).T

        slot = (jnp.arange(mps) == quarter)[:, None, None]
        qkv_sum = scatter(jnp.where(slot, dot_tn(low, normed)[None], 0.0))
        mixed = jnp.stack([pick(heads, me ^ h) for h in range(mps)])
        mixed = mixed.transpose(0, 2, 1, 3).reshape(mps, rows, -1)
        attn_sum = scatter(jnp.stack([dot_tn(mixed[h], middle_low) for h in range(mps)]))
        ffn_sum = ffn_sum.reshape(mps, wide, 3 * units, LANES).transpose(0, 2, 1, 3)
        ffn_sum = scatter(ffn_sum.reshape(mps, 3 * units, model).astype(F32))
        vhat, scale = norm_stats(layer_input.astype(F32))
        input_grad = middle_grad + norm_back(vhat, scale, attn_gain, normed_grad)
        small = small.at[0].set(jnp.sum(normed_grad * vhat, axis=0))
        small = lax.psum(small, ("dp", "mp"))
    rms_values = jnp.sqrt(small[2, :4] / (small[2, 4] * model))

    qkv_sum = qkv_sum.reshape(pairs, 3, LANES, -1).transpose(3, 1, 0, 2)
    ffn_sum = ffn_sum.reshape(3, units, -1)
    return (
        layer_output,
        input_grad,
        qkv_sum.reshape(-1, 3, head_cols),
        attn_sum.T,
        ffn_sum[:2].transpose(2, 0, 1),
        ffn_sum[2].T,
        small[0],
        small[1],
        rms_values,
    )


def solution(mesh):
    sizes = (mesh.shape["dp"], mesh.shape["mp"])
    both = ("dp", "mp")
    whole = (P(both, None), P("dp", None, "mp"), P("dp", "mp"))
    return jax.shard_map(
        functools.partial(local, sizes),
        mesh=mesh,
        in_specs=(
            whole[0],
            P("dp", None),
            whole[0],
            whole[1],
            whole[2],
            whole[1],
            whole[2],
            P(),
            P(),
        ),
        out_specs=(
            whole[0],
            whole[0],
            whole[1],
            whole[2],
            whole[1],
            whole[2],
            P(),
            P(),
            P(),
        ),
        check_vma=False,
    )
```

```python
import functools
import math

import jax
import jax.numpy as jnp
from jax import lax
from jax.experimental import pallas as pl
from jax.experimental.pallas import tpu as pltpu
from jax.sharding import PartitionSpec as P

HEAD_DIM = 64
NORM_EPS = 1e-05
ROPE_BASE = 160000.0
BIG = 1e30
LANES = 128
WAYS = 4
BF = jnp.bfloat16
F32 = jnp.float32
VMEM_LIMIT = 56 * 1024 * 1024


def dot_nn(a, b):
    return lax.dot_general(a, b, (((1,), (0,)), ((), ())), preferred_element_type=F32)


def dot_nt(a, b):
    return lax.dot_general(a, b, (((1,), (1,)), ((), ())), preferred_element_type=F32)


def dot_tn(a, b):
    return lax.dot_general(a, b, (((0,), (0,)), ((), ())), preferred_element_type=F32)


def norm_stats(values):
    centre = jnp.mean(values, axis=-1, keepdims=True)
    shifted = values - centre
    spread = jnp.mean(shifted * shifted, axis=-1, keepdims=True)
    scale = lax.rsqrt(spread + NORM_EPS)
    return shifted * scale, scale


def norm_back(vhat, scale, gain, grad):
    u = grad * gain
    mean_u = jnp.mean(u, axis=-1, keepdims=True)
    mean_uv = jnp.mean(u * vhat, axis=-1, keepdims=True)
    return scale * (u - mean_u - vhat * mean_uv)


def swap_halves(values):
    lane = lax.broadcasted_iota(jnp.int32, values.shape, 1)
    first = lane % HEAD_DIM < HEAD_DIM // 2
    back = pltpu.roll(values, LANES - HEAD_DIM // 2, 1)
    ahead = pltpu.roll(values, HEAD_DIM // 2, 1)
    return jnp.where(first, back, ahead)


def choose(at, values):
    out = values[0]
    for i in range(1, len(values)):
        out = jnp.where(at == i, values[i], out)
    return out


def params():
    return pltpu.CompilerParams(vmem_limit_bytes=VMEM_LIMIT)


def cost(flops, mib):
    return pl.CostEstimate(flops=int(flops), bytes_accessed=int(mib * 2**20), transcendentals=0)


def call(kernel, scalars, grid, in_specs, out_specs, out_shape, scratch, estimate, name):
    spec = pltpu.PrefetchScalarGridSpec(
        num_scalar_prefetch=1,
        grid=grid,
        in_specs=in_specs,
        out_specs=out_specs,
        scratch_shapes=scratch,
    )
    return functools.partial(
        pl.pallas_call(
            kernel,
            grid_spec=spec,
            out_shape=out_shape,
            compiler_params=params(),
            cost_estimate=estimate,
            name=name,
        ),
        scalars,
    )


def full(shape):
    return pl.BlockSpec(shape, lambda i, s: (0,) * len(shape))


def shape_of(shape, dtype):
    return jax.ShapeDtypeStruct(shape, dtype)


def side_by_side(ref, *at):
    return jnp.concatenate([ref[(d, *at)] for d in range(ref.shape[0])], axis=-1)


STEP = 256


def doc_starts(pieces):
    number = lax.broadcasted_iota(jnp.int32, (1, LANES), 1).astype(F32)
    total = jnp.zeros((1, LANES), F32)
    for piece in pieces:
        before = jnp.logical_and(piece > 0.0, piece < number)
        total += jnp.sum(jnp.where(before, 1.0, 0.0), axis=0, keepdims=True)
    return total


def table_piece(m, segment, first, starts, out):
    rows = segment.shape[0]
    here = slice(m * rows, (m + 1) * rows)
    number = lax.broadcasted_iota(jnp.int32, (1, LANES), 1).astype(F32)
    start = jnp.sum(jnp.where(segment == number, starts, 0.0), axis=-1, keepdims=True)
    place = lax.broadcasted_iota(jnp.int32, (rows, 1), 0) + first
    position = place.astype(F32) - start
    lane = lax.broadcasted_iota(jnp.int32, (1, LANES), 1)
    half = HEAD_DIM // 2
    frequency = jnp.exp((lane % half).astype(F32) * (-2.0 * math.log(ROPE_BASE) / HEAD_DIM))
    angle = position * frequency
    sine = jnp.sin(angle)
    out.cosine[here, :] = jnp.cos(angle)
    out.sine[here, :] = jnp.where(lane % HEAD_DIM < half, -sine, sine)
    t = lane % HEAD_DIM
    same = segment == t.astype(F32)
    masked = jnp.where(same, 0.0, -BIG)
    out.qaux[here, :] = jnp.where(t >= 16, 0.0, masked).astype(BF)
    found = jnp.where(same, 1.0, 0.0)
    counted = jnp.where(t < 19, 1.0, 0.0)
    out.kaux[here, :] = jnp.where(t < 16, found, counted).astype(BF)
    out.live[here, :] = jnp.where(segment[:, 0:1] != 0.0, 1.0, 0.0)


def qkv_piece(m, x, gain, weight, out):
    rows = x.shape[0]
    here = slice(m * rows, (m + 1) * rows)
    vhat, unused = norm_stats(x.astype(F32))
    normed = (vhat * gain).astype(BF)
    out.normed[here, :] = normed
    flat = dot_nt(normed, weight)
    cosine, sine = out.cosine[here, :], out.sine[here, :]
    kaux = out.kaux[here, :]
    lane = lax.broadcasted_iota(jnp.int32, (rows, LANES), 1)
    for pair in range(flat.shape[1] // (3 * LANES)):
        q, k, v = [
            flat[:, at : at + LANES] for at in range(pair * 3 * LANES, (pair + 1) * 3 * LANES, LANES)
        ]
        q = (q * cosine + swap_halves(q) * sine).astype(BF)
        k = (k * cosine + swap_halves(k) * sine).astype(BF)
        out.q[pair, here, :] = q * jnp.asarray(HEAD_DIM**-0.5, BF)
        out.ka[pair, 0, here, :] = jnp.where(lane < HEAD_DIM, k, kaux)
        out.ka[pair, 1, here, :] = jnp.where(lane >= HEAD_DIM, k, kaux)
        out.v[pair, here, :] = v.astype(BF)


def attn_step(pair, step, out):
    tokens = out.v.shape[1]
    chunk = 512
    here = pl.ds(pl.multiple_of(step * STEP, STEP), STEP)
    lane = lax.broadcasted_iota(jnp.int32, (STEP, LANES), 1)
    t = lane % HEAD_DIM
    q = out.q[pair, here, :]
    qaux = out.qaux[here, :]
    live = out.live[here, :]
    outs = []
    for head in range(2):
        mine = (lane < HEAD_DIM) if head == 0 else (lane >= HEAD_DIM)
        qa = jnp.where(mine, q, qaux)
        top = None
        for at in range(0, tokens, chunk):
            s = dot_nt(qa, out.ka[pair, head, at : at + chunk, :])
            out.scores[:, at : at + chunk] = s
            part = jnp.max(s, axis=-1, keepdims=True)
            top = part if top is None else jnp.maximum(top, part)
        total = jnp.zeros((STEP, 1), F32)
        mixed = jnp.zeros((STEP, LANES), F32)
        for at in range(0, tokens, chunk):
            p = jnp.exp(out.scores[:, at : at + chunk] - top)
            total += jnp.sum(p, axis=-1, keepdims=True)
            mixed += dot_nn(p.astype(BF), out.v[pair, at : at + chunk, :])
        outs.append(mixed * (live / total))
        log_sum = jnp.where(live > 0, top + jnp.log(total), BIG)
        high = log_sum.astype(BF)
        rest = log_sum - high.astype(F32)
        mid = rest.astype(BF)
        low = (rest - mid.astype(F32)).astype(BF)
        aux = jnp.where(t == 16, -high, jnp.where(t == 17, -mid, jnp.where(t == 18, -low, qaux)))
        out.qa[pair, head, here, :] = jnp.where(mine, q, aux)
    out.o[pair, here, :] = jnp.where(lane < HEAD_DIM, outs[0], outs[1]).astype(BF)


class Kept:
    names = ("normed", "cosine", "sine", "qa", "ka", "v", "o", "q", "qaux", "kaux", "live", "scores")

    def __init__(self, refs):
        for name, ref in zip(self.names, refs):
            setattr(self, name, ref)


def kept_shapes(tokens, model, pairs):
    outs = [
        shape_of((tokens, model), BF),
        shape_of((tokens, LANES), F32),
        shape_of((tokens, LANES), F32),
        shape_of((pairs, 2, tokens, LANES), BF),
        shape_of((pairs, 2, tokens, LANES), BF),
        shape_of((pairs, tokens, LANES), BF),
        shape_of((pairs, tokens, LANES), BF),
    ]
    scratch = [
        pltpu.VMEM((pairs, tokens, LANES), BF),
        pltpu.VMEM((tokens, LANES), BF),
        pltpu.VMEM((tokens, LANES), BF),
        pltpu.VMEM((tokens, 1), F32),
        pltpu.VMEM((STEP, tokens), F32),
    ]
    return outs, scratch


def alone_kernel(quarter_ref, x_ref, info_ref, gain_ref, w_ref, *refs):
    out = Kept(refs)
    starts = doc_starts([info_ref[t] for t in range(WAYS)])
    for m in range(WAYS):
        t = quarter_ref[0] ^ m
        table_piece(m, info_ref[t], t * info_ref.shape[1], starts, out)
        qkv_piece(m, x_ref[m], gain_ref[...], side_by_side(w_ref), out)

    def body(step, carry):
        per = out.v.shape[1] // STEP
        attn_step(step // per, step % per, out)
        return carry

    lax.fori_loop(0, out.v.shape[0] * out.v.shape[1] // STEP, body, 0)


def alone_call(quarter, x, info, gain, weight, pairs):
    outs, scratch = kept_shapes(WAYS * x.shape[1], x.shape[2], pairs)
    return pl.pallas_call(
        alone_kernel,
        in_specs=[pl.BlockSpec(memory_space=pltpu.SMEM)]
        + [pl.BlockSpec(memory_space=pltpu.VMEM)] * 4,
        out_specs=[pl.BlockSpec(memory_space=pltpu.VMEM)] * len(outs),
        out_shape=outs,
        scratch_shapes=scratch,
        compiler_params=params(),
        name="forward",
    )(quarter.reshape(1), x, info, gain, weight)


def piece_block(m, rows, per):
    return pl.BlockSpec((rows, LANES), lambda i, s: (jnp.clip(i - per * m, 0, per - 1), 0))


def attn_bwd_kernel(s_ref, *refs):
    qa_ref, ka_ref, v_ref, o_ref, do_refs = refs[0], refs[1], refs[2], refs[3], refs[4:8]
    cosq_ref, sinq_ref, cosk_ref, sink_ref = refs[8:12]
    out_refs = refs[12:16]
    va_ref, kt_ref, dk_acc, dv_acc = refs[16:20]
    step = pl.program_id(0)
    rows = do_refs[0].shape[0]
    chunk = v_ref.shape[0] // WAYS
    per = chunk // rows
    piece = step // per
    lane_k = lax.broadcasted_iota(jnp.int32, (chunk, LANES), 1)
    lane = lax.broadcasted_iota(jnp.int32, (rows, LANES), 1)
    zero = jnp.zeros((), BF)

    @pl.when(step == 0)
    def _():
        ones = jnp.where(lane_k % HEAD_DIM < 3, jnp.ones((), BF), zero)
        for m in range(WAYS):
            some = slice(m * chunk, (m + 1) * chunk)
            v = v_ref[some, :]
            for head in range(2):
                mine = (lane_k < HEAD_DIM) if head == 0 else (lane_k >= HEAD_DIM)
                va_ref[head, some, :] = jnp.where(mine, v, ones)
                own = jnp.where(mine, ka_ref[head, some, :], zero).astype(F32)
                kt_ref[head, :, some] = own.T.astype(BF)
        dk_acc[...] = jnp.zeros_like(dk_acc)
        dv_acc[...] = jnp.zeros_like(dv_acc)

    grad = choose(piece, [r[...] for r in do_refs])
    out = o_ref[...]
    product = grad.astype(F32) * out.astype(F32)
    turned = jnp.zeros((LANES, rows), F32)
    for head in range(2):
        mine = (lane < HEAD_DIM) if head == 0 else (lane >= HEAD_DIM)
        delta = jnp.sum(jnp.where(mine, product, 0.0), axis=-1, keepdims=True)
        high = delta.astype(BF)
        rest = delta - high.astype(F32)
        mid = rest.astype(BF)
        low = (rest - mid.astype(F32)).astype(BF)
        t = lane % HEAD_DIM
        aux = jnp.where(t == 0, -high, jnp.where(t == 1, -mid, jnp.where(t == 2, -low, zero)))
        grad_aug = jnp.where(mine, grad, aux)
        grad_own = jnp.where(mine, grad, zero)
        qa = qa_ref[head]
        q_own = jnp.where(mine, qa, zero)
        for m in range(WAYS):
            some = slice(m * chunk, (m + 1) * chunk)
            prob = jnp.exp(dot_nt(ka_ref[head, some, :], qa))
            back = dot_nt(va_ref[head, some, :], grad_aug)
            score_grad = (prob * back).astype(BF)
            dv_acc[some, :] += dot_nn(prob.astype(BF), grad_own)
            dk_acc[some, :] += dot_nn(score_grad, q_own)
            turned += dot_nn(kt_ref[head, :, some], score_grad)
    dq = turned.T * (HEAD_DIM**-0.5)
    dq = (dq * cosq_ref[...] - swap_halves(dq) * sinq_ref[...]).astype(BF)
    for m in range(WAYS):

        @pl.when(piece == m)
        def _(m=m):
            here = pl.ds(pl.multiple_of((step - m * per) * rows, rows), rows)
            out_refs[m][here, :LANES] = dq

    @pl.when(step == pl.num_programs(0) - 1)
    def _():
        for m in range(WAYS):
            some = slice(m * chunk, (m + 1) * chunk)
            dk = dk_acc[some, :]
            dk = dk * cosk_ref[some, :] - swap_halves(dk) * sink_ref[some, :]
            out_refs[m][:, LANES : 2 * LANES] = dk.astype(BF)
            out_refs[m][:, 2 * LANES :] = dv_acc[some, :].astype(BF)


def attn_bwd_call(scalars, qa, ka, v, grad, o, cosine, sine, pair):
    tokens = v.shape[1]
    chunk = tokens // WAYS
    rows = 256
    per = chunk // rows
    moving = [piece_block(m, rows, per) for m in range(WAYS)]
    block = pl.BlockSpec((rows, LANES), lambda i, s: (i, 0))
    return call(
        attn_bwd_kernel,
        scalars,
        (tokens // rows,),
        [
            pl.BlockSpec((None, 2, rows, LANES), lambda i, s: (pair, 0, i, 0)),
            pl.BlockSpec((None, 2, tokens, LANES), lambda i, s: (pair, 0, 0, 0)),
            pl.BlockSpec((None, tokens, LANES), lambda i, s: (pair, 0, 0)),
            pl.BlockSpec((None, rows, LANES), lambda i, s: (pair, i, 0)),
        ]
        + moving
        + [block, block, full((tokens, LANES)), full((tokens, LANES))],
        [full((chunk, 3 * LANES))] * WAYS,
        [shape_of((chunk, 3 * LANES), BF)] * WAYS,
        [
            pltpu.VMEM((2, tokens, LANES), BF),
            pltpu.VMEM((2, LANES, tokens), BF),
            pltpu.VMEM((tokens, LANES), F32),
            pltpu.VMEM((tokens, LANES), F32),
        ],
        cost(28 * tokens * tokens * LANES, 8),
        "attn_bwd",
    )(qa, ka, v, o, *grad, cosine, sine, cosine, sine)


def own_first(core, values):
    cut = [values[:, at : at + LANES] for at in range(0, values.shape[1], LANES)]
    turned = [cut[i ^ 1] for i in range(len(cut))]
    return jnp.where(core == 0, values, jnp.concatenate(turned, axis=-1))


MESH = pl.DeviceIdType.MESH
UP, DOWN, TO_X, TO_Y, TO_D, CORE_OWN, CORE_X, CORE_Y, CORE_D = range(9)
FROM_Z, FROM_X, FROM_Y, FROM_D = range(4)
CHUNKS = 4


class Place:
    def __init__(self):
        self.dp, self.z = lax.axis_index("dp"), lax.axis_index("mp")
        self.core, self.x, self.y = self.dp % 2, (self.dp // 2) % 2, self.dp // 4
        self.at_c = self.dp + 1 - 2 * self.core
        self.at_x = self.dp + 2 - 4 * self.x
        self.at_y = self.dp + 4 - 8 * self.y
        self.at_d = self.at_x + self.at_y - self.dp
        self.group = self.z // 2
        self.far_z = self.z + 2 - 4 * self.group
        self.quarter = self.z + self.core * (self.far_z - self.z)

    @staticmethod
    def mix(q, m):
        return (q + m) % 2 + 2 * ((q // 2 + m // 2) % 2)

    def stays(self, a, b):
        return jnp.logical_and(a == self.dp, b == self.z)

    def attention_of(self, m):
        h = self.mix(self.z, m)
        a, b = self.dp - self.core + (h // 2 + self.core) % 2, 2 * self.core + h % 2
        return a, b, self.stays(a, b)

    def owner_of(self, m):
        a, b = self.dp - self.core + self.group, self.mix(self.quarter, m)
        return a, b, self.stays(a, b)


def remote(src, dst, send, recv, device):
    return pltpu.make_async_remote_copy(
        src_ref=src, dst_ref=dst, send_sem=send, recv_sem=recv,
        device_id=device, device_id_type=MESH,
    )


class Move:
    def __init__(self, src, dst, send, recv, place):
        a, b, self.stays = place
        self.far = lambda: remote(src, dst, send, recv, (a, b))
        self.near = lambda: pltpu.make_async_copy(src, dst, recv)

    def start(self):
        pl.when(self.stays)(lambda: self.near().start())
        pl.when(jnp.logical_not(self.stays))(lambda: self.far().start())

    def wait_recv(self):
        self.far().wait_recv()

    def wait_send(self):
        pl.when(jnp.logical_not(self.stays))(lambda: self.far().wait_send())


def forward_kernel(x_ref, info_ref, gain_ref, qkv_ref, *refs, packs):
    parts, outs, heads_ref = refs[:packs], refs[packs : 2 * packs], refs[2 * packs]
    saved, refs = refs[2 * packs + 1 : 2 * packs + 7], refs[2 * packs + 7 :]
    qa, o, normed, cosine, sine, ka, v, q, qaux, kaux, live, scores = refs[:12]
    kept = Kept((normed, cosine, sine, qa, ka, v, o, q, qaux, kaux, live, scores))
    x_all, w_ref, infos = refs[12:15]
    (
        sends, recvs, cores, locals_, token_send, token_recv, relay_send, info_sem,
        head_send, head_recv,
        q_send, q_recv, save_sem,
    ) = refs[15:]
    dp, z = lax.axis_index("dp"), lax.axis_index("mp")
    core, xb, yb = dp % 2, (dp // 2) % 2, dp // 4
    at_c, at_x, at_y = dp + 1 - 2 * core, dp + 2 - 4 * xb, dp + 4 - 8 * yb
    at_d = at_x + at_y - dp
    group = z // 2
    far_z = z + 2 - 4 * group
    quarter = z + core * (far_z - z)

    def mix(q, m):
        return (q + m) % 2 + 2 * ((q // 2 + m // 2) % 2)

    def attention_of(m):
        h = mix(z, m)
        return dp - core + (h // 2 + core) % 2, 2 * core + h % 2

    def owner_of(m):
        return dp - core + group, mix(quarter, m)

    barrier = pltpu.get_barrier_semaphore()

    def greet(device, when=None):
        def signal():
            pl.semaphore_signal(barrier, inc=1, device_id=device, device_id_type=MESH)

        signal() if when is None else pl.when(when)(signal)

    greet((at_c, z))
    greet((at_x, z))
    greet((at_y, z))
    greet((dp, far_z))
    greet((dp, z + 1), z < WAYS - 1)
    greet((dp, z - 1), z > 0)
    count = 4 + (z < WAYS - 1).astype(jnp.int32) + (z > 0).astype(jnp.int32)
    here, there = [], []
    for m in range(WAYS):
        for of, found in ((attention_of, here), (owner_of, there)):
            a, b = of(m)
            stays = jnp.logical_and(a == dp, b == z)
            found.append((a, b, stays))
            greet((a, b), jnp.logical_not(stays))
            count += 1 - stays.astype(jnp.int32)
    pl.semaphore_wait(barrier, count)

    def remote(src, dst, send, recv, device):
        return pltpu.make_async_remote_copy(
            src_ref=src, dst_ref=dst, send_sem=send, recv_sem=recv,
            device_id=device, device_id_type=MESH,
        )

    def copy(p, kind, s, src=None):
        who = {CORE_X: at_x, CORE_Y: at_y, CORE_D: at_d}.get(kind, dp)
        if kind == TO_D:
            who = jnp.where(s < 2, at_x, at_y)
        slab = outs[p].at[who, s]
        send = sends.at[p, kind, s]
        if kind == UP:
            recv, device = recvs.at[p, FROM_Z, s], (dp, z + 1)
        elif kind == DOWN:
            recv, device = recvs.at[p, FROM_Z, s], (dp, z - 1)
        elif kind == TO_X:
            recv, device = recvs.at[p, FROM_X, s], (at_x, z)
        elif kind == TO_Y:
            recv, device = recvs.at[p, FROM_Y, s], (at_y, z)
        elif kind == TO_D:
            recv, device = recvs.at[p, FROM_D, s], (jnp.where(s < 2, at_y, at_x), z)
        else:
            recv, device = cores.at[p, kind - CORE_OWN, s], (at_c, z)
        return remote(slab if src is None else src, slab, send, recv, device)

    def arrived(p, sem, who, s):
        slab = outs[p].at[who, s]
        remote(slab, slab, sends.at[p, UP, s], sem, (at_c, z)).wait_recv()

    def spread(p, s, src=None):
        copy(p, TO_X, s, src).start()
        copy(p, TO_Y, s, src).start()
        copy(p, CORE_OWN, s, src).start()

    def begin(p):
        src = parts[p]
        spread(p, z, src)
        pltpu.make_async_copy(src, outs[p].at[dp, z], locals_.at[p]).start()

    def begin_line(p):
        src = parts[p]
        pl.when(z < WAYS - 1)(lambda: copy(p, UP, z, src).start())
        pl.when(z > 0)(lambda: copy(p, DOWN, z, src).start())

    def reach(p, hop):
        def one(s):
            arrived(p, recvs.at[p, FROM_Z, s], dp, s)
            spread(p, s)

        pl.when(z >= hop)(lambda: one(z - hop))
        pl.when(z + hop < WAYS)(lambda: one(z + hop))

    def ahead(p, hop):
        pl.when(jnp.logical_and(z >= hop, z < WAYS - 1))(lambda: copy(p, UP, z - hop).start())
        pl.when(jnp.logical_and(z + hop < WAYS, z > 0))(lambda: copy(p, DOWN, z + hop).start())

    def line(p, hop):
        reach(p, hop)
        if hop < WAYS - 1:
            ahead(p, hop)

    def plane(p, hop):
        def one(s):
            arrived(p, recvs.at[p, FROM_X, s], at_x, s)
            copy(p, CORE_X, s).start()
            pl.when(s < 2)(lambda: copy(p, TO_D, s).start())
            arrived(p, recvs.at[p, FROM_Y, s], at_y, s)
            copy(p, CORE_Y, s).start()
            pl.when(s >= 2)(lambda: copy(p, TO_D, s).start())

        if hop == 0:
            one(z)
        else:
            pl.when(z >= hop)(lambda: one(z - hop))
            pl.when(z + hop < WAYS)(lambda: one(z + hop))

    def corner(p, hop):
        def one(s):
            arrived(p, recvs.at[p, FROM_D, s], at_d, s)
            copy(p, CORE_D, s).start()

        if hop == 0:
            one(z)
        else:
            pl.when(z >= hop)(lambda: one(z - hop))
            pl.when(z + hop < WAYS)(lambda: one(z + hop))

    def from_core(p):
        for s in range(WAYS):
            for kind in range(4):
                twin = (at_c, at_x + at_c - dp, at_y + at_c - dp, at_d + at_c - dp)[kind]
                arrived(p, cores.at[p, kind, s], twin, s)
        pltpu.make_async_copy(parts[p], outs[p].at[dp, z], locals_.at[p]).wait()

    def finish(p):
        for s in range(WAYS):
            pl.when(jnp.logical_and(z < WAYS - 1, s <= z))(lambda s=s: copy(p, UP, s).wait_send())
            pl.when(jnp.logical_and(z > 0, s >= z))(lambda s=s: copy(p, DOWN, s).wait_send())
            for kind in range(TO_X, CORE_D + 1):
                copy(p, kind, s).wait_send()

    far = (z // 2 + core) % 2 == 1
    straight = (z + 1 + core) % 2
    relays = jnp.logical_and(core == 1, jnp.logical_and(z > 0, z < WAYS - 1))
    beside = (dp, z + 1 - 2 * (z % 2))
    cut = x_ref.shape[0] // CHUNKS

    def token(m, c):
        to_dp, to_z, stays = here[m]
        some = pl.ds(c * cut, cut)
        src, dst = x_ref.at[some], x_all.at[m, some]

        def direct():
            return remote(src, dst, token_send.at[m, c], token_recv.at[m, c], (to_dp, to_z))

        def near():
            return pltpu.make_async_copy(src, dst, token_recv.at[m, c])

        goes = jnp.logical_and(
            jnp.logical_not(stays), jnp.logical_or(jnp.logical_not(far), straight == m)
        )
        return direct, near, stays, goes

    def relay(m, c):
        some = pl.ds(c * cut, cut)
        return remote(
            x_all.at[m, some], x_all.at[1 - m, some],
            relay_send.at[m, c], token_recv.at[1 - m, c], beside,
        )

    def pass_on(m, c):
        some = pl.ds(c * cut, cut)
        return remote(
            x_all.at[m, some], x_all.at[m + 2, some],
            token_send.at[m + 2, c], token_recv.at[m + 2, c], (at_c, z),
        )

    def take_tokens(c):
        for m in range(2):
            token(m, c)[0]().wait_recv()
            pl.when(relays)(lambda m=m: relay(m, c).start())
            pass_on(m, c).start()

    def early(*chunks):
        def run():
            for c in chunks:
                take_tokens(c)

        pl.when(relays)(run)

    def swap_info():
        return remote(info_ref, infos.at[1], info_sem.at[0], info_sem.at[1], (at_c, z))

    def own_info():
        return pltpu.make_async_copy(info_ref, infos.at[0], locals_.at[packs])

    def q_copy(kind, i=0, src=None):
        who = {"z": dp, "x": dp, "y": dp, "c": dp, "cx": at_x, "cy": at_y, "cd": at_d}.get(kind)
        if kind == "d":
            who = at_x if i == 0 else at_y
        device = {"z": (dp, far_z), "x": (at_x, z), "y": (at_y, z)}.get(kind, (at_c, z))
        if kind == "d":
            device = (at_y, z) if i == 0 else (at_x, z)
        slot = {"z": 0, "x": 1, "y": 3, "d": 5, "c": 7, "cx": 8, "cy": 9, "cd": 10}[kind]
        if kind in ("x", "y", "d"):
            slot += i
        if kind == "z":
            i = 1
        if kind[0] == "c":
            i = 1 - core
        dst = w_ref.at[i, who]
        return remote(dst if src is None else src, dst, q_send.at[slot], q_recv.at[slot], device)

    def q_arrived(kind, i=0):
        q_copy(kind, i).wait_recv()

    def own_q():
        return pltpu.make_async_copy(qkv_ref, w_ref.at[0, dp], locals_.at[packs + 1])

    q_kinds = [("z", 0), ("x", 0), ("x", 1), ("y", 0), ("y", 1), ("d", 0), ("d", 1)]
    q_kinds += [("c", 0), ("cx", 0), ("cy", 0), ("cd", 0)]

    keeps = [w_ref.at[core], normed, cosine, sine, ka, v]

    def save(i):
        return pltpu.make_async_copy(keeps[i], saved[i], save_sem.at[i])

    rows = x_ref.shape[0]

    def head(pair, m, owner):
        src = kept.o.at[pair, pl.ds(m * rows, rows)]
        dst = heads_ref.at[m, pair]
        to_dp, to_z, stays = owner

        def far():
            return remote(
                src, dst, head_send.at[m, pair], head_recv.at[m, pair], (to_dp, to_z)
            )

        def near():
            return pltpu.make_async_copy(src, dst, head_recv.at[m, pair])

        return far, near, stays

    def start(item):
        far, near, stays = item
        pl.when(stays)(lambda: near().start())
        pl.when(jnp.logical_not(stays))(lambda: far().start())

    def end_send(item):
        far, near, stays = item
        pl.when(jnp.logical_not(stays))(lambda: far().wait_send())

    q_copy("z", 0, qkv_ref).start()
    q_copy("x", 0, qkv_ref).start()
    q_copy("y", 0, qkv_ref).start()
    own_q().start()
    for c in range(CHUNKS):
        for m in range(2):
            direct, near, stays, goes = token(m, c)
            pl.when(stays)(lambda: near().start())
            pl.when(goes)(lambda: direct().start())
    swap_info().start()
    own_info().start()
    for p in range(packs):
        begin(p)
        begin_line(p)
    own_info().wait()
    swap_info().wait()
    own_q().wait()
    q_arrived("x", 0)
    q_copy("d", 0).start()
    q_arrived("z")
    q_copy("x", 1).start()
    q_copy("y", 1).start()
    early(0)
    away = (group + core) % 2
    starts = doc_starts([infos[away, t] for t in range(WAYS)])
    for m in range(WAYS):
        t = mix(quarter, m)
        table_piece(m, infos[away, t], t * x_ref.shape[0], starts, kept)
    q_arrived("y", 0)
    q_copy("c").start()
    plane(0, 0)
    q_arrived("x", 1)
    q_copy("cx").start()
    q_arrived("y", 1)
    q_copy("d", 1).start()
    q_copy("cy").start()
    early(1)
    plane(1, 0)
    q_arrived("d", 0)
    q_arrived("d", 1)
    q_copy("cd").start()
    early(2)
    reach(0, 1)
    corner(0, 0)
    reach(1, 1)
    corner(1, 0)
    for kind in ("c", "cx", "cy", "cd"):
        q_arrived(kind)
    save(0).start()
    save(2).start()
    save(3).start()
    early(3)
    @pl.when(jnp.logical_not(relays))
    def _():
        for c in range(CHUNKS):
            take_tokens(c)

    for p in range(packs):
        ahead(p, 1)
        plane(p, 1)
    for m in range(WAYS):
        if m >= 2:
            for c in range(CHUNKS):
                pass_on(m - 2, c).wait_recv()
        weight = jnp.concatenate([w_ref[core, d] for d in range(w_ref.shape[1])], axis=-1)
        qkv_piece(m, x_all[m], gain_ref[...], weight, kept)
        if m == 2:
            line(0, 2)
            corner(0, 1)
    save(1).start()
    save(4).start()
    save(5).start()

    events = {
        1: [(line, 1, 2), (corner, 1, 1)],
        4: [(line, 0, 3), (plane, 0, 2)],
        7: [(line, 1, 3), (plane, 1, 2)],
        9: [(corner, 0, 2)],
        11: [(plane, 0, 3)],
        13: [(corner, 1, 2)],
    }
    steps = kept.v.shape[1] // STEP
    pairs = kept.v.shape[0]
    per = steps // WAYS

    def body(i, carry):
        for at, todo in events.items():

            @pl.when(i == at)
            def _(todo=todo):
                for what, p, hop in todo:
                    what(p, hop)

        pair = i // steps
        step = i % steps
        attn_step(pair, step, kept)
        m = step // per

        @pl.when(step % per == per - 1)
        def _():
            a, b = dp - core + group, mix(quarter, m)
            start(head(pair, m, (a, b, jnp.logical_and(a == dp, b == z))))

        return carry

    lax.fori_loop(0, pairs * steps, body, 0)
    plane(1, 3)
    corner(0, 3)
    corner(1, 3)
    for p in range(packs):
        from_core(p)
    for m in range(WAYS):
        for pair in range(pairs):
            head(pair, m, there[m])[0]().wait_recv()
            end_send(head(pair, m, there[m]))
    for c in range(CHUNKS):
        for m in range(2):
            pass_on(m, c).wait_send()
            direct, near, stays, goes = token(m, c)
            pl.when(goes)(lambda: direct().wait_send())
            pl.when(relays)(lambda m=m, c=c: relay(m, c).wait_send())
    for p in range(packs):
        finish(p)
    for kind, i in q_kinds:
        q_copy(kind, i).wait_send()
    for i in range(len(keeps)):
        save(i).wait()


def forward_call(x, info, gain, qkv_part, parts, dps, pairs):
    rows, model = x.shape
    packs = len(parts)
    anywhere = pl.BlockSpec(memory_space=pl.ANY)
    vmem = pl.BlockSpec(memory_space=pltpu.VMEM)
    outs, scratch = kept_shapes(WAYS * rows, model, pairs)
    normed, cosine, sine, qa, ka, v, o = outs
    hold = [normed, cosine, sine, ka, v]
    weight = (dps,) + qkv_part.shape
    out = pl.pallas_call(
        functools.partial(forward_kernel, packs=packs),
        in_specs=[anywhere, anywhere, vmem] + [anywhere] * (1 + packs),
        out_specs=[anywhere] * (packs + 7) + [vmem] * 2,
        out_shape=[shape_of((dps, WAYS) + part.shape, BF) for part in parts]
        + [shape_of((WAYS, pairs, rows, LANES), BF), shape_of(weight, BF)]
        + hold
        + [qa, o],
        scratch_shapes=[pltpu.VMEM(h.shape, h.dtype) for h in hold]
        + scratch
        + [
            pltpu.VMEM((WAYS, rows, model), BF),
            pltpu.VMEM((2,) + weight, BF),
            pltpu.VMEM((2, WAYS, rows, LANES), F32),
            pltpu.SemaphoreType.DMA((packs, 9, WAYS)),
            pltpu.SemaphoreType.DMA((packs, 4, WAYS)),
            pltpu.SemaphoreType.DMA((packs, 4, WAYS)),
            pltpu.SemaphoreType.DMA((packs + 2,)),
            pltpu.SemaphoreType.DMA((WAYS, CHUNKS)),
            pltpu.SemaphoreType.DMA((WAYS, CHUNKS)),
            pltpu.SemaphoreType.DMA((2, CHUNKS)),
            pltpu.SemaphoreType.DMA((2,)),
            pltpu.SemaphoreType.DMA((WAYS, pairs)),
            pltpu.SemaphoreType.DMA((WAYS, pairs)),
            pltpu.SemaphoreType.DMA((11,)),
            pltpu.SemaphoreType.DMA((11,)),
            pltpu.SemaphoreType.DMA((6,)),
        ],
        compiler_params=pltpu.CompilerParams(
            collective_id=0, has_side_effects=True, vmem_limit_bytes=VMEM_LIMIT
        ),
        name="forward",
    )(x, info, gain, qkv_part, *parts)
    packs_out, out = out[:packs], out[packs:]
    heads, weight, normed, cosine, sine, ka, v, qa, o = out
    return packs_out, heads, weight, (normed, cosine, sine, qa, ka, v, o)


def attn_back_begin(pair, k):
    chunk = 512
    lane = lax.broadcasted_iota(jnp.int32, (chunk, LANES), 1)
    zero = jnp.zeros((), BF)
    ones = jnp.where(lane % HEAD_DIM < 3, jnp.ones((), BF), zero)
    for at in range(0, k.dk.shape[0], chunk):
        some = slice(at, at + chunk)
        v = k.v[pair, some, :]
        for head in range(2):
            mine = (lane < HEAD_DIM) if head == 0 else (lane >= HEAD_DIM)
            k.va[head, some, :] = jnp.where(mine, v, ones)
            own = jnp.where(mine, k.ka[pair, head, some, :], zero).astype(F32)
            k.kt[head, :, some] = own.T.astype(BF)
    k.dk[...] = jnp.zeros_like(k.dk)
    k.dv[...] = jnp.zeros_like(k.dv)


def attn_back_step(pair, step, grad, k):
    chunk = 512
    here = pl.ds(pl.multiple_of(step * STEP, STEP), STEP)
    lane = lax.broadcasted_iota(jnp.int32, (STEP, LANES), 1)
    zero = jnp.zeros((), BF)
    t = lane % HEAD_DIM
    product = grad.astype(F32) * k.o[pair, here, :].astype(F32)
    turned = jnp.zeros((LANES, STEP), F32)
    for head in range(2):
        mine = (lane < HEAD_DIM) if head == 0 else (lane >= HEAD_DIM)
        delta = jnp.sum(jnp.where(mine, product, 0.0), axis=-1, keepdims=True)
        high = delta.astype(BF)
        rest = delta - high.astype(F32)
        mid = rest.astype(BF)
        low = (rest - mid.astype(F32)).astype(BF)
        aux = jnp.where(t == 0, -high, jnp.where(t == 1, -mid, jnp.where(t == 2, -low, zero)))
        grad_aug = jnp.where(mine, grad, aux)
        grad_own = jnp.where(mine, grad, zero)
        qa = k.qa[pair, head, here, :]
        q_own = jnp.where(mine, qa, zero)
        for at in range(0, k.dk.shape[0], chunk):
            some = slice(at, at + chunk)
            prob = jnp.exp(dot_nt(k.ka[pair, head, some, :], qa))
            back = dot_nt(k.va[head, some, :], grad_aug)
            score_grad = (prob * back).astype(BF)
            k.dv[some, :] += dot_nn(prob.astype(BF), grad_own)
            k.dk[some, :] += dot_nn(score_grad, q_own)
            turned += dot_nn(k.kt[head, :, some], score_grad)
    dq = turned.T * (HEAD_DIM**-0.5)
    dq = dq * k.cosine[here, :] - swap_halves(dq) * k.sine[here, :]
    k.low[pair, 0, here, :] = dq.astype(BF)


def attn_back_end(pair, m, k, rows):
    some = slice(m * rows, (m + 1) * rows)
    dk = k.dk[some, :]
    dk = dk * k.cosine[some, :] - swap_halves(dk) * k.sine[some, :]
    k.low[pair, 1, some, :] = dk.astype(BF)
    k.low[pair, 2, some, :] = k.dv[some, :].astype(BF)


def low_piece(pair, m, k, rows):
    some = slice(m * rows, (m + 1) * rows)
    return jnp.concatenate([k.low[pair, c, some, :] for c in range(3)], axis=-1)


class Back:
    names = ("qa", "ka", "v", "o", "cosine", "sine", "low", "va", "kt", "dk", "dv")

    def __init__(self, refs):
        for name, ref in zip(self.names, refs):
            setattr(self, name, ref)


class Chain:
    def __init__(self, p, source, kept, r1, r2, rz, send, recv):
        self.p, self.source, self.kept = p, source, kept
        self.r1, self.r2, self.rz, self.send, self.recv = r1, r2, rz, send, recv

    def slab(self, q, slot, away):
        x, y = self.p.x, self.p.y
        if q < 2:
            return (y if slot else 1 - y) * 2 + (1 - x if away else x)
        return (1 - y if away else y) * 2 + (x if slot else 1 - x)

    def near(self, q, second=False):
        p = self.p
        return (p.at_x, p.z) if (q < 2) != second else (p.at_y, p.z)

    def stage1(self, q, slot):
        src = self.source(q, self.slab(q, slot, True))
        at = q * 2 + slot
        return remote(src, self.r1.at[q, slot], self.send.at[at], self.recv.at[at], self.near(q))

    def stage2(self, q):
        at = 8 + q
        src = self.kept(q, 0, self.slab(q, 0, False))
        return remote(src, self.r2.at[q], self.send.at[at], self.recv.at[at], self.near(q, True))

    def first(self, q):
        self.stage1(q, 0).start()
        self.stage1(q, 1).start()

    def second(self, q, done=False):
        if not done:
            self.stage1(q, 0).wait_recv()
        ref = self.kept(q, 0, self.slab(q, 0, False))
        ref[...] += self.r1[q, 0]
        self.stage2(q).start()
        if not done:
            self.stage1(q, 1).wait_recv()
        self.own(q)[...] += self.r1[q, 1]

    def own(self, q):
        return self.kept(q, 1, self.slab(q, 1, False))

    def third(self, q):
        self.stage2(q).wait_recv()
        self.own(q)[...] += self.r2[q]

    def lined(self, q, down):
        z = self.p.z
        at = q if down else q + 1
        return remote(
            self.own(q), self.rz.at[at], self.send.at[12 + q], self.recv.at[12 + at],
            (self.p.dp, z - 1 if down else z + 1),
        )

    def line(self, hop, quarters):
        z = self.p.z
        for q in quarters:
            if q < WAYS - hop:

                @pl.when(z == WAYS - hop)
                def _(q=q):
                    if hop > 1:
                        self.lined(q, True).wait_recv()
                        self.own(q)[...] += self.rz[q]
                    self.lined(q, True).start()

            if q > hop - 1:

                @pl.when(z == hop - 1)
                def _(q=q):
                    if hop > 1:
                        self.lined(q, False).wait_recv()
                        self.own(q)[...] += self.rz[q + 1]
                    self.lined(q, False).start()

    def last(self, out_ref):
        z = self.p.z
        for q in range(WAYS):

            @pl.when(z == q)
            def _(q=q):
                total = self.own(q)[...].astype(F32)
                if q < WAYS - 1:
                    self.lined(q, True).wait_recv()
                    total += self.rz[q].astype(F32)
                if q > 0:
                    self.lined(q, False).wait_recv()
                    total += self.rz[q + 1].astype(F32)
                out_ref[...] = total

    def finish(self, done=()):
        z = self.p.z
        for q in range(WAYS):
            if q not in done:
                self.stage1(q, 0).wait_send()
                self.stage1(q, 1).wait_send()
            self.stage2(q).wait_send()
            pl.when(q < z)(lambda q=q: self.lined(q, True).wait_send())
            pl.when(q > z)(lambda q=q: self.lined(q, False).wait_send())


DONE = (0, 2)


def turn_of(step):
    return 2 * (step % 2) + step // 2


def mlp_kernel(
    s_ref, heads_ref, x_ref, g_ref, gain_ref, live_ref, pack_ref, qkv_ref, wa_ref, wb_ref,
    output_ref, mgrad_ref, low_ref, small_ref, hg_ref, sum_ref, r1_ref, w_ref, *scratch, swap
):
    w_attn, middle, inner, mlp, back, grads, segment, load_sem = scratch[:8]
    step = pl.program_id(0)
    steps = pl.num_programs(0)
    quarter = turn_of(step)
    units = wb_ref.shape[2] // 2
    skip = wa_ref.shape[2] - units
    z = s_ref[0]
    core = s_ref[1]
    load = pltpu.make_async_copy(pack_ref.at[:, :, :skip], w_attn, load_sem.at[0])

    def alive():
        return jnp.where(segment[:, 0:1] != 0.0, 1.0, 0.0)

    if swap:
        away, got, send_sem, recv_sem, f_send, f_recv, w_send, w_recv = scratch[8:]
        p = Place()
        core, z = p.core, p.z
        other = (p.at_c, z)
        chain = Chain(
            p, lambda q, i: grads.at[q, i], None, None, None, None, f_send, f_recv
        )

        beside = (p.dp, p.z + 1 - 2 * (p.z % 2))

        def weight_copy(i):
            src, device = ((qkv_ref, beside), (qkv_ref, other), (w_ref.at[1], other))[i]
            return remote(src, w_ref.at[i + 1], w_send.at[i], w_recv.at[i], device)

        def weight_own():
            return pltpu.make_async_copy(qkv_ref, w_ref.at[0], w_send.at[3])

        @pl.when(step == 0)
        def _():
            barrier = pltpu.get_barrier_semaphore()
            for device in (other, (p.at_x, p.z), (p.at_y, p.z), beside):
                pl.semaphore_signal(barrier, inc=1, device_id=device, device_id_type=MESH)
            pl.semaphore_wait(barrier, 4)
            weight_copy(0).start()
            weight_copy(1).start()
            weight_own().start()

        def give(i):
            return remote(
                away.at[i % 2], got.at[i % 2], send_sem.at[i % 2], recv_sem.at[i % 2], other
            )

        def stage1(i, slot):
            q = DONE[i]
            at = i * 2 + slot
            return remote(
                grads.at[q, chain.slab(q, slot, True)], r1_ref.at[i, slot],
                f_send.at[at], f_recv.at[at], chain.near(q),
            )

        def take(i):
            q = turn_of(i)
            give(i).wait_recv()
            for d in range(grads.shape[1]):
                grads[q, d] += got[i % 2, d]
            pltpu.make_async_copy(grads.at[q], sum_ref.at[q], load_sem.at[1 + i]).start()
            for j in range(len(DONE)):

                @pl.when(i == j)
                def _(j=j):
                    stage1(j, 0).start()
                    stage1(j, 1).start()

    @pl.when(step == 0)
    def _():
        load.start()
        load_live = pltpu.make_async_copy(live_ref.at[z], segment, load_sem.at[1 + WAYS])
        load_live.start()
        tokens = x_ref[...].astype(F32)
        attn_out = jnp.zeros(tokens.shape, F32)
        load_live.wait()
        load.wait()
        for m in range(WAYS):
            o = jnp.concatenate([heads_ref[m, 0], heads_ref[m, 1]], axis=-1)
            attn_out += dot_nn(o, side_by_side(w_attn, z ^ m))
        total = tokens + attn_out
        vhat, unused = norm_stats(total)
        middle[...] = total
        inner[...] = (vhat * gain_ref[...]).astype(BF)
        live = alive()
        lane = lax.broadcasted_iota(jnp.int32, (1, tokens.shape[1]), 1)
        sums = jnp.where(lane == 4, jnp.sum(live), 0.0)
        for i, values in enumerate((tokens, attn_out, total)):
            sums = jnp.where(lane == i, jnp.sum(live * values * values), sums)
        small_ref[...] = jnp.zeros_like(small_ref)
        small_ref[2:3, :] = sums

    w_act = side_by_side(wa_ref, 0, slice(skip, skip + units))
    w_lin = side_by_side(wb_ref, 0, slice(0, units))
    w_out = side_by_side(wb_ref, 0, slice(units, 2 * units))
    x = inner[...]
    grad = g_ref[...]
    act_in = dot_nt(w_act, x)
    linear = dot_nt(w_lin, x)
    hidden_grad = dot_nt(w_out, grad)
    cdf = 0.5 * (1.0 + lax.erf(act_in * (2.0**-0.5)))
    act = act_in * cdf
    slope = cdf + act_in * jnp.exp(-0.5 * act_in * act_in) * ((2.0 * math.pi) ** -0.5)
    hidden = (act * linear).astype(BF)
    d_act = (hidden_grad * linear * slope).astype(BF)
    d_lin = (hidden_grad * act).astype(BF)
    if swap:
        pl.when(step >= 1)(lambda: take(step - 1))
        pl.when(step >= 2)(lambda: give(step - 2).wait_send())

        @pl.when(step == steps - 1)
        def _():
            weight_copy(0).wait_recv()
            weight_copy(2).start()

    x_mine = own_first(core, x)
    g_mine = own_first(core, grad)
    pieces = (dot_nn(d_act, x_mine), dot_nn(d_lin, x_mine), dot_nn(hidden, g_mine))
    for part, value in enumerate(pieces):
        some = slice(part * units, (part + 1) * units)
        value = value.astype(BF)
        for d in range(value.shape[1] // LANES):
            slab = value[:, d * LANES : (d + 1) * LANES]
            if not swap:
                sum_ref[quarter, d // 2, d % 2, some] = slab
            elif d % 2:
                away[step % 2, d // 2, some] = slab
            else:
                grads[quarter, d // 2, some] = slab
    if swap:
        give(step).start()
    more_mlp = dot_tn(hidden, w_out)
    more_back = dot_tn(d_act, w_act) + dot_tn(d_lin, w_lin)

    @pl.when(step == 0)
    def _():
        mlp[...] = more_mlp
        back[...] = more_back

    @pl.when(step > 0)
    def _():
        mlp[...] += more_mlp
        back[...] += more_back

    @pl.when(step == steps - 1)
    def _():
        vhat, scale = norm_stats(middle[...])
        into = back[...]
        middle_grad = g_ref[...].astype(F32) + norm_back(vhat, scale, gain_ref[...], into)
        low = middle_grad.astype(BF)
        for m in range(WAYS):
            hg = dot_nt(low, side_by_side(w_attn, z ^ m)).astype(BF)
            hg_ref[m, 0] = hg[:, :LANES]
            hg_ref[m, 1] = hg[:, LANES:]
        mgrad_ref[...] = middle_grad
        low_ref[...] = low
        out = mlp[...]
        output_ref[...] = (middle[...] + out).astype(BF)
        lane = lax.broadcasted_iota(jnp.int32, (1, out.shape[1]), 1)
        square = jnp.sum(alive() * out * out)
        small_ref[2:3, :] = jnp.where(lane == 3, square, small_ref[2:3, :])
        small_ref[1:2, :] = jnp.sum(into * vhat, axis=0, keepdims=True)
        if swap:
            take(step)
            give(step - 1).wait_send()
            give(step).wait_send()
            for i in range(WAYS):
                q = turn_of(i)
                pltpu.make_async_copy(grads.at[q], sum_ref.at[q], load_sem.at[1 + i]).wait()
            for i in range(len(DONE)):
                for slot in range(2):
                    stage1(i, slot).wait()
            weight_copy(0).wait_send()
            weight_copy(1).wait()
            weight_copy(2).wait()
            weight_own().wait()


def mlp_call(scalars, heads, x, grad, gain, live, pack_a, pack_b, qkv, swap):
    tokens, model = x.shape
    wide, quarters, depth_a, unused = pack_a.shape
    units = pack_b.shape[2] // 2
    depth = model // WAYS
    out = (quarters, wide // 2) + (() if swap else (2,)) + (3 * units, LANES)
    whole = pl.BlockSpec(memory_space=pltpu.VMEM)
    anywhere = pl.BlockSpec(memory_space=pl.ANY)
    weight = lambda rows: pl.BlockSpec((wide, 1, rows, LANES), lambda i, s: (0, turn_of(i), 0, 0))
    sems = lambda *shape: pltpu.SemaphoreType.DMA(shape)
    scratch = [
        pltpu.VMEM((wide, quarters, depth, LANES), BF),
        pltpu.VMEM((tokens, model), F32),
        pltpu.VMEM((tokens, model), BF),
        pltpu.VMEM((tokens, model), F32),
        pltpu.VMEM((tokens, model), F32),
        pltpu.VMEM(out if swap else (8, LANES), BF),
        pltpu.VMEM((tokens, LANES), F32),
        sems(2 + WAYS),
    ]
    if swap:
        scratch += [pltpu.VMEM((2,) + out[1:], BF)] * 2
        scratch += [sems(2), sems(2), sems(6), sems(6), sems(4), sems(3)]
    r1 = (len(DONE), 2, 3 * units, LANES) if swap else (8, LANES)
    spec = pltpu.PrefetchScalarGridSpec(
        num_scalar_prefetch=1,
        grid=(quarters,),
        in_specs=[whole] * 4 + [anywhere] * 3 + [weight(depth_a), weight(2 * units)],
        out_specs=[whole] * 5 + [anywhere if swap else whole, anywhere, anywhere],
        scratch_shapes=scratch,
    )
    extra = dict(collective_id=1, has_side_effects=True) if swap else {}
    return pl.pallas_call(
        functools.partial(mlp_kernel, swap=swap),
        grid_spec=spec,
        out_shape=[
            shape_of((tokens, model), BF),
            shape_of((tokens, model), F32),
            shape_of((tokens, model), BF),
            shape_of((8, model), F32),
            shape_of((WAYS, depth // LANES, tokens, LANES), BF),
            shape_of(out, BF),
            shape_of(r1, BF),
            shape_of((WAYS,) + qkv.shape if swap else (8, LANES), BF),
        ],
        compiler_params=pltpu.CompilerParams(vmem_limit_bytes=62 * 1024 * 1024, **extra),
        cost_estimate=cost(22 * tokens * model * units * quarters, 40),
        name="mlp",
    )(scalars, heads, x, grad, gain, live, pack_a, qkv, pack_a, pack_b)


def backward_kernel(
    hg_ref, sum_ref, r1_ref, normed_ref, w_ref, x_ref, mgrad_ref, low_ref, heads_ref,
    qa, ka, v, o, cosine, sine, gain_ref, small_ref,
    grad_ref, inner_ref, outer_ref, attn_ref, qkv_ref, gain_a_ref, gain_m_ref, rms_ref,
    do_ref, low, va, kt, dk, dv, normed, weight, x_in,
    f_kept0, f_r10, f_r20, f_rz0, f_kept1, f_r11, f_r21, f_rz1,
    a_sum, a_got, a_r1, a_r2, a_rz,
    q_sum, q_rx, q_ry, q_rz, ret, s_own, s_dp, s_mp,
    load_sem, do_send, do_recv, f_send, f_recv, a_send, a_recv, c_send, c_recv,
    q_send, q_recv, g_send, g_recv, s_send, s_recv,
):
    p = Place()
    dp, z, core = p.dp, p.z, p.core
    rows = x_ref.shape[0]
    pairs = v.shape[0]
    k = Back((qa, ka, v, o, cosine, sine, low, va, kt, dk, dv))

    def qkv_to(turn):
        a, b = dp - core + (p.group + turn) % 2, p.quarter
        return a, b, p.stays(a, b)

    def qkv_from(g):
        a, b = dp - core + (z // 2 + g) % 2, 2 * g + z % 2
        return a, b, p.stays(a, b)

    def other_dp(turn):
        return (dp + turn) % 8, z

    def other_mp(turn):
        return dp, (z + turn) % WAYS

    barrier = pltpu.get_barrier_semaphore()
    count = jnp.int32(0)

    def greet(device, skip=None):
        def signal():
            pl.semaphore_signal(barrier, inc=1, device_id=device, device_id_type=MESH)

        if skip is None:
            signal()
            return 1
        pl.when(jnp.logical_not(skip))(signal)
        return 1 - skip.astype(jnp.int32)

    for turn in range(1, 8):
        count += greet(other_dp(turn))
    for turn in range(1, WAYS):
        count += greet(other_mp(turn))
    for m in range(WAYS):
        for a, b, stays in (p.attention_of(m), p.owner_of(m)):
            count += greet((a, b), stays)
    for i in range(2):
        for a, b, stays in (qkv_to(i), qkv_from(i)):
            count += greet((a, b), stays)
    pl.semaphore_wait(barrier, count)

    def head_grad(m, pair, place):
        return Move(
            hg_ref.at[m, pair], do_ref.at[m, pair], do_send.at[m, pair], do_recv.at[m, pair], place
        )

    for pair in range(pairs):
        for m in range(WAYS):
            head_grad(m, pair, p.attention_of(m)).start()

    def half(h):
        kept, r1, r2, rz = ((f_kept0, f_r10, f_r20, f_rz0), (f_kept1, f_r11, f_r21, f_rz1))[h]
        some = pl.ds(h * f_kept0.shape[2], kept.shape[2])
        return Chain(
            p, lambda q, i: sum_ref.at[q, i, some], lambda q, slot, i: kept.at[q, slot],
            r1, r2, rz, f_send.at[h], f_recv.at[h],
        )

    ffn = [half(0), half(1)]
    loads = []

    def load(src, dst):
        copy = pltpu.make_async_copy(src, dst, load_sem.at[len(loads)])
        copy.start()
        loads.append(copy)
        return copy

    def fetch(h, q):
        kept, r1 = (f_kept0, f_r10) if h == 0 else (f_kept1, f_r11)
        some = pl.ds(h * f_kept0.shape[2], kept.shape[2])
        copies = []
        for slot in range(2):
            copies.append(load(sum_ref.at[q, ffn[h].slab(q, slot, False), some], kept.at[q, slot]))
        if q in DONE:
            copies.append(load(r1_ref.at[DONE.index(q), :, some], r1.at[q]))
        return copies

    fetched = {(h, q): fetch(h, q) for q in (0, 2, 1, 3) for h in range(2)}

    def second(h, q):
        for copy in fetched[h, q]:
            copy.wait()
        ffn[h].second(q, q in DONE)

    def third(h, *quarters):
        for q in quarters:
            ffn[h].third(q)

    def line(h, hop, *quarters):
        ffn[h].line(hop, quarters)

    for h in range(2):
        second(h, 0)
        second(h, 2)
        ffn[h].first(1)
        ffn[h].first(3)
    low_load = load(low_ref, x_in)
    late = [load(normed_ref, normed), load(w_ref, weight)]
    late.append(load(mgrad_ref, grad_ref))

    low_load.wait()
    low_here = own_first(core, x_in[...])
    for m in range(WAYS):
        mixed = jnp.concatenate([heads_ref[m, 0], heads_ref[m, 1]], axis=-1)
        value = dot_tn(mixed, low_here).astype(BF)
        h = p.mix(z, m)
        for d in range(value.shape[1] // LANES):
            a_sum[d % 2, h, d // 2] = value[:, d * LANES : (d + 1) * LANES]
    late.append(load(x_ref, x_in))
    swap = remote(a_sum.at[1], a_got, c_send.at[0], c_recv.at[0], (p.at_c, z))
    swap.start()
    attn_back_begin(0, k)
    swap.wait()
    for q in range(WAYS):
        a_sum[0, q] += a_got[q]
    attn = Chain(
        p, lambda q, i: a_sum.at[0, q, i], lambda q, slot, i: a_sum.at[0, q, i],
        a_r1, a_r2, a_rz, a_send, a_recv,
    )
    for q in range(WAYS):
        attn.first(q)

    def qkv_x(pair, yy):
        at = (p.y if yy else 1 - p.y) * 4 + (1 - p.x) * 2
        return remote(
            q_sum.at[pair, pl.ds(at, 2)], q_rx.at[pair, yy],
            q_send.at[pair, yy], q_recv.at[pair, yy], (p.at_x, z),
        )

    def qkv_y(pair):
        at = (1 - p.y) * 4 + p.x * 2
        return remote(
            q_sum.at[pair, pl.ds(at, 2)], q_ry.at[pair],
            q_send.at[pair, 2], q_recv.at[pair, 2], (p.at_y, z),
        )

    def qkv_z(pair, turn, g, place):
        at = p.y * 4 + p.x * 2 + (p.group + turn) % 2
        return Move(
            q_sum.at[pair, at], q_rz.at[pair, g],
            q_send.at[pair, 3 + turn], q_recv.at[pair, 3 + g], place,
        )

    def qkv_first(pair):
        total = None
        for m in range(WAYS):
            part = dot_tn(low_piece(pair, m, k, rows), normed[m * rows : (m + 1) * rows, :])
            total = part if total is None else total + part
        value = total.astype(BF)
        for d in range(value.shape[1] // LANES):
            q_sum[pair, d] = value[:, d * LANES : (d + 1) * LANES]
        qkv_x(pair, 0).start()
        qkv_x(pair, 1).start()

    def qkv_second(pair):
        qkv_x(pair, 0).wait_recv()
        at = (1 - p.y) * 4 + p.x * 2
        for i in range(2):
            q_sum[pair, at + i] += q_rx[pair, 0, i]
        qkv_y(pair).start()
        qkv_x(pair, 1).wait_recv()
        at = p.y * 4 + p.x * 2
        for i in range(2):
            q_sum[pair, at + i] += q_rx[pair, 1, i]

    def qkv_third(pair):
        qkv_y(pair).wait_recv()
        at = p.y * 4 + p.x * 2
        for i in range(2):
            q_sum[pair, at + i] += q_ry[pair, i]
        for turn in range(2):
            qkv_z(pair, turn, p.group, qkv_to(turn)).start()

    def give_back(pair, m, part, place):
        some = pl.ds(m * rows, rows)
        if part == 0:
            src, dst = low.at[pair, 0, some], ret.at[m, pair, 0]
        else:
            src, dst = low.at[pair, pl.ds(1, 2), some], ret.at[m, pair, pl.ds(1, 2)]
        return Move(src, dst, g_send.at[m, pair, part], g_recv.at[m, pair, part], place)

    def finish_pair(pair):
        for m in range(WAYS):
            attn_back_end(pair, m, k, rows)
            give_back(pair, m, 1, p.owner_of(m)).start()

    def pair_end():
        finish_pair(0)
        attn_back_begin(1, k)
        for copy in late:
            copy.wait()
        qkv_first(0)

    every = range(WAYS)
    events = {
        1: [(third, 0, 0, 2), (line, 0, 1, 0, 2)],
        2: [(third, 1, 0, 2), (line, 1, 1, 0, 2)],
        3: [(line, 0, 2, 0, 2)],
        4: [(attn.second, q) for q in every],
        5: [(second, 0, 1), (second, 0, 3), (line, 1, 2, 0, 2)],
        6: [(line, 0, 3, 0, 2)] + [(attn.third, q) for q in every] + [(attn.line, 1, every)],
        7: [(line, 1, 3, 0, 2), (attn.line, 2, every)],
        8: [(second, 1, 1), (second, 1, 3), (attn.line, 3, every), (pair_end,)],
        9: [(third, 0, 1, 3), (line, 0, 1, 1, 3)],
        10: [(qkv_second, 0)],
        11: [(line, 0, 2, 1, 3), (third, 1, 1, 3), (line, 1, 1, 1, 3)],
        12: [(qkv_third, 0)],
        13: [(line, 0, 3, 1, 3), (line, 1, 2, 1, 3)],
        15: [(line, 1, 3, 1, 3)],
    }
    steps = v.shape[1] // STEP
    per = rows // STEP

    def body(i, carry):
        for at, todo in events.items():

            @pl.when(i == at)
            def _(todo=todo):
                for what, *args in todo:
                    what(*args)

        pair, step = i // steps, i % steps
        m = step // per

        @pl.when(step % per == 0)
        def _():
            head_grad(m, pair, p.owner_of(0)).wait_recv()

        at = pl.multiple_of((step - m * per) * STEP, STEP)
        attn_back_step(pair, step, do_ref[m, pair, pl.ds(at, STEP), :], k)

        @pl.when(step % per == per - 1)
        def _():
            give_back(pair, m, 0, p.owner_of(m)).start()

        return carry

    lax.fori_loop(0, pairs * steps, body, 0)
    finish_pair(1)
    qkv_first(1)

    def normed_part(pair, m):
        slot = p.mix(m, 2 * core)
        at = pair * 3 * LANES
        w = [weight[slot, d, at : at + 3 * LANES, :] for d in range(weight.shape[1])]
        grads = jnp.concatenate([ret[m, pair, c] for c in range(3)], axis=-1)
        return dot_nn(grads, jnp.concatenate(w, axis=-1))

    normed_grad = None
    for m in range(WAYS):
        for part in range(2):
            give_back(0, m, part, p.attention_of(m)).wait_recv()
        add = normed_part(0, m)
        normed_grad = add if normed_grad is None else normed_grad + add
    qkv_second(1)
    depth = a_r2.shape[1]
    attn.last(dv.at[:depth])
    attn_ref[...] = dv[:depth, :].T
    qkv_third(1)
    cut = f_kept0.shape[2]
    units = outer_ref.shape[1]
    ffn[0].last(dk.at[:cut])
    ffn[1].last(dk.at[cut : 3 * units])
    inner_ref[0] = dk[:units, :].T
    inner_ref[1] = dk[units : 2 * units, :].T
    outer_ref[...] = dk[2 * units : 3 * units, :].T
    vhat, scale = norm_stats(x_in[...].astype(F32))
    for pair in range(pairs):
        for g in range(2):
            qkv_z(pair, 0, g, qkv_from(g)).wait_recv()
        total = q_rz[pair, 0].astype(F32) + q_rz[pair, 1].astype(F32)
        for c in range(3):
            part = total[c * LANES : (c + 1) * LANES, :]
            qkv_ref[c, :, pair * LANES : (pair + 1) * LANES] = part.T
    for m in range(WAYS):
        for part in range(2):
            give_back(1, m, part, p.attention_of(m)).wait_recv()
        normed_grad += normed_part(1, m)
    gain_part = jnp.sum(normed_grad * vhat, axis=0, keepdims=True)
    s_own[...] = jnp.concatenate([gain_part, small_ref[1:, :]], axis=0)

    def sum_dp(turn):
        return remote(
            s_own, s_dp.at[turn], s_send.at[turn], s_recv.at[turn], other_dp(turn)
        )

    def sum_mp(turn):
        return remote(
            s_dp.at[0], s_mp.at[turn], s_send.at[8 + turn], s_recv.at[8 + turn], other_mp(turn)
        )

    for turn in range(1, 8):
        sum_dp(turn).start()
    grad_ref[...] += norm_back(vhat, scale, gain_ref[...], normed_grad)
    total = s_own[...]
    for turn in range(1, 8):
        sum_dp(turn).wait_recv()
        total += s_dp[turn]
    s_dp[0] = total
    for turn in range(1, WAYS):
        sum_mp(turn).start()
    for turn in range(1, WAYS):
        sum_mp(turn).wait_recv()
        total += s_mp[turn]
    gain_a_ref[...] = total[0:1, :]
    gain_m_ref[...] = total[1:2, :]
    squares = total[2:3, :LANES]
    lane = lax.broadcasted_iota(jnp.int32, squares.shape, 1)
    count = jnp.sum(jnp.where(lane == 4, squares, 0.0)) * x_ref.shape[1]
    rms_ref[...] = jnp.sqrt(squares / count)

    for turn in range(1, 8):
        sum_dp(turn).wait_send()
    for turn in range(1, WAYS):
        sum_mp(turn).wait_send()
    for m in range(WAYS):
        for pair in range(pairs):
            for part in range(2):
                give_back(pair, m, part, p.owner_of(m)).wait_send()
    for m in range(WAYS):
        for pair in range(pairs):
            head_grad(m, pair, p.attention_of(m)).wait_send()
    for pair in range(pairs):
        qkv_x(pair, 0).wait_send()
        qkv_x(pair, 1).wait_send()
        qkv_y(pair).wait_send()
        for turn in range(2):
            qkv_z(pair, turn, p.group, qkv_to(turn)).wait_send()
    ffn[0].finish(DONE)
    ffn[1].finish(DONE)
    attn.finish()


def backward_call(heads_grad, ffn_sum, r1, kept, weight, x, middle_grad, low, heads, gain, small):
    normed, cosine, sine, qa, ka, v, o = kept
    rows, model = x.shape
    pairs, tokens, unused = v.shape
    unused, wide, cols3, unused = weight.shape
    units = ffn_sum.shape[2]
    depth = model // WAYS
    third = cols3 // pairs
    part = (units // 32 + 1) * 16
    anywhere = pl.BlockSpec(memory_space=pl.ANY)
    vmem = pl.BlockSpec(memory_space=pltpu.VMEM)
    buf = lambda *shape, kind=BF: pltpu.VMEM(shape, kind)
    sems = lambda *shape: pltpu.SemaphoreType.DMA(shape)
    return pl.pallas_call(
        backward_kernel,
        in_specs=[anywhere] * 8 + [vmem] * 9,
        out_specs=[vmem] * 8,
        out_shape=[
            shape_of((rows, model), F32),
            shape_of((2, LANES, units // 3), F32),
            shape_of((LANES, units // 3), F32),
            shape_of((LANES, depth), F32),
            shape_of((3, LANES, pairs * LANES), F32),
            shape_of((1, model), F32),
            shape_of((1, model), F32),
            shape_of((1, LANES), F32),
        ],
        scratch_shapes=[
            buf(WAYS, pairs, rows, LANES),
            buf(pairs, 3, tokens, LANES),
            buf(2, tokens, LANES),
            buf(2, LANES, tokens),
            buf(tokens, LANES, kind=F32),
            buf(tokens, LANES, kind=F32),
            buf(tokens, model),
            buf(WAYS, wide, cols3, LANES),
            buf(rows, model),
            *[
                buf(*lead, cut, LANES)
                for cut in (part, units - part)
                for lead in ((WAYS, 2), (WAYS, 2), (WAYS,), (WAYS + 1,))
            ],
            buf(2, WAYS, wide // 2, depth, LANES),
            buf(WAYS, wide // 2, depth, LANES),
            buf(WAYS, 2, depth, LANES),
            buf(WAYS, depth, LANES),
            buf(WAYS + 1, depth, LANES),
            buf(pairs, wide, third, LANES),
            buf(pairs, 2, 2, third, LANES),
            buf(pairs, 2, third, LANES),
            buf(pairs, 2, third, LANES),
            buf(WAYS, pairs, 3, rows, LANES),
            buf(*small.shape, kind=F32),
            buf(8, *small.shape, kind=F32),
            buf(WAYS, *small.shape, kind=F32),
            sems(27),
            sems(WAYS, pairs),
            sems(WAYS, pairs),
            sems(2, 16),
            sems(2, 17),
            sems(16),
            sems(17),
            sems(1),
            sems(1),
            sems(pairs, 5),
            sems(pairs, 5),
            sems(WAYS, pairs, 2),
            sems(WAYS, pairs, 2),
            sems(12),
            sems(12),
        ],
        compiler_params=pltpu.CompilerParams(
            collective_id=2, has_side_effects=True, vmem_limit_bytes=62 * 1024 * 1024
        ),
        name="backward",
    )(
        heads_grad, ffn_sum, r1, normed, weight, x, middle_grad, low, heads,
        qa, ka, v, o, cosine, sine, gain, small,
    )


def pick(values, at, axis=0):
    return lax.dynamic_index_in_dim(values, at, axis, keepdims=False)


def flip(values, bit, dps):
    return lax.ppermute(values, "dp", [(i, i ^ bit) for i in range(dps)])


def to_attention(values, m, dps, back=False):
    pairs = []
    for dp in range(dps):
        group = dp % 2
        for t in range(WAYS):
            quarter = t ^ m
            there = (dp - group + ((quarter // 2) ^ group)) * WAYS + 2 * group + quarter % 2
            pairs.append((there, dp * WAYS + t) if back else (dp * WAYS + t, there))
    return lax.ppermute(values, ("dp", "mp"), pairs)


def local(
    sizes,
    layer_input,
    segment_ids,
    grad_out,
    qkv_weight,
    attn_weight,
    inner_weight,
    outer_weight,
    attn_gain,
    mlp_gain,
):
    dps, mps = sizes
    rows, model = layer_input.shape
    head_cols = qkv_weight.shape[2]
    units = inner_weight.shape[2]
    pairs = head_cols // LANES
    wide = model // LANES
    special = dps == wide
    me = lax.axis_index("mp")
    dp = lax.axis_index("dp")
    core = dp % 2
    group = me // 2
    quarter = me ^ (2 * core)
    scalars = jnp.stack([me, core if special else 0, quarter]).astype(jnp.int32)

    def every(values):
        got = lax.all_gather(values.T, "dp", axis=0, tiled=True).T
        got = got.reshape(-1, wide, LANES).transpose(1, 0, 2)
        return lax.all_gather(got, "mp", axis=1)

    qkv_part = qkv_weight.transpose(1, 2, 0).reshape(3, pairs, LANES, -1)
    qkv_part = qkv_part.transpose(1, 0, 2, 3).reshape(3 * head_cols, -1)
    inner_t = inner_weight.transpose(1, 2, 0)
    outer_t = outer_weight.T
    attn_depth = model // mps
    part_a = jnp.concatenate([attn_weight.T, inner_t[0]], axis=0)
    part_b = jnp.concatenate([inner_t[1], outer_t], axis=0)
    mine = segment_ids[0]
    info = jnp.broadcast_to(mine.astype(F32)[:, None], (mine.shape[0], LANES))
    info = info.reshape(WAYS, rows, LANES)
    if special:
        (pack_a, pack_b), heads, qkv_own, kept = forward_call(
            layer_input, info, attn_gain[None], qkv_part, [part_a, part_b], dps, pairs
        )
    else:
        x_all = jnp.stack([to_attention(layer_input, m, dps) for m in range(WAYS)])
        qkv_all, pack_a, pack_b = every(qkv_part), every(part_a), every(part_b)
        info = jnp.where(group == core, info, flip(info, 1, dps))
        qkv_own = qkv_all
        kept = alone_call(
            quarter, x_all, info, attn_gain[None], pick(qkv_all, quarter, 1), pairs)
        heads = kept[6].reshape(pairs, WAYS, rows, LANES)
        heads = [to_attention(heads[:, m], m, dps, back=True) for m in range(WAYS)]
        heads = jnp.stack(heads)
    normed, cosine, sine, qa, ka, v, o = kept

    outs = mlp_call(
        scalars, heads, layer_input, grad_out, mlp_gain[None], info, pack_a, pack_b,
        qkv_own, special,
    )
    layer_output, middle_grad, middle_low, small, heads_grad, ffn_sum, ffn_got, qkv_whole = outs
    if special:
        input_grad, inner_sum, outer_sum, attn_sum, qkv_sum, gain_a, gain_m, rms = backward_call(
            heads_grad, ffn_sum, ffn_got, kept, qkv_whole, layer_input, middle_grad, middle_low, heads,
            attn_gain[None], small,
        )
        return (
            layer_output,
            input_grad,
            qkv_sum.transpose(1, 0, 2),
            attn_sum,
            inner_sum.transpose(1, 0, 2),
            outer_sum,
            gain_a[0],
            gain_m[0],
            rms[0, :4],
        )
    else:
        lows = []
        for pair in range(pairs):
            grad = [to_attention(heads_grad[m, pair], m, dps) for m in range(WAYS)]
            low = attn_bwd_call(scalars, qa, ka, v, grad, o, cosine, sine, pair)
            lows.append(jnp.concatenate(low, axis=0))
        low = jnp.concatenate(lows, axis=1)
        own = pick(qkv_all, quarter, 1)
        own = jnp.concatenate([own[d] for d in range(wide)], axis=-1)
        normed_grad = dot_nn(low, own).astype(BF).reshape(WAYS, rows, model)
        normed_grad = sum(
            to_attention(normed_grad[m], m, dps, back=True).astype(F32) for m in range(WAYS)
        )

        def scatter(values):
            cut = lax.psum_scatter(values, "mp", scatter_dimension=0)
            return lax.psum_scatter(cut.T, "dp", scatter_dimension=0, tiled=True).T

        slot = (jnp.arange(mps) == quarter)[:, None, None]
        qkv_sum = scatter(jnp.where(slot, dot_tn(low, normed)[None], 0.0))
        mixed = jnp.stack([pick(heads, me ^ h) for h in range(mps)])
        mixed = mixed.transpose(0, 2, 1, 3).reshape(mps, rows, -1)
        attn_sum = scatter(jnp.stack([dot_tn(mixed[h], middle_low) for h in range(mps)]))
        ffn_sum = ffn_sum.reshape(mps, wide, 3 * units, LANES).transpose(0, 2, 1, 3)
        ffn_sum = scatter(ffn_sum.reshape(mps, 3 * units, model).astype(F32))
        vhat, scale = norm_stats(layer_input.astype(F32))
        input_grad = middle_grad + norm_back(vhat, scale, attn_gain, normed_grad)
        small = small.at[0].set(jnp.sum(normed_grad * vhat, axis=0))
        small = lax.psum(small, ("dp", "mp"))
    rms_values = jnp.sqrt(small[2, :4] / (small[2, 4] * model))

    qkv_sum = qkv_sum.reshape(pairs, 3, LANES, -1).transpose(3, 1, 0, 2)
    ffn_sum = ffn_sum.reshape(3, units, -1)
    return (
        layer_output,
        input_grad,
        qkv_sum.reshape(-1, 3, head_cols),
        attn_sum.T,
        ffn_sum[:2].transpose(2, 0, 1),
        ffn_sum[2].T,
        small[0],
        small[1],
        rms_values,
    )


def solution(mesh):
    sizes = (mesh.shape["dp"], mesh.shape["mp"])
    both = ("dp", "mp")
    whole = (P(both, None), P("dp", None, "mp"), P("dp", "mp"))
    return jax.shard_map(
        functools.partial(local, sizes),
        mesh=mesh,
        in_specs=(
            whole[0],
            P("dp", None),
            whole[0],
            whole[1],
            whole[2],
            whole[1],
            whole[2],
            P(),
            P(),
        ),
        out_specs=(
            whole[0],
            whole[0],
            whole[1],
            whole[2],
            whole[1],
            whole[2],
            P(),
            P(),
            P(),
        ),
        check_vma=False,
    )
```

```python
import functools
import math

import jax
import jax.numpy as jnp
from jax import lax
from jax.experimental import pallas as pl
from jax.experimental.pallas import tpu as pltpu
from jax.sharding import PartitionSpec as P

HEAD_DIM = 64
NORM_EPS = 1e-05
ROPE_BASE = 160000.0
BIG = 1e30
LANES = 128
WAYS = 4
BF = jnp.bfloat16
F32 = jnp.float32
VMEM_LIMIT = 56 * 1024 * 1024


def dot_nn(a, b):
    return lax.dot_general(a, b, (((1,), (0,)), ((), ())), preferred_element_type=F32)


def dot_nt(a, b):
    return lax.dot_general(a, b, (((1,), (1,)), ((), ())), preferred_element_type=F32)


def dot_tn(a, b):
    return lax.dot_general(a, b, (((0,), (0,)), ((), ())), preferred_element_type=F32)


def norm_stats(values):
    centre = jnp.mean(values, axis=-1, keepdims=True)
    shifted = values - centre
    spread = jnp.mean(shifted * shifted, axis=-1, keepdims=True)
    scale = lax.rsqrt(spread + NORM_EPS)
    return shifted * scale, scale


def norm_back(vhat, scale, gain, grad):
    u = grad * gain
    mean_u = jnp.mean(u, axis=-1, keepdims=True)
    mean_uv = jnp.mean(u * vhat, axis=-1, keepdims=True)
    return scale * (u - mean_u - vhat * mean_uv)


def swap_halves(values):
    lane = lax.broadcasted_iota(jnp.int32, values.shape, 1)
    first = lane % HEAD_DIM < HEAD_DIM // 2
    back = pltpu.roll(values, LANES - HEAD_DIM // 2, 1)
    ahead = pltpu.roll(values, HEAD_DIM // 2, 1)
    return jnp.where(first, back, ahead)


def choose(at, values):
    out = values[0]
    for i in range(1, len(values)):
        out = jnp.where(at == i, values[i], out)
    return out


def params():
    return pltpu.CompilerParams(vmem_limit_bytes=VMEM_LIMIT)


def cost(flops, mib):
    return pl.CostEstimate(flops=int(flops), bytes_accessed=int(mib * 2**20), transcendentals=0)


def call(kernel, scalars, grid, in_specs, out_specs, out_shape, scratch, estimate, name):
    spec = pltpu.PrefetchScalarGridSpec(
        num_scalar_prefetch=1,
        grid=grid,
        in_specs=in_specs,
        out_specs=out_specs,
        scratch_shapes=scratch,
    )
    return functools.partial(
        pl.pallas_call(
            kernel,
            grid_spec=spec,
            out_shape=out_shape,
            compiler_params=params(),
            cost_estimate=estimate,
            name=name,
        ),
        scalars,
    )


def full(shape):
    return pl.BlockSpec(shape, lambda i, s: (0,) * len(shape))


def shape_of(shape, dtype):
    return jax.ShapeDtypeStruct(shape, dtype)


def side_by_side(ref, *at):
    return jnp.concatenate([ref[(d, *at)] for d in range(ref.shape[0])], axis=-1)


STEP = 256


def doc_starts(pieces):
    number = lax.broadcasted_iota(jnp.int32, (1, LANES), 1).astype(F32)
    total = jnp.zeros((1, LANES), F32)
    for piece in pieces:
        before = jnp.logical_and(piece > 0.0, piece < number)
        total += jnp.sum(jnp.where(before, 1.0, 0.0), axis=0, keepdims=True)
    return total


def table_piece(m, segment, first, starts, out):
    rows = segment.shape[0]
    here = slice(m * rows, (m + 1) * rows)
    number = lax.broadcasted_iota(jnp.int32, (1, LANES), 1).astype(F32)
    start = jnp.sum(jnp.where(segment == number, starts, 0.0), axis=-1, keepdims=True)
    place = lax.broadcasted_iota(jnp.int32, (rows, 1), 0) + first
    position = place.astype(F32) - start
    lane = lax.broadcasted_iota(jnp.int32, (1, LANES), 1)
    half = HEAD_DIM // 2
    frequency = jnp.exp((lane % half).astype(F32) * (-2.0 * math.log(ROPE_BASE) / HEAD_DIM))
    angle = position * frequency
    sine = jnp.sin(angle)
    out.cosine[here, :] = jnp.cos(angle)
    out.sine[here, :] = jnp.where(lane % HEAD_DIM < half, -sine, sine)
    t = lane % HEAD_DIM
    same = segment == t.astype(F32)
    masked = jnp.where(same, 0.0, -BIG)
    out.qaux[here, :] = jnp.where(t >= 16, 0.0, masked).astype(BF)
    found = jnp.where(same, 1.0, 0.0)
    counted = jnp.where(t < 19, 1.0, 0.0)
    out.kaux[here, :] = jnp.where(t < 16, found, counted).astype(BF)
    out.live[here, :] = jnp.where(segment[:, 0:1] != 0.0, 1.0, 0.0)


def qkv_piece(m, x, gain, weight, out):
    rows = x.shape[0]
    here = slice(m * rows, (m + 1) * rows)
    vhat, unused = norm_stats(x.astype(F32))
    normed = (vhat * gain).astype(BF)
    out.normed[here, :] = normed
    flat = dot_nt(normed, weight)
    cosine, sine = out.cosine[here, :], out.sine[here, :]
    kaux = out.kaux[here, :]
    lane = lax.broadcasted_iota(jnp.int32, (rows, LANES), 1)
    for pair in range(flat.shape[1] // (3 * LANES)):
        q, k, v = [
            flat[:, at : at + LANES] for at in range(pair * 3 * LANES, (pair + 1) * 3 * LANES, LANES)
        ]
        q = (q * cosine + swap_halves(q) * sine).astype(BF)
        k = (k * cosine + swap_halves(k) * sine).astype(BF)
        out.q[pair, here, :] = q * jnp.asarray(HEAD_DIM**-0.5, BF)
        out.ka[pair, 0, here, :] = jnp.where(lane < HEAD_DIM, k, kaux)
        out.ka[pair, 1, here, :] = jnp.where(lane >= HEAD_DIM, k, kaux)
        out.v[pair, here, :] = v.astype(BF)


def attn_step(pair, step, out):
    tokens = out.v.shape[1]
    chunk = 512
    here = pl.ds(pl.multiple_of(step * STEP, STEP), STEP)
    lane = lax.broadcasted_iota(jnp.int32, (STEP, LANES), 1)
    t = lane % HEAD_DIM
    q = out.q[pair, here, :]
    qaux = out.qaux[here, :]
    live = out.live[here, :]
    outs = []
    for head in range(2):
        mine = (lane < HEAD_DIM) if head == 0 else (lane >= HEAD_DIM)
        qa = jnp.where(mine, q, qaux)
        top = None
        for at in range(0, tokens, chunk):
            s = dot_nt(qa, out.ka[pair, head, at : at + chunk, :])
            out.scores[:, at : at + chunk] = s
            part = jnp.max(s, axis=-1, keepdims=True)
            top = part if top is None else jnp.maximum(top, part)
        total = jnp.zeros((STEP, 1), F32)
        mixed = jnp.zeros((STEP, LANES), F32)
        for at in range(0, tokens, chunk):
            p = jnp.exp(out.scores[:, at : at + chunk] - top)
            total += jnp.sum(p, axis=-1, keepdims=True)
            mixed += dot_nn(p.astype(BF), out.v[pair, at : at + chunk, :])
        outs.append(mixed * (live / total))
        log_sum = jnp.where(live > 0, top + jnp.log(total), BIG)
        high = log_sum.astype(BF)
        rest = log_sum - high.astype(F32)
        mid = rest.astype(BF)
        low = (rest - mid.astype(F32)).astype(BF)
        aux = jnp.where(t == 16, -high, jnp.where(t == 17, -mid, jnp.where(t == 18, -low, qaux)))
        out.qa[pair, head, here, :] = jnp.where(mine, q, aux)
    out.o[pair, here, :] = jnp.where(lane < HEAD_DIM, outs[0], outs[1]).astype(BF)


class Kept:
    names = ("normed", "cosine", "sine", "qa", "ka", "v", "o", "q", "qaux", "kaux", "live", "scores")

    def __init__(self, refs):
        for name, ref in zip(self.names, refs):
            setattr(self, name, ref)


def kept_shapes(tokens, model, pairs):
    outs = [
        shape_of((tokens, model), BF),
        shape_of((tokens, LANES), F32),
        shape_of((tokens, LANES), F32),
        shape_of((pairs, 2, tokens, LANES), BF),
        shape_of((pairs, 2, tokens, LANES), BF),
        shape_of((pairs, tokens, LANES), BF),
        shape_of((pairs, tokens, LANES), BF),
    ]
    scratch = [
        pltpu.VMEM((pairs, tokens, LANES), BF),
        pltpu.VMEM((tokens, LANES), BF),
        pltpu.VMEM((tokens, LANES), BF),
        pltpu.VMEM((tokens, 1), F32),
        pltpu.VMEM((STEP, tokens), F32),
    ]
    return outs, scratch


def alone_kernel(quarter_ref, x_ref, info_ref, gain_ref, w_ref, *refs):
    out = Kept(refs)
    starts = doc_starts([info_ref[t] for t in range(WAYS)])
    for m in range(WAYS):
        t = quarter_ref[0] ^ m
        table_piece(m, info_ref[t], t * info_ref.shape[1], starts, out)
        qkv_piece(m, x_ref[m], gain_ref[...], side_by_side(w_ref), out)

    def body(step, carry):
        per = out.v.shape[1] // STEP
        attn_step(step // per, step % per, out)
        return carry

    lax.fori_loop(0, out.v.shape[0] * out.v.shape[1] // STEP, body, 0)


def alone_call(quarter, x, info, gain, weight, pairs):
    outs, scratch = kept_shapes(WAYS * x.shape[1], x.shape[2], pairs)
    return pl.pallas_call(
        alone_kernel,
        in_specs=[pl.BlockSpec(memory_space=pltpu.SMEM)]
        + [pl.BlockSpec(memory_space=pltpu.VMEM)] * 4,
        out_specs=[pl.BlockSpec(memory_space=pltpu.VMEM)] * len(outs),
        out_shape=outs,
        scratch_shapes=scratch,
        compiler_params=params(),
        name="forward",
    )(quarter.reshape(1), x, info, gain, weight)


def piece_block(m, rows, per):
    return pl.BlockSpec((rows, LANES), lambda i, s: (jnp.clip(i - per * m, 0, per - 1), 0))


def attn_bwd_kernel(s_ref, *refs):
    qa_ref, ka_ref, v_ref, o_ref, do_refs = refs[0], refs[1], refs[2], refs[3], refs[4:8]
    cosq_ref, sinq_ref, cosk_ref, sink_ref = refs[8:12]
    out_refs = refs[12:16]
    va_ref, kt_ref, dk_acc, dv_acc = refs[16:20]
    step = pl.program_id(0)
    rows = do_refs[0].shape[0]
    chunk = v_ref.shape[0] // WAYS
    per = chunk // rows
    piece = step // per
    lane_k = lax.broadcasted_iota(jnp.int32, (chunk, LANES), 1)
    lane = lax.broadcasted_iota(jnp.int32, (rows, LANES), 1)
    zero = jnp.zeros((), BF)

    @pl.when(step == 0)
    def _():
        ones = jnp.where(lane_k % HEAD_DIM < 3, jnp.ones((), BF), zero)
        for m in range(WAYS):
            some = slice(m * chunk, (m + 1) * chunk)
            v = v_ref[some, :]
            for head in range(2):
                mine = (lane_k < HEAD_DIM) if head == 0 else (lane_k >= HEAD_DIM)
                va_ref[head, some, :] = jnp.where(mine, v, ones)
                own = jnp.where(mine, ka_ref[head, some, :], zero).astype(F32)
                kt_ref[head, :, some] = own.T.astype(BF)
        dk_acc[...] = jnp.zeros_like(dk_acc)
        dv_acc[...] = jnp.zeros_like(dv_acc)

    grad = choose(piece, [r[...] for r in do_refs])
    out = o_ref[...]
    product = grad.astype(F32) * out.astype(F32)
    turned = jnp.zeros((LANES, rows), F32)
    for head in range(2):
        mine = (lane < HEAD_DIM) if head == 0 else (lane >= HEAD_DIM)
        delta = jnp.sum(jnp.where(mine, product, 0.0), axis=-1, keepdims=True)
        high = delta.astype(BF)
        rest = delta - high.astype(F32)
        mid = rest.astype(BF)
        low = (rest - mid.astype(F32)).astype(BF)
        t = lane % HEAD_DIM
        aux = jnp.where(t == 0, -high, jnp.where(t == 1, -mid, jnp.where(t == 2, -low, zero)))
        grad_aug = jnp.where(mine, grad, aux)
        grad_own = jnp.where(mine, grad, zero)
        qa = qa_ref[head]
        q_own = jnp.where(mine, qa, zero)
        for m in range(WAYS):
            some = slice(m * chunk, (m + 1) * chunk)
            prob = jnp.exp(dot_nt(ka_ref[head, some, :], qa))
            back = dot_nt(va_ref[head, some, :], grad_aug)
            score_grad = (prob * back).astype(BF)
            dv_acc[some, :] += dot_nn(prob.astype(BF), grad_own)
            dk_acc[some, :] += dot_nn(score_grad, q_own)
            turned += dot_nn(kt_ref[head, :, some], score_grad)
    dq = turned.T * (HEAD_DIM**-0.5)
    dq = (dq * cosq_ref[...] - swap_halves(dq) * sinq_ref[...]).astype(BF)
    for m in range(WAYS):

        @pl.when(piece == m)
        def _(m=m):
            here = pl.ds(pl.multiple_of((step - m * per) * rows, rows), rows)
            out_refs[m][here, :LANES] = dq

    @pl.when(step == pl.num_programs(0) - 1)
    def _():
        for m in range(WAYS):
            some = slice(m * chunk, (m + 1) * chunk)
            dk = dk_acc[some, :]
            dk = dk * cosk_ref[some, :] - swap_halves(dk) * sink_ref[some, :]
            out_refs[m][:, LANES : 2 * LANES] = dk.astype(BF)
            out_refs[m][:, 2 * LANES :] = dv_acc[some, :].astype(BF)


def attn_bwd_call(scalars, qa, ka, v, grad, o, cosine, sine, pair):
    tokens = v.shape[1]
    chunk = tokens // WAYS
    rows = 256
    per = chunk // rows
    moving = [piece_block(m, rows, per) for m in range(WAYS)]
    block = pl.BlockSpec((rows, LANES), lambda i, s: (i, 0))
    return call(
        attn_bwd_kernel,
        scalars,
        (tokens // rows,),
        [
            pl.BlockSpec((None, 2, rows, LANES), lambda i, s: (pair, 0, i, 0)),
            pl.BlockSpec((None, 2, tokens, LANES), lambda i, s: (pair, 0, 0, 0)),
            pl.BlockSpec((None, tokens, LANES), lambda i, s: (pair, 0, 0)),
            pl.BlockSpec((None, rows, LANES), lambda i, s: (pair, i, 0)),
        ]
        + moving
        + [block, block, full((tokens, LANES)), full((tokens, LANES))],
        [full((chunk, 3 * LANES))] * WAYS,
        [shape_of((chunk, 3 * LANES), BF)] * WAYS,
        [
            pltpu.VMEM((2, tokens, LANES), BF),
            pltpu.VMEM((2, LANES, tokens), BF),
            pltpu.VMEM((tokens, LANES), F32),
            pltpu.VMEM((tokens, LANES), F32),
        ],
        cost(28 * tokens * tokens * LANES, 8),
        "attn_bwd",
    )(qa, ka, v, o, *grad, cosine, sine, cosine, sine)


def own_first(core, values):
    cut = [values[:, at : at + LANES] for at in range(0, values.shape[1], LANES)]
    turned = [cut[i ^ 1] for i in range(len(cut))]
    return jnp.where(core == 0, values, jnp.concatenate(turned, axis=-1))


MESH = pl.DeviceIdType.MESH
UP, DOWN, TO_X, TO_Y, TO_D, CORE_OWN, CORE_X, CORE_Y, CORE_D = range(9)
FROM_Z, FROM_X, FROM_Y, FROM_D = range(4)
CHUNKS = 4


class Place:
    def __init__(self):
        self.dp, self.z = lax.axis_index("dp"), lax.axis_index("mp")
        self.core, self.x, self.y = self.dp % 2, (self.dp // 2) % 2, self.dp // 4
        self.at_c = self.dp + 1 - 2 * self.core
        self.at_x = self.dp + 2 - 4 * self.x
        self.at_y = self.dp + 4 - 8 * self.y
        self.at_d = self.at_x + self.at_y - self.dp
        self.group = self.z // 2
        self.far_z = self.z + 2 - 4 * self.group
        self.quarter = self.z + self.core * (self.far_z - self.z)

    @staticmethod
    def mix(q, m):
        return (q + m) % 2 + 2 * ((q // 2 + m // 2) % 2)

    def stays(self, a, b):
        return jnp.logical_and(a == self.dp, b == self.z)

    def attention_of(self, m):
        h = self.mix(self.z, m)
        a, b = self.dp - self.core + (h // 2 + self.core) % 2, 2 * self.core + h % 2
        return a, b, self.stays(a, b)

    def owner_of(self, m):
        a, b = self.dp - self.core + self.group, self.mix(self.quarter, m)
        return a, b, self.stays(a, b)


def remote(src, dst, send, recv, device):
    return pltpu.make_async_remote_copy(
        src_ref=src, dst_ref=dst, send_sem=send, recv_sem=recv,
        device_id=device, device_id_type=MESH,
    )


class Move:
    def __init__(self, src, dst, send, recv, place):
        a, b, self.stays = place
        self.far = lambda: remote(src, dst, send, recv, (a, b))
        self.near = lambda: pltpu.make_async_copy(src, dst, recv)

    def start(self):
        pl.when(self.stays)(lambda: self.near().start())
        pl.when(jnp.logical_not(self.stays))(lambda: self.far().start())

    def wait_recv(self):
        self.far().wait_recv()

    def wait_send(self):
        pl.when(jnp.logical_not(self.stays))(lambda: self.far().wait_send())


def forward_kernel(x_ref, info_ref, gain_ref, qkv_ref, *refs, packs):
    parts, outs, heads_ref = refs[:packs], refs[packs : 2 * packs], refs[2 * packs]
    saved, refs = refs[2 * packs + 1 : 2 * packs + 7], refs[2 * packs + 7 :]
    qa, o, normed, cosine, sine, ka, v, q, qaux, kaux, live, scores = refs[:12]
    kept = Kept((normed, cosine, sine, qa, ka, v, o, q, qaux, kaux, live, scores))
    x_all, w_ref, infos = refs[12:15]
    (
        sends, recvs, cores, locals_, token_send, token_recv, relay_send, info_sem,
        head_send, head_recv,
        q_send, q_recv, save_sem,
    ) = refs[15:]
    dp, z = lax.axis_index("dp"), lax.axis_index("mp")
    core, xb, yb = dp % 2, (dp // 2) % 2, dp // 4
    at_c, at_x, at_y = dp + 1 - 2 * core, dp + 2 - 4 * xb, dp + 4 - 8 * yb
    at_d = at_x + at_y - dp
    group = z // 2
    far_z = z + 2 - 4 * group
    quarter = z + core * (far_z - z)

    def mix(q, m):
        return (q + m) % 2 + 2 * ((q // 2 + m // 2) % 2)

    def attention_of(m):
        h = mix(z, m)
        return dp - core + (h // 2 + core) % 2, 2 * core + h % 2

    def owner_of(m):
        return dp - core + group, mix(quarter, m)

    barrier = pltpu.get_barrier_semaphore()

    def greet(device, when=None):
        def signal():
            pl.semaphore_signal(barrier, inc=1, device_id=device, device_id_type=MESH)

        signal() if when is None else pl.when(when)(signal)

    greet((at_c, z))
    greet((at_x, z))
    greet((at_y, z))
    greet((dp, far_z))
    greet((dp, z + 1), z < WAYS - 1)
    greet((dp, z - 1), z > 0)
    count = 4 + (z < WAYS - 1).astype(jnp.int32) + (z > 0).astype(jnp.int32)
    here, there = [], []
    for m in range(WAYS):
        for of, found in ((attention_of, here), (owner_of, there)):
            a, b = of(m)
            stays = jnp.logical_and(a == dp, b == z)
            found.append((a, b, stays))
            greet((a, b), jnp.logical_not(stays))
            count += 1 - stays.astype(jnp.int32)
    pl.semaphore_wait(barrier, count)

    def remote(src, dst, send, recv, device):
        return pltpu.make_async_remote_copy(
            src_ref=src, dst_ref=dst, send_sem=send, recv_sem=recv,
            device_id=device, device_id_type=MESH,
        )

    def copy(p, kind, s, src=None):
        who = {CORE_X: at_x, CORE_Y: at_y, CORE_D: at_d}.get(kind, dp)
        if kind == TO_D:
            who = jnp.where(s < 2, at_x, at_y)
        slab = outs[p].at[who, s]
        send = sends.at[p, kind, s]
        if kind == UP:
            recv, device = recvs.at[p, FROM_Z, s], (dp, z + 1)
        elif kind == DOWN:
            recv, device = recvs.at[p, FROM_Z, s], (dp, z - 1)
        elif kind == TO_X:
            recv, device = recvs.at[p, FROM_X, s], (at_x, z)
        elif kind == TO_Y:
            recv, device = recvs.at[p, FROM_Y, s], (at_y, z)
        elif kind == TO_D:
            recv, device = recvs.at[p, FROM_D, s], (jnp.where(s < 2, at_y, at_x), z)
        else:
            recv, device = cores.at[p, kind - CORE_OWN, s], (at_c, z)
        return remote(slab if src is None else src, slab, send, recv, device)

    def arrived(p, sem, who, s):
        slab = outs[p].at[who, s]
        remote(slab, slab, sends.at[p, UP, s], sem, (at_c, z)).wait_recv()

    def spread(p, s, src=None):
        copy(p, TO_X, s, src).start()
        copy(p, TO_Y, s, src).start()
        copy(p, CORE_OWN, s, src).start()

    def begin(p):
        src = parts[p]
        spread(p, z, src)
        pltpu.make_async_copy(src, outs[p].at[dp, z], locals_.at[p]).start()

    def begin_line(p):
        src = parts[p]
        pl.when(z < WAYS - 1)(lambda: copy(p, UP, z, src).start())
        pl.when(z > 0)(lambda: copy(p, DOWN, z, src).start())

    def reach(p, hop):
        def one(s):
            arrived(p, recvs.at[p, FROM_Z, s], dp, s)
            spread(p, s)

        pl.when(z >= hop)(lambda: one(z - hop))
        pl.when(z + hop < WAYS)(lambda: one(z + hop))

    def ahead(p, hop):
        pl.when(jnp.logical_and(z >= hop, z < WAYS - 1))(lambda: copy(p, UP, z - hop).start())
        pl.when(jnp.logical_and(z + hop < WAYS, z > 0))(lambda: copy(p, DOWN, z + hop).start())

    def line(p, hop):
        reach(p, hop)
        if hop < WAYS - 1:
            ahead(p, hop)

    def plane(p, hop):
        def one(s):
            arrived(p, recvs.at[p, FROM_X, s], at_x, s)
            copy(p, CORE_X, s).start()
            pl.when(s < 2)(lambda: copy(p, TO_D, s).start())
            arrived(p, recvs.at[p, FROM_Y, s], at_y, s)
            copy(p, CORE_Y, s).start()
            pl.when(s >= 2)(lambda: copy(p, TO_D, s).start())

        if hop == 0:
            one(z)
        else:
            pl.when(z >= hop)(lambda: one(z - hop))
            pl.when(z + hop < WAYS)(lambda: one(z + hop))

    def corner(p, hop):
        def one(s):
            arrived(p, recvs.at[p, FROM_D, s], at_d, s)
            copy(p, CORE_D, s).start()

        if hop == 0:
            one(z)
        else:
            pl.when(z >= hop)(lambda: one(z - hop))
            pl.when(z + hop < WAYS)(lambda: one(z + hop))

    def from_core(p):
        for s in range(WAYS):
            for kind in range(4):
                twin = (at_c, at_x + at_c - dp, at_y + at_c - dp, at_d + at_c - dp)[kind]
                arrived(p, cores.at[p, kind, s], twin, s)
        pltpu.make_async_copy(parts[p], outs[p].at[dp, z], locals_.at[p]).wait()

    def finish(p):
        for s in range(WAYS):
            pl.when(jnp.logical_and(z < WAYS - 1, s <= z))(lambda s=s: copy(p, UP, s).wait_send())
            pl.when(jnp.logical_and(z > 0, s >= z))(lambda s=s: copy(p, DOWN, s).wait_send())
            for kind in range(TO_X, CORE_D + 1):
                copy(p, kind, s).wait_send()

    far = (z // 2 + core) % 2 == 1
    straight = (z + 1 + core) % 2
    relays = jnp.logical_and(core == 1, jnp.logical_and(z > 0, z < WAYS - 1))
    beside = (dp, z + 1 - 2 * (z % 2))
    cut = x_ref.shape[0] // CHUNKS

    def token(m, c):
        to_dp, to_z, stays = here[m]
        some = pl.ds(c * cut, cut)
        src, dst = x_ref.at[some], x_all.at[m, some]

        def direct():
            return remote(src, dst, token_send.at[m, c], token_recv.at[m, c], (to_dp, to_z))

        def near():
            return pltpu.make_async_copy(src, dst, token_recv.at[m, c])

        goes = jnp.logical_and(
            jnp.logical_not(stays), jnp.logical_or(jnp.logical_not(far), straight == m)
        )
        return direct, near, stays, goes

    def relay(m, c):
        some = pl.ds(c * cut, cut)
        return remote(
            x_all.at[m, some], x_all.at[1 - m, some],
            relay_send.at[m, c], token_recv.at[1 - m, c], beside,
        )

    def pass_on(m, c):
        some = pl.ds(c * cut, cut)
        return remote(
            x_all.at[m, some], x_all.at[m + 2, some],
            token_send.at[m + 2, c], token_recv.at[m + 2, c], (at_c, z),
        )

    def take_tokens(c):
        for m in range(2):
            token(m, c)[0]().wait_recv()
            pl.when(relays)(lambda m=m: relay(m, c).start())
            pass_on(m, c).start()

    def early(*chunks):
        def run():
            for c in chunks:
                take_tokens(c)

        pl.when(relays)(run)

    def swap_info():
        return remote(info_ref, infos.at[1], info_sem.at[0], info_sem.at[1], (at_c, z))

    def own_info():
        return pltpu.make_async_copy(info_ref, infos.at[0], locals_.at[packs])

    def q_copy(kind, i=0, src=None):
        who = {"z": dp, "x": dp, "y": dp, "c": dp, "cx": at_x, "cy": at_y, "cd": at_d}.get(kind)
        if kind == "d":
            who = at_x if i == 0 else at_y
        device = {"z": (dp, far_z), "x": (at_x, z), "y": (at_y, z)}.get(kind, (at_c, z))
        if kind == "d":
            device = (at_y, z) if i == 0 else (at_x, z)
        slot = {"z": 0, "x": 1, "y": 3, "d": 5, "c": 7, "cx": 8, "cy": 9, "cd": 10}[kind]
        if kind in ("x", "y", "d"):
            slot += i
        if kind == "z":
            i = 1
        if kind[0] == "c":
            i = 1 - core
        dst = w_ref.at[i, who]
        return remote(dst if src is None else src, dst, q_send.at[slot], q_recv.at[slot], device)

    def q_arrived(kind, i=0):
        q_copy(kind, i).wait_recv()

    def own_q():
        return pltpu.make_async_copy(qkv_ref, w_ref.at[0, dp], locals_.at[packs + 1])

    q_kinds = [("z", 0), ("x", 0), ("x", 1), ("y", 0), ("y", 1), ("d", 0), ("d", 1)]
    q_kinds += [("c", 0), ("cx", 0), ("cy", 0), ("cd", 0)]

    keeps = [w_ref.at[core], normed, cosine, sine, ka, v]

    def save(i):
        return pltpu.make_async_copy(keeps[i], saved[i], save_sem.at[i])

    rows = x_ref.shape[0]

    def head(pair, m, owner):
        src = kept.o.at[pair, pl.ds(m * rows, rows)]
        dst = heads_ref.at[m, pair]
        to_dp, to_z, stays = owner

        def far():
            return remote(
                src, dst, head_send.at[m, pair], head_recv.at[m, pair], (to_dp, to_z)
            )

        def near():
            return pltpu.make_async_copy(src, dst, head_recv.at[m, pair])

        return far, near, stays

    def start(item):
        far, near, stays = item
        pl.when(stays)(lambda: near().start())
        pl.when(jnp.logical_not(stays))(lambda: far().start())

    def end_send(item):
        far, near, stays = item
        pl.when(jnp.logical_not(stays))(lambda: far().wait_send())

    q_copy("z", 0, qkv_ref).start()
    q_copy("x", 0, qkv_ref).start()
    q_copy("y", 0, qkv_ref).start()
    own_q().start()
    for c in range(CHUNKS):
        for m in range(2):
            direct, near, stays, goes = token(m, c)
            pl.when(stays)(lambda: near().start())
            pl.when(goes)(lambda: direct().start())
    swap_info().start()
    own_info().start()
    for p in range(packs):
        begin(p)
        begin_line(p)
    own_info().wait()
    swap_info().wait()
    own_q().wait()
    q_arrived("x", 0)
    q_copy("d", 0).start()
    q_arrived("z")
    q_copy("x", 1).start()
    q_copy("y", 1).start()
    early(0)
    away = (group + core) % 2
    starts = doc_starts([infos[away, t] for t in range(WAYS)])
    for m in range(WAYS):
        t = mix(quarter, m)
        table_piece(m, infos[away, t], t * x_ref.shape[0], starts, kept)
    q_arrived("y", 0)
    q_copy("c").start()
    plane(0, 0)
    q_arrived("x", 1)
    q_copy("cx").start()
    q_arrived("y", 1)
    q_copy("d", 1).start()
    q_copy("cy").start()
    early(1)
    plane(1, 0)
    q_arrived("d", 0)
    q_arrived("d", 1)
    q_copy("cd").start()
    early(2)
    reach(0, 1)
    corner(0, 0)
    reach(1, 1)
    corner(1, 0)
    for kind in ("c", "cx", "cy", "cd"):
        q_arrived(kind)
    save(0).start()
    save(2).start()
    save(3).start()
    early(3)
    @pl.when(jnp.logical_not(relays))
    def _():
        for c in range(CHUNKS):
            take_tokens(c)

    for p in range(packs):
        ahead(p, 1)
        plane(p, 1)
    for m in range(WAYS):
        if m >= 2:
            for c in range(CHUNKS):
                pass_on(m - 2, c).wait_recv()
        weight = jnp.concatenate([w_ref[core, d] for d in range(w_ref.shape[1])], axis=-1)
        qkv_piece(m, x_all[m], gain_ref[...], weight, kept)
        if m == 2:
            line(0, 2)
            corner(0, 1)
    save(1).start()
    save(4).start()
    save(5).start()

    events = {
        1: [(line, 1, 2)],
        2: [(line, 0, 3), (corner, 1, 1)],
        4: [(plane, 0, 2)],
        5: [(line, 1, 3)],
        7: [(plane, 1, 2)],
        9: [(corner, 0, 2)],
        11: [(plane, 0, 3)],
        13: [(corner, 1, 2)],
        15: [(plane, 1, 3)],
    }
    steps = kept.v.shape[1] // STEP
    pairs = kept.v.shape[0]
    per = steps // WAYS

    def body(i, carry):
        for at, todo in events.items():

            @pl.when(i == at)
            def _(todo=todo):
                for what, p, hop in todo:
                    what(p, hop)

        pair = i // steps
        step = i % steps
        attn_step(pair, step, kept)
        m = step // per

        @pl.when(step % per == per - 1)
        def _():
            a, b = dp - core + group, mix(quarter, m)
            start(head(pair, m, (a, b, jnp.logical_and(a == dp, b == z))))

        return carry

    lax.fori_loop(0, pairs * steps, body, 0)
    corner(0, 3)
    corner(1, 3)
    for p in range(packs):
        from_core(p)
    for m in range(WAYS):
        for pair in range(pairs):
            head(pair, m, there[m])[0]().wait_recv()
            end_send(head(pair, m, there[m]))
    for c in range(CHUNKS):
        for m in range(2):
            pass_on(m, c).wait_send()
            direct, near, stays, goes = token(m, c)
            pl.when(goes)(lambda: direct().wait_send())
            pl.when(relays)(lambda m=m, c=c: relay(m, c).wait_send())
    for p in range(packs):
        finish(p)
    for kind, i in q_kinds:
        q_copy(kind, i).wait_send()
    for i in range(len(keeps)):
        save(i).wait()


def forward_call(x, info, gain, qkv_part, parts, dps, pairs):
    rows, model = x.shape
    packs = len(parts)
    anywhere = pl.BlockSpec(memory_space=pl.ANY)
    vmem = pl.BlockSpec(memory_space=pltpu.VMEM)
    outs, scratch = kept_shapes(WAYS * rows, model, pairs)
    normed, cosine, sine, qa, ka, v, o = outs
    hold = [normed, cosine, sine, ka, v]
    weight = (dps,) + qkv_part.shape
    out = pl.pallas_call(
        functools.partial(forward_kernel, packs=packs),
        in_specs=[anywhere, anywhere, vmem] + [anywhere] * (1 + packs),
        out_specs=[anywhere] * (packs + 7) + [vmem] * 2,
        out_shape=[shape_of((dps, WAYS) + part.shape, BF) for part in parts]
        + [shape_of((WAYS, pairs, rows, LANES), BF), shape_of(weight, BF)]
        + hold
        + [qa, o],
        scratch_shapes=[pltpu.VMEM(h.shape, h.dtype) for h in hold]
        + scratch
        + [
            pltpu.VMEM((WAYS, rows, model), BF),
            pltpu.VMEM((2,) + weight, BF),
            pltpu.VMEM((2, WAYS, rows, LANES), F32),
            pltpu.SemaphoreType.DMA((packs, 9, WAYS)),
            pltpu.SemaphoreType.DMA((packs, 4, WAYS)),
            pltpu.SemaphoreType.DMA((packs, 4, WAYS)),
            pltpu.SemaphoreType.DMA((packs + 2,)),
            pltpu.SemaphoreType.DMA((WAYS, CHUNKS)),
            pltpu.SemaphoreType.DMA((WAYS, CHUNKS)),
            pltpu.SemaphoreType.DMA((2, CHUNKS)),
            pltpu.SemaphoreType.DMA((2,)),
            pltpu.SemaphoreType.DMA((WAYS, pairs)),
            pltpu.SemaphoreType.DMA((WAYS, pairs)),
            pltpu.SemaphoreType.DMA((11,)),
            pltpu.SemaphoreType.DMA((11,)),
            pltpu.SemaphoreType.DMA((6,)),
        ],
        compiler_params=pltpu.CompilerParams(
            collective_id=0, has_side_effects=True, vmem_limit_bytes=VMEM_LIMIT
        ),
        name="forward",
    )(x, info, gain, qkv_part, *parts)
    packs_out, out = out[:packs], out[packs:]
    heads, weight, normed, cosine, sine, ka, v, qa, o = out
    return packs_out, heads, weight, (normed, cosine, sine, qa, ka, v, o)


def attn_back_begin(pair, k):
    chunk = 512
    lane = lax.broadcasted_iota(jnp.int32, (chunk, LANES), 1)
    zero = jnp.zeros((), BF)
    ones = jnp.where(lane % HEAD_DIM < 3, jnp.ones((), BF), zero)
    for at in range(0, k.dk.shape[0], chunk):
        some = slice(at, at + chunk)
        v = k.v[pair, some, :]
        for head in range(2):
            mine = (lane < HEAD_DIM) if head == 0 else (lane >= HEAD_DIM)
            k.va[head, some, :] = jnp.where(mine, v, ones)
            own = jnp.where(mine, k.ka[pair, head, some, :], zero).astype(F32)
            k.kt[head, :, some] = own.T.astype(BF)
    k.dk[...] = jnp.zeros_like(k.dk)
    k.dv[...] = jnp.zeros_like(k.dv)


def attn_back_step(pair, step, grad, k):
    chunk = 512
    here = pl.ds(pl.multiple_of(step * STEP, STEP), STEP)
    lane = lax.broadcasted_iota(jnp.int32, (STEP, LANES), 1)
    zero = jnp.zeros((), BF)
    t = lane % HEAD_DIM
    product = grad.astype(F32) * k.o[pair, here, :].astype(F32)
    turned = jnp.zeros((LANES, STEP), F32)
    for head in range(2):
        mine = (lane < HEAD_DIM) if head == 0 else (lane >= HEAD_DIM)
        delta = jnp.sum(jnp.where(mine, product, 0.0), axis=-1, keepdims=True)
        high = delta.astype(BF)
        rest = delta - high.astype(F32)
        mid = rest.astype(BF)
        low = (rest - mid.astype(F32)).astype(BF)
        aux = jnp.where(t == 0, -high, jnp.where(t == 1, -mid, jnp.where(t == 2, -low, zero)))
        grad_aug = jnp.where(mine, grad, aux)
        grad_own = jnp.where(mine, grad, zero)
        qa = k.qa[pair, head, here, :]
        q_own = jnp.where(mine, qa, zero)
        for at in range(0, k.dk.shape[0], chunk):
            some = slice(at, at + chunk)
            prob = jnp.exp(dot_nt(k.ka[pair, head, some, :], qa))
            back = dot_nt(k.va[head, some, :], grad_aug)
            score_grad = (prob * back).astype(BF)
            k.dv[some, :] += dot_nn(prob.astype(BF), grad_own)
            k.dk[some, :] += dot_nn(score_grad, q_own)
            turned += dot_nn(k.kt[head, :, some], score_grad)
    dq = turned.T * (HEAD_DIM**-0.5)
    dq = dq * k.cosine[here, :] - swap_halves(dq) * k.sine[here, :]
    k.low[pair, 0, here, :] = dq.astype(BF)


def attn_back_end(pair, m, k, rows):
    some = slice(m * rows, (m + 1) * rows)
    dk = k.dk[some, :]
    dk = dk * k.cosine[some, :] - swap_halves(dk) * k.sine[some, :]
    k.low[pair, 1, some, :] = dk.astype(BF)
    k.low[pair, 2, some, :] = k.dv[some, :].astype(BF)


def low_piece(pair, m, k, rows):
    some = slice(m * rows, (m + 1) * rows)
    return jnp.concatenate([k.low[pair, c, some, :] for c in range(3)], axis=-1)


class Back:
    names = ("qa", "ka", "v", "o", "cosine", "sine", "low", "va", "kt", "dk", "dv")

    def __init__(self, refs):
        for name, ref in zip(self.names, refs):
            setattr(self, name, ref)


class Chain:
    def __init__(self, p, source, kept, r1, r2, rz, send, recv):
        self.p, self.source, self.kept = p, source, kept
        self.r1, self.r2, self.rz, self.send, self.recv = r1, r2, rz, send, recv

    def slab(self, q, slot, away):
        x, y = self.p.x, self.p.y
        if q < 2:
            return (y if slot else 1 - y) * 2 + (1 - x if away else x)
        return (1 - y if away else y) * 2 + (x if slot else 1 - x)

    def near(self, q, second=False):
        p = self.p
        return (p.at_x, p.z) if (q < 2) != second else (p.at_y, p.z)

    def stage1(self, q, slot):
        src = self.source(q, self.slab(q, slot, True))
        at = q * 2 + slot
        return remote(src, self.r1.at[q, slot], self.send.at[at], self.recv.at[at], self.near(q))

    def stage2(self, q):
        at = 8 + q
        src = self.kept(q, 0, self.slab(q, 0, False))
        return remote(src, self.r2.at[q], self.send.at[at], self.recv.at[at], self.near(q, True))

    def first(self, q):
        self.stage1(q, 0).start()
        self.stage1(q, 1).start()

    def second(self, q, done=False):
        if not done:
            self.stage1(q, 0).wait_recv()
        ref = self.kept(q, 0, self.slab(q, 0, False))
        ref[...] += self.r1[q, 0]
        self.stage2(q).start()
        if not done:
            self.stage1(q, 1).wait_recv()
        self.own(q)[...] += self.r1[q, 1]

    def own(self, q):
        return self.kept(q, 1, self.slab(q, 1, False))

    def third(self, q):
        self.stage2(q).wait_recv()
        self.own(q)[...] += self.r2[q]

    def lined(self, q, down):
        z = self.p.z
        at = q if down else q + 1
        return remote(
            self.own(q), self.rz.at[at], self.send.at[12 + q], self.recv.at[12 + at],
            (self.p.dp, z - 1 if down else z + 1),
        )

    def line(self, hop, quarters):
        z = self.p.z
        for q in quarters:
            if q < WAYS - hop:

                @pl.when(z == WAYS - hop)
                def _(q=q):
                    if hop > 1:
                        self.lined(q, True).wait_recv()
                        self.own(q)[...] += self.rz[q]
                    self.lined(q, True).start()

            if q > hop - 1:

                @pl.when(z == hop - 1)
                def _(q=q):
                    if hop > 1:
                        self.lined(q, False).wait_recv()
                        self.own(q)[...] += self.rz[q + 1]
                    self.lined(q, False).start()

    def last(self, out_ref):
        z = self.p.z
        for q in range(WAYS):

            @pl.when(z == q)
            def _(q=q):
                total = self.own(q)[...].astype(F32)
                if q < WAYS - 1:
                    self.lined(q, True).wait_recv()
                    total += self.rz[q].astype(F32)
                if q > 0:
                    self.lined(q, False).wait_recv()
                    total += self.rz[q + 1].astype(F32)
                out_ref[...] = total

    def finish(self, done=()):
        z = self.p.z
        for q in range(WAYS):
            if q not in done:
                self.stage1(q, 0).wait_send()
                self.stage1(q, 1).wait_send()
            self.stage2(q).wait_send()
            pl.when(q < z)(lambda q=q: self.lined(q, True).wait_send())
            pl.when(q > z)(lambda q=q: self.lined(q, False).wait_send())


DONE = (0, 2)


def turn_of(step):
    return 2 * (step % 2) + step // 2


def mlp_kernel(
    s_ref, heads_ref, x_ref, g_ref, gain_ref, live_ref, pack_ref, qkv_ref, wa_ref, wb_ref,
    output_ref, mgrad_ref, low_ref, small_ref, hg_ref, sum_ref, r1_ref, w_ref, *scratch, swap
):
    w_attn, middle, inner, mlp, back, grads, segment, load_sem = scratch[:8]
    step = pl.program_id(0)
    steps = pl.num_programs(0)
    quarter = turn_of(step)
    units = wb_ref.shape[2] // 2
    skip = wa_ref.shape[2] - units
    z = s_ref[0]
    core = s_ref[1]
    load = pltpu.make_async_copy(pack_ref.at[:, :, :skip], w_attn, load_sem.at[0])

    def alive():
        return jnp.where(segment[:, 0:1] != 0.0, 1.0, 0.0)

    if swap:
        away, got, send_sem, recv_sem, f_send, f_recv, w_send, w_recv = scratch[8:]
        p = Place()
        core, z = p.core, p.z
        other = (p.at_c, z)
        chain = Chain(
            p, lambda q, i: grads.at[q, i], None, None, None, None, f_send, f_recv
        )

        beside = (p.dp, p.z + 1 - 2 * (p.z % 2))

        def weight_copy(i):
            src, device = ((qkv_ref, beside), (qkv_ref, other), (w_ref.at[1], other))[i]
            return remote(src, w_ref.at[i + 1], w_send.at[i], w_recv.at[i], device)

        def weight_own():
            return pltpu.make_async_copy(qkv_ref, w_ref.at[0], w_send.at[3])

        @pl.when(step == 0)
        def _():
            barrier = pltpu.get_barrier_semaphore()
            for device in (other, (p.at_x, p.z), (p.at_y, p.z), beside):
                pl.semaphore_signal(barrier, inc=1, device_id=device, device_id_type=MESH)
            pl.semaphore_wait(barrier, 4)
            weight_copy(0).start()
            weight_copy(1).start()
            weight_own().start()

        def give(i):
            return remote(
                away.at[i % 2], got.at[i % 2], send_sem.at[i % 2], recv_sem.at[i % 2], other
            )

        def stage1(i, slot):
            q = DONE[i]
            at = i * 2 + slot
            return remote(
                grads.at[q, chain.slab(q, slot, True)], r1_ref.at[i, slot],
                f_send.at[at], f_recv.at[at], chain.near(q),
            )

        def take(i):
            q = turn_of(i)
            give(i).wait_recv()
            for d in range(grads.shape[1]):
                grads[q, d] += got[i % 2, d]
            pltpu.make_async_copy(grads.at[q], sum_ref.at[q], load_sem.at[1 + i]).start()
            for j in range(len(DONE)):

                @pl.when(i == j)
                def _(j=j):
                    stage1(j, 0).start()
                    stage1(j, 1).start()

    @pl.when(step == 0)
    def _():
        load.start()
        load_live = pltpu.make_async_copy(live_ref.at[z], segment, load_sem.at[1 + WAYS])
        load_live.start()
        tokens = x_ref[...].astype(F32)
        attn_out = jnp.zeros(tokens.shape, F32)
        load_live.wait()
        load.wait()
        for m in range(WAYS):
            o = jnp.concatenate([heads_ref[m, 0], heads_ref[m, 1]], axis=-1)
            attn_out += dot_nn(o, side_by_side(w_attn, z ^ m))
        total = tokens + attn_out
        vhat, unused = norm_stats(total)
        middle[...] = total
        inner[...] = (vhat * gain_ref[...]).astype(BF)
        live = alive()
        lane = lax.broadcasted_iota(jnp.int32, (1, tokens.shape[1]), 1)
        sums = jnp.where(lane == 4, jnp.sum(live), 0.0)
        for i, values in enumerate((tokens, attn_out, total)):
            sums = jnp.where(lane == i, jnp.sum(live * values * values), sums)
        small_ref[...] = jnp.zeros_like(small_ref)
        small_ref[2:3, :] = sums

    w_act = side_by_side(wa_ref, 0, slice(skip, skip + units))
    w_lin = side_by_side(wb_ref, 0, slice(0, units))
    w_out = side_by_side(wb_ref, 0, slice(units, 2 * units))
    x = inner[...]
    grad = g_ref[...]
    act_in = dot_nt(w_act, x)
    linear = dot_nt(w_lin, x)
    hidden_grad = dot_nt(w_out, grad)
    cdf = 0.5 * (1.0 + lax.erf(act_in * (2.0**-0.5)))
    act = act_in * cdf
    slope = cdf + act_in * jnp.exp(-0.5 * act_in * act_in) * ((2.0 * math.pi) ** -0.5)
    hidden = (act * linear).astype(BF)
    d_act = (hidden_grad * linear * slope).astype(BF)
    d_lin = (hidden_grad * act).astype(BF)
    if swap:
        pl.when(step >= 1)(lambda: take(step - 1))
        pl.when(step >= 2)(lambda: give(step - 2).wait_send())

        @pl.when(step == steps - 1)
        def _():
            weight_copy(0).wait_recv()
            weight_copy(2).start()

    x_mine = own_first(core, x)
    g_mine = own_first(core, grad)
    pieces = (dot_nn(d_act, x_mine), dot_nn(d_lin, x_mine), dot_nn(hidden, g_mine))
    for part, value in enumerate(pieces):
        some = slice(part * units, (part + 1) * units)
        value = value.astype(BF)
        for d in range(value.shape[1] // LANES):
            slab = value[:, d * LANES : (d + 1) * LANES]
            if not swap:
                sum_ref[quarter, d // 2, d % 2, some] = slab
            elif d % 2:
                away[step % 2, d // 2, some] = slab
            else:
                grads[quarter, d // 2, some] = slab
    if swap:
        give(step).start()
    more_mlp = dot_tn(hidden, w_out)
    more_back = dot_tn(d_act, w_act) + dot_tn(d_lin, w_lin)

    @pl.when(step == 0)
    def _():
        mlp[...] = more_mlp
        back[...] = more_back

    @pl.when(step > 0)
    def _():
        mlp[...] += more_mlp
        back[...] += more_back

    @pl.when(step == steps - 1)
    def _():
        vhat, scale = norm_stats(middle[...])
        into = back[...]
        middle_grad = g_ref[...].astype(F32) + norm_back(vhat, scale, gain_ref[...], into)
        low = middle_grad.astype(BF)
        for m in range(WAYS):
            hg = dot_nt(low, side_by_side(w_attn, z ^ m)).astype(BF)
            hg_ref[m, 0] = hg[:, :LANES]
            hg_ref[m, 1] = hg[:, LANES:]
        mgrad_ref[...] = middle_grad
        low_ref[...] = low
        out = mlp[...]
        output_ref[...] = (middle[...] + out).astype(BF)
        lane = lax.broadcasted_iota(jnp.int32, (1, out.shape[1]), 1)
        square = jnp.sum(alive() * out * out)
        small_ref[2:3, :] = jnp.where(lane == 3, square, small_ref[2:3, :])
        small_ref[1:2, :] = jnp.sum(into * vhat, axis=0, keepdims=True)
        if swap:
            take(step)
            give(step - 1).wait_send()
            give(step).wait_send()
            for i in range(WAYS):
                q = turn_of(i)
                pltpu.make_async_copy(grads.at[q], sum_ref.at[q], load_sem.at[1 + i]).wait()
            for i in range(len(DONE)):
                for slot in range(2):
                    stage1(i, slot).wait()
            weight_copy(0).wait_send()
            weight_copy(1).wait()
            weight_copy(2).wait()
            weight_own().wait()


def mlp_call(scalars, heads, x, grad, gain, live, pack_a, pack_b, qkv, swap):
    tokens, model = x.shape
    wide, quarters, depth_a, unused = pack_a.shape
    units = pack_b.shape[2] // 2
    depth = model // WAYS
    out = (quarters, wide // 2) + (() if swap else (2,)) + (3 * units, LANES)
    whole = pl.BlockSpec(memory_space=pltpu.VMEM)
    anywhere = pl.BlockSpec(memory_space=pl.ANY)
    weight = lambda rows: pl.BlockSpec((wide, 1, rows, LANES), lambda i, s: (0, turn_of(i), 0, 0))
    sems = lambda *shape: pltpu.SemaphoreType.DMA(shape)
    scratch = [
        pltpu.VMEM((wide, quarters, depth, LANES), BF),
        pltpu.VMEM((tokens, model), F32),
        pltpu.VMEM((tokens, model), BF),
        pltpu.VMEM((tokens, model), F32),
        pltpu.VMEM((tokens, model), F32),
        pltpu.VMEM(out if swap else (8, LANES), BF),
        pltpu.VMEM((tokens, LANES), F32),
        sems(2 + WAYS),
    ]
    if swap:
        scratch += [pltpu.VMEM((2,) + out[1:], BF)] * 2
        scratch += [sems(2), sems(2), sems(6), sems(6), sems(4), sems(3)]
    r1 = (len(DONE), 2, 3 * units, LANES) if swap else (8, LANES)
    spec = pltpu.PrefetchScalarGridSpec(
        num_scalar_prefetch=1,
        grid=(quarters,),
        in_specs=[whole] * 4 + [anywhere] * 3 + [weight(depth_a), weight(2 * units)],
        out_specs=[whole] * 5 + [anywhere if swap else whole, anywhere, anywhere],
        scratch_shapes=scratch,
    )
    extra = dict(collective_id=1, has_side_effects=True) if swap else {}
    return pl.pallas_call(
        functools.partial(mlp_kernel, swap=swap),
        grid_spec=spec,
        out_shape=[
            shape_of((tokens, model), BF),
            shape_of((tokens, model), F32),
            shape_of((tokens, model), BF),
            shape_of((8, model), F32),
            shape_of((WAYS, depth // LANES, tokens, LANES), BF),
            shape_of(out, BF),
            shape_of(r1, BF),
            shape_of((WAYS,) + qkv.shape if swap else (8, LANES), BF),
        ],
        compiler_params=pltpu.CompilerParams(vmem_limit_bytes=62 * 1024 * 1024, **extra),
        cost_estimate=cost(22 * tokens * model * units * quarters, 40),
        name="mlp",
    )(scalars, heads, x, grad, gain, live, pack_a, qkv, pack_a, pack_b)


def backward_kernel(
    hg_ref, sum_ref, r1_ref, normed_ref, w_ref, x_ref, mgrad_ref, low_ref, heads_ref,
    qa, ka, v, o, cosine, sine, gain_ref, small_ref,
    grad_ref, inner_ref, outer_ref, attn_ref, qkv_ref, gain_a_ref, gain_m_ref, rms_ref,
    do_ref, low, va, kt, dk, dv, normed, weight, x_in,
    f_kept0, f_r10, f_r20, f_rz0, f_kept1, f_r11, f_r21, f_rz1,
    a_sum, a_got, a_r1, a_r2, a_rz,
    q_sum, q_rx, q_ry, q_rz, ret, s_own, s_dp, s_mp,
    load_sem, do_send, do_recv, f_send, f_recv, a_send, a_recv, c_send, c_recv,
    q_send, q_recv, g_send, g_recv, s_send, s_recv,
):
    p = Place()
    dp, z, core = p.dp, p.z, p.core
    rows = x_ref.shape[0]
    pairs = v.shape[0]
    k = Back((qa, ka, v, o, cosine, sine, low, va, kt, dk, dv))

    def qkv_to(turn):
        a, b = dp - core + (p.group + turn) % 2, p.quarter
        return a, b, p.stays(a, b)

    def qkv_from(g):
        a, b = dp - core + (z // 2 + g) % 2, 2 * g + z % 2
        return a, b, p.stays(a, b)

    def other_dp(turn):
        return (dp + turn) % 8, z

    def other_mp(turn):
        return dp, (z + turn) % WAYS

    barrier = pltpu.get_barrier_semaphore()
    count = jnp.int32(0)

    def greet(device, skip=None):
        def signal():
            pl.semaphore_signal(barrier, inc=1, device_id=device, device_id_type=MESH)

        if skip is None:
            signal()
            return 1
        pl.when(jnp.logical_not(skip))(signal)
        return 1 - skip.astype(jnp.int32)

    for turn in range(1, 8):
        count += greet(other_dp(turn))
    for turn in range(1, WAYS):
        count += greet(other_mp(turn))
    for m in range(WAYS):
        for a, b, stays in (p.attention_of(m), p.owner_of(m)):
            count += greet((a, b), stays)
    for i in range(2):
        for a, b, stays in (qkv_to(i), qkv_from(i)):
            count += greet((a, b), stays)
    pl.semaphore_wait(barrier, count)

    def head_grad(m, pair, place):
        return Move(
            hg_ref.at[m, pair], do_ref.at[m, pair], do_send.at[m, pair], do_recv.at[m, pair], place
        )

    for pair in range(pairs):
        for m in range(WAYS):
            head_grad(m, pair, p.attention_of(m)).start()

    def half(h):
        kept, r1, r2, rz = ((f_kept0, f_r10, f_r20, f_rz0), (f_kept1, f_r11, f_r21, f_rz1))[h]
        some = pl.ds(h * f_kept0.shape[2], kept.shape[2])
        return Chain(
            p, lambda q, i: sum_ref.at[q, i, some], lambda q, slot, i: kept.at[q, slot],
            r1, r2, rz, f_send.at[h], f_recv.at[h],
        )

    ffn = [half(0), half(1)]
    loads = []

    def load(src, dst):
        copy = pltpu.make_async_copy(src, dst, load_sem.at[len(loads)])
        copy.start()
        loads.append(copy)
        return copy

    def fetch(h, q):
        kept, r1 = (f_kept0, f_r10) if h == 0 else (f_kept1, f_r11)
        some = pl.ds(h * f_kept0.shape[2], kept.shape[2])
        copies = []
        for slot in range(2):
            copies.append(load(sum_ref.at[q, ffn[h].slab(q, slot, False), some], kept.at[q, slot]))
        if q in DONE:
            copies.append(load(r1_ref.at[DONE.index(q), :, some], r1.at[q]))
        return copies

    fetched = {(h, q): fetch(h, q) for q in (0, 2, 1, 3) for h in range(2)}

    def second(h, q):
        for copy in fetched[h, q]:
            copy.wait()
        ffn[h].second(q, q in DONE)

    def third(h, *quarters):
        for q in quarters:
            ffn[h].third(q)

    def line(h, hop, *quarters):
        ffn[h].line(hop, quarters)

    for h in range(2):
        second(h, 0)
        second(h, 2)
    low_load = load(low_ref, x_in)
    late = [load(normed_ref, normed), load(w_ref, weight)]
    late.append(load(mgrad_ref, grad_ref))

    low_load.wait()
    low_here = own_first(core, x_in[...])
    for m in range(WAYS):
        mixed = jnp.concatenate([heads_ref[m, 0], heads_ref[m, 1]], axis=-1)
        value = dot_tn(mixed, low_here).astype(BF)
        h = p.mix(z, m)
        for d in range(value.shape[1] // LANES):
            a_sum[d % 2, h, d // 2] = value[:, d * LANES : (d + 1) * LANES]
    late.append(load(x_ref, x_in))
    swap = remote(a_sum.at[1], a_got, c_send.at[0], c_recv.at[0], (p.at_c, z))
    swap.start()
    attn_back_begin(0, k)
    swap.wait()
    for q in range(WAYS):
        a_sum[0, q] += a_got[q]
    attn = Chain(
        p, lambda q, i: a_sum.at[0, q, i], lambda q, slot, i: a_sum.at[0, q, i],
        a_r1, a_r2, a_rz, a_send, a_recv,
    )

    def qkv_x(pair, yy):
        at = (p.y if yy else 1 - p.y) * 4 + (1 - p.x) * 2
        return remote(
            q_sum.at[pair, pl.ds(at, 2)], q_rx.at[pair, yy],
            q_send.at[pair, yy], q_recv.at[pair, yy], (p.at_x, z),
        )

    def qkv_y(pair):
        at = (1 - p.y) * 4 + p.x * 2
        return remote(
            q_sum.at[pair, pl.ds(at, 2)], q_ry.at[pair],
            q_send.at[pair, 2], q_recv.at[pair, 2], (p.at_y, z),
        )

    def qkv_z(pair, turn, g, place):
        at = p.y * 4 + p.x * 2 + (p.group + turn) % 2
        return Move(
            q_sum.at[pair, at], q_rz.at[pair, g],
            q_send.at[pair, 3 + turn], q_recv.at[pair, 3 + g], place,
        )

    def qkv_first(pair):
        total = None
        for m in range(WAYS):
            part = dot_tn(low_piece(pair, m, k, rows), normed[m * rows : (m + 1) * rows, :])
            total = part if total is None else total + part
        value = total.astype(BF)
        for d in range(value.shape[1] // LANES):
            q_sum[pair, d] = value[:, d * LANES : (d + 1) * LANES]
        qkv_x(pair, 0).start()
        qkv_x(pair, 1).start()

    def qkv_second(pair):
        qkv_x(pair, 0).wait_recv()
        at = (1 - p.y) * 4 + p.x * 2
        for i in range(2):
            q_sum[pair, at + i] += q_rx[pair, 0, i]
        qkv_y(pair).start()
        qkv_x(pair, 1).wait_recv()
        at = p.y * 4 + p.x * 2
        for i in range(2):
            q_sum[pair, at + i] += q_rx[pair, 1, i]

    def qkv_third(pair):
        qkv_y(pair).wait_recv()
        at = p.y * 4 + p.x * 2
        for i in range(2):
            q_sum[pair, at + i] += q_ry[pair, i]
        for turn in range(2):
            qkv_z(pair, turn, p.group, qkv_to(turn)).start()

    def give_back(pair, m, part, place):
        some = pl.ds(m * rows, rows)
        if part == 0:
            src, dst = low.at[pair, 0, some], ret.at[m, pair, 0]
        else:
            src, dst = low.at[pair, pl.ds(1, 2), some], ret.at[m, pair, pl.ds(1, 2)]
        return Move(src, dst, g_send.at[m, pair, part], g_recv.at[m, pair, part], place)

    def finish_pair(pair):
        for m in range(WAYS):
            attn_back_end(pair, m, k, rows)
            give_back(pair, m, 1, p.owner_of(m)).start()

    def pair_end():
        finish_pair(0)
        attn_back_begin(1, k)
        for copy in late:
            copy.wait()
        qkv_first(0)

    every = range(WAYS)
    events = {
        1: [(third, 0, 0, 2), (ffn[0].first, 1), (ffn[0].first, 3), (line, 0, 1, 0, 2)],
        3: [(third, 1, 0, 2), (line, 1, 1, 0, 2)],
        4: [(line, 0, 2, 0, 2), (second, 0, 1), (second, 0, 3), (ffn[1].first, 1), (ffn[1].first, 3)],
        6: [(line, 1, 2, 0, 2)] + [(attn.first, q) for q in every],
        7: [(third, 0, 1, 3), (line, 0, 1, 1, 3), (line, 0, 3, 0, 2)],
        8: [(second, 1, 1), (second, 1, 3), (pair_end,)],
        9: [(line, 1, 3, 0, 2), (line, 0, 2, 1, 3)] + [(attn.second, q) for q in every],
        10: [(qkv_second, 0)],
        11: [(line, 0, 3, 1, 3), (third, 1, 1, 3), (line, 1, 1, 1, 3)] + [(attn.third, q) for q in every] + [(attn.line, 1, every)],
        12: [(qkv_third, 0)],
        13: [(line, 1, 2, 1, 3), (attn.line, 2, every)],
        15: [(line, 1, 3, 1, 3), (attn.line, 3, every)],
    }
    steps = v.shape[1] // STEP
    per = rows // STEP

    def body(i, carry):
        for at, todo in events.items():

            @pl.when(i == at)
            def _(todo=todo):
                for what, *args in todo:
                    what(*args)

        pair, step = i // steps, i % steps
        m = step // per

        @pl.when(step % per == 0)
        def _():
            head_grad(m, pair, p.owner_of(0)).wait_recv()

        at = pl.multiple_of((step - m * per) * STEP, STEP)
        attn_back_step(pair, step, do_ref[m, pair, pl.ds(at, STEP), :], k)

        @pl.when(step % per == per - 1)
        def _():
            give_back(pair, m, 0, p.owner_of(m)).start()

        return carry

    lax.fori_loop(0, pairs * steps, body, 0)
    finish_pair(1)
    qkv_first(1)

    def normed_part(pair, m):
        slot = p.mix(m, 2 * core)
        at = pair * 3 * LANES
        w = [weight[slot, d, at : at + 3 * LANES, :] for d in range(weight.shape[1])]
        grads = jnp.concatenate([ret[m, pair, c] for c in range(3)], axis=-1)
        return dot_nn(grads, jnp.concatenate(w, axis=-1))

    normed_grad = None
    for m in range(WAYS):
        for part in range(2):
            give_back(0, m, part, p.attention_of(m)).wait_recv()
        add = normed_part(0, m)
        normed_grad = add if normed_grad is None else normed_grad + add
    qkv_second(1)
    depth = a_r2.shape[1]
    attn.last(dv.at[:depth])
    attn_ref[...] = dv[:depth, :].T
    qkv_third(1)
    cut = f_kept0.shape[2]
    units = outer_ref.shape[1]
    ffn[0].last(dk.at[:cut])
    ffn[1].last(dk.at[cut : 3 * units])
    inner_ref[0] = dk[:units, :].T
    inner_ref[1] = dk[units : 2 * units, :].T
    outer_ref[...] = dk[2 * units : 3 * units, :].T
    vhat, scale = norm_stats(x_in[...].astype(F32))
    for pair in range(pairs):
        for g in range(2):
            qkv_z(pair, 0, g, qkv_from(g)).wait_recv()
        total = q_rz[pair, 0].astype(F32) + q_rz[pair, 1].astype(F32)
        for c in range(3):
            part = total[c * LANES : (c + 1) * LANES, :]
            qkv_ref[c, :, pair * LANES : (pair + 1) * LANES] = part.T
    for m in range(WAYS):
        for part in range(2):
            give_back(1, m, part, p.attention_of(m)).wait_recv()
        normed_grad += normed_part(1, m)
    gain_part = jnp.sum(normed_grad * vhat, axis=0, keepdims=True)
    s_own[...] = jnp.concatenate([gain_part, small_ref[1:, :]], axis=0)

    def sum_dp(turn):
        return remote(
            s_own, s_dp.at[turn], s_send.at[turn], s_recv.at[turn], other_dp(turn)
        )

    def sum_mp(turn):
        return remote(
            s_dp.at[0], s_mp.at[turn], s_send.at[8 + turn], s_recv.at[8 + turn], other_mp(turn)
        )

    for turn in range(1, 8):
        sum_dp(turn).start()
    grad_ref[...] += norm_back(vhat, scale, gain_ref[...], normed_grad)
    total = s_own[...]
    for turn in range(1, 8):
        sum_dp(turn).wait_recv()
        total += s_dp[turn]
    s_dp[0] = total
    for turn in range(1, WAYS):
        sum_mp(turn).start()
    for turn in range(1, WAYS):
        sum_mp(turn).wait_recv()
        total += s_mp[turn]
    gain_a_ref[...] = total[0:1, :]
    gain_m_ref[...] = total[1:2, :]
    squares = total[2:3, :LANES]
    lane = lax.broadcasted_iota(jnp.int32, squares.shape, 1)
    count = jnp.sum(jnp.where(lane == 4, squares, 0.0)) * x_ref.shape[1]
    rms_ref[...] = jnp.sqrt(squares / count)

    for turn in range(1, 8):
        sum_dp(turn).wait_send()
    for turn in range(1, WAYS):
        sum_mp(turn).wait_send()
    for m in range(WAYS):
        for pair in range(pairs):
            for part in range(2):
                give_back(pair, m, part, p.owner_of(m)).wait_send()
    for m in range(WAYS):
        for pair in range(pairs):
            head_grad(m, pair, p.attention_of(m)).wait_send()
    for pair in range(pairs):
        qkv_x(pair, 0).wait_send()
        qkv_x(pair, 1).wait_send()
        qkv_y(pair).wait_send()
        for turn in range(2):
            qkv_z(pair, turn, p.group, qkv_to(turn)).wait_send()
    ffn[0].finish(DONE)
    ffn[1].finish(DONE)
    attn.finish()


def backward_call(heads_grad, ffn_sum, r1, kept, weight, x, middle_grad, low, heads, gain, small):
    normed, cosine, sine, qa, ka, v, o = kept
    rows, model = x.shape
    pairs, tokens, unused = v.shape
    unused, wide, cols3, unused = weight.shape
    units = ffn_sum.shape[2]
    depth = model // WAYS
    third = cols3 // pairs
    part = (units // 32 + 1) * 16
    anywhere = pl.BlockSpec(memory_space=pl.ANY)
    vmem = pl.BlockSpec(memory_space=pltpu.VMEM)
    buf = lambda *shape, kind=BF: pltpu.VMEM(shape, kind)
    sems = lambda *shape: pltpu.SemaphoreType.DMA(shape)
    return pl.pallas_call(
        backward_kernel,
        in_specs=[anywhere] * 8 + [vmem] * 9,
        out_specs=[vmem] * 8,
        out_shape=[
            shape_of((rows, model), F32),
            shape_of((2, LANES, units // 3), F32),
            shape_of((LANES, units // 3), F32),
            shape_of((LANES, depth), F32),
            shape_of((3, LANES, pairs * LANES), F32),
            shape_of((1, model), F32),
            shape_of((1, model), F32),
            shape_of((1, LANES), F32),
        ],
        scratch_shapes=[
            buf(WAYS, pairs, rows, LANES),
            buf(pairs, 3, tokens, LANES),
            buf(2, tokens, LANES),
            buf(2, LANES, tokens),
            buf(tokens, LANES, kind=F32),
            buf(tokens, LANES, kind=F32),
            buf(tokens, model),
            buf(WAYS, wide, cols3, LANES),
            buf(rows, model),
            *[
                buf(*lead, cut, LANES)
                for cut in (part, units - part)
                for lead in ((WAYS, 2), (WAYS, 2), (WAYS,), (WAYS + 1,))
            ],
            buf(2, WAYS, wide // 2, depth, LANES),
            buf(WAYS, wide // 2, depth, LANES),
            buf(WAYS, 2, depth, LANES),
            buf(WAYS, depth, LANES),
            buf(WAYS + 1, depth, LANES),
            buf(pairs, wide, third, LANES),
            buf(pairs, 2, 2, third, LANES),
            buf(pairs, 2, third, LANES),
            buf(pairs, 2, third, LANES),
            buf(WAYS, pairs, 3, rows, LANES),
            buf(*small.shape, kind=F32),
            buf(8, *small.shape, kind=F32),
            buf(WAYS, *small.shape, kind=F32),
            sems(27),
            sems(WAYS, pairs),
            sems(WAYS, pairs),
            sems(2, 16),
            sems(2, 17),
            sems(16),
            sems(17),
            sems(1),
            sems(1),
            sems(pairs, 5),
            sems(pairs, 5),
            sems(WAYS, pairs, 2),
            sems(WAYS, pairs, 2),
            sems(12),
            sems(12),
        ],
        compiler_params=pltpu.CompilerParams(
            collective_id=2, has_side_effects=True, vmem_limit_bytes=62 * 1024 * 1024
        ),
        name="backward",
    )(
        heads_grad, ffn_sum, r1, normed, weight, x, middle_grad, low, heads,
        qa, ka, v, o, cosine, sine, gain, small,
    )


def pick(values, at, axis=0):
    return lax.dynamic_index_in_dim(values, at, axis, keepdims=False)


def flip(values, bit, dps):
    return lax.ppermute(values, "dp", [(i, i ^ bit) for i in range(dps)])


def to_attention(values, m, dps, back=False):
    pairs = []
    for dp in range(dps):
        group = dp % 2
        for t in range(WAYS):
            quarter = t ^ m
            there = (dp - group + ((quarter // 2) ^ group)) * WAYS + 2 * group + quarter % 2
            pairs.append((there, dp * WAYS + t) if back else (dp * WAYS + t, there))
    return lax.ppermute(values, ("dp", "mp"), pairs)


def local(
    sizes,
    layer_input,
    segment_ids,
    grad_out,
    qkv_weight,
    attn_weight,
    inner_weight,
    outer_weight,
    attn_gain,
    mlp_gain,
):
    dps, mps = sizes
    rows, model = layer_input.shape
    head_cols = qkv_weight.shape[2]
    units = inner_weight.shape[2]
    pairs = head_cols // LANES
    wide = model // LANES
    special = dps == wide
    me = lax.axis_index("mp")
    dp = lax.axis_index("dp")
    core = dp % 2
    group = me // 2
    quarter = me ^ (2 * core)
    scalars = jnp.stack([me, core if special else 0, quarter]).astype(jnp.int32)

    def every(values):
        got = lax.all_gather(values.T, "dp", axis=0, tiled=True).T
        got = got.reshape(-1, wide, LANES).transpose(1, 0, 2)
        return lax.all_gather(got, "mp", axis=1)

    qkv_part = qkv_weight.transpose(1, 2, 0).reshape(3, pairs, LANES, -1)
    qkv_part = qkv_part.transpose(1, 0, 2, 3).reshape(3 * head_cols, -1)
    inner_t = inner_weight.transpose(1, 2, 0)
    outer_t = outer_weight.T
    attn_depth = model // mps
    part_a = jnp.concatenate([attn_weight.T, inner_t[0]], axis=0)
    part_b = jnp.concatenate([inner_t[1], outer_t], axis=0)
    mine = segment_ids[0]
    info = jnp.broadcast_to(mine.astype(F32)[:, None], (mine.shape[0], LANES))
    info = info.reshape(WAYS, rows, LANES)
    if special:
        (pack_a, pack_b), heads, qkv_own, kept = forward_call(
            layer_input, info, attn_gain[None], qkv_part, [part_a, part_b], dps, pairs
        )
    else:
        x_all = jnp.stack([to_attention(layer_input, m, dps) for m in range(WAYS)])
        qkv_all, pack_a, pack_b = every(qkv_part), every(part_a), every(part_b)
        info = jnp.where(group == core, info, flip(info, 1, dps))
        qkv_own = qkv_all
        kept = alone_call(
            quarter, x_all, info, attn_gain[None], pick(qkv_all, quarter, 1), pairs)
        heads = kept[6].reshape(pairs, WAYS, rows, LANES)
        heads = [to_attention(heads[:, m], m, dps, back=True) for m in range(WAYS)]
        heads = jnp.stack(heads)
    normed, cosine, sine, qa, ka, v, o = kept

    outs = mlp_call(
        scalars, heads, layer_input, grad_out, mlp_gain[None], info, pack_a, pack_b,
        qkv_own, special,
    )
    layer_output, middle_grad, middle_low, small, heads_grad, ffn_sum, ffn_got, qkv_whole = outs
    if special:
        input_grad, inner_sum, outer_sum, attn_sum, qkv_sum, gain_a, gain_m, rms = backward_call(
            heads_grad, ffn_sum, ffn_got, kept, qkv_whole, layer_input, middle_grad, middle_low, heads,
            attn_gain[None], small,
        )
        return (
            layer_output,
            input_grad,
            qkv_sum.transpose(1, 0, 2),
            attn_sum,
            inner_sum.transpose(1, 0, 2),
            outer_sum,
            gain_a[0],
            gain_m[0],
            rms[0, :4],
        )
    else:
        lows = []
        for pair in range(pairs):
            grad = [to_attention(heads_grad[m, pair], m, dps) for m in range(WAYS)]
            low = attn_bwd_call(scalars, qa, ka, v, grad, o, cosine, sine, pair)
            lows.append(jnp.concatenate(low, axis=0))
        low = jnp.concatenate(lows, axis=1)
        own = pick(qkv_all, quarter, 1)
        own = jnp.concatenate([own[d] for d in range(wide)], axis=-1)
        normed_grad = dot_nn(low, own).astype(BF).reshape(WAYS, rows, model)
        normed_grad = sum(
            to_attention(normed_grad[m], m, dps, back=True).astype(F32) for m in range(WAYS)
        )

        def scatter(values):
            cut = lax.psum_scatter(values, "mp", scatter_dimension=0)
            return lax.psum_scatter(cut.T, "dp", scatter_dimension=0, tiled=True).T

        slot = (jnp.arange(mps) == quarter)[:, None, None]
        qkv_sum = scatter(jnp.where(slot, dot_tn(low, normed)[None], 0.0))
        mixed = jnp.stack([pick(heads, me ^ h) for h in range(mps)])
        mixed = mixed.transpose(0, 2, 1, 3).reshape(mps, rows, -1)
        attn_sum = scatter(jnp.stack([dot_tn(mixed[h], middle_low) for h in range(mps)]))
        ffn_sum = ffn_sum.reshape(mps, wide, 3 * units, LANES).transpose(0, 2, 1, 3)
        ffn_sum = scatter(ffn_sum.reshape(mps, 3 * units, model).astype(F32))
        vhat, scale = norm_stats(layer_input.astype(F32))
        input_grad = middle_grad + norm_back(vhat, scale, attn_gain, normed_grad)
        small = small.at[0].set(jnp.sum(normed_grad * vhat, axis=0))
        small = lax.psum(small, ("dp", "mp"))
    rms_values = jnp.sqrt(small[2, :4] / (small[2, 4] * model))

    qkv_sum = qkv_sum.reshape(pairs, 3, LANES, -1).transpose(3, 1, 0, 2)
    ffn_sum = ffn_sum.reshape(3, units, -1)
    return (
        layer_output,
        input_grad,
        qkv_sum.reshape(-1, 3, head_cols),
        attn_sum.T,
        ffn_sum[:2].transpose(2, 0, 1),
        ffn_sum[2].T,
        small[0],
        small[1],
        rms_values,
    )


def solution(mesh):
    sizes = (mesh.shape["dp"], mesh.shape["mp"])
    both = ("dp", "mp")
    whole = (P(both, None), P("dp", None, "mp"), P("dp", "mp"))
    return jax.shard_map(
        functools.partial(local, sizes),
        mesh=mesh,
        in_specs=(
            whole[0],
            P("dp", None),
            whole[0],
            whole[1],
            whole[2],
            whole[1],
            whole[2],
            P(),
            P(),
        ),
        out_specs=(
            whole[0],
            whole[0],
            whole[1],
            whole[2],
            whole[1],
            whole[2],
            P(),
            P(),
            P(),
        ),
        check_vma=False,
    )
```

```python
import functools
import math

import jax
import jax.numpy as jnp
from jax import lax
from jax.experimental import pallas as pl
from jax.experimental.pallas import tpu as pltpu
from jax.sharding import PartitionSpec as P

HEAD_DIM = 64
NORM_EPS = 1e-05
ROPE_BASE = 160000.0
BIG = 1e30
LANES = 128
WAYS = 4
BF = jnp.bfloat16
F32 = jnp.float32
VMEM_LIMIT = 56 * 1024 * 1024


def dot_nn(a, b):
    return lax.dot_general(a, b, (((1,), (0,)), ((), ())), preferred_element_type=F32)


def dot_nt(a, b):
    return lax.dot_general(a, b, (((1,), (1,)), ((), ())), preferred_element_type=F32)


def dot_tn(a, b):
    return lax.dot_general(a, b, (((0,), (0,)), ((), ())), preferred_element_type=F32)


def norm_stats(values):
    centre = jnp.mean(values, axis=-1, keepdims=True)
    shifted = values - centre
    spread = jnp.mean(shifted * shifted, axis=-1, keepdims=True)
    scale = lax.rsqrt(spread + NORM_EPS)
    return shifted * scale, scale


def norm_back(vhat, scale, gain, grad):
    u = grad * gain
    mean_u = jnp.mean(u, axis=-1, keepdims=True)
    mean_uv = jnp.mean(u * vhat, axis=-1, keepdims=True)
    return scale * (u - mean_u - vhat * mean_uv)


def swap_halves(values):
    lane = lax.broadcasted_iota(jnp.int32, values.shape, 1)
    first = lane % HEAD_DIM < HEAD_DIM // 2
    back = pltpu.roll(values, LANES - HEAD_DIM // 2, 1)
    ahead = pltpu.roll(values, HEAD_DIM // 2, 1)
    return jnp.where(first, back, ahead)


def choose(at, values):
    out = values[0]
    for i in range(1, len(values)):
        out = jnp.where(at == i, values[i], out)
    return out


def params():
    return pltpu.CompilerParams(vmem_limit_bytes=VMEM_LIMIT)


def cost(flops, mib):
    return pl.CostEstimate(flops=int(flops), bytes_accessed=int(mib * 2**20), transcendentals=0)


def call(kernel, scalars, grid, in_specs, out_specs, out_shape, scratch, estimate, name):
    spec = pltpu.PrefetchScalarGridSpec(
        num_scalar_prefetch=1,
        grid=grid,
        in_specs=in_specs,
        out_specs=out_specs,
        scratch_shapes=scratch,
    )
    return functools.partial(
        pl.pallas_call(
            kernel,
            grid_spec=spec,
            out_shape=out_shape,
            compiler_params=params(),
            cost_estimate=estimate,
            name=name,
        ),
        scalars,
    )


def full(shape):
    return pl.BlockSpec(shape, lambda i, s: (0,) * len(shape))


def shape_of(shape, dtype):
    return jax.ShapeDtypeStruct(shape, dtype)


def side_by_side(ref, *at):
    return jnp.concatenate([ref[(d, *at)] for d in range(ref.shape[0])], axis=-1)


STEP = 256


def doc_starts(pieces):
    number = lax.broadcasted_iota(jnp.int32, (1, LANES), 1).astype(F32)
    total = jnp.zeros((1, LANES), F32)
    for piece in pieces:
        before = jnp.logical_and(piece > 0.0, piece < number)
        total += jnp.sum(jnp.where(before, 1.0, 0.0), axis=0, keepdims=True)
    return total


def table_piece(m, segment, first, starts, out):
    rows = segment.shape[0]
    here = slice(m * rows, (m + 1) * rows)
    number = lax.broadcasted_iota(jnp.int32, (1, LANES), 1).astype(F32)
    start = jnp.sum(jnp.where(segment == number, starts, 0.0), axis=-1, keepdims=True)
    place = lax.broadcasted_iota(jnp.int32, (rows, 1), 0) + first
    position = place.astype(F32) - start
    lane = lax.broadcasted_iota(jnp.int32, (1, LANES), 1)
    half = HEAD_DIM // 2
    frequency = jnp.exp((lane % half).astype(F32) * (-2.0 * math.log(ROPE_BASE) / HEAD_DIM))
    angle = position * frequency
    sine = jnp.sin(angle)
    out.cosine[here, :] = jnp.cos(angle)
    out.sine[here, :] = jnp.where(lane % HEAD_DIM < half, -sine, sine)
    t = lane % HEAD_DIM
    same = segment == t.astype(F32)
    masked = jnp.where(same, 0.0, -BIG)
    out.qaux[here, :] = jnp.where(t >= 16, 0.0, masked).astype(BF)
    found = jnp.where(same, 1.0, 0.0)
    counted = jnp.where(t < 19, 1.0, 0.0)
    out.kaux[here, :] = jnp.where(t < 16, found, counted).astype(BF)
    out.live[here, :] = jnp.where(segment[:, 0:1] != 0.0, 1.0, 0.0)


def qkv_piece(m, x, gain, weight, out):
    rows = x.shape[0]
    here = slice(m * rows, (m + 1) * rows)
    vhat, unused = norm_stats(x.astype(F32))
    normed = (vhat * gain).astype(BF)
    out.normed[here, :] = normed
    flat = dot_nt(normed, weight)
    cosine, sine = out.cosine[here, :], out.sine[here, :]
    kaux = out.kaux[here, :]
    lane = lax.broadcasted_iota(jnp.int32, (rows, LANES), 1)
    for pair in range(flat.shape[1] // (3 * LANES)):
        q, k, v = [
            flat[:, at : at + LANES] for at in range(pair * 3 * LANES, (pair + 1) * 3 * LANES, LANES)
        ]
        q = (q * cosine + swap_halves(q) * sine).astype(BF)
        k = (k * cosine + swap_halves(k) * sine).astype(BF)
        out.q[pair, here, :] = q * jnp.asarray(HEAD_DIM**-0.5, BF)
        out.ka[pair, 0, here, :] = jnp.where(lane < HEAD_DIM, k, kaux)
        out.ka[pair, 1, here, :] = jnp.where(lane >= HEAD_DIM, k, kaux)
        out.v[pair, here, :] = v.astype(BF)


def attn_step(pair, step, out):
    tokens = out.v.shape[1]
    chunk = 512
    here = pl.ds(pl.multiple_of(step * STEP, STEP), STEP)
    lane = lax.broadcasted_iota(jnp.int32, (STEP, LANES), 1)
    t = lane % HEAD_DIM
    q = out.q[pair, here, :]
    qaux = out.qaux[here, :]
    live = out.live[here, :]
    outs = []
    for head in range(2):
        mine = (lane < HEAD_DIM) if head == 0 else (lane >= HEAD_DIM)
        qa = jnp.where(mine, q, qaux)
        top = None
        for at in range(0, tokens, chunk):
            s = dot_nt(qa, out.ka[pair, head, at : at + chunk, :])
            out.scores[:, at : at + chunk] = s
            part = jnp.max(s, axis=-1, keepdims=True)
            top = part if top is None else jnp.maximum(top, part)
        total = jnp.zeros((STEP, 1), F32)
        mixed = jnp.zeros((STEP, LANES), F32)
        for at in range(0, tokens, chunk):
            p = jnp.exp(out.scores[:, at : at + chunk] - top)
            total += jnp.sum(p, axis=-1, keepdims=True)
            mixed += dot_nn(p.astype(BF), out.v[pair, at : at + chunk, :])
        outs.append(mixed * (live / total))
        log_sum = jnp.where(live > 0, top + jnp.log(total), BIG)
        high = log_sum.astype(BF)
        rest = log_sum - high.astype(F32)
        mid = rest.astype(BF)
        low = (rest - mid.astype(F32)).astype(BF)
        aux = jnp.where(t == 16, -high, jnp.where(t == 17, -mid, jnp.where(t == 18, -low, qaux)))
        out.qa[pair, head, here, :] = jnp.where(mine, q, aux)
    out.o[pair, here, :] = jnp.where(lane < HEAD_DIM, outs[0], outs[1]).astype(BF)


class Kept:
    names = ("normed", "cosine", "sine", "qa", "ka", "v", "o", "q", "qaux", "kaux", "live", "scores")

    def __init__(self, refs):
        for name, ref in zip(self.names, refs):
            setattr(self, name, ref)


def kept_shapes(tokens, model, pairs):
    outs = [
        shape_of((tokens, model), BF),
        shape_of((tokens, LANES), F32),
        shape_of((tokens, LANES), F32),
        shape_of((pairs, 2, tokens, LANES), BF),
        shape_of((pairs, 2, tokens, LANES), BF),
        shape_of((pairs, tokens, LANES), BF),
        shape_of((pairs, tokens, LANES), BF),
    ]
    scratch = [
        pltpu.VMEM((pairs, tokens, LANES), BF),
        pltpu.VMEM((tokens, LANES), BF),
        pltpu.VMEM((tokens, LANES), BF),
        pltpu.VMEM((tokens, 1), F32),
        pltpu.VMEM((STEP, tokens), F32),
    ]
    return outs, scratch


def alone_kernel(quarter_ref, x_ref, info_ref, gain_ref, w_ref, *refs):
    out = Kept(refs)
    starts = doc_starts([info_ref[t] for t in range(WAYS)])
    for m in range(WAYS):
        t = quarter_ref[0] ^ m
        table_piece(m, info_ref[t], t * info_ref.shape[1], starts, out)
        qkv_piece(m, x_ref[m], gain_ref[...], side_by_side(w_ref), out)

    def body(step, carry):
        per = out.v.shape[1] // STEP
        attn_step(step // per, step % per, out)
        return carry

    lax.fori_loop(0, out.v.shape[0] * out.v.shape[1] // STEP, body, 0)


def alone_call(quarter, x, info, gain, weight, pairs):
    outs, scratch = kept_shapes(WAYS * x.shape[1], x.shape[2], pairs)
    return pl.pallas_call(
        alone_kernel,
        in_specs=[pl.BlockSpec(memory_space=pltpu.SMEM)]
        + [pl.BlockSpec(memory_space=pltpu.VMEM)] * 4,
        out_specs=[pl.BlockSpec(memory_space=pltpu.VMEM)] * len(outs),
        out_shape=outs,
        scratch_shapes=scratch,
        compiler_params=params(),
        name="forward",
    )(quarter.reshape(1), x, info, gain, weight)


def piece_block(m, rows, per):
    return pl.BlockSpec((rows, LANES), lambda i, s: (jnp.clip(i - per * m, 0, per - 1), 0))


def attn_bwd_kernel(s_ref, *refs):
    qa_ref, ka_ref, v_ref, o_ref, do_refs = refs[0], refs[1], refs[2], refs[3], refs[4:8]
    cosq_ref, sinq_ref, cosk_ref, sink_ref = refs[8:12]
    out_refs = refs[12:16]
    va_ref, kt_ref, dk_acc, dv_acc = refs[16:20]
    step = pl.program_id(0)
    rows = do_refs[0].shape[0]
    chunk = v_ref.shape[0] // WAYS
    per = chunk // rows
    piece = step // per
    lane_k = lax.broadcasted_iota(jnp.int32, (chunk, LANES), 1)
    lane = lax.broadcasted_iota(jnp.int32, (rows, LANES), 1)
    zero = jnp.zeros((), BF)

    @pl.when(step == 0)
    def _():
        ones = jnp.where(lane_k % HEAD_DIM < 3, jnp.ones((), BF), zero)
        for m in range(WAYS):
            some = slice(m * chunk, (m + 1) * chunk)
            v = v_ref[some, :]
            for head in range(2):
                mine = (lane_k < HEAD_DIM) if head == 0 else (lane_k >= HEAD_DIM)
                va_ref[head, some, :] = jnp.where(mine, v, ones)
                own = jnp.where(mine, ka_ref[head, some, :], zero).astype(F32)
                kt_ref[head, :, some] = own.T.astype(BF)
        dk_acc[...] = jnp.zeros_like(dk_acc)
        dv_acc[...] = jnp.zeros_like(dv_acc)

    grad = choose(piece, [r[...] for r in do_refs])
    out = o_ref[...]
    product = grad.astype(F32) * out.astype(F32)
    turned = jnp.zeros((LANES, rows), F32)
    for head in range(2):
        mine = (lane < HEAD_DIM) if head == 0 else (lane >= HEAD_DIM)
        delta = jnp.sum(jnp.where(mine, product, 0.0), axis=-1, keepdims=True)
        high = delta.astype(BF)
        rest = delta - high.astype(F32)
        mid = rest.astype(BF)
        low = (rest - mid.astype(F32)).astype(BF)
        t = lane % HEAD_DIM
        aux = jnp.where(t == 0, -high, jnp.where(t == 1, -mid, jnp.where(t == 2, -low, zero)))
        grad_aug = jnp.where(mine, grad, aux)
        grad_own = jnp.where(mine, grad, zero)
        qa = qa_ref[head]
        q_own = jnp.where(mine, qa, zero)
        for m in range(WAYS):
            some = slice(m * chunk, (m + 1) * chunk)
            prob = jnp.exp(dot_nt(ka_ref[head, some, :], qa))
            back = dot_nt(va_ref[head, some, :], grad_aug)
            score_grad = (prob * back).astype(BF)
            dv_acc[some, :] += dot_nn(prob.astype(BF), grad_own)
            dk_acc[some, :] += dot_nn(score_grad, q_own)
            turned += dot_nn(kt_ref[head, :, some], score_grad)
    dq = turned.T * (HEAD_DIM**-0.5)
    dq = (dq * cosq_ref[...] - swap_halves(dq) * sinq_ref[...]).astype(BF)
    for m in range(WAYS):

        @pl.when(piece == m)
        def _(m=m):
            here = pl.ds(pl.multiple_of((step - m * per) * rows, rows), rows)
            out_refs[m][here, :LANES] = dq

    @pl.when(step == pl.num_programs(0) - 1)
    def _():
        for m in range(WAYS):
            some = slice(m * chunk, (m + 1) * chunk)
            dk = dk_acc[some, :]
            dk = dk * cosk_ref[some, :] - swap_halves(dk) * sink_ref[some, :]
            out_refs[m][:, LANES : 2 * LANES] = dk.astype(BF)
            out_refs[m][:, 2 * LANES :] = dv_acc[some, :].astype(BF)


def attn_bwd_call(scalars, qa, ka, v, grad, o, cosine, sine, pair):
    tokens = v.shape[1]
    chunk = tokens // WAYS
    rows = 256
    per = chunk // rows
    moving = [piece_block(m, rows, per) for m in range(WAYS)]
    block = pl.BlockSpec((rows, LANES), lambda i, s: (i, 0))
    return call(
        attn_bwd_kernel,
        scalars,
        (tokens // rows,),
        [
            pl.BlockSpec((None, 2, rows, LANES), lambda i, s: (pair, 0, i, 0)),
            pl.BlockSpec((None, 2, tokens, LANES), lambda i, s: (pair, 0, 0, 0)),
            pl.BlockSpec((None, tokens, LANES), lambda i, s: (pair, 0, 0)),
            pl.BlockSpec((None, rows, LANES), lambda i, s: (pair, i, 0)),
        ]
        + moving
        + [block, block, full((tokens, LANES)), full((tokens, LANES))],
        [full((chunk, 3 * LANES))] * WAYS,
        [shape_of((chunk, 3 * LANES), BF)] * WAYS,
        [
            pltpu.VMEM((2, tokens, LANES), BF),
            pltpu.VMEM((2, LANES, tokens), BF),
            pltpu.VMEM((tokens, LANES), F32),
            pltpu.VMEM((tokens, LANES), F32),
        ],
        cost(28 * tokens * tokens * LANES, 8),
        "attn_bwd",
    )(qa, ka, v, o, *grad, cosine, sine, cosine, sine)


def own_first(core, values):
    cut = [values[:, at : at + LANES] for at in range(0, values.shape[1], LANES)]
    turned = [cut[i ^ 1] for i in range(len(cut))]
    return jnp.where(core == 0, values, jnp.concatenate(turned, axis=-1))


MESH = pl.DeviceIdType.MESH
UP, DOWN, TO_X, TO_Y, TO_D, CORE_OWN, CORE_X, CORE_Y, CORE_D = range(9)
FROM_Z, FROM_X, FROM_Y, FROM_D = range(4)
CHUNKS = 4


class Place:
    def __init__(self):
        self.dp, self.z = lax.axis_index("dp"), lax.axis_index("mp")
        self.core, self.x, self.y = self.dp % 2, (self.dp // 2) % 2, self.dp // 4
        self.at_c = self.dp + 1 - 2 * self.core
        self.at_x = self.dp + 2 - 4 * self.x
        self.at_y = self.dp + 4 - 8 * self.y
        self.at_d = self.at_x + self.at_y - self.dp
        self.group = self.z // 2
        self.far_z = self.z + 2 - 4 * self.group
        self.quarter = self.z + self.core * (self.far_z - self.z)

    @staticmethod
    def mix(q, m):
        return (q + m) % 2 + 2 * ((q // 2 + m // 2) % 2)

    def stays(self, a, b):
        return jnp.logical_and(a == self.dp, b == self.z)

    def attention_of(self, m):
        h = self.mix(self.z, m)
        a, b = self.dp - self.core + (h // 2 + self.core) % 2, 2 * self.core + h % 2
        return a, b, self.stays(a, b)

    def owner_of(self, m):
        a, b = self.dp - self.core + self.group, self.mix(self.quarter, m)
        return a, b, self.stays(a, b)


def remote(src, dst, send, recv, device):
    return pltpu.make_async_remote_copy(
        src_ref=src, dst_ref=dst, send_sem=send, recv_sem=recv,
        device_id=device, device_id_type=MESH,
    )


class Move:
    def __init__(self, src, dst, send, recv, place):
        a, b, self.stays = place
        self.far = lambda: remote(src, dst, send, recv, (a, b))
        self.near = lambda: pltpu.make_async_copy(src, dst, recv)

    def start(self):
        pl.when(self.stays)(lambda: self.near().start())
        pl.when(jnp.logical_not(self.stays))(lambda: self.far().start())

    def wait_recv(self):
        self.far().wait_recv()

    def wait_send(self):
        pl.when(jnp.logical_not(self.stays))(lambda: self.far().wait_send())


def forward_kernel(x_ref, info_ref, gain_ref, qkv_ref, *refs, packs):
    parts, outs, heads_ref = refs[:packs], refs[packs : 2 * packs], refs[2 * packs]
    saved, refs = refs[2 * packs + 1 : 2 * packs + 7], refs[2 * packs + 7 :]
    qa, o, normed, cosine, sine, ka, v, q, qaux, kaux, live, scores = refs[:12]
    kept = Kept((normed, cosine, sine, qa, ka, v, o, q, qaux, kaux, live, scores))
    x_all, w_ref, infos = refs[12:15]
    (
        sends, recvs, cores, locals_, token_send, token_recv, relay_send, info_sem,
        head_send, head_recv,
        q_send, q_recv, save_sem,
    ) = refs[15:]
    dp, z = lax.axis_index("dp"), lax.axis_index("mp")
    core, xb, yb = dp % 2, (dp // 2) % 2, dp // 4
    at_c, at_x, at_y = dp + 1 - 2 * core, dp + 2 - 4 * xb, dp + 4 - 8 * yb
    at_d = at_x + at_y - dp
    group = z // 2
    far_z = z + 2 - 4 * group
    quarter = z + core * (far_z - z)

    def mix(q, m):
        return (q + m) % 2 + 2 * ((q // 2 + m // 2) % 2)

    def attention_of(m):
        h = mix(z, m)
        return dp - core + (h // 2 + core) % 2, 2 * core + h % 2

    def owner_of(m):
        return dp - core + group, mix(quarter, m)

    barrier = pltpu.get_barrier_semaphore()

    def greet(device, when=None):
        def signal():
            pl.semaphore_signal(barrier, inc=1, device_id=device, device_id_type=MESH)

        signal() if when is None else pl.when(when)(signal)

    greet((at_c, z))
    greet((at_x, z))
    greet((at_y, z))
    greet((dp, far_z))
    greet((dp, z + 1), z < WAYS - 1)
    greet((dp, z - 1), z > 0)
    count = 4 + (z < WAYS - 1).astype(jnp.int32) + (z > 0).astype(jnp.int32)
    here, there = [], []
    for m in range(WAYS):
        for of, found in ((attention_of, here), (owner_of, there)):
            a, b = of(m)
            stays = jnp.logical_and(a == dp, b == z)
            found.append((a, b, stays))
            greet((a, b), jnp.logical_not(stays))
            count += 1 - stays.astype(jnp.int32)
    pl.semaphore_wait(barrier, count)

    def remote(src, dst, send, recv, device):
        return pltpu.make_async_remote_copy(
            src_ref=src, dst_ref=dst, send_sem=send, recv_sem=recv,
            device_id=device, device_id_type=MESH,
        )

    def copy(p, kind, s, src=None):
        who = {CORE_X: at_x, CORE_Y: at_y, CORE_D: at_d}.get(kind, dp)
        if kind == TO_D:
            who = jnp.where(s < 2, at_x, at_y)
        slab = outs[p].at[who, s]
        send = sends.at[p, kind, s]
        if kind == UP:
            recv, device = recvs.at[p, FROM_Z, s], (dp, z + 1)
        elif kind == DOWN:
            recv, device = recvs.at[p, FROM_Z, s], (dp, z - 1)
        elif kind == TO_X:
            recv, device = recvs.at[p, FROM_X, s], (at_x, z)
        elif kind == TO_Y:
            recv, device = recvs.at[p, FROM_Y, s], (at_y, z)
        elif kind == TO_D:
            recv, device = recvs.at[p, FROM_D, s], (jnp.where(s < 2, at_y, at_x), z)
        else:
            recv, device = cores.at[p, kind - CORE_OWN, s], (at_c, z)
        return remote(slab if src is None else src, slab, send, recv, device)

    def arrived(p, sem, who, s):
        slab = outs[p].at[who, s]
        remote(slab, slab, sends.at[p, UP, s], sem, (at_c, z)).wait_recv()

    def spread(p, s, src=None):
        copy(p, TO_X, s, src).start()
        copy(p, TO_Y, s, src).start()
        copy(p, CORE_OWN, s, src).start()

    def begin(p):
        src = parts[p]
        spread(p, z, src)
        pltpu.make_async_copy(src, outs[p].at[dp, z], locals_.at[p]).start()

    def begin_line(p):
        src = parts[p]
        pl.when(z < WAYS - 1)(lambda: copy(p, UP, z, src).start())
        pl.when(z > 0)(lambda: copy(p, DOWN, z, src).start())

    def reach(p, hop):
        def one(s):
            arrived(p, recvs.at[p, FROM_Z, s], dp, s)
            spread(p, s)

        pl.when(z >= hop)(lambda: one(z - hop))
        pl.when(z + hop < WAYS)(lambda: one(z + hop))

    def ahead(p, hop):
        pl.when(jnp.logical_and(z >= hop, z < WAYS - 1))(lambda: copy(p, UP, z - hop).start())
        pl.when(jnp.logical_and(z + hop < WAYS, z > 0))(lambda: copy(p, DOWN, z + hop).start())

    def line(p, hop):
        reach(p, hop)
        if hop < WAYS - 1:
            ahead(p, hop)

    def plane(p, hop):
        def one(s):
            arrived(p, recvs.at[p, FROM_X, s], at_x, s)
            copy(p, CORE_X, s).start()
            pl.when(s < 2)(lambda: copy(p, TO_D, s).start())
            arrived(p, recvs.at[p, FROM_Y, s], at_y, s)
            copy(p, CORE_Y, s).start()
            pl.when(s >= 2)(lambda: copy(p, TO_D, s).start())

        if hop == 0:
            one(z)
        else:
            pl.when(z >= hop)(lambda: one(z - hop))
            pl.when(z + hop < WAYS)(lambda: one(z + hop))

    def corner(p, hop):
        def one(s):
            arrived(p, recvs.at[p, FROM_D, s], at_d, s)
            copy(p, CORE_D, s).start()

        if hop == 0:
            one(z)
        else:
            pl.when(z >= hop)(lambda: one(z - hop))
            pl.when(z + hop < WAYS)(lambda: one(z + hop))

    def from_core(p):
        for s in range(WAYS):
            for kind in range(4):
                twin = (at_c, at_x + at_c - dp, at_y + at_c - dp, at_d + at_c - dp)[kind]
                arrived(p, cores.at[p, kind, s], twin, s)
        pltpu.make_async_copy(parts[p], outs[p].at[dp, z], locals_.at[p]).wait()

    def finish(p):
        for s in range(WAYS):
            pl.when(jnp.logical_and(z < WAYS - 1, s <= z))(lambda s=s: copy(p, UP, s).wait_send())
            pl.when(jnp.logical_and(z > 0, s >= z))(lambda s=s: copy(p, DOWN, s).wait_send())
            for kind in range(TO_X, CORE_D + 1):
                copy(p, kind, s).wait_send()

    far = (z // 2 + core) % 2 == 1
    straight = (z + 1 + core) % 2
    relays = jnp.logical_and(core == 1, jnp.logical_and(z > 0, z < WAYS - 1))
    beside = (dp, z + 1 - 2 * (z % 2))
    cut = x_ref.shape[0] // CHUNKS

    def token(m, c):
        to_dp, to_z, stays = here[m]
        some = pl.ds(c * cut, cut)
        src, dst = x_ref.at[some], x_all.at[m, some]

        def direct():
            return remote(src, dst, token_send.at[m, c], token_recv.at[m, c], (to_dp, to_z))

        def near():
            return pltpu.make_async_copy(src, dst, token_recv.at[m, c])

        goes = jnp.logical_and(
            jnp.logical_not(stays), jnp.logical_or(jnp.logical_not(far), straight == m)
        )
        return direct, near, stays, goes

    def relay(m, c):
        some = pl.ds(c * cut, cut)
        return remote(
            x_all.at[m, some], x_all.at[1 - m, some],
            relay_send.at[m, c], token_recv.at[1 - m, c], beside,
        )

    def pass_on(m, c):
        some = pl.ds(c * cut, cut)
        return remote(
            x_all.at[m, some], x_all.at[m + 2, some],
            token_send.at[m + 2, c], token_recv.at[m + 2, c], (at_c, z),
        )

    def take_tokens(c):
        for m in range(2):
            token(m, c)[0]().wait_recv()
            pl.when(relays)(lambda m=m: relay(m, c).start())
            pass_on(m, c).start()

    def early(*chunks):
        def run():
            for c in chunks:
                take_tokens(c)

        pl.when(relays)(run)

    def swap_info():
        return remote(info_ref, infos.at[1], info_sem.at[0], info_sem.at[1], (at_c, z))

    def own_info():
        return pltpu.make_async_copy(info_ref, infos.at[0], locals_.at[packs])

    def q_copy(kind, i=0, src=None):
        who = {"z": dp, "x": dp, "y": dp, "c": dp, "cx": at_x, "cy": at_y, "cd": at_d}.get(kind)
        if kind == "d":
            who = at_x if i == 0 else at_y
        device = {"z": (dp, far_z), "x": (at_x, z), "y": (at_y, z)}.get(kind, (at_c, z))
        if kind == "d":
            device = (at_y, z) if i == 0 else (at_x, z)
        slot = {"z": 0, "x": 1, "y": 3, "d": 5, "c": 7, "cx": 8, "cy": 9, "cd": 10}[kind]
        if kind in ("x", "y", "d"):
            slot += i
        if kind == "z":
            i = 1
        if kind[0] == "c":
            i = 1 - core
        dst = w_ref.at[i, who]
        return remote(dst if src is None else src, dst, q_send.at[slot], q_recv.at[slot], device)

    def q_arrived(kind, i=0):
        q_copy(kind, i).wait_recv()

    def own_q():
        return pltpu.make_async_copy(qkv_ref, w_ref.at[0, dp], locals_.at[packs + 1])

    q_kinds = [("z", 0), ("x", 0), ("x", 1), ("y", 0), ("y", 1), ("d", 0), ("d", 1)]
    q_kinds += [("c", 0), ("cx", 0), ("cy", 0), ("cd", 0)]

    keeps = [w_ref.at[core], normed, cosine, sine, ka, v]

    def save(i):
        return pltpu.make_async_copy(keeps[i], saved[i], save_sem.at[i])

    rows = x_ref.shape[0]

    def head(pair, m, owner):
        src = kept.o.at[pair, pl.ds(m * rows, rows)]
        dst = heads_ref.at[m, pair]
        to_dp, to_z, stays = owner

        def far():
            return remote(
                src, dst, head_send.at[m, pair], head_recv.at[m, pair], (to_dp, to_z)
            )

        def near():
            return pltpu.make_async_copy(src, dst, head_recv.at[m, pair])

        return far, near, stays

    def start(item):
        far, near, stays = item
        pl.when(stays)(lambda: near().start())
        pl.when(jnp.logical_not(stays))(lambda: far().start())

    def end_send(item):
        far, near, stays = item
        pl.when(jnp.logical_not(stays))(lambda: far().wait_send())

    q_copy("z", 0, qkv_ref).start()
    q_copy("x", 0, qkv_ref).start()
    q_copy("y", 0, qkv_ref).start()
    own_q().start()
    for c in range(CHUNKS):
        for m in range(2):
            direct, near, stays, goes = token(m, c)
            pl.when(stays)(lambda: near().start())
            pl.when(goes)(lambda: direct().start())
    swap_info().start()
    own_info().start()
    for p in range(packs):
        begin(p)
        begin_line(p)
    own_info().wait()
    swap_info().wait()
    own_q().wait()
    q_arrived("x", 0)
    q_copy("d", 0).start()
    q_arrived("z")
    q_copy("x", 1).start()
    q_copy("y", 1).start()
    early(0)
    away = (group + core) % 2
    starts = doc_starts([infos[away, t] for t in range(WAYS)])
    for m in range(WAYS):
        t = mix(quarter, m)
        table_piece(m, infos[away, t], t * x_ref.shape[0], starts, kept)
    q_arrived("y", 0)
    q_copy("c").start()
    plane(0, 0)
    q_arrived("x", 1)
    q_copy("cx").start()
    q_arrived("y", 1)
    q_copy("d", 1).start()
    q_copy("cy").start()
    early(1)
    plane(1, 0)
    q_arrived("d", 0)
    q_arrived("d", 1)
    q_copy("cd").start()
    early(2)
    reach(0, 1)
    corner(0, 0)
    reach(1, 1)
    corner(1, 0)
    for kind in ("c", "cx", "cy", "cd"):
        q_arrived(kind)
    save(0).start()
    save(2).start()
    save(3).start()
    early(3)
    @pl.when(jnp.logical_not(relays))
    def _():
        for c in range(CHUNKS):
            take_tokens(c)

    for p in range(packs):
        ahead(p, 1)
        plane(p, 1)
    for m in range(WAYS):
        if m >= 2:
            for c in range(CHUNKS):
                pass_on(m - 2, c).wait_recv()
        weight = jnp.concatenate([w_ref[core, d] for d in range(w_ref.shape[1])], axis=-1)
        qkv_piece(m, x_all[m], gain_ref[...], weight, kept)
        if m == 2:
            line(0, 2)
            corner(0, 1)
    save(1).start()
    save(4).start()
    save(5).start()

    events = {
        1: [(line, 1, 2)],
        2: [(line, 0, 3), (corner, 1, 1)],
        4: [(plane, 0, 2)],
        5: [(line, 1, 3)],
        7: [(plane, 1, 2)],
        9: [(corner, 0, 2)],
        11: [(plane, 0, 3)],
        13: [(corner, 1, 2)],
        15: [(plane, 1, 3)],
    }
    steps = kept.v.shape[1] // STEP
    pairs = kept.v.shape[0]
    per = steps // WAYS

    def body(i, carry):
        for at, todo in events.items():

            @pl.when(i == at)
            def _(todo=todo):
                for what, p, hop in todo:
                    what(p, hop)

        pair = i // steps
        step = i % steps
        attn_step(pair, step, kept)
        m = step // per

        @pl.when(step % per == per - 1)
        def _():
            a, b = dp - core + group, mix(quarter, m)
            start(head(pair, m, (a, b, jnp.logical_and(a == dp, b == z))))

        return carry

    lax.fori_loop(0, pairs * steps, body, 0)
    corner(0, 3)
    corner(1, 3)
    for p in range(packs):
        from_core(p)
    for m in range(WAYS):
        for pair in range(pairs):
            head(pair, m, there[m])[0]().wait_recv()
            end_send(head(pair, m, there[m]))
    for c in range(CHUNKS):
        for m in range(2):
            pass_on(m, c).wait_send()
            direct, near, stays, goes = token(m, c)
            pl.when(goes)(lambda: direct().wait_send())
            pl.when(relays)(lambda m=m, c=c: relay(m, c).wait_send())
    for p in range(packs):
        finish(p)
    for kind, i in q_kinds:
        q_copy(kind, i).wait_send()
    for i in range(len(keeps)):
        save(i).wait()


def forward_call(x, info, gain, qkv_part, parts, dps, pairs):
    rows, model = x.shape
    packs = len(parts)
    anywhere = pl.BlockSpec(memory_space=pl.ANY)
    vmem = pl.BlockSpec(memory_space=pltpu.VMEM)
    outs, scratch = kept_shapes(WAYS * rows, model, pairs)
    normed, cosine, sine, qa, ka, v, o = outs
    hold = [normed, cosine, sine, ka, v]
    weight = (dps,) + qkv_part.shape
    out = pl.pallas_call(
        functools.partial(forward_kernel, packs=packs),
        in_specs=[anywhere, anywhere, vmem] + [anywhere] * (1 + packs),
        out_specs=[anywhere] * (packs + 7) + [vmem] * 2,
        out_shape=[shape_of((dps, WAYS) + part.shape, BF) for part in parts]
        + [shape_of((WAYS, pairs, rows, LANES), BF), shape_of(weight, BF)]
        + hold
        + [qa, o],
        scratch_shapes=[pltpu.VMEM(h.shape, h.dtype) for h in hold]
        + scratch
        + [
            pltpu.VMEM((WAYS, rows, model), BF),
            pltpu.VMEM((2,) + weight, BF),
            pltpu.VMEM((2, WAYS, rows, LANES), F32),
            pltpu.SemaphoreType.DMA((packs, 9, WAYS)),
            pltpu.SemaphoreType.DMA((packs, 4, WAYS)),
            pltpu.SemaphoreType.DMA((packs, 4, WAYS)),
            pltpu.SemaphoreType.DMA((packs + 2,)),
            pltpu.SemaphoreType.DMA((WAYS, CHUNKS)),
            pltpu.SemaphoreType.DMA((WAYS, CHUNKS)),
            pltpu.SemaphoreType.DMA((2, CHUNKS)),
            pltpu.SemaphoreType.DMA((2,)),
            pltpu.SemaphoreType.DMA((WAYS, pairs)),
            pltpu.SemaphoreType.DMA((WAYS, pairs)),
            pltpu.SemaphoreType.DMA((11,)),
            pltpu.SemaphoreType.DMA((11,)),
            pltpu.SemaphoreType.DMA((6,)),
        ],
        compiler_params=pltpu.CompilerParams(
            collective_id=0, has_side_effects=True, vmem_limit_bytes=VMEM_LIMIT
        ),
        name="forward",
    )(x, info, gain, qkv_part, *parts)
    packs_out, out = out[:packs], out[packs:]
    heads, weight, normed, cosine, sine, ka, v, qa, o = out
    return packs_out, heads, weight, (normed, cosine, sine, qa, ka, v, o)


def attn_back_begin(pair, k):
    chunk = 512
    lane = lax.broadcasted_iota(jnp.int32, (chunk, LANES), 1)
    zero = jnp.zeros((), BF)
    ones = jnp.where(lane % HEAD_DIM < 3, jnp.ones((), BF), zero)
    for at in range(0, k.dk.shape[0], chunk):
        some = slice(at, at + chunk)
        v = k.v[pair, some, :]
        for head in range(2):
            mine = (lane < HEAD_DIM) if head == 0 else (lane >= HEAD_DIM)
            k.va[head, some, :] = jnp.where(mine, v, ones)
            own = jnp.where(mine, k.ka[pair, head, some, :], zero).astype(F32)
            k.kt[head, :, some] = own.T.astype(BF)
    k.dk[...] = jnp.zeros_like(k.dk)
    k.dv[...] = jnp.zeros_like(k.dv)


def attn_back_step(pair, step, grad, k):
    chunk = 512
    here = pl.ds(pl.multiple_of(step * STEP, STEP), STEP)
    lane = lax.broadcasted_iota(jnp.int32, (STEP, LANES), 1)
    zero = jnp.zeros((), BF)
    t = lane % HEAD_DIM
    product = grad.astype(F32) * k.o[pair, here, :].astype(F32)
    turned = jnp.zeros((LANES, STEP), F32)
    for head in range(2):
        mine = (lane < HEAD_DIM) if head == 0 else (lane >= HEAD_DIM)
        delta = jnp.sum(jnp.where(mine, product, 0.0), axis=-1, keepdims=True)
        high = delta.astype(BF)
        rest = delta - high.astype(F32)
        mid = rest.astype(BF)
        low = (rest - mid.astype(F32)).astype(BF)
        aux = jnp.where(t == 0, -high, jnp.where(t == 1, -mid, jnp.where(t == 2, -low, zero)))
        grad_aug = jnp.where(mine, grad, aux)
        grad_own = jnp.where(mine, grad, zero)
        qa = k.qa[pair, head, here, :]
        q_own = jnp.where(mine, qa, zero)
        for at in range(0, k.dk.shape[0], chunk):
            some = slice(at, at + chunk)
            prob = jnp.exp(dot_nt(k.ka[pair, head, some, :], qa))
            back = dot_nt(k.va[head, some, :], grad_aug)
            score_grad = (prob * back).astype(BF)
            k.dv[some, :] += dot_nn(prob.astype(BF), grad_own)
            k.dk[some, :] += dot_nn(score_grad, q_own)
            turned += dot_nn(k.kt[head, :, some], score_grad)
    dq = turned.T * (HEAD_DIM**-0.5)
    dq = dq * k.cosine[here, :] - swap_halves(dq) * k.sine[here, :]
    k.low[pair, 0, here, :] = dq.astype(BF)


def attn_back_end(pair, m, k, rows):
    some = slice(m * rows, (m + 1) * rows)
    dk = k.dk[some, :]
    dk = dk * k.cosine[some, :] - swap_halves(dk) * k.sine[some, :]
    k.low[pair, 1, some, :] = dk.astype(BF)
    k.low[pair, 2, some, :] = k.dv[some, :].astype(BF)


def low_piece(pair, m, k, rows):
    some = slice(m * rows, (m + 1) * rows)
    return jnp.concatenate([k.low[pair, c, some, :] for c in range(3)], axis=-1)


class Back:
    names = ("qa", "ka", "v", "o", "cosine", "sine", "low", "va", "kt", "dk", "dv")

    def __init__(self, refs):
        for name, ref in zip(self.names, refs):
            setattr(self, name, ref)


class Chain:
    def __init__(self, p, source, kept, r1, r2, rz, send, recv):
        self.p, self.source, self.kept = p, source, kept
        self.r1, self.r2, self.rz, self.send, self.recv = r1, r2, rz, send, recv

    def slab(self, q, slot, away):
        x, y = self.p.x, self.p.y
        if q < 2:
            return (y if slot else 1 - y) * 2 + (1 - x if away else x)
        return (1 - y if away else y) * 2 + (x if slot else 1 - x)

    def near(self, q, second=False):
        p = self.p
        return (p.at_x, p.z) if (q < 2) != second else (p.at_y, p.z)

    def stage1(self, q, slot):
        src = self.source(q, self.slab(q, slot, True))
        at = q * 2 + slot
        return remote(src, self.r1.at[q, slot], self.send.at[at], self.recv.at[at], self.near(q))

    def stage2(self, q):
        at = 8 + q
        src = self.kept(q, 0, self.slab(q, 0, False))
        return remote(src, self.r2.at[q], self.send.at[at], self.recv.at[at], self.near(q, True))

    def first(self, q):
        self.stage1(q, 0).start()
        self.stage1(q, 1).start()

    def second(self, q, done=False):
        if not done:
            self.stage1(q, 0).wait_recv()
        ref = self.kept(q, 0, self.slab(q, 0, False))
        ref[...] += self.r1[q, 0]
        self.stage2(q).start()
        if not done:
            self.stage1(q, 1).wait_recv()
        self.own(q)[...] += self.r1[q, 1]

    def own(self, q):
        return self.kept(q, 1, self.slab(q, 1, False))

    def third(self, q):
        self.stage2(q).wait_recv()
        self.own(q)[...] += self.r2[q]

    def lined(self, q, down):
        z = self.p.z
        at = q if down else q + 1
        return remote(
            self.own(q), self.rz.at[at], self.send.at[12 + q], self.recv.at[12 + at],
            (self.p.dp, z - 1 if down else z + 1),
        )

    def line(self, hop, quarters):
        z = self.p.z
        for q in quarters:
            if q < WAYS - hop:

                @pl.when(z == WAYS - hop)
                def _(q=q):
                    if hop > 1:
                        self.lined(q, True).wait_recv()
                        self.own(q)[...] += self.rz[q]
                    self.lined(q, True).start()

            if q > hop - 1:

                @pl.when(z == hop - 1)
                def _(q=q):
                    if hop > 1:
                        self.lined(q, False).wait_recv()
                        self.own(q)[...] += self.rz[q + 1]
                    self.lined(q, False).start()

    def last(self, out_ref):
        z = self.p.z
        for q in range(WAYS):

            @pl.when(z == q)
            def _(q=q):
                total = self.own(q)[...].astype(F32)
                if q < WAYS - 1:
                    self.lined(q, True).wait_recv()
                    total += self.rz[q].astype(F32)
                if q > 0:
                    self.lined(q, False).wait_recv()
                    total += self.rz[q + 1].astype(F32)
                out_ref[...] = total

    def finish(self, done=()):
        z = self.p.z
        for q in range(WAYS):
            if q not in done:
                self.stage1(q, 0).wait_send()
                self.stage1(q, 1).wait_send()
            self.stage2(q).wait_send()
            pl.when(q < z)(lambda q=q: self.lined(q, True).wait_send())
            pl.when(q > z)(lambda q=q: self.lined(q, False).wait_send())


DONE = (0, 2)


def turn_of(step):
    return 2 * (step % 2) + step // 2


def mlp_kernel(
    s_ref, heads_ref, x_ref, g_ref, gain_ref, live_ref, pack_ref, qkv_ref, wa_ref, wb_ref,
    output_ref, mgrad_ref, low_ref, small_ref, hg_ref, sum_ref, r1_ref, w_ref, *scratch, swap
):
    w_attn, middle, inner, mlp, back, grads, segment, load_sem = scratch[:8]
    step = pl.program_id(0)
    steps = pl.num_programs(0)
    quarter = turn_of(step)
    units = wb_ref.shape[2] // 2
    skip = wa_ref.shape[2] - units
    z = s_ref[0]
    core = s_ref[1]
    load = pltpu.make_async_copy(pack_ref.at[:, :, :skip], w_attn, load_sem.at[0])

    def alive():
        return jnp.where(segment[:, 0:1] != 0.0, 1.0, 0.0)

    if swap:
        away, got, send_sem, recv_sem, f_send, f_recv, w_send, w_recv = scratch[8:]
        p = Place()
        core, z = p.core, p.z
        other = (p.at_c, z)
        chain = Chain(
            p, lambda q, i: grads.at[q, i], None, None, None, None, f_send, f_recv
        )

        beside = (p.dp, p.z + 1 - 2 * (p.z % 2))

        def weight_copy(i):
            src, device = ((qkv_ref, beside), (qkv_ref, other), (w_ref.at[1], other))[i]
            return remote(src, w_ref.at[i + 1], w_send.at[i], w_recv.at[i], device)

        def weight_own():
            return pltpu.make_async_copy(qkv_ref, w_ref.at[0], w_send.at[3])

        @pl.when(step == 0)
        def _():
            barrier = pltpu.get_barrier_semaphore()
            for device in (other, (p.at_x, p.z), (p.at_y, p.z), beside):
                pl.semaphore_signal(barrier, inc=1, device_id=device, device_id_type=MESH)
            pl.semaphore_wait(barrier, 4)
            weight_copy(0).start()
            weight_copy(1).start()
            weight_own().start()

        def give(i):
            return remote(
                away.at[i % 2], got.at[i % 2], send_sem.at[i % 2], recv_sem.at[i % 2], other
            )

        def stage1(i, slot):
            q = DONE[i]
            at = i * 2 + slot
            return remote(
                grads.at[q, chain.slab(q, slot, True)], r1_ref.at[i, slot],
                f_send.at[at], f_recv.at[at], chain.near(q),
            )

        def take(i):
            q = turn_of(i)
            give(i).wait_recv()
            for d in range(grads.shape[1]):
                grads[q, d] += got[i % 2, d]
            pltpu.make_async_copy(grads.at[q], sum_ref.at[q], load_sem.at[1 + i]).start()
            for j in range(len(DONE)):

                @pl.when(i == j)
                def _(j=j):
                    stage1(j, 0).start()
                    stage1(j, 1).start()

    @pl.when(step == 0)
    def _():
        load.start()
        load_live = pltpu.make_async_copy(live_ref.at[z], segment, load_sem.at[1 + WAYS])
        load_live.start()
        tokens = x_ref[...].astype(F32)
        attn_out = jnp.zeros(tokens.shape, F32)
        load_live.wait()
        load.wait()
        for m in range(WAYS):
            o = jnp.concatenate([heads_ref[m, 0], heads_ref[m, 1]], axis=-1)
            attn_out += dot_nn(o, side_by_side(w_attn, z ^ m))
        total = tokens + attn_out
        vhat, unused = norm_stats(total)
        middle[...] = total
        inner[...] = (vhat * gain_ref[...]).astype(BF)
        live = alive()
        lane = lax.broadcasted_iota(jnp.int32, (1, tokens.shape[1]), 1)
        sums = jnp.where(lane == 4, jnp.sum(live), 0.0)
        for i, values in enumerate((tokens, attn_out, total)):
            sums = jnp.where(lane == i, jnp.sum(live * values * values), sums)
        small_ref[...] = jnp.zeros_like(small_ref)
        small_ref[2:3, :] = sums

    w_act = side_by_side(wa_ref, 0, slice(skip, skip + units))
    w_lin = side_by_side(wb_ref, 0, slice(0, units))
    w_out = side_by_side(wb_ref, 0, slice(units, 2 * units))
    x = inner[...]
    grad = g_ref[...]
    act_in = dot_nt(w_act, x)
    linear = dot_nt(w_lin, x)
    hidden_grad = dot_nt(w_out, grad)
    cdf = 0.5 * (1.0 + lax.erf(act_in * (2.0**-0.5)))
    act = act_in * cdf
    slope = cdf + act_in * jnp.exp(-0.5 * act_in * act_in) * ((2.0 * math.pi) ** -0.5)
    hidden = (act * linear).astype(BF)
    d_act = (hidden_grad * linear * slope).astype(BF)
    d_lin = (hidden_grad * act).astype(BF)
    if swap:
        pl.when(step >= 1)(lambda: take(step - 1))
        pl.when(step >= 2)(lambda: give(step - 2).wait_send())

        @pl.when(step == steps - 1)
        def _():
            weight_copy(0).wait_recv()
            weight_copy(2).start()

    x_mine = own_first(core, x)
    g_mine = own_first(core, grad)
    pieces = (dot_nn(d_act, x_mine), dot_nn(d_lin, x_mine), dot_nn(hidden, g_mine))
    for part, value in enumerate(pieces):
        some = slice(part * units, (part + 1) * units)
        value = value.astype(BF)
        for d in range(value.shape[1] // LANES):
            slab = value[:, d * LANES : (d + 1) * LANES]
            if not swap:
                sum_ref[quarter, d // 2, d % 2, some] = slab
            elif d % 2:
                away[step % 2, d // 2, some] = slab
            else:
                grads[quarter, d // 2, some] = slab
    if swap:
        give(step).start()
    more_mlp = dot_tn(hidden, w_out)
    more_back = dot_tn(d_act, w_act) + dot_tn(d_lin, w_lin)

    @pl.when(step == 0)
    def _():
        mlp[...] = more_mlp
        back[...] = more_back

    @pl.when(step > 0)
    def _():
        mlp[...] += more_mlp
        back[...] += more_back

    @pl.when(step == steps - 1)
    def _():
        vhat, scale = norm_stats(middle[...])
        into = back[...]
        middle_grad = g_ref[...].astype(F32) + norm_back(vhat, scale, gain_ref[...], into)
        low = middle_grad.astype(BF)
        for m in range(WAYS):
            hg = dot_nt(low, side_by_side(w_attn, z ^ m)).astype(BF)
            hg_ref[m, 0] = hg[:, :LANES]
            hg_ref[m, 1] = hg[:, LANES:]
        mgrad_ref[...] = middle_grad
        low_ref[...] = low
        out = mlp[...]
        output_ref[...] = (middle[...] + out).astype(BF)
        lane = lax.broadcasted_iota(jnp.int32, (1, out.shape[1]), 1)
        square = jnp.sum(alive() * out * out)
        small_ref[2:3, :] = jnp.where(lane == 3, square, small_ref[2:3, :])
        small_ref[1:2, :] = jnp.sum(into * vhat, axis=0, keepdims=True)
        if swap:
            take(step)
            give(step - 1).wait_send()
            give(step).wait_send()
            for i in range(WAYS):
                q = turn_of(i)
                pltpu.make_async_copy(grads.at[q], sum_ref.at[q], load_sem.at[1 + i]).wait()
            for i in range(len(DONE)):
                for slot in range(2):
                    stage1(i, slot).wait()
            weight_copy(0).wait_send()
            weight_copy(1).wait()
            weight_copy(2).wait()
            weight_own().wait()


def mlp_call(scalars, heads, x, grad, gain, live, pack_a, pack_b, qkv, swap):
    tokens, model = x.shape
    wide, quarters, depth_a, unused = pack_a.shape
    units = pack_b.shape[2] // 2
    depth = model // WAYS
    out = (quarters, wide // 2) + (() if swap else (2,)) + (3 * units, LANES)
    whole = pl.BlockSpec(memory_space=pltpu.VMEM)
    anywhere = pl.BlockSpec(memory_space=pl.ANY)
    weight = lambda rows: pl.BlockSpec((wide, 1, rows, LANES), lambda i, s: (0, turn_of(i), 0, 0))
    sems = lambda *shape: pltpu.SemaphoreType.DMA(shape)
    scratch = [
        pltpu.VMEM((wide, quarters, depth, LANES), BF),
        pltpu.VMEM((tokens, model), F32),
        pltpu.VMEM((tokens, model), BF),
        pltpu.VMEM((tokens, model), F32),
        pltpu.VMEM((tokens, model), F32),
        pltpu.VMEM(out if swap else (8, LANES), BF),
        pltpu.VMEM((tokens, LANES), F32),
        sems(2 + WAYS),
    ]
    if swap:
        scratch += [pltpu.VMEM((2,) + out[1:], BF)] * 2
        scratch += [sems(2), sems(2), sems(6), sems(6), sems(4), sems(3)]
    r1 = (len(DONE), 2, 3 * units, LANES) if swap else (8, LANES)
    spec = pltpu.PrefetchScalarGridSpec(
        num_scalar_prefetch=1,
        grid=(quarters,),
        in_specs=[whole] * 4 + [anywhere] * 3 + [weight(depth_a), weight(2 * units)],
        out_specs=[whole] * 5 + [anywhere if swap else whole, anywhere, anywhere],
        scratch_shapes=scratch,
    )
    extra = dict(collective_id=1, has_side_effects=True) if swap else {}
    return pl.pallas_call(
        functools.partial(mlp_kernel, swap=swap),
        grid_spec=spec,
        out_shape=[
            shape_of((tokens, model), BF),
            shape_of((tokens, model), F32),
            shape_of((tokens, model), BF),
            shape_of((8, model), F32),
            shape_of((WAYS, depth // LANES, tokens, LANES), BF),
            shape_of(out, BF),
            shape_of(r1, BF),
            shape_of((WAYS,) + qkv.shape if swap else (8, LANES), BF),
        ],
        compiler_params=pltpu.CompilerParams(vmem_limit_bytes=62 * 1024 * 1024, **extra),
        cost_estimate=cost(22 * tokens * model * units * quarters, 40),
        name="mlp",
    )(scalars, heads, x, grad, gain, live, pack_a, qkv, pack_a, pack_b)


def backward_kernel(
    hg_ref, sum_ref, r1_ref, normed_ref, w_ref, x_ref, mgrad_ref, low_ref, heads_ref,
    qa, ka, v, o, cosine, sine, gain_ref, small_ref,
    grad_ref, inner_ref, outer_ref, attn_ref, qkv_ref, gain_a_ref, gain_m_ref, rms_ref,
    do_ref, low, va, kt, dk, dv, normed, weight, x_in,
    f_kept0, f_r10, f_r20, f_rz0, f_kept1, f_r11, f_r21, f_rz1,
    a_sum, a_got, a_r1, a_r2, a_rz,
    q_sum, q_rx, q_ry, q_rz, ret, s_own, s_dp, s_mp,
    load_sem, do_send, do_recv, f_send, f_recv, a_send, a_recv, c_send, c_recv,
    q_send, q_recv, g_send, g_recv, s_send, s_recv,
):
    p = Place()
    dp, z, core = p.dp, p.z, p.core
    rows = x_ref.shape[0]
    pairs = v.shape[0]
    k = Back((qa, ka, v, o, cosine, sine, low, va, kt, dk, dv))

    def qkv_to(turn):
        a, b = dp - core + (p.group + turn) % 2, p.quarter
        return a, b, p.stays(a, b)

    def qkv_from(g):
        a, b = dp - core + (z // 2 + g) % 2, 2 * g + z % 2
        return a, b, p.stays(a, b)

    def other_dp(turn):
        return (dp + turn) % 8, z

    def other_mp(turn):
        return dp, (z + turn) % WAYS

    barrier = pltpu.get_barrier_semaphore()
    count = jnp.int32(0)

    def greet(device, skip=None):
        def signal():
            pl.semaphore_signal(barrier, inc=1, device_id=device, device_id_type=MESH)

        if skip is None:
            signal()
            return 1
        pl.when(jnp.logical_not(skip))(signal)
        return 1 - skip.astype(jnp.int32)

    for turn in range(1, 8):
        count += greet(other_dp(turn))
    for turn in range(1, WAYS):
        count += greet(other_mp(turn))
    for m in range(WAYS):
        for a, b, stays in (p.attention_of(m), p.owner_of(m)):
            count += greet((a, b), stays)
    for i in range(2):
        for a, b, stays in (qkv_to(i), qkv_from(i)):
            count += greet((a, b), stays)
    pl.semaphore_wait(barrier, count)

    def head_grad(m, pair, place):
        return Move(
            hg_ref.at[m, pair], do_ref.at[m, pair], do_send.at[m, pair], do_recv.at[m, pair], place
        )

    for pair in range(pairs):
        for m in range(WAYS):
            head_grad(m, pair, p.attention_of(m)).start()

    def half(h):
        kept, r1, r2, rz = ((f_kept0, f_r10, f_r20, f_rz0), (f_kept1, f_r11, f_r21, f_rz1))[h]
        some = pl.ds(h * f_kept0.shape[2], kept.shape[2])
        return Chain(
            p, lambda q, i: sum_ref.at[q, i, some], lambda q, slot, i: kept.at[q, slot],
            r1, r2, rz, f_send.at[h], f_recv.at[h],
        )

    ffn = [half(0), half(1)]
    loads = []

    def load(src, dst):
        copy = pltpu.make_async_copy(src, dst, load_sem.at[len(loads)])
        copy.start()
        loads.append(copy)
        return copy

    def fetch(h, q):
        kept, r1 = (f_kept0, f_r10) if h == 0 else (f_kept1, f_r11)
        some = pl.ds(h * f_kept0.shape[2], kept.shape[2])
        copies = []
        for slot in range(2):
            copies.append(load(sum_ref.at[q, ffn[h].slab(q, slot, False), some], kept.at[q, slot]))
        if q in DONE:
            copies.append(load(r1_ref.at[DONE.index(q), :, some], r1.at[q]))
        return copies

    fetched = {(h, q): fetch(h, q) for q in (0, 2, 1, 3) for h in range(2)}

    def second(h, q):
        for copy in fetched[h, q]:
            copy.wait()
        ffn[h].second(q, q in DONE)

    def third(h, *quarters):
        for q in quarters:
            ffn[h].third(q)

    def line(h, hop, *quarters):
        ffn[h].line(hop, quarters)

    for h in range(2):
        second(h, 0)
        second(h, 2)
    low_load = load(low_ref, x_in)
    late = [load(normed_ref, normed), load(w_ref, weight)]
    late.append(load(mgrad_ref, grad_ref))

    low_load.wait()
    low_here = own_first(core, x_in[...])
    for m in range(WAYS):
        mixed = jnp.concatenate([heads_ref[m, 0], heads_ref[m, 1]], axis=-1)
        value = dot_tn(mixed, low_here).astype(BF)
        h = p.mix(z, m)
        for d in range(value.shape[1] // LANES):
            a_sum[d % 2, h, d // 2] = value[:, d * LANES : (d + 1) * LANES]
    late.append(load(x_ref, x_in))
    swap = remote(a_sum.at[1], a_got, c_send.at[0], c_recv.at[0], (p.at_c, z))
    swap.start()
    attn_back_begin(0, k)
    swap.wait()
    for q in range(WAYS):
        a_sum[0, q] += a_got[q]
    attn = Chain(
        p, lambda q, i: a_sum.at[0, q, i], lambda q, slot, i: a_sum.at[0, q, i],
        a_r1, a_r2, a_rz, a_send, a_recv,
    )

    def qkv_x(pair, yy):
        at = (p.y if yy else 1 - p.y) * 4 + (1 - p.x) * 2
        return remote(
            q_sum.at[pair, pl.ds(at, 2)], q_rx.at[pair, yy],
            q_send.at[pair, yy], q_recv.at[pair, yy], (p.at_x, z),
        )

    def qkv_y(pair):
        at = (1 - p.y) * 4 + p.x * 2
        return remote(
            q_sum.at[pair, pl.ds(at, 2)], q_ry.at[pair],
            q_send.at[pair, 2], q_recv.at[pair, 2], (p.at_y, z),
        )

    def qkv_z(pair, turn, g, place):
        at = p.y * 4 + p.x * 2 + (p.group + turn) % 2
        return Move(
            q_sum.at[pair, at], q_rz.at[pair, g],
            q_send.at[pair, 3 + turn], q_recv.at[pair, 3 + g], place,
        )

    def qkv_first(pair):
        total = None
        for m in range(WAYS):
            part = dot_tn(low_piece(pair, m, k, rows), normed[m * rows : (m + 1) * rows, :])
            total = part if total is None else total + part
        value = total.astype(BF)
        for d in range(value.shape[1] // LANES):
            q_sum[pair, d] = value[:, d * LANES : (d + 1) * LANES]
        qkv_x(pair, 0).start()
        qkv_x(pair, 1).start()

    def qkv_second(pair):
        qkv_x(pair, 0).wait_recv()
        at = (1 - p.y) * 4 + p.x * 2
        for i in range(2):
            q_sum[pair, at + i] += q_rx[pair, 0, i]
        qkv_y(pair).start()
        qkv_x(pair, 1).wait_recv()
        at = p.y * 4 + p.x * 2
        for i in range(2):
            q_sum[pair, at + i] += q_rx[pair, 1, i]

    def qkv_third(pair):
        qkv_y(pair).wait_recv()
        at = p.y * 4 + p.x * 2
        for i in range(2):
            q_sum[pair, at + i] += q_ry[pair, i]
        for turn in range(2):
            qkv_z(pair, turn, p.group, qkv_to(turn)).start()

    def give_back(pair, m, part, place):
        some = pl.ds(m * rows, rows)
        if part == 0:
            src, dst = low.at[pair, 0, some], ret.at[m, pair, 0]
        else:
            src, dst = low.at[pair, pl.ds(1, 2), some], ret.at[m, pair, pl.ds(1, 2)]
        return Move(src, dst, g_send.at[m, pair, part], g_recv.at[m, pair, part], place)

    def finish_pair(pair):
        for m in range(WAYS):
            attn_back_end(pair, m, k, rows)
            give_back(pair, m, 1, p.owner_of(m)).start()

    def pair_end():
        finish_pair(0)
        attn_back_begin(1, k)
        for copy in late:
            copy.wait()
        qkv_first(0)

    every = range(WAYS)
    events = {
        1: [(third, 0, 0, 2), (ffn[0].first, 1), (ffn[0].first, 3), (line, 0, 1, 0, 2)],
        3: [(third, 1, 0, 2), (line, 1, 1, 0, 2)],
        4: [(line, 0, 2, 0, 2)],
        5: [(second, 0, 1), (second, 0, 3), (ffn[1].first, 1), (ffn[1].first, 3)],
        6: [(line, 1, 2, 0, 2)] + [(attn.first, q) for q in every],
        7: [(line, 0, 3, 0, 2)],
        8: [(pair_end,), (third, 0, 1, 3)],
        9: [(line, 0, 1, 1, 3), (second, 1, 1), (second, 1, 3), (line, 1, 3, 0, 2)],
        10: [(attn.second, q) for q in every],
        11: [(qkv_second, 0), (line, 0, 2, 1, 3)] + [(attn.third, q) for q in every] + [(attn.line, 1, every)],
        12: [(third, 1, 1, 3)],
        13: [(qkv_third, 0), (line, 0, 3, 1, 3), (line, 1, 1, 1, 3), (attn.line, 2, every)],
        15: [(line, 1, 2, 1, 3), (attn.line, 3, every)],
    }
    steps = v.shape[1] // STEP
    per = rows // STEP

    def body(i, carry):
        for at, todo in events.items():

            @pl.when(i == at)
            def _(todo=todo):
                for what, *args in todo:
                    what(*args)

        pair, step = i // steps, i % steps
        m = step // per

        @pl.when(step % per == 0)
        def _():
            head_grad(m, pair, p.owner_of(0)).wait_recv()

        at = pl.multiple_of((step - m * per) * STEP, STEP)
        attn_back_step(pair, step, do_ref[m, pair, pl.ds(at, STEP), :], k)

        @pl.when(step % per == per - 1)
        def _():
            give_back(pair, m, 0, p.owner_of(m)).start()

        return carry

    lax.fori_loop(0, pairs * steps, body, 0)
    finish_pair(1)
    qkv_first(1)

    def normed_part(pair, m):
        slot = p.mix(m, 2 * core)
        at = pair * 3 * LANES
        w = [weight[slot, d, at : at + 3 * LANES, :] for d in range(weight.shape[1])]
        grads = jnp.concatenate([ret[m, pair, c] for c in range(3)], axis=-1)
        return dot_nn(grads, jnp.concatenate(w, axis=-1))

    normed_grad = None
    for m in range(WAYS):
        for part in range(2):
            give_back(0, m, part, p.attention_of(m)).wait_recv()
        add = normed_part(0, m)
        normed_grad = add if normed_grad is None else normed_grad + add
    qkv_second(1)
    line(1, 3, 1, 3)
    depth = a_r2.shape[1]
    attn.last(dv.at[:depth])
    attn_ref[...] = dv[:depth, :].T
    qkv_third(1)
    cut = f_kept0.shape[2]
    units = outer_ref.shape[1]
    ffn[0].last(dk.at[:cut])
    ffn[1].last(dk.at[cut : 3 * units])
    inner_ref[0] = dk[:units, :].T
    inner_ref[1] = dk[units : 2 * units, :].T
    outer_ref[...] = dk[2 * units : 3 * units, :].T
    vhat, scale = norm_stats(x_in[...].astype(F32))
    for pair in range(pairs):
        for g in range(2):
            qkv_z(pair, 0, g, qkv_from(g)).wait_recv()
        total = q_rz[pair, 0].astype(F32) + q_rz[pair, 1].astype(F32)
        for c in range(3):
            part = total[c * LANES : (c + 1) * LANES, :]
            qkv_ref[c, :, pair * LANES : (pair + 1) * LANES] = part.T
    for m in range(WAYS):
        for part in range(2):
            give_back(1, m, part, p.attention_of(m)).wait_recv()
        normed_grad += normed_part(1, m)
    gain_part = jnp.sum(normed_grad * vhat, axis=0, keepdims=True)
    s_own[...] = jnp.concatenate([gain_part, small_ref[1:, :]], axis=0)

    def sum_dp(turn):
        return remote(
            s_own, s_dp.at[turn], s_send.at[turn], s_recv.at[turn], other_dp(turn)
        )

    def sum_mp(turn):
        return remote(
            s_dp.at[0], s_mp.at[turn], s_send.at[8 + turn], s_recv.at[8 + turn], other_mp(turn)
        )

    for turn in range(1, 8):
        sum_dp(turn).start()
    grad_ref[...] += norm_back(vhat, scale, gain_ref[...], normed_grad)
    total = s_own[...]
    for turn in range(1, 8):
        sum_dp(turn).wait_recv()
        total += s_dp[turn]
    s_dp[0] = total
    for turn in range(1, WAYS):
        sum_mp(turn).start()
    for turn in range(1, WAYS):
        sum_mp(turn).wait_recv()
        total += s_mp[turn]
    gain_a_ref[...] = total[0:1, :]
    gain_m_ref[...] = total[1:2, :]
    squares = total[2:3, :LANES]
    lane = lax.broadcasted_iota(jnp.int32, squares.shape, 1)
    count = jnp.sum(jnp.where(lane == 4, squares, 0.0)) * x_ref.shape[1]
    rms_ref[...] = jnp.sqrt(squares / count)

    for turn in range(1, 8):
        sum_dp(turn).wait_send()
    for turn in range(1, WAYS):
        sum_mp(turn).wait_send()
    for m in range(WAYS):
        for pair in range(pairs):
            for part in range(2):
                give_back(pair, m, part, p.owner_of(m)).wait_send()
    for m in range(WAYS):
        for pair in range(pairs):
            head_grad(m, pair, p.attention_of(m)).wait_send()
    for pair in range(pairs):
        qkv_x(pair, 0).wait_send()
        qkv_x(pair, 1).wait_send()
        qkv_y(pair).wait_send()
        for turn in range(2):
            qkv_z(pair, turn, p.group, qkv_to(turn)).wait_send()
    ffn[0].finish(DONE)
    ffn[1].finish(DONE)
    attn.finish()


def backward_call(heads_grad, ffn_sum, r1, kept, weight, x, middle_grad, low, heads, gain, small):
    normed, cosine, sine, qa, ka, v, o = kept
    rows, model = x.shape
    pairs, tokens, unused = v.shape
    unused, wide, cols3, unused = weight.shape
    units = ffn_sum.shape[2]
    depth = model // WAYS
    third = cols3 // pairs
    part = (units // 32 + 1) * 16
    anywhere = pl.BlockSpec(memory_space=pl.ANY)
    vmem = pl.BlockSpec(memory_space=pltpu.VMEM)
    buf = lambda *shape, kind=BF: pltpu.VMEM(shape, kind)
    sems = lambda *shape: pltpu.SemaphoreType.DMA(shape)
    return pl.pallas_call(
        backward_kernel,
        in_specs=[anywhere] * 8 + [vmem] * 9,
        out_specs=[vmem] * 8,
        out_shape=[
            shape_of((rows, model), F32),
            shape_of((2, LANES, units // 3), F32),
            shape_of((LANES, units // 3), F32),
            shape_of((LANES, depth), F32),
            shape_of((3, LANES, pairs * LANES), F32),
            shape_of((1, model), F32),
            shape_of((1, model), F32),
            shape_of((1, LANES), F32),
        ],
        scratch_shapes=[
            buf(WAYS, pairs, rows, LANES),
            buf(pairs, 3, tokens, LANES),
            buf(2, tokens, LANES),
            buf(2, LANES, tokens),
            buf(tokens, LANES, kind=F32),
            buf(tokens, LANES, kind=F32),
            buf(tokens, model),
            buf(WAYS, wide, cols3, LANES),
            buf(rows, model),
            *[
                buf(*lead, cut, LANES)
                for cut in (part, units - part)
                for lead in ((WAYS, 2), (WAYS, 2), (WAYS,), (WAYS + 1,))
            ],
            buf(2, WAYS, wide // 2, depth, LANES),
            buf(WAYS, wide // 2, depth, LANES),
            buf(WAYS, 2, depth, LANES),
            buf(WAYS, depth, LANES),
            buf(WAYS + 1, depth, LANES),
            buf(pairs, wide, third, LANES),
            buf(pairs, 2, 2, third, LANES),
            buf(pairs, 2, third, LANES),
            buf(pairs, 2, third, LANES),
            buf(WAYS, pairs, 3, rows, LANES),
            buf(*small.shape, kind=F32),
            buf(8, *small.shape, kind=F32),
            buf(WAYS, *small.shape, kind=F32),
            sems(27),
            sems(WAYS, pairs),
            sems(WAYS, pairs),
            sems(2, 16),
            sems(2, 17),
            sems(16),
            sems(17),
            sems(1),
            sems(1),
            sems(pairs, 5),
            sems(pairs, 5),
            sems(WAYS, pairs, 2),
            sems(WAYS, pairs, 2),
            sems(12),
            sems(12),
        ],
        compiler_params=pltpu.CompilerParams(
            collective_id=2, has_side_effects=True, vmem_limit_bytes=62 * 1024 * 1024
        ),
        name="backward",
    )(
        heads_grad, ffn_sum, r1, normed, weight, x, middle_grad, low, heads,
        qa, ka, v, o, cosine, sine, gain, small,
    )


def pick(values, at, axis=0):
    return lax.dynamic_index_in_dim(values, at, axis, keepdims=False)


def flip(values, bit, dps):
    return lax.ppermute(values, "dp", [(i, i ^ bit) for i in range(dps)])


def to_attention(values, m, dps, back=False):
    pairs = []
    for dp in range(dps):
        group = dp % 2
        for t in range(WAYS):
            quarter = t ^ m
            there = (dp - group + ((quarter // 2) ^ group)) * WAYS + 2 * group + quarter % 2
            pairs.append((there, dp * WAYS + t) if back else (dp * WAYS + t, there))
    return lax.ppermute(values, ("dp", "mp"), pairs)


def local(
    sizes,
    layer_input,
    segment_ids,
    grad_out,
    qkv_weight,
    attn_weight,
    inner_weight,
    outer_weight,
    attn_gain,
    mlp_gain,
):
    dps, mps = sizes
    rows, model = layer_input.shape
    head_cols = qkv_weight.shape[2]
    units = inner_weight.shape[2]
    pairs = head_cols // LANES
    wide = model // LANES
    special = dps == wide
    me = lax.axis_index("mp")
    dp = lax.axis_index("dp")
    core = dp % 2
    group = me // 2
    quarter = me ^ (2 * core)
    scalars = jnp.stack([me, core if special else 0, quarter]).astype(jnp.int32)

    def every(values):
        got = lax.all_gather(values.T, "dp", axis=0, tiled=True).T
        got = got.reshape(-1, wide, LANES).transpose(1, 0, 2)
        return lax.all_gather(got, "mp", axis=1)

    qkv_part = qkv_weight.transpose(1, 2, 0).reshape(3, pairs, LANES, -1)
    qkv_part = qkv_part.transpose(1, 0, 2, 3).reshape(3 * head_cols, -1)
    inner_t = inner_weight.transpose(1, 2, 0)
    outer_t = outer_weight.T
    attn_depth = model // mps
    part_a = jnp.concatenate([attn_weight.T, inner_t[0]], axis=0)
    part_b = jnp.concatenate([inner_t[1], outer_t], axis=0)
    mine = segment_ids[0]
    info = jnp.broadcast_to(mine.astype(F32)[:, None], (mine.shape[0], LANES))
    info = info.reshape(WAYS, rows, LANES)
    if special:
        (pack_a, pack_b), heads, qkv_own, kept = forward_call(
            layer_input, info, attn_gain[None], qkv_part, [part_a, part_b], dps, pairs
        )
    else:
        x_all = jnp.stack([to_attention(layer_input, m, dps) for m in range(WAYS)])
        qkv_all, pack_a, pack_b = every(qkv_part), every(part_a), every(part_b)
        info = jnp.where(group == core, info, flip(info, 1, dps))
        qkv_own = qkv_all
        kept = alone_call(
            quarter, x_all, info, attn_gain[None], pick(qkv_all, quarter, 1), pairs)
        heads = kept[6].reshape(pairs, WAYS, rows, LANES)
        heads = [to_attention(heads[:, m], m, dps, back=True) for m in range(WAYS)]
        heads = jnp.stack(heads)
    normed, cosine, sine, qa, ka, v, o = kept

    outs = mlp_call(
        scalars, heads, layer_input, grad_out, mlp_gain[None], info, pack_a, pack_b,
        qkv_own, special,
    )
    layer_output, middle_grad, middle_low, small, heads_grad, ffn_sum, ffn_got, qkv_whole = outs
    if special:
        input_grad, inner_sum, outer_sum, attn_sum, qkv_sum, gain_a, gain_m, rms = backward_call(
            heads_grad, ffn_sum, ffn_got, kept, qkv_whole, layer_input, middle_grad, middle_low, heads,
            attn_gain[None], small,
        )
        return (
            layer_output,
            input_grad,
            qkv_sum.transpose(1, 0, 2),
            attn_sum,
            inner_sum.transpose(1, 0, 2),
            outer_sum,
            gain_a[0],
            gain_m[0],
            rms[0, :4],
        )
    else:
        lows = []
        for pair in range(pairs):
            grad = [to_attention(heads_grad[m, pair], m, dps) for m in range(WAYS)]
            low = attn_bwd_call(scalars, qa, ka, v, grad, o, cosine, sine, pair)
            lows.append(jnp.concatenate(low, axis=0))
        low = jnp.concatenate(lows, axis=1)
        own = pick(qkv_all, quarter, 1)
        own = jnp.concatenate([own[d] for d in range(wide)], axis=-1)
        normed_grad = dot_nn(low, own).astype(BF).reshape(WAYS, rows, model)
        normed_grad = sum(
            to_attention(normed_grad[m], m, dps, back=True).astype(F32) for m in range(WAYS)
        )

        def scatter(values):
            cut = lax.psum_scatter(values, "mp", scatter_dimension=0)
            return lax.psum_scatter(cut.T, "dp", scatter_dimension=0, tiled=True).T

        slot = (jnp.arange(mps) == quarter)[:, None, None]
        qkv_sum = scatter(jnp.where(slot, dot_tn(low, normed)[None], 0.0))
        mixed = jnp.stack([pick(heads, me ^ h) for h in range(mps)])
        mixed = mixed.transpose(0, 2, 1, 3).reshape(mps, rows, -1)
        attn_sum = scatter(jnp.stack([dot_tn(mixed[h], middle_low) for h in range(mps)]))
        ffn_sum = ffn_sum.reshape(mps, wide, 3 * units, LANES).transpose(0, 2, 1, 3)
        ffn_sum = scatter(ffn_sum.reshape(mps, 3 * units, model).astype(F32))
        vhat, scale = norm_stats(layer_input.astype(F32))
        input_grad = middle_grad + norm_back(vhat, scale, attn_gain, normed_grad)
        small = small.at[0].set(jnp.sum(normed_grad * vhat, axis=0))
        small = lax.psum(small, ("dp", "mp"))
    rms_values = jnp.sqrt(small[2, :4] / (small[2, 4] * model))

    qkv_sum = qkv_sum.reshape(pairs, 3, LANES, -1).transpose(3, 1, 0, 2)
    ffn_sum = ffn_sum.reshape(3, units, -1)
    return (
        layer_output,
        input_grad,
        qkv_sum.reshape(-1, 3, head_cols),
        attn_sum.T,
        ffn_sum[:2].transpose(2, 0, 1),
        ffn_sum[2].T,
        small[0],
        small[1],
        rms_values,
    )


def solution(mesh):
    sizes = (mesh.shape["dp"], mesh.shape["mp"])
    both = ("dp", "mp")
    whole = (P(both, None), P("dp", None, "mp"), P("dp", "mp"))
    return jax.shard_map(
        functools.partial(local, sizes),
        mesh=mesh,
        in_specs=(
            whole[0],
            P("dp", None),
            whole[0],
            whole[1],
            whole[2],
            whole[1],
            whole[2],
            P(),
            P(),
        ),
        out_specs=(
            whole[0],
            whole[0],
            whole[1],
            whole[2],
            whole[1],
            whole[2],
            P(),
            P(),
            P(),
        ),
        check_vma=False,
    )
```

```python
import functools
import math

import jax
import jax.numpy as jnp
from jax import lax
from jax.experimental import pallas as pl
from jax.experimental.pallas import tpu as pltpu
from jax.sharding import PartitionSpec as P

HEAD_DIM = 64
NORM_EPS = 1e-05
ROPE_BASE = 160000.0
BIG = 1e30
LANES = 128
WAYS = 4
BF = jnp.bfloat16
F32 = jnp.float32
VMEM_LIMIT = 56 * 1024 * 1024


def dot_nn(a, b):
    return lax.dot_general(a, b, (((1,), (0,)), ((), ())), preferred_element_type=F32)


def dot_nt(a, b):
    return lax.dot_general(a, b, (((1,), (1,)), ((), ())), preferred_element_type=F32)


def dot_tn(a, b):
    return lax.dot_general(a, b, (((0,), (0,)), ((), ())), preferred_element_type=F32)


def norm_stats(values):
    centre = jnp.mean(values, axis=-1, keepdims=True)
    shifted = values - centre
    spread = jnp.mean(shifted * shifted, axis=-1, keepdims=True)
    scale = lax.rsqrt(spread + NORM_EPS)
    return shifted * scale, scale


def norm_back(vhat, scale, gain, grad):
    u = grad * gain
    mean_u = jnp.mean(u, axis=-1, keepdims=True)
    mean_uv = jnp.mean(u * vhat, axis=-1, keepdims=True)
    return scale * (u - mean_u - vhat * mean_uv)


def swap_halves(values):
    lane = lax.broadcasted_iota(jnp.int32, values.shape, 1)
    first = lane % HEAD_DIM < HEAD_DIM // 2
    back = pltpu.roll(values, LANES - HEAD_DIM // 2, 1)
    ahead = pltpu.roll(values, HEAD_DIM // 2, 1)
    return jnp.where(first, back, ahead)


def choose(at, values):
    out = values[0]
    for i in range(1, len(values)):
        out = jnp.where(at == i, values[i], out)
    return out


def params():
    return pltpu.CompilerParams(vmem_limit_bytes=VMEM_LIMIT)


def cost(flops, mib):
    return pl.CostEstimate(flops=int(flops), bytes_accessed=int(mib * 2**20), transcendentals=0)


def call(kernel, scalars, grid, in_specs, out_specs, out_shape, scratch, estimate, name):
    spec = pltpu.PrefetchScalarGridSpec(
        num_scalar_prefetch=1,
        grid=grid,
        in_specs=in_specs,
        out_specs=out_specs,
        scratch_shapes=scratch,
    )
    return functools.partial(
        pl.pallas_call(
            kernel,
            grid_spec=spec,
            out_shape=out_shape,
            compiler_params=params(),
            cost_estimate=estimate,
            name=name,
        ),
        scalars,
    )


def full(shape):
    return pl.BlockSpec(shape, lambda i, s: (0,) * len(shape))


def shape_of(shape, dtype):
    return jax.ShapeDtypeStruct(shape, dtype)


def side_by_side(ref, *at):
    return jnp.concatenate([ref[(d, *at)] for d in range(ref.shape[0])], axis=-1)


STEP = 256


def doc_starts(pieces):
    number = lax.broadcasted_iota(jnp.int32, (1, LANES), 1).astype(F32)
    total = jnp.zeros((1, LANES), F32)
    for piece in pieces:
        before = jnp.logical_and(piece > 0.0, piece < number)
        total += jnp.sum(jnp.where(before, 1.0, 0.0), axis=0, keepdims=True)
    return total


def table_piece(m, segment, first, starts, out):
    rows = segment.shape[0]
    here = slice(m * rows, (m + 1) * rows)
    number = lax.broadcasted_iota(jnp.int32, (1, LANES), 1).astype(F32)
    start = jnp.sum(jnp.where(segment == number, starts, 0.0), axis=-1, keepdims=True)
    place = lax.broadcasted_iota(jnp.int32, (rows, 1), 0) + first
    position = place.astype(F32) - start
    lane = lax.broadcasted_iota(jnp.int32, (1, LANES), 1)
    half = HEAD_DIM // 2
    frequency = jnp.exp((lane % half).astype(F32) * (-2.0 * math.log(ROPE_BASE) / HEAD_DIM))
    angle = position * frequency
    sine = jnp.sin(angle)
    out.cosine[here, :] = jnp.cos(angle)
    out.sine[here, :] = jnp.where(lane % HEAD_DIM < half, -sine, sine)
    t = lane % HEAD_DIM
    same = segment == t.astype(F32)
    masked = jnp.where(same, 0.0, -BIG)
    out.qaux[here, :] = jnp.where(t >= 16, 0.0, masked).astype(BF)
    found = jnp.where(same, 1.0, 0.0)
    counted = jnp.where(t < 19, 1.0, 0.0)
    out.kaux[here, :] = jnp.where(t < 16, found, counted).astype(BF)
    out.live[here, :] = jnp.where(segment[:, 0:1] != 0.0, 1.0, 0.0)


def qkv_piece(m, x, gain, weight, out):
    rows = x.shape[0]
    here = slice(m * rows, (m + 1) * rows)
    vhat, unused = norm_stats(x.astype(F32))
    normed = (vhat * gain).astype(BF)
    out.normed[here, :] = normed
    flat = dot_nt(normed, weight)
    cosine, sine = out.cosine[here, :], out.sine[here, :]
    kaux = out.kaux[here, :]
    lane = lax.broadcasted_iota(jnp.int32, (rows, LANES), 1)
    for pair in range(flat.shape[1] // (3 * LANES)):
        q, k, v = [
            flat[:, at : at + LANES] for at in range(pair * 3 * LANES, (pair + 1) * 3 * LANES, LANES)
        ]
        q = (q * cosine + swap_halves(q) * sine).astype(BF)
        k = (k * cosine + swap_halves(k) * sine).astype(BF)
        out.q[pair, here, :] = q * jnp.asarray(HEAD_DIM**-0.5, BF)
        out.ka[pair, 0, here, :] = jnp.where(lane < HEAD_DIM, k, kaux)
        out.ka[pair, 1, here, :] = jnp.where(lane >= HEAD_DIM, k, kaux)
        out.v[pair, here, :] = v.astype(BF)


def attn_step(pair, step, out):
    tokens = out.v.shape[1]
    chunk = 512
    here = pl.ds(pl.multiple_of(step * STEP, STEP), STEP)
    lane = lax.broadcasted_iota(jnp.int32, (STEP, LANES), 1)
    t = lane % HEAD_DIM
    q = out.q[pair, here, :]
    qaux = out.qaux[here, :]
    live = out.live[here, :]
    outs = []
    for head in range(2):
        mine = (lane < HEAD_DIM) if head == 0 else (lane >= HEAD_DIM)
        qa = jnp.where(mine, q, qaux)
        top = None
        for at in range(0, tokens, chunk):
            s = dot_nt(qa, out.ka[pair, head, at : at + chunk, :])
            out.scores[:, at : at + chunk] = s
            part = jnp.max(s, axis=-1, keepdims=True)
            top = part if top is None else jnp.maximum(top, part)
        total = jnp.zeros((STEP, 1), F32)
        mixed = jnp.zeros((STEP, LANES), F32)
        for at in range(0, tokens, chunk):
            p = jnp.exp(out.scores[:, at : at + chunk] - top)
            total += jnp.sum(p, axis=-1, keepdims=True)
            mixed += dot_nn(p.astype(BF), out.v[pair, at : at + chunk, :])
        outs.append(mixed * (live / total))
        log_sum = jnp.where(live > 0, top + jnp.log(total), BIG)
        high = log_sum.astype(BF)
        rest = log_sum - high.astype(F32)
        mid = rest.astype(BF)
        low = (rest - mid.astype(F32)).astype(BF)
        aux = jnp.where(t == 16, -high, jnp.where(t == 17, -mid, jnp.where(t == 18, -low, qaux)))
        out.qa[pair, head, here, :] = jnp.where(mine, q, aux)
    out.o[pair, here, :] = jnp.where(lane < HEAD_DIM, outs[0], outs[1]).astype(BF)


class Kept:
    names = ("normed", "cosine", "sine", "qa", "ka", "v", "o", "q", "qaux", "kaux", "live", "scores")

    def __init__(self, refs):
        for name, ref in zip(self.names, refs):
            setattr(self, name, ref)


def kept_shapes(tokens, model, pairs):
    outs = [
        shape_of((tokens, model), BF),
        shape_of((tokens, LANES), F32),
        shape_of((tokens, LANES), F32),
        shape_of((pairs, 2, tokens, LANES), BF),
        shape_of((pairs, 2, tokens, LANES), BF),
        shape_of((pairs, tokens, LANES), BF),
        shape_of((pairs, tokens, LANES), BF),
    ]
    scratch = [
        pltpu.VMEM((pairs, tokens, LANES), BF),
        pltpu.VMEM((tokens, LANES), BF),
        pltpu.VMEM((tokens, LANES), BF),
        pltpu.VMEM((tokens, 1), F32),
        pltpu.VMEM((STEP, tokens), F32),
    ]
    return outs, scratch


def alone_kernel(quarter_ref, x_ref, info_ref, gain_ref, w_ref, *refs):
    out = Kept(refs)
    starts = doc_starts([info_ref[t] for t in range(WAYS)])
    for m in range(WAYS):
        t = quarter_ref[0] ^ m
        table_piece(m, info_ref[t], t * info_ref.shape[1], starts, out)
        qkv_piece(m, x_ref[m], gain_ref[...], side_by_side(w_ref), out)

    def body(step, carry):
        per = out.v.shape[1] // STEP
        attn_step(step // per, step % per, out)
        return carry

    lax.fori_loop(0, out.v.shape[0] * out.v.shape[1] // STEP, body, 0)


def alone_call(quarter, x, info, gain, weight, pairs):
    outs, scratch = kept_shapes(WAYS * x.shape[1], x.shape[2], pairs)
    return pl.pallas_call(
        alone_kernel,
        in_specs=[pl.BlockSpec(memory_space=pltpu.SMEM)]
        + [pl.BlockSpec(memory_space=pltpu.VMEM)] * 4,
        out_specs=[pl.BlockSpec(memory_space=pltpu.VMEM)] * len(outs),
        out_shape=outs,
        scratch_shapes=scratch,
        compiler_params=params(),
        name="forward",
    )(quarter.reshape(1), x, info, gain, weight)


def piece_block(m, rows, per):
    return pl.BlockSpec((rows, LANES), lambda i, s: (jnp.clip(i - per * m, 0, per - 1), 0))


def attn_bwd_kernel(s_ref, *refs):
    qa_ref, ka_ref, v_ref, o_ref, do_refs = refs[0], refs[1], refs[2], refs[3], refs[4:8]
    cosq_ref, sinq_ref, cosk_ref, sink_ref = refs[8:12]
    out_refs = refs[12:16]
    va_ref, kt_ref, dk_acc, dv_acc = refs[16:20]
    step = pl.program_id(0)
    rows = do_refs[0].shape[0]
    chunk = v_ref.shape[0] // WAYS
    per = chunk // rows
    piece = step // per
    lane_k = lax.broadcasted_iota(jnp.int32, (chunk, LANES), 1)
    lane = lax.broadcasted_iota(jnp.int32, (rows, LANES), 1)
    zero = jnp.zeros((), BF)

    @pl.when(step == 0)
    def _():
        ones = jnp.where(lane_k % HEAD_DIM < 3, jnp.ones((), BF), zero)
        for m in range(WAYS):
            some = slice(m * chunk, (m + 1) * chunk)
            v = v_ref[some, :]
            for head in range(2):
                mine = (lane_k < HEAD_DIM) if head == 0 else (lane_k >= HEAD_DIM)
                va_ref[head, some, :] = jnp.where(mine, v, ones)
                own = jnp.where(mine, ka_ref[head, some, :], zero).astype(F32)
                kt_ref[head, :, some] = own.T.astype(BF)
        dk_acc[...] = jnp.zeros_like(dk_acc)
        dv_acc[...] = jnp.zeros_like(dv_acc)

    grad = choose(piece, [r[...] for r in do_refs])
    out = o_ref[...]
    product = grad.astype(F32) * out.astype(F32)
    turned = jnp.zeros((LANES, rows), F32)
    for head in range(2):
        mine = (lane < HEAD_DIM) if head == 0 else (lane >= HEAD_DIM)
        delta = jnp.sum(jnp.where(mine, product, 0.0), axis=-1, keepdims=True)
        high = delta.astype(BF)
        rest = delta - high.astype(F32)
        mid = rest.astype(BF)
        low = (rest - mid.astype(F32)).astype(BF)
        t = lane % HEAD_DIM
        aux = jnp.where(t == 0, -high, jnp.where(t == 1, -mid, jnp.where(t == 2, -low, zero)))
        grad_aug = jnp.where(mine, grad, aux)
        grad_own = jnp.where(mine, grad, zero)
        qa = qa_ref[head]
        q_own = jnp.where(mine, qa, zero)
        for m in range(WAYS):
            some = slice(m * chunk, (m + 1) * chunk)
            prob = jnp.exp(dot_nt(ka_ref[head, some, :], qa))
            back = dot_nt(va_ref[head, some, :], grad_aug)
            score_grad = (prob * back).astype(BF)
            dv_acc[some, :] += dot_nn(prob.astype(BF), grad_own)
            dk_acc[some, :] += dot_nn(score_grad, q_own)
            turned += dot_nn(kt_ref[head, :, some], score_grad)
    dq = turned.T * (HEAD_DIM**-0.5)
    dq = (dq * cosq_ref[...] - swap_halves(dq) * sinq_ref[...]).astype(BF)
    for m in range(WAYS):

        @pl.when(piece == m)
        def _(m=m):
            here = pl.ds(pl.multiple_of((step - m * per) * rows, rows), rows)
            out_refs[m][here, :LANES] = dq

    @pl.when(step == pl.num_programs(0) - 1)
    def _():
        for m in range(WAYS):
            some = slice(m * chunk, (m + 1) * chunk)
            dk = dk_acc[some, :]
            dk = dk * cosk_ref[some, :] - swap_halves(dk) * sink_ref[some, :]
            out_refs[m][:, LANES : 2 * LANES] = dk.astype(BF)
            out_refs[m][:, 2 * LANES :] = dv_acc[some, :].astype(BF)


def attn_bwd_call(scalars, qa, ka, v, grad, o, cosine, sine, pair):
    tokens = v.shape[1]
    chunk = tokens // WAYS
    rows = 256
    per = chunk // rows
    moving = [piece_block(m, rows, per) for m in range(WAYS)]
    block = pl.BlockSpec((rows, LANES), lambda i, s: (i, 0))
    return call(
        attn_bwd_kernel,
        scalars,
        (tokens // rows,),
        [
            pl.BlockSpec((None, 2, rows, LANES), lambda i, s: (pair, 0, i, 0)),
            pl.BlockSpec((None, 2, tokens, LANES), lambda i, s: (pair, 0, 0, 0)),
            pl.BlockSpec((None, tokens, LANES), lambda i, s: (pair, 0, 0)),
            pl.BlockSpec((None, rows, LANES), lambda i, s: (pair, i, 0)),
        ]
        + moving
        + [block, block, full((tokens, LANES)), full((tokens, LANES))],
        [full((chunk, 3 * LANES))] * WAYS,
        [shape_of((chunk, 3 * LANES), BF)] * WAYS,
        [
            pltpu.VMEM((2, tokens, LANES), BF),
            pltpu.VMEM((2, LANES, tokens), BF),
            pltpu.VMEM((tokens, LANES), F32),
            pltpu.VMEM((tokens, LANES), F32),
        ],
        cost(28 * tokens * tokens * LANES, 8),
        "attn_bwd",
    )(qa, ka, v, o, *grad, cosine, sine, cosine, sine)


def own_first(core, values):
    cut = [values[:, at : at + LANES] for at in range(0, values.shape[1], LANES)]
    turned = [cut[i ^ 1] for i in range(len(cut))]
    return jnp.where(core == 0, values, jnp.concatenate(turned, axis=-1))


MESH = pl.DeviceIdType.MESH
UP, DOWN, TO_X, TO_Y, TO_D, CORE_OWN, CORE_X, CORE_Y, CORE_D = range(9)
FROM_Z, FROM_X, FROM_Y, FROM_D = range(4)
CHUNKS = 4


class Place:
    def __init__(self):
        self.dp, self.z = lax.axis_index("dp"), lax.axis_index("mp")
        self.core, self.x, self.y = self.dp % 2, (self.dp // 2) % 2, self.dp // 4
        self.at_c = self.dp + 1 - 2 * self.core
        self.at_x = self.dp + 2 - 4 * self.x
        self.at_y = self.dp + 4 - 8 * self.y
        self.at_d = self.at_x + self.at_y - self.dp
        self.group = self.z // 2
        self.far_z = self.z + 2 - 4 * self.group
        self.quarter = self.z + self.core * (self.far_z - self.z)

    @staticmethod
    def mix(q, m):
        return (q + m) % 2 + 2 * ((q // 2 + m // 2) % 2)

    def stays(self, a, b):
        return jnp.logical_and(a == self.dp, b == self.z)

    def attention_of(self, m):
        h = self.mix(self.z, m)
        a, b = self.dp - self.core + (h // 2 + self.core) % 2, 2 * self.core + h % 2
        return a, b, self.stays(a, b)

    def owner_of(self, m):
        a, b = self.dp - self.core + self.group, self.mix(self.quarter, m)
        return a, b, self.stays(a, b)


def remote(src, dst, send, recv, device):
    return pltpu.make_async_remote_copy(
        src_ref=src, dst_ref=dst, send_sem=send, recv_sem=recv,
        device_id=device, device_id_type=MESH,
    )


class Move:
    def __init__(self, src, dst, send, recv, place):
        a, b, self.stays = place
        self.far = lambda: remote(src, dst, send, recv, (a, b))
        self.near = lambda: pltpu.make_async_copy(src, dst, recv)

    def start(self):
        pl.when(self.stays)(lambda: self.near().start())
        pl.when(jnp.logical_not(self.stays))(lambda: self.far().start())

    def wait_recv(self):
        self.far().wait_recv()

    def wait_send(self):
        pl.when(jnp.logical_not(self.stays))(lambda: self.far().wait_send())


def forward_kernel(x_ref, info_ref, gain_ref, qkv_ref, *refs, packs):
    parts, outs, heads_ref = refs[:packs], refs[packs : 2 * packs], refs[2 * packs]
    saved, refs = refs[2 * packs + 1 : 2 * packs + 7], refs[2 * packs + 7 :]
    qa, o, normed, cosine, sine, ka, v, q, qaux, kaux, live, scores = refs[:12]
    kept = Kept((normed, cosine, sine, qa, ka, v, o, q, qaux, kaux, live, scores))
    x_all, w_ref, infos = refs[12:15]
    (
        sends, recvs, cores, locals_, token_send, token_recv, relay_send, info_sem,
        head_send, head_recv,
        q_send, q_recv, save_sem,
    ) = refs[15:]
    dp, z = lax.axis_index("dp"), lax.axis_index("mp")
    core, xb, yb = dp % 2, (dp // 2) % 2, dp // 4
    at_c, at_x, at_y = dp + 1 - 2 * core, dp + 2 - 4 * xb, dp + 4 - 8 * yb
    at_d = at_x + at_y - dp
    group = z // 2
    far_z = z + 2 - 4 * group
    quarter = z + core * (far_z - z)

    def mix(q, m):
        return (q + m) % 2 + 2 * ((q // 2 + m // 2) % 2)

    def attention_of(m):
        h = mix(z, m)
        return dp - core + (h // 2 + core) % 2, 2 * core + h % 2

    def owner_of(m):
        return dp - core + group, mix(quarter, m)

    barrier = pltpu.get_barrier_semaphore()

    def greet(device, when=None):
        def signal():
            pl.semaphore_signal(barrier, inc=1, device_id=device, device_id_type=MESH)

        signal() if when is None else pl.when(when)(signal)

    greet((at_c, z))
    greet((at_x, z))
    greet((at_y, z))
    greet((dp, far_z))
    greet((dp, z + 1), z < WAYS - 1)
    greet((dp, z - 1), z > 0)
    count = 4 + (z < WAYS - 1).astype(jnp.int32) + (z > 0).astype(jnp.int32)
    here, there = [], []
    for m in range(WAYS):
        for of, found in ((attention_of, here), (owner_of, there)):
            a, b = of(m)
            stays = jnp.logical_and(a == dp, b == z)
            found.append((a, b, stays))
            greet((a, b), jnp.logical_not(stays))
            count += 1 - stays.astype(jnp.int32)
    pl.semaphore_wait(barrier, count)

    def remote(src, dst, send, recv, device):
        return pltpu.make_async_remote_copy(
            src_ref=src, dst_ref=dst, send_sem=send, recv_sem=recv,
            device_id=device, device_id_type=MESH,
        )

    def copy(p, kind, s, src=None):
        who = {CORE_X: at_x, CORE_Y: at_y, CORE_D: at_d}.get(kind, dp)
        if kind == TO_D:
            who = jnp.where(s < 2, at_x, at_y)
        slab = outs[p].at[who, s]
        send = sends.at[p, kind, s]
        if kind == UP:
            recv, device = recvs.at[p, FROM_Z, s], (dp, z + 1)
        elif kind == DOWN:
            recv, device = recvs.at[p, FROM_Z, s], (dp, z - 1)
        elif kind == TO_X:
            recv, device = recvs.at[p, FROM_X, s], (at_x, z)
        elif kind == TO_Y:
            recv, device = recvs.at[p, FROM_Y, s], (at_y, z)
        elif kind == TO_D:
            recv, device = recvs.at[p, FROM_D, s], (jnp.where(s < 2, at_y, at_x), z)
        else:
            recv, device = cores.at[p, kind - CORE_OWN, s], (at_c, z)
        return remote(slab if src is None else src, slab, send, recv, device)

    def arrived(p, sem, who, s):
        slab = outs[p].at[who, s]
        remote(slab, slab, sends.at[p, UP, s], sem, (at_c, z)).wait_recv()

    def spread(p, s, src=None):
        copy(p, TO_X, s, src).start()
        copy(p, TO_Y, s, src).start()
        copy(p, CORE_OWN, s, src).start()

    def begin(p):
        src = parts[p]
        spread(p, z, src)
        pltpu.make_async_copy(src, outs[p].at[dp, z], locals_.at[p]).start()

    def begin_line(p):
        src = parts[p]
        pl.when(z < WAYS - 1)(lambda: copy(p, UP, z, src).start())
        pl.when(z > 0)(lambda: copy(p, DOWN, z, src).start())

    def reach(p, hop):
        def one(s):
            arrived(p, recvs.at[p, FROM_Z, s], dp, s)
            spread(p, s)

        pl.when(z >= hop)(lambda: one(z - hop))
        pl.when(z + hop < WAYS)(lambda: one(z + hop))

    def ahead(p, hop):
        pl.when(jnp.logical_and(z >= hop, z < WAYS - 1))(lambda: copy(p, UP, z - hop).start())
        pl.when(jnp.logical_and(z + hop < WAYS, z > 0))(lambda: copy(p, DOWN, z + hop).start())

    def line(p, hop):
        reach(p, hop)
        if hop < WAYS - 1:
            ahead(p, hop)

    def plane(p, hop):
        def one(s):
            arrived(p, recvs.at[p, FROM_X, s], at_x, s)
            copy(p, CORE_X, s).start()
            pl.when(s < 2)(lambda: copy(p, TO_D, s).start())
            arrived(p, recvs.at[p, FROM_Y, s], at_y, s)
            copy(p, CORE_Y, s).start()
            pl.when(s >= 2)(lambda: copy(p, TO_D, s).start())

        if hop == 0:
            one(z)
        else:
            pl.when(z >= hop)(lambda: one(z - hop))
            pl.when(z + hop < WAYS)(lambda: one(z + hop))

    def corner(p, hop):
        def one(s):
            arrived(p, recvs.at[p, FROM_D, s], at_d, s)
            copy(p, CORE_D, s).start()

        if hop == 0:
            one(z)
        else:
            pl.when(z >= hop)(lambda: one(z - hop))
            pl.when(z + hop < WAYS)(lambda: one(z + hop))

    def from_core(p):
        for s in range(WAYS):
            for kind in range(4):
                twin = (at_c, at_x + at_c - dp, at_y + at_c - dp, at_d + at_c - dp)[kind]
                arrived(p, cores.at[p, kind, s], twin, s)
        pltpu.make_async_copy(parts[p], outs[p].at[dp, z], locals_.at[p]).wait()

    def finish(p):
        for s in range(WAYS):
            pl.when(jnp.logical_and(z < WAYS - 1, s <= z))(lambda s=s: copy(p, UP, s).wait_send())
            pl.when(jnp.logical_and(z > 0, s >= z))(lambda s=s: copy(p, DOWN, s).wait_send())
            for kind in range(TO_X, CORE_D + 1):
                copy(p, kind, s).wait_send()

    far = (z // 2 + core) % 2 == 1
    straight = (z + 1 + core) % 2
    relays = jnp.logical_and(core == 1, jnp.logical_and(z > 0, z < WAYS - 1))
    beside = (dp, z + 1 - 2 * (z % 2))
    cut = x_ref.shape[0] // CHUNKS

    def token(m, c):
        to_dp, to_z, stays = here[m]
        some = pl.ds(c * cut, cut)
        src, dst = x_ref.at[some], x_all.at[m, some]

        def direct():
            return remote(src, dst, token_send.at[m, c], token_recv.at[m, c], (to_dp, to_z))

        def near():
            return pltpu.make_async_copy(src, dst, token_recv.at[m, c])

        goes = jnp.logical_and(
            jnp.logical_not(stays), jnp.logical_or(jnp.logical_not(far), straight == m)
        )
        return direct, near, stays, goes

    def relay(m, c):
        some = pl.ds(c * cut, cut)
        return remote(
            x_all.at[m, some], x_all.at[1 - m, some],
            relay_send.at[m, c], token_recv.at[1 - m, c], beside,
        )

    def pass_on(m, c):
        some = pl.ds(c * cut, cut)
        return remote(
            x_all.at[m, some], x_all.at[m + 2, some],
            token_send.at[m + 2, c], token_recv.at[m + 2, c], (at_c, z),
        )

    def take_tokens(c):
        for m in range(2):
            token(m, c)[0]().wait_recv()
            pl.when(relays)(lambda m=m: relay(m, c).start())
            pass_on(m, c).start()

    def early(*chunks):
        def run():
            for c in chunks:
                take_tokens(c)

        pl.when(relays)(run)

    def swap_info():
        return remote(info_ref, infos.at[1], info_sem.at[0], info_sem.at[1], (at_c, z))

    def own_info():
        return pltpu.make_async_copy(info_ref, infos.at[0], locals_.at[packs])

    def q_copy(kind, i=0, src=None):
        who = {"z": dp, "x": dp, "y": dp, "c": dp, "cx": at_x, "cy": at_y, "cd": at_d}.get(kind)
        if kind == "d":
            who = at_x if i == 0 else at_y
        device = {"z": (dp, far_z), "x": (at_x, z), "y": (at_y, z)}.get(kind, (at_c, z))
        if kind == "d":
            device = (at_y, z) if i == 0 else (at_x, z)
        slot = {"z": 0, "x": 1, "y": 3, "d": 5, "c": 7, "cx": 8, "cy": 9, "cd": 10}[kind]
        if kind in ("x", "y", "d"):
            slot += i
        if kind == "z":
            i = 1
        if kind[0] == "c":
            i = 1 - core
        dst = w_ref.at[i, who]
        return remote(dst if src is None else src, dst, q_send.at[slot], q_recv.at[slot], device)

    def q_arrived(kind, i=0):
        q_copy(kind, i).wait_recv()

    def own_q():
        return pltpu.make_async_copy(qkv_ref, w_ref.at[0, dp], locals_.at[packs + 1])

    q_kinds = [("z", 0), ("x", 0), ("x", 1), ("y", 0), ("y", 1), ("d", 0), ("d", 1)]
    q_kinds += [("c", 0), ("cx", 0), ("cy", 0), ("cd", 0)]

    keeps = [w_ref.at[core], normed, cosine, sine, ka, v]

    def save(i):
        return pltpu.make_async_copy(keeps[i], saved[i], save_sem.at[i])

    rows = x_ref.shape[0]

    def head(pair, m, owner):
        src = kept.o.at[pair, pl.ds(m * rows, rows)]
        dst = heads_ref.at[m, pair]
        to_dp, to_z, stays = owner

        def far():
            return remote(
                src, dst, head_send.at[m, pair], head_recv.at[m, pair], (to_dp, to_z)
            )

        def near():
            return pltpu.make_async_copy(src, dst, head_recv.at[m, pair])

        return far, near, stays

    def start(item):
        far, near, stays = item
        pl.when(stays)(lambda: near().start())
        pl.when(jnp.logical_not(stays))(lambda: far().start())

    def end_send(item):
        far, near, stays = item
        pl.when(jnp.logical_not(stays))(lambda: far().wait_send())

    q_copy("z", 0, qkv_ref).start()
    q_copy("x", 0, qkv_ref).start()
    q_copy("y", 0, qkv_ref).start()
    own_q().start()
    for c in range(CHUNKS):
        for m in range(2):
            direct, near, stays, goes = token(m, c)
            pl.when(stays)(lambda: near().start())
            pl.when(goes)(lambda: direct().start())
    swap_info().start()
    own_info().start()
    for p in range(packs):
        begin(p)
        begin_line(p)
    own_info().wait()
    swap_info().wait()
    own_q().wait()
    q_arrived("x", 0)
    q_copy("d", 0).start()
    q_arrived("z")
    q_copy("x", 1).start()
    q_copy("y", 1).start()
    early(0)
    away = (group + core) % 2
    starts = doc_starts([infos[away, t] for t in range(WAYS)])
    for m in range(WAYS):
        t = mix(quarter, m)
        table_piece(m, infos[away, t], t * x_ref.shape[0], starts, kept)
    q_arrived("y", 0)
    q_copy("c").start()
    plane(0, 0)
    q_arrived("x", 1)
    q_copy("cx").start()
    q_arrived("y", 1)
    q_copy("d", 1).start()
    q_copy("cy").start()
    early(1)
    plane(1, 0)
    q_arrived("d", 0)
    q_arrived("d", 1)
    q_copy("cd").start()
    early(2)
    reach(0, 1)
    corner(0, 0)
    reach(1, 1)
    corner(1, 0)
    for kind in ("c", "cx", "cy", "cd"):
        q_arrived(kind)
    save(0).start()
    save(2).start()
    save(3).start()
    early(3)
    @pl.when(jnp.logical_not(relays))
    def _():
        for c in range(CHUNKS):
            take_tokens(c)

    for p in range(packs):
        ahead(p, 1)
        plane(p, 1)
    for m in range(WAYS):
        if m >= 2:
            for c in range(CHUNKS):
                pass_on(m - 2, c).wait_recv()
        weight = jnp.concatenate([w_ref[core, d] for d in range(w_ref.shape[1])], axis=-1)
        qkv_piece(m, x_all[m], gain_ref[...], weight, kept)
        if m == 2:
            line(0, 2)
            corner(0, 1)
    save(1).start()
    save(4).start()
    save(5).start()

    events = {
        1: [(line, 1, 2)],
        2: [(line, 0, 3), (corner, 1, 1)],
        4: [(plane, 0, 2)],
        5: [(line, 1, 3)],
        7: [(plane, 1, 2)],
        9: [(corner, 0, 2)],
        11: [(plane, 0, 3)],
        13: [(corner, 1, 2)],
        15: [(plane, 1, 3)],
    }
    steps = kept.v.shape[1] // STEP
    pairs = kept.v.shape[0]
    per = steps // WAYS

    def body(i, carry):
        for at, todo in events.items():

            @pl.when(i == at)
            def _(todo=todo):
                for what, p, hop in todo:
                    what(p, hop)

        pair = i // steps
        step = i % steps
        attn_step(pair, step, kept)
        m = step // per

        @pl.when(step % per == per - 1)
        def _():
            a, b = dp - core + group, mix(quarter, m)
            start(head(pair, m, (a, b, jnp.logical_and(a == dp, b == z))))

        return carry

    lax.fori_loop(0, pairs * steps, body, 0)
    corner(0, 3)
    corner(1, 3)
    for p in range(packs):
        from_core(p)
    for m in range(WAYS):
        for pair in range(pairs):
            head(pair, m, there[m])[0]().wait_recv()
            end_send(head(pair, m, there[m]))
    for c in range(CHUNKS):
        for m in range(2):
            pass_on(m, c).wait_send()
            direct, near, stays, goes = token(m, c)
            pl.when(goes)(lambda: direct().wait_send())
            pl.when(relays)(lambda m=m, c=c: relay(m, c).wait_send())
    for p in range(packs):
        finish(p)
    for kind, i in q_kinds:
        q_copy(kind, i).wait_send()
    for i in range(len(keeps)):
        save(i).wait()


def forward_call(x, info, gain, qkv_part, parts, dps, pairs):
    rows, model = x.shape
    packs = len(parts)
    anywhere = pl.BlockSpec(memory_space=pl.ANY)
    vmem = pl.BlockSpec(memory_space=pltpu.VMEM)
    outs, scratch = kept_shapes(WAYS * rows, model, pairs)
    normed, cosine, sine, qa, ka, v, o = outs
    hold = [normed, cosine, sine, ka, v]
    weight = (dps,) + qkv_part.shape
    out = pl.pallas_call(
        functools.partial(forward_kernel, packs=packs),
        in_specs=[anywhere, anywhere, vmem] + [anywhere] * (1 + packs),
        out_specs=[anywhere] * (packs + 7) + [vmem] * 2,
        out_shape=[shape_of((dps, WAYS) + part.shape, BF) for part in parts]
        + [shape_of((WAYS, pairs, rows, LANES), BF), shape_of(weight, BF)]
        + hold
        + [qa, o],
        scratch_shapes=[pltpu.VMEM(h.shape, h.dtype) for h in hold]
        + scratch
        + [
            pltpu.VMEM((WAYS, rows, model), BF),
            pltpu.VMEM((2,) + weight, BF),
            pltpu.VMEM((2, WAYS, rows, LANES), F32),
            pltpu.SemaphoreType.DMA((packs, 9, WAYS)),
            pltpu.SemaphoreType.DMA((packs, 4, WAYS)),
            pltpu.SemaphoreType.DMA((packs, 4, WAYS)),
            pltpu.SemaphoreType.DMA((packs + 2,)),
            pltpu.SemaphoreType.DMA((WAYS, CHUNKS)),
            pltpu.SemaphoreType.DMA((WAYS, CHUNKS)),
            pltpu.SemaphoreType.DMA((2, CHUNKS)),
            pltpu.SemaphoreType.DMA((2,)),
            pltpu.SemaphoreType.DMA((WAYS, pairs)),
            pltpu.SemaphoreType.DMA((WAYS, pairs)),
            pltpu.SemaphoreType.DMA((11,)),
            pltpu.SemaphoreType.DMA((11,)),
            pltpu.SemaphoreType.DMA((6,)),
        ],
        compiler_params=pltpu.CompilerParams(
            collective_id=0, has_side_effects=True, vmem_limit_bytes=VMEM_LIMIT
        ),
        name="forward",
    )(x, info, gain, qkv_part, *parts)
    packs_out, out = out[:packs], out[packs:]
    heads, weight, normed, cosine, sine, ka, v, qa, o = out
    return packs_out, heads, weight, (normed, cosine, sine, qa, ka, v, o)


def attn_back_begin(pair, k):
    chunk = 512
    lane = lax.broadcasted_iota(jnp.int32, (chunk, LANES), 1)
    zero = jnp.zeros((), BF)
    ones = jnp.where(lane % HEAD_DIM < 3, jnp.ones((), BF), zero)
    for at in range(0, k.dk.shape[0], chunk):
        some = slice(at, at + chunk)
        v = k.v[pair, some, :]
        for head in range(2):
            mine = (lane < HEAD_DIM) if head == 0 else (lane >= HEAD_DIM)
            k.va[head, some, :] = jnp.where(mine, v, ones)
            own = jnp.where(mine, k.ka[pair, head, some, :], zero).astype(F32)
            k.kt[head, :, some] = own.T.astype(BF)
    k.dk[...] = jnp.zeros_like(k.dk)
    k.dv[...] = jnp.zeros_like(k.dv)


def attn_back_step(pair, step, grad, k):
    chunk = 512
    here = pl.ds(pl.multiple_of(step * STEP, STEP), STEP)
    lane = lax.broadcasted_iota(jnp.int32, (STEP, LANES), 1)
    zero = jnp.zeros((), BF)
    t = lane % HEAD_DIM
    product = grad.astype(F32) * k.o[pair, here, :].astype(F32)
    turned = jnp.zeros((LANES, STEP), F32)
    for head in range(2):
        mine = (lane < HEAD_DIM) if head == 0 else (lane >= HEAD_DIM)
        delta = jnp.sum(jnp.where(mine, product, 0.0), axis=-1, keepdims=True)
        high = delta.astype(BF)
        rest = delta - high.astype(F32)
        mid = rest.astype(BF)
        low = (rest - mid.astype(F32)).astype(BF)
        aux = jnp.where(t == 0, -high, jnp.where(t == 1, -mid, jnp.where(t == 2, -low, zero)))
        grad_aug = jnp.where(mine, grad, aux)
        grad_own = jnp.where(mine, grad, zero)
        qa = k.qa[pair, head, here, :]
        q_own = jnp.where(mine, qa, zero)
        for at in range(0, k.dk.shape[0], chunk):
            some = slice(at, at + chunk)
            prob = jnp.exp(dot_nt(k.ka[pair, head, some, :], qa))
            back = dot_nt(k.va[head, some, :], grad_aug)
            score_grad = (prob * back).astype(BF)
            k.dv[some, :] += dot_nn(prob.astype(BF), grad_own)
            k.dk[some, :] += dot_nn(score_grad, q_own)
            turned += dot_nn(k.kt[head, :, some], score_grad)
    dq = turned.T * (HEAD_DIM**-0.5)
    dq = dq * k.cosine[here, :] - swap_halves(dq) * k.sine[here, :]
    k.low[pair, 0, here, :] = dq.astype(BF)


def attn_back_end(pair, m, k, rows):
    some = slice(m * rows, (m + 1) * rows)
    dk = k.dk[some, :]
    dk = dk * k.cosine[some, :] - swap_halves(dk) * k.sine[some, :]
    k.low[pair, 1, some, :] = dk.astype(BF)
    k.low[pair, 2, some, :] = k.dv[some, :].astype(BF)


def low_piece(pair, m, k, rows):
    some = slice(m * rows, (m + 1) * rows)
    return jnp.concatenate([k.low[pair, c, some, :] for c in range(3)], axis=-1)


class Back:
    names = ("qa", "ka", "v", "o", "cosine", "sine", "low", "va", "kt", "dk", "dv")

    def __init__(self, refs):
        for name, ref in zip(self.names, refs):
            setattr(self, name, ref)


class Chain:
    def __init__(self, p, source, kept, r1, r2, rz, send, recv):
        self.p, self.source, self.kept = p, source, kept
        self.r1, self.r2, self.rz, self.send, self.recv = r1, r2, rz, send, recv

    def slab(self, q, slot, away):
        x, y = self.p.x, self.p.y
        if q < 2:
            return (y if slot else 1 - y) * 2 + (1 - x if away else x)
        return (1 - y if away else y) * 2 + (x if slot else 1 - x)

    def near(self, q, second=False):
        p = self.p
        return (p.at_x, p.z) if (q < 2) != second else (p.at_y, p.z)

    def stage1(self, q, slot):
        src = self.source(q, self.slab(q, slot, True))
        at = q * 2 + slot
        return remote(src, self.r1.at[q, slot], self.send.at[at], self.recv.at[at], self.near(q))

    def stage2(self, q):
        at = 8 + q
        src = self.kept(q, 0, self.slab(q, 0, False))
        return remote(src, self.r2.at[q], self.send.at[at], self.recv.at[at], self.near(q, True))

    def first(self, q):
        self.stage1(q, 0).start()
        self.stage1(q, 1).start()

    def second(self, q, done=False):
        if not done:
            self.stage1(q, 0).wait_recv()
        ref = self.kept(q, 0, self.slab(q, 0, False))
        ref[...] += self.r1[q, 0]
        self.stage2(q).start()
        if not done:
            self.stage1(q, 1).wait_recv()
        self.own(q)[...] += self.r1[q, 1]

    def own(self, q):
        return self.kept(q, 1, self.slab(q, 1, False))

    def third(self, q):
        self.stage2(q).wait_recv()
        self.own(q)[...] += self.r2[q]

    def lined(self, q, down):
        z = self.p.z
        at = q if down else q + 1
        return remote(
            self.own(q), self.rz.at[at], self.send.at[12 + q], self.recv.at[12 + at],
            (self.p.dp, z - 1 if down else z + 1),
        )

    def line(self, hop, quarters):
        z = self.p.z
        for q in quarters:
            if q < WAYS - hop:

                @pl.when(z == WAYS - hop)
                def _(q=q):
                    if hop > 1:
                        self.lined(q, True).wait_recv()
                        self.own(q)[...] += self.rz[q]
                    self.lined(q, True).start()

            if q > hop - 1:

                @pl.when(z == hop - 1)
                def _(q=q):
                    if hop > 1:
                        self.lined(q, False).wait_recv()
                        self.own(q)[...] += self.rz[q + 1]
                    self.lined(q, False).start()

    def last(self, out_ref):
        z = self.p.z
        for q in range(WAYS):

            @pl.when(z == q)
            def _(q=q):
                total = self.own(q)[...].astype(F32)
                if q < WAYS - 1:
                    self.lined(q, True).wait_recv()
                    total += self.rz[q].astype(F32)
                if q > 0:
                    self.lined(q, False).wait_recv()
                    total += self.rz[q + 1].astype(F32)
                out_ref[...] = total

    def finish(self, done=()):
        z = self.p.z
        for q in range(WAYS):
            if q not in done:
                self.stage1(q, 0).wait_send()
                self.stage1(q, 1).wait_send()
            self.stage2(q).wait_send()
            pl.when(q < z)(lambda q=q: self.lined(q, True).wait_send())
            pl.when(q > z)(lambda q=q: self.lined(q, False).wait_send())


DONE = (0, 2)


def turn_of(step):
    return 2 * (step % 2) + step // 2


def mlp_kernel(
    s_ref, heads_ref, x_ref, g_ref, gain_ref, live_ref, pack_ref, qkv_ref, wa_ref, wb_ref,
    output_ref, mgrad_ref, low_ref, small_ref, hg_ref, sum_ref, r1_ref, w_ref, *scratch, swap
):
    w_attn, middle, inner, mlp, back, grads, segment, load_sem = scratch[:8]
    step = pl.program_id(0)
    steps = pl.num_programs(0)
    quarter = turn_of(step)
    units = wb_ref.shape[2] // 2
    skip = wa_ref.shape[2] - units
    z = s_ref[0]
    core = s_ref[1]
    load = pltpu.make_async_copy(pack_ref.at[:, :, :skip], w_attn, load_sem.at[0])

    def alive():
        return jnp.where(segment[:, 0:1] != 0.0, 1.0, 0.0)

    if swap:
        away, got, send_sem, recv_sem, f_send, f_recv, w_send, w_recv = scratch[8:]
        p = Place()
        core, z = p.core, p.z
        other = (p.at_c, z)
        chain = Chain(
            p, lambda q, i: grads.at[q, i], None, None, None, None, f_send, f_recv
        )

        beside = (p.dp, p.z + 1 - 2 * (p.z % 2))

        def weight_copy(i):
            src, device = ((qkv_ref, beside), (qkv_ref, other), (w_ref.at[1], other))[i]
            return remote(src, w_ref.at[i + 1], w_send.at[i], w_recv.at[i], device)

        def weight_own():
            return pltpu.make_async_copy(qkv_ref, w_ref.at[0], w_send.at[3])

        @pl.when(step == 0)
        def _():
            barrier = pltpu.get_barrier_semaphore()
            for device in (other, (p.at_x, p.z), (p.at_y, p.z), beside):
                pl.semaphore_signal(barrier, inc=1, device_id=device, device_id_type=MESH)
            pl.semaphore_wait(barrier, 4)
            weight_copy(0).start()
            weight_copy(1).start()
            weight_own().start()

        def give(i):
            return remote(
                away.at[i % 2], got.at[i % 2], send_sem.at[i % 2], recv_sem.at[i % 2], other
            )

        def stage1(i, slot):
            q = DONE[i]
            at = i * 2 + slot
            return remote(
                grads.at[q, chain.slab(q, slot, True)], r1_ref.at[i, slot],
                f_send.at[at], f_recv.at[at], chain.near(q),
            )

        def take(i):
            q = turn_of(i)
            give(i).wait_recv()
            for d in range(grads.shape[1]):
                grads[q, d] += got[i % 2, d]
            pltpu.make_async_copy(grads.at[q], sum_ref.at[q], load_sem.at[1 + i]).start()
            for j in range(len(DONE)):

                @pl.when(i == j)
                def _(j=j):
                    stage1(j, 0).start()
                    stage1(j, 1).start()

    @pl.when(step == 0)
    def _():
        load.start()
        load_live = pltpu.make_async_copy(live_ref.at[z], segment, load_sem.at[1 + WAYS])
        load_live.start()
        tokens = x_ref[...].astype(F32)
        attn_out = jnp.zeros(tokens.shape, F32)
        load_live.wait()
        load.wait()
        for m in range(WAYS):
            o = jnp.concatenate([heads_ref[m, 0], heads_ref[m, 1]], axis=-1)
            attn_out += dot_nn(o, side_by_side(w_attn, z ^ m))
        total = tokens + attn_out
        vhat, unused = norm_stats(total)
        middle[...] = total
        inner[...] = (vhat * gain_ref[...]).astype(BF)
        live = alive()
        lane = lax.broadcasted_iota(jnp.int32, (1, tokens.shape[1]), 1)
        sums = jnp.where(lane == 4, jnp.sum(live), 0.0)
        for i, values in enumerate((tokens, attn_out, total)):
            sums = jnp.where(lane == i, jnp.sum(live * values * values), sums)
        small_ref[...] = jnp.zeros_like(small_ref)
        small_ref[2:3, :] = sums

    w_act = side_by_side(wa_ref, 0, slice(skip, skip + units))
    w_lin = side_by_side(wb_ref, 0, slice(0, units))
    w_out = side_by_side(wb_ref, 0, slice(units, 2 * units))
    x = inner[...]
    grad = g_ref[...]
    act_in = dot_nt(w_act, x)
    linear = dot_nt(w_lin, x)
    hidden_grad = dot_nt(w_out, grad)
    cdf = 0.5 * (1.0 + lax.erf(act_in * (2.0**-0.5)))
    act = act_in * cdf
    slope = cdf + act_in * jnp.exp(-0.5 * act_in * act_in) * ((2.0 * math.pi) ** -0.5)
    hidden = (act * linear).astype(BF)
    d_act = (hidden_grad * linear * slope).astype(BF)
    d_lin = (hidden_grad * act).astype(BF)
    if swap:
        pl.when(step >= 1)(lambda: take(step - 1))
        pl.when(step >= 2)(lambda: give(step - 2).wait_send())

        @pl.when(step == steps - 1)
        def _():
            weight_copy(0).wait_recv()
            weight_copy(2).start()

    x_mine = own_first(core, x)
    g_mine = own_first(core, grad)
    pieces = (dot_nn(d_act, x_mine), dot_nn(d_lin, x_mine), dot_nn(hidden, g_mine))
    for part, value in enumerate(pieces):
        some = slice(part * units, (part + 1) * units)
        value = value.astype(BF)
        for d in range(value.shape[1] // LANES):
            slab = value[:, d * LANES : (d + 1) * LANES]
            if not swap:
                sum_ref[quarter, d // 2, d % 2, some] = slab
            elif d % 2:
                away[step % 2, d // 2, some] = slab
            else:
                grads[quarter, d // 2, some] = slab
    if swap:
        give(step).start()
    more_mlp = dot_tn(hidden, w_out)
    more_back = dot_tn(d_act, w_act) + dot_tn(d_lin, w_lin)

    @pl.when(step == 0)
    def _():
        mlp[...] = more_mlp
        back[...] = more_back

    @pl.when(step > 0)
    def _():
        mlp[...] += more_mlp
        back[...] += more_back

    @pl.when(step == steps - 1)
    def _():
        vhat, scale = norm_stats(middle[...])
        into = back[...]
        middle_grad = g_ref[...].astype(F32) + norm_back(vhat, scale, gain_ref[...], into)
        low = middle_grad.astype(BF)
        for m in range(WAYS):
            hg = dot_nt(low, side_by_side(w_attn, z ^ m)).astype(BF)
            hg_ref[m, 0] = hg[:, :LANES]
            hg_ref[m, 1] = hg[:, LANES:]
        mgrad_ref[...] = middle_grad
        low_ref[...] = low
        out = mlp[...]
        output_ref[...] = (middle[...] + out).astype(BF)
        lane = lax.broadcasted_iota(jnp.int32, (1, out.shape[1]), 1)
        square = jnp.sum(alive() * out * out)
        small_ref[2:3, :] = jnp.where(lane == 3, square, small_ref[2:3, :])
        small_ref[1:2, :] = jnp.sum(into * vhat, axis=0, keepdims=True)
        if swap:
            take(step)
            give(step - 1).wait_send()
            give(step).wait_send()
            for i in range(WAYS):
                q = turn_of(i)
                pltpu.make_async_copy(grads.at[q], sum_ref.at[q], load_sem.at[1 + i]).wait()
            for i in range(len(DONE)):
                for slot in range(2):
                    stage1(i, slot).wait()
            weight_copy(0).wait_send()
            weight_copy(1).wait()
            weight_copy(2).wait()
            weight_own().wait()


def mlp_call(scalars, heads, x, grad, gain, live, pack_a, pack_b, qkv, swap):
    tokens, model = x.shape
    wide, quarters, depth_a, unused = pack_a.shape
    units = pack_b.shape[2] // 2
    depth = model // WAYS
    out = (quarters, wide // 2) + (() if swap else (2,)) + (3 * units, LANES)
    whole = pl.BlockSpec(memory_space=pltpu.VMEM)
    anywhere = pl.BlockSpec(memory_space=pl.ANY)
    weight = lambda rows: pl.BlockSpec((wide, 1, rows, LANES), lambda i, s: (0, turn_of(i), 0, 0))
    sems = lambda *shape: pltpu.SemaphoreType.DMA(shape)
    scratch = [
        pltpu.VMEM((wide, quarters, depth, LANES), BF),
        pltpu.VMEM((tokens, model), F32),
        pltpu.VMEM((tokens, model), BF),
        pltpu.VMEM((tokens, model), F32),
        pltpu.VMEM((tokens, model), F32),
        pltpu.VMEM(out if swap else (8, LANES), BF),
        pltpu.VMEM((tokens, LANES), F32),
        sems(2 + WAYS),
    ]
    if swap:
        scratch += [pltpu.VMEM((2,) + out[1:], BF)] * 2
        scratch += [sems(2), sems(2), sems(6), sems(6), sems(4), sems(3)]
    r1 = (len(DONE), 2, 3 * units, LANES) if swap else (8, LANES)
    spec = pltpu.PrefetchScalarGridSpec(
        num_scalar_prefetch=1,
        grid=(quarters,),
        in_specs=[whole] * 4 + [anywhere] * 3 + [weight(depth_a), weight(2 * units)],
        out_specs=[whole] * 5 + [anywhere if swap else whole, anywhere, anywhere],
        scratch_shapes=scratch,
    )
    extra = dict(collective_id=1, has_side_effects=True) if swap else {}
    return pl.pallas_call(
        functools.partial(mlp_kernel, swap=swap),
        grid_spec=spec,
        out_shape=[
            shape_of((tokens, model), BF),
            shape_of((tokens, model), F32),
            shape_of((tokens, model), BF),
            shape_of((8, model), F32),
            shape_of((WAYS, depth // LANES, tokens, LANES), BF),
            shape_of(out, BF),
            shape_of(r1, BF),
            shape_of((WAYS,) + qkv.shape if swap else (8, LANES), BF),
        ],
        compiler_params=pltpu.CompilerParams(vmem_limit_bytes=62 * 1024 * 1024, **extra),
        cost_estimate=cost(22 * tokens * model * units * quarters, 40),
        name="mlp",
    )(scalars, heads, x, grad, gain, live, pack_a, qkv, pack_a, pack_b)


def backward_kernel(
    hg_ref, sum_ref, r1_ref, normed_ref, w_ref, x_ref, mgrad_ref, low_ref, heads_ref,
    qa, ka, v, o, cosine, sine, gain_ref, small_ref,
    grad_ref, inner_ref, outer_ref, attn_ref, qkv_ref, gain_a_ref, gain_m_ref, rms_ref,
    do_ref, low, va, kt, dk, dv, normed, weight, x_in,
    f_kept0, f_r10, f_r20, f_rz0, f_kept1, f_r11, f_r21, f_rz1,
    a_sum, a_got, a_r1, a_r2, a_rz,
    q_sum, q_rx, q_ry, q_rz, ret, s_own, s_dp, s_mp,
    load_sem, do_send, do_recv, f_send, f_recv, a_send, a_recv, c_send, c_recv,
    q_send, q_recv, g_send, g_recv, s_send, s_recv,
):
    p = Place()
    dp, z, core = p.dp, p.z, p.core
    rows = x_ref.shape[0]
    pairs = v.shape[0]
    k = Back((qa, ka, v, o, cosine, sine, low, va, kt, dk, dv))

    def qkv_to(turn):
        a, b = dp - core + (p.group + turn) % 2, p.quarter
        return a, b, p.stays(a, b)

    def qkv_from(g):
        a, b = dp - core + (z // 2 + g) % 2, 2 * g + z % 2
        return a, b, p.stays(a, b)

    def other_dp(turn):
        return (dp + turn) % 8, z

    def other_mp(turn):
        return dp, (z + turn) % WAYS

    barrier = pltpu.get_barrier_semaphore()
    count = jnp.int32(0)

    def greet(device, skip=None):
        def signal():
            pl.semaphore_signal(barrier, inc=1, device_id=device, device_id_type=MESH)

        if skip is None:
            signal()
            return 1
        pl.when(jnp.logical_not(skip))(signal)
        return 1 - skip.astype(jnp.int32)

    for turn in range(1, 8):
        count += greet(other_dp(turn))
    for turn in range(1, WAYS):
        count += greet(other_mp(turn))
    for m in range(WAYS):
        for a, b, stays in (p.attention_of(m), p.owner_of(m)):
            count += greet((a, b), stays)
    for i in range(2):
        for a, b, stays in (qkv_to(i), qkv_from(i)):
            count += greet((a, b), stays)
    pl.semaphore_wait(barrier, count)

    def head_grad(m, pair, place):
        return Move(
            hg_ref.at[m, pair], do_ref.at[m, pair], do_send.at[m, pair], do_recv.at[m, pair], place
        )

    for pair in range(pairs):
        for m in range(WAYS):
            head_grad(m, pair, p.attention_of(m)).start()

    def half(h):
        kept, r1, r2, rz = ((f_kept0, f_r10, f_r20, f_rz0), (f_kept1, f_r11, f_r21, f_rz1))[h]
        some = pl.ds(h * f_kept0.shape[2], kept.shape[2])
        return Chain(
            p, lambda q, i: sum_ref.at[q, i, some], lambda q, slot, i: kept.at[q, slot],
            r1, r2, rz, f_send.at[h], f_recv.at[h],
        )

    ffn = [half(0), half(1)]
    loads = []

    def load(src, dst):
        copy = pltpu.make_async_copy(src, dst, load_sem.at[len(loads)])
        copy.start()
        loads.append(copy)
        return copy

    def fetch(h, q):
        kept, r1 = (f_kept0, f_r10) if h == 0 else (f_kept1, f_r11)
        some = pl.ds(h * f_kept0.shape[2], kept.shape[2])
        copies = []
        for slot in range(2):
            copies.append(load(sum_ref.at[q, ffn[h].slab(q, slot, False), some], kept.at[q, slot]))
        if q in DONE:
            copies.append(load(r1_ref.at[DONE.index(q), :, some], r1.at[q]))
        return copies

    fetched = {(h, q): fetch(h, q) for q in (0, 2, 1, 3) for h in range(2)}

    def second(h, q):
        for copy in fetched[h, q]:
            copy.wait()
        ffn[h].second(q, q in DONE)

    def third(h, *quarters):
        for q in quarters:
            ffn[h].third(q)

    def line(h, hop, *quarters):
        ffn[h].line(hop, quarters)

    for h in range(2):
        second(h, 0)
        second(h, 2)
    low_load = load(low_ref, x_in)
    late = [load(normed_ref, normed), load(w_ref, weight)]
    late.append(load(mgrad_ref, grad_ref))

    low_load.wait()
    low_here = own_first(core, x_in[...])
    for m in range(WAYS):
        mixed = jnp.concatenate([heads_ref[m, 0], heads_ref[m, 1]], axis=-1)
        value = dot_tn(mixed, low_here).astype(BF)
        h = p.mix(z, m)
        for d in range(value.shape[1] // LANES):
            a_sum[d % 2, h, d // 2] = value[:, d * LANES : (d + 1) * LANES]
    late.append(load(x_ref, x_in))
    swap = remote(a_sum.at[1], a_got, c_send.at[0], c_recv.at[0], (p.at_c, z))
    swap.start()
    attn_back_begin(0, k)
    swap.wait()
    for q in range(WAYS):
        a_sum[0, q] += a_got[q]
    attn = Chain(
        p, lambda q, i: a_sum.at[0, q, i], lambda q, slot, i: a_sum.at[0, q, i],
        a_r1, a_r2, a_rz, a_send, a_recv,
    )

    def qkv_x(pair, yy):
        at = (p.y if yy else 1 - p.y) * 4 + (1 - p.x) * 2
        return remote(
            q_sum.at[pair, pl.ds(at, 2)], q_rx.at[pair, yy],
            q_send.at[pair, yy], q_recv.at[pair, yy], (p.at_x, z),
        )

    def qkv_y(pair):
        at = (1 - p.y) * 4 + p.x * 2
        return remote(
            q_sum.at[pair, pl.ds(at, 2)], q_ry.at[pair],
            q_send.at[pair, 2], q_recv.at[pair, 2], (p.at_y, z),
        )

    def qkv_z(pair, turn, g, place):
        at = p.y * 4 + p.x * 2 + (p.group + turn) % 2
        return Move(
            q_sum.at[pair, at], q_rz.at[pair, g],
            q_send.at[pair, 3 + turn], q_recv.at[pair, 3 + g], place,
        )

    def qkv_first(pair):
        total = None
        for m in range(WAYS):
            part = dot_tn(low_piece(pair, m, k, rows), normed[m * rows : (m + 1) * rows, :])
            total = part if total is None else total + part
        value = total.astype(BF)
        for d in range(value.shape[1] // LANES):
            q_sum[pair, d] = value[:, d * LANES : (d + 1) * LANES]
        qkv_x(pair, 0).start()
        qkv_x(pair, 1).start()

    def qkv_second(pair):
        qkv_x(pair, 0).wait_recv()
        at = (1 - p.y) * 4 + p.x * 2
        for i in range(2):
            q_sum[pair, at + i] += q_rx[pair, 0, i]
        qkv_y(pair).start()
        qkv_x(pair, 1).wait_recv()
        at = p.y * 4 + p.x * 2
        for i in range(2):
            q_sum[pair, at + i] += q_rx[pair, 1, i]

    def qkv_third(pair):
        qkv_y(pair).wait_recv()
        at = p.y * 4 + p.x * 2
        for i in range(2):
            q_sum[pair, at + i] += q_ry[pair, i]
        for turn in range(2):
            qkv_z(pair, turn, p.group, qkv_to(turn)).start()

    def give_back(pair, m, part, place):
        some = pl.ds(m * rows, rows)
        if part == 0:
            src, dst = low.at[pair, 0, some], ret.at[m, pair, 0]
        else:
            src, dst = low.at[pair, pl.ds(1, 2), some], ret.at[m, pair, pl.ds(1, 2)]
        return Move(src, dst, g_send.at[m, pair, part], g_recv.at[m, pair, part], place)

    def finish_pair(pair):
        for m in range(WAYS):
            attn_back_end(pair, m, k, rows)
            give_back(pair, m, 1, p.owner_of(m)).start()

    def pair_end():
        finish_pair(0)
        attn_back_begin(1, k)
        for copy in late:
            copy.wait()
        qkv_first(0)

    every = range(WAYS)
    events = {
        1: [(third, 0, 0, 2), (ffn[0].first, 1), (ffn[0].first, 3), (line, 0, 1, 0, 2)],
        3: [(third, 1, 0, 2), (line, 1, 1, 0, 2)],
        4: [(line, 0, 2, 0, 2)],
        5: [(second, 0, 1), (second, 0, 3), (ffn[1].first, 1), (ffn[1].first, 3)],
        6: [(line, 1, 2, 0, 2)] + [(attn.first, q) for q in every],
        7: [(line, 0, 3, 0, 2)],
        8: [(pair_end,), (third, 0, 1, 3)],
        9: [(line, 0, 1, 1, 3), (second, 1, 1), (second, 1, 3), (line, 1, 3, 0, 2)],
        10: [(attn.second, q) for q in every],
        11: [(qkv_second, 0), (line, 0, 2, 1, 3)] + [(attn.third, q) for q in every] + [(attn.line, 1, every)],
        12: [(third, 1, 1, 3)],
        13: [(qkv_third, 0), (line, 0, 3, 1, 3), (line, 1, 1, 1, 3), (attn.line, 2, every)],
        15: [(line, 1, 2, 1, 3), (attn.line, 3, every)],
    }
    steps = v.shape[1] // STEP
    per = rows // STEP

    def body(i, carry):
        for at, todo in events.items():

            @pl.when(i == at)
            def _(todo=todo):
                for what, *args in todo:
                    what(*args)

        pair, step = i // steps, i % steps
        m = step // per

        @pl.when(step % per == 0)
        def _():
            head_grad(m, pair, p.owner_of(0)).wait_recv()

        at = pl.multiple_of((step - m * per) * STEP, STEP)
        attn_back_step(pair, step, do_ref[m, pair, pl.ds(at, STEP), :], k)

        @pl.when(step % per == per - 1)
        def _():
            give_back(pair, m, 0, p.owner_of(m)).start()

        return carry

    lax.fori_loop(0, pairs * steps, body, 0)
    finish_pair(1)
    qkv_first(1)

    def normed_part(pair, m):
        slot = p.mix(m, 2 * core)
        at = pair * 3 * LANES
        w = [weight[slot, d, at : at + 3 * LANES, :] for d in range(weight.shape[1])]
        grads = jnp.concatenate([ret[m, pair, c] for c in range(3)], axis=-1)
        return dot_nn(grads, jnp.concatenate(w, axis=-1))

    normed_grad = None
    for m in range(WAYS):
        for part in range(2):
            give_back(0, m, part, p.attention_of(m)).wait_recv()
        add = normed_part(0, m)
        normed_grad = add if normed_grad is None else normed_grad + add
    qkv_second(1)
    line(1, 3, 1, 3)
    depth = a_r2.shape[1]
    attn.last(dv.at[:depth])
    attn_ref[...] = dv[:depth, :].T
    qkv_third(1)
    cut = f_kept0.shape[2]
    units = outer_ref.shape[1]
    ffn[0].last(dk.at[:cut])
    ffn[1].last(dk.at[cut : 3 * units])
    inner_ref[0] = dk[:units, :].T
    inner_ref[1] = dk[units : 2 * units, :].T
    outer_ref[...] = dk[2 * units : 3 * units, :].T
    vhat, scale = norm_stats(x_in[...].astype(F32))
    for pair in range(pairs):
        for g in range(2):
            qkv_z(pair, 0, g, qkv_from(g)).wait_recv()
        total = q_rz[pair, 0].astype(F32) + q_rz[pair, 1].astype(F32)
        for c in range(3):
            part = total[c * LANES : (c + 1) * LANES, :]
            qkv_ref[c, :, pair * LANES : (pair + 1) * LANES] = part.T
    for m in range(WAYS):
        for part in range(2):
            give_back(1, m, part, p.attention_of(m)).wait_recv()
        normed_grad += normed_part(1, m)
    gain_part = jnp.sum(normed_grad * vhat, axis=0, keepdims=True)
    s_own[...] = jnp.concatenate([gain_part, small_ref[1:, :]], axis=0)

    def sum_dp(turn):
        return remote(
            s_own, s_dp.at[turn], s_send.at[turn], s_recv.at[turn], other_dp(turn)
        )

    def sum_mp(turn):
        return remote(
            s_dp.at[0], s_mp.at[turn], s_send.at[8 + turn], s_recv.at[8 + turn], other_mp(turn)
        )

    for turn in range(1, 8):
        sum_dp(turn).start()
    grad_ref[...] += norm_back(vhat, scale, gain_ref[...], normed_grad)
    total = s_own[...]
    for turn in range(1, 8):
        sum_dp(turn).wait_recv()
        total += s_dp[turn]
    s_dp[0] = total
    for turn in range(1, WAYS):
        sum_mp(turn).start()
    for turn in range(1, WAYS):
        sum_mp(turn).wait_recv()
        total += s_mp[turn]
    gain_a_ref[...] = total[0:1, :]
    gain_m_ref[...] = total[1:2, :]
    squares = total[2:3, :LANES]
    lane = lax.broadcasted_iota(jnp.int32, squares.shape, 1)
    count = jnp.sum(jnp.where(lane == 4, squares, 0.0)) * x_ref.shape[1]
    rms_ref[...] = jnp.sqrt(squares / count)

    for turn in range(1, 8):
        sum_dp(turn).wait_send()
    for turn in range(1, WAYS):
        sum_mp(turn).wait_send()
    for m in range(WAYS):
        for pair in range(pairs):
            for part in range(2):
                give_back(pair, m, part, p.owner_of(m)).wait_send()
    for m in range(WAYS):
        for pair in range(pairs):
            head_grad(m, pair, p.attention_of(m)).wait_send()
    for pair in range(pairs):
        qkv_x(pair, 0).wait_send()
        qkv_x(pair, 1).wait_send()
        qkv_y(pair).wait_send()
        for turn in range(2):
            qkv_z(pair, turn, p.group, qkv_to(turn)).wait_send()
    ffn[0].finish(DONE)
    ffn[1].finish(DONE)
    attn.finish()


def backward_call(heads_grad, ffn_sum, r1, kept, weight, x, middle_grad, low, heads, gain, small):
    normed, cosine, sine, qa, ka, v, o = kept
    rows, model = x.shape
    pairs, tokens, unused = v.shape
    unused, wide, cols3, unused = weight.shape
    units = ffn_sum.shape[2]
    depth = model // WAYS
    third = cols3 // pairs
    part = (units // 32 + 1) * 16
    anywhere = pl.BlockSpec(memory_space=pl.ANY)
    vmem = pl.BlockSpec(memory_space=pltpu.VMEM)
    buf = lambda *shape, kind=BF: pltpu.VMEM(shape, kind)
    sems = lambda *shape: pltpu.SemaphoreType.DMA(shape)
    return pl.pallas_call(
        backward_kernel,
        in_specs=[anywhere] * 8 + [vmem] * 9,
        out_specs=[vmem] * 8,
        out_shape=[
            shape_of((rows, model), F32),
            shape_of((2, LANES, units // 3), F32),
            shape_of((LANES, units // 3), F32),
            shape_of((LANES, depth), F32),
            shape_of((3, LANES, pairs * LANES), F32),
            shape_of((1, model), F32),
            shape_of((1, model), F32),
            shape_of((1, LANES), F32),
        ],
        scratch_shapes=[
            buf(WAYS, pairs, rows, LANES),
            buf(pairs, 3, tokens, LANES),
            buf(2, tokens, LANES),
            buf(2, LANES, tokens),
            buf(tokens, LANES, kind=F32),
            buf(tokens, LANES, kind=F32),
            buf(tokens, model),
            buf(WAYS, wide, cols3, LANES),
            buf(rows, model),
            *[
                buf(*lead, cut, LANES)
                for cut in (part, units - part)
                for lead in ((WAYS, 2), (WAYS, 2), (WAYS,), (WAYS + 1,))
            ],
            buf(2, WAYS, wide // 2, depth, LANES),
            buf(WAYS, wide // 2, depth, LANES),
            buf(WAYS, 2, depth, LANES),
            buf(WAYS, depth, LANES),
            buf(WAYS + 1, depth, LANES),
            buf(pairs, wide, third, LANES),
            buf(pairs, 2, 2, third, LANES),
            buf(pairs, 2, third, LANES),
            buf(pairs, 2, third, LANES),
            buf(WAYS, pairs, 3, rows, LANES),
            buf(*small.shape, kind=F32),
            buf(8, *small.shape, kind=F32),
            buf(WAYS, *small.shape, kind=F32),
            sems(27),
            sems(WAYS, pairs),
            sems(WAYS, pairs),
            sems(2, 16),
            sems(2, 17),
            sems(16),
            sems(17),
            sems(1),
            sems(1),
            sems(pairs, 5),
            sems(pairs, 5),
            sems(WAYS, pairs, 2),
            sems(WAYS, pairs, 2),
            sems(12),
            sems(12),
        ],
        compiler_params=pltpu.CompilerParams(
            collective_id=2, has_side_effects=True, vmem_limit_bytes=62 * 1024 * 1024
        ),
        name="backward",
    )(
        heads_grad, ffn_sum, r1, normed, weight, x, middle_grad, low, heads,
        qa, ka, v, o, cosine, sine, gain, small,
    )


def pick(values, at, axis=0):
    return lax.dynamic_index_in_dim(values, at, axis, keepdims=False)


def flip(values, bit, dps):
    return lax.ppermute(values, "dp", [(i, i ^ bit) for i in range(dps)])


def to_attention(values, m, dps, back=False):
    pairs = []
    for dp in range(dps):
        group = dp % 2
        for t in range(WAYS):
            quarter = t ^ m
            there = (dp - group + ((quarter // 2) ^ group)) * WAYS + 2 * group + quarter % 2
            pairs.append((there, dp * WAYS + t) if back else (dp * WAYS + t, there))
    return lax.ppermute(values, ("dp", "mp"), pairs)


def local(
    sizes,
    layer_input,
    segment_ids,
    grad_out,
    qkv_weight,
    attn_weight,
    inner_weight,
    outer_weight,
    attn_gain,
    mlp_gain,
):
    dps, mps = sizes
    rows, model = layer_input.shape
    head_cols = qkv_weight.shape[2]
    units = inner_weight.shape[2]
    pairs = head_cols // LANES
    wide = model // LANES
    special = dps == wide
    me = lax.axis_index("mp")
    dp = lax.axis_index("dp")
    core = dp % 2
    group = me // 2
    quarter = me ^ (2 * core)
    scalars = jnp.zeros((3,), jnp.int32)
    if not special:
        scalars = jnp.stack([me, 0, quarter]).astype(jnp.int32)

    def every(values):
        got = lax.all_gather(values.T, "dp", axis=0, tiled=True).T
        got = got.reshape(-1, wide, LANES).transpose(1, 0, 2)
        return lax.all_gather(got, "mp", axis=1)

    qkv_part = qkv_weight.transpose(1, 2, 0).reshape(3, pairs, LANES, -1)
    qkv_part = qkv_part.transpose(1, 0, 2, 3).reshape(3 * head_cols, -1)
    inner_t = inner_weight.transpose(1, 2, 0)
    outer_t = outer_weight.T
    attn_depth = model // mps
    part_a = jnp.concatenate([attn_weight.T, inner_t[0]], axis=0)
    part_b = jnp.concatenate([inner_t[1], outer_t], axis=0)
    mine = segment_ids[0]
    info = jnp.broadcast_to(mine.astype(F32)[:, None], (mine.shape[0], LANES))
    info = info.reshape(WAYS, rows, LANES)
    if special:
        (pack_a, pack_b), heads, qkv_own, kept = forward_call(
            layer_input, info, attn_gain[None], qkv_part, [part_a, part_b], dps, pairs
        )
    else:
        x_all = jnp.stack([to_attention(layer_input, m, dps) for m in range(WAYS)])
        qkv_all, pack_a, pack_b = every(qkv_part), every(part_a), every(part_b)
        info = jnp.where(group == core, info, flip(info, 1, dps))
        qkv_own = qkv_all
        kept = alone_call(
            quarter, x_all, info, attn_gain[None], pick(qkv_all, quarter, 1), pairs)
        heads = kept[6].reshape(pairs, WAYS, rows, LANES)
        heads = [to_attention(heads[:, m], m, dps, back=True) for m in range(WAYS)]
        heads = jnp.stack(heads)
    normed, cosine, sine, qa, ka, v, o = kept

    outs = mlp_call(
        scalars, heads, layer_input, grad_out, mlp_gain[None], info, pack_a, pack_b,
        qkv_own, special,
    )
    layer_output, middle_grad, middle_low, small, heads_grad, ffn_sum, ffn_got, qkv_whole = outs
    if special:
        input_grad, inner_sum, outer_sum, attn_sum, qkv_sum, gain_a, gain_m, rms = backward_call(
            heads_grad, ffn_sum, ffn_got, kept, qkv_whole, layer_input, middle_grad, middle_low, heads,
            attn_gain[None], small,
        )
        return (
            layer_output,
            input_grad,
            qkv_sum.transpose(1, 0, 2),
            attn_sum,
            inner_sum.transpose(1, 0, 2),
            outer_sum,
            gain_a[0],
            gain_m[0],
            rms[0, :4],
        )
    else:
        lows = []
        for pair in range(pairs):
            grad = [to_attention(heads_grad[m, pair], m, dps) for m in range(WAYS)]
            low = attn_bwd_call(scalars, qa, ka, v, grad, o, cosine, sine, pair)
            lows.append(jnp.concatenate(low, axis=0))
        low = jnp.concatenate(lows, axis=1)
        own = pick(qkv_all, quarter, 1)
        own = jnp.concatenate([own[d] for d in range(wide)], axis=-1)
        normed_grad = dot_nn(low, own).astype(BF).reshape(WAYS, rows, model)
        normed_grad = sum(
            to_attention(normed_grad[m], m, dps, back=True).astype(F32) for m in range(WAYS)
        )

        def scatter(values):
            cut = lax.psum_scatter(values, "mp", scatter_dimension=0)
            return lax.psum_scatter(cut.T, "dp", scatter_dimension=0, tiled=True).T

        slot = (jnp.arange(mps) == quarter)[:, None, None]
        qkv_sum = scatter(jnp.where(slot, dot_tn(low, normed)[None], 0.0))
        mixed = jnp.stack([pick(heads, me ^ h) for h in range(mps)])
        mixed = mixed.transpose(0, 2, 1, 3).reshape(mps, rows, -1)
        attn_sum = scatter(jnp.stack([dot_tn(mixed[h], middle_low) for h in range(mps)]))
        ffn_sum = ffn_sum.reshape(mps, wide, 3 * units, LANES).transpose(0, 2, 1, 3)
        ffn_sum = scatter(ffn_sum.reshape(mps, 3 * units, model).astype(F32))
        vhat, scale = norm_stats(layer_input.astype(F32))
        input_grad = middle_grad + norm_back(vhat, scale, attn_gain, normed_grad)
        small = small.at[0].set(jnp.sum(normed_grad * vhat, axis=0))
        small = lax.psum(small, ("dp", "mp"))
    rms_values = jnp.sqrt(small[2, :4] / (small[2, 4] * model))

    qkv_sum = qkv_sum.reshape(pairs, 3, LANES, -1).transpose(3, 1, 0, 2)
    ffn_sum = ffn_sum.reshape(3, units, -1)
    return (
        layer_output,
        input_grad,
        qkv_sum.reshape(-1, 3, head_cols),
        attn_sum.T,
        ffn_sum[:2].transpose(2, 0, 1),
        ffn_sum[2].T,
        small[0],
        small[1],
        rms_values,
    )


def solution(mesh):
    sizes = (mesh.shape["dp"], mesh.shape["mp"])
    both = ("dp", "mp")
    whole = (P(both, None), P("dp", None, "mp"), P("dp", "mp"))
    return jax.shard_map(
        functools.partial(local, sizes),
        mesh=mesh,
        in_specs=(
            whole[0],
            P("dp", None),
            whole[0],
            whole[1],
            whole[2],
            whole[1],
            whole[2],
            P(),
            P(),
        ),
        out_specs=(
            whole[0],
            whole[0],
            whole[1],
            whole[2],
            whole[1],
            whole[2],
            P(),
            P(),
            P(),
        ),
        check_vma=False,
    )
```
